32 devices in a mesh: dp: 1 (over z), depth: 4 (over y), col: 4 (over x), row: 2 (over core).
Axes of the slice: x: 4, y: 4, z: 1, core: 2. Of those that a mesh axis runs over, the one named last changes fastest.
The devices are a block of a 4x4x8 slice.
Arguments:
- x_in: bfloat16 [16384, 2048], P(('dp', 'depth', 'row'), 'col')
- ln_gamma: float32 [2048], P('col')
- ln_beta: float32 [2048], P('col')
- w_up: bfloat16 [2048, 8192], P('row', 'col')
- b_up: bfloat16 [8192], P('col')
- w_down: bfloat16 [8192, 2048], P('row', 'col')
- b_down: bfloat16 [2048], P('col')
- grad_out: bfloat16 [16384, 2048], P(('dp', 'depth', 'row'), 'col')
Outputs:
- output 1: bfloat16 [16384, 2048], P(('dp', 'depth', 'row'), 'col')
- output 2: bfloat16 [16384, 2048], P(('dp', 'depth', 'row'), 'col')
- output 3: float32 [2048], P(('dp', 'col'))
- output 4: float32 [2048], P(('dp', 'col'))
- output 5: bfloat16 [2048, 8192], P(('dp', 'row'), 'col')
- output 6: float32 [8192], P(('dp', 'col'))
- output 7: bfloat16 [8192, 2048], P(('dp', 'row'), 'col')
- output 8: float32 [2048], P(('dp', 'col'))
All inputs are finite; a program needn't handle non-finite values.
Results may differ from the reference program's by a relative error of at most 0.0111579.
Values are sent between devices in bfloat16 or wider.
A program may use at most 768 MiB of HBM per device.

```python
import jax
import jax.numpy as jnp
from jax import lax

ROWS = 2048
WIDTH = 2048
FFN = 8192
TOKENS = 16384
SEGMENTS = 64
NUM_BLOCKS = TOKENS // ROWS
SEG_WIDTH = WIDTH // SEGMENTS
LN_EPS = 1e-5


def gelu_tanh(values):
    return jax.nn.gelu(values, approximate=True)


def setup_inputs(seed: int = 0, part: int = 0) -> dict:
    base_key = jax.random.key(seed)
    part_key = jax.random.fold_in(base_key, part)
    key_mean, key_scale, key_noise, key_grad = jax.random.split(part_key, 4)
    shared_key = jax.random.key(seed + 1)
    key_gamma, key_beta, key_wup, key_bup, key_wdown, key_bdown = jax.random.split(shared_key, 6)
    seg_mean = jax.random.normal(key_mean, (TOKENS, SEGMENTS), jnp.float32)
    seg_scale = jax.random.uniform(key_scale, (TOKENS, SEGMENTS), jnp.float32, 0.5, 2.0)
    white_noise = jax.random.normal(key_noise, (TOKENS, WIDTH), jnp.float32)
    x_in = jnp.repeat(seg_mean, SEG_WIDTH, axis=1) + jnp.repeat(seg_scale, SEG_WIDTH, axis=1) * white_noise
    grad_out = jax.random.normal(key_grad, (TOKENS, WIDTH), jnp.float32)
    ln_gamma = jax.random.uniform(key_gamma, (WIDTH,), jnp.float32, 0.5, 1.5)
    ln_beta = 0.5 * jax.random.normal(key_beta, (WIDTH,), jnp.float32)
    w_up = jax.random.normal(key_wup, (WIDTH, FFN), jnp.float32) * WIDTH ** -0.5
    b_up = 0.5 * jax.random.normal(key_bup, (FFN,), jnp.float32)
    w_down = jax.random.normal(key_wdown, (FFN, WIDTH), jnp.float32) * FFN ** -0.5
    b_down = 0.5 * jax.random.normal(key_bdown, (WIDTH,), jnp.float32)
    return {
        'x_in': x_in.astype(jnp.bfloat16),
        'ln_gamma': ln_gamma,
        'ln_beta': ln_beta,
        'w_up': w_up.astype(jnp.bfloat16),
        'b_up': b_up.astype(jnp.bfloat16),
        'w_down': w_down.astype(jnp.bfloat16),
        'b_down': b_down.astype(jnp.bfloat16),
        'grad_out': grad_out.astype(jnp.bfloat16),
    }


def block_pass(x_blk, dy_blk, ln_gamma, ln_beta, w_up, b_up, w_down, b_down):
    x_f32 = x_blk.astype(jnp.float32)
    row_mean = jnp.mean(x_f32, axis=1, keepdims=True)
    centered = x_f32 - row_mean
    row_var = jnp.mean(centered * centered, axis=1, keepdims=True)
    inv_std = lax.rsqrt(row_var + LN_EPS)
    x_hat = centered * inv_std
    x_norm = (x_hat * ln_gamma + ln_beta).astype(jnp.bfloat16)
    pre_act = (jnp.dot(x_norm, w_up, preferred_element_type=jnp.float32) + b_up.astype(jnp.float32)).astype(jnp.bfloat16)
    act_f32, gelu_vjp = jax.vjp(gelu_tanh, pre_act.astype(jnp.float32))
    hidden = act_f32.astype(jnp.bfloat16)
    y_blk = (x_f32 + jnp.dot(hidden, w_down, preferred_element_type=jnp.float32) + b_down.astype(jnp.float32)).astype(jnp.bfloat16)
    dy_f32 = dy_blk.astype(jnp.float32)
    sum_w_down = jnp.dot(hidden.T, dy_blk, preferred_element_type=jnp.float32)
    grad_hidden = jnp.dot(dy_blk, w_down.T, preferred_element_type=jnp.float32)
    grad_pre = gelu_vjp(grad_hidden)[0].astype(jnp.bfloat16)
    sum_w_up = jnp.dot(x_norm.T, grad_pre, preferred_element_type=jnp.float32)
    grad_norm = jnp.dot(grad_pre, w_up.T, preferred_element_type=jnp.float32)
    grad_hat = grad_norm * ln_gamma
    mean_plain = jnp.mean(grad_hat, axis=1, keepdims=True)
    mean_proj = jnp.mean(grad_hat * x_hat, axis=1, keepdims=True)
    dx_blk = (dy_f32 + inv_std * (grad_hat - mean_plain - x_hat * mean_proj)).astype(jnp.bfloat16)
    block_sums = (
        jnp.sum(grad_norm * x_hat, axis=0),
        jnp.sum(grad_norm, axis=0),
        sum_w_up,
        jnp.sum(grad_pre.astype(jnp.float32), axis=0),
        sum_w_down,
        jnp.sum(dy_f32, axis=0),
    )
    return y_blk, dx_blk, block_sums


def reference(x_in, ln_gamma, ln_beta, w_up, b_up, w_down, b_down, grad_out):
    x_blocks = x_in.reshape(NUM_BLOCKS, ROWS, WIDTH)
    dy_blocks = grad_out.reshape(NUM_BLOCKS, ROWS, WIDTH)

    def scan_body(run_sums, blocks):
        y_blk, dx_blk, block_sums = block_pass(blocks[0], blocks[1], ln_gamma, ln_beta, w_up, b_up, w_down, b_down)
        new_sums = jax.tree.map(lambda total, update: total + update, run_sums, block_sums)
        return new_sums, (y_blk, dx_blk)

    init_sums = (
        jnp.zeros((WIDTH,), jnp.float32),
        jnp.zeros((WIDTH,), jnp.float32),
        jnp.zeros((WIDTH, FFN), jnp.float32),
        jnp.zeros((FFN,), jnp.float32),
        jnp.zeros((FFN, WIDTH), jnp.float32),
        jnp.zeros((WIDTH,), jnp.float32),
    )
    final_sums, outputs = lax.scan(scan_body, init_sums, (x_blocks, dy_blocks))
    y_blocks, dx_blocks = outputs
    grad_gamma, grad_beta, sum_w_up, grad_b_up, sum_w_down, grad_b_down = final_sums
    return (
        y_blocks.reshape(TOKENS, WIDTH),
        dx_blocks.reshape(TOKENS, WIDTH),
        grad_gamma,
        grad_beta,
        sum_w_up.astype(jnp.bfloat16),
        grad_b_up,
        sum_w_down.astype(jnp.bfloat16),
        grad_b_down,
    )
```

```python
import jax
import jax.numpy as jnp
from jax import lax
from jax.sharding import PartitionSpec as P

LN_EPS = 1e-5
F32 = jnp.float32
BF16 = jnp.bfloat16


def gelu_tanh(values):
    return jax.nn.gelu(values, approximate=True)


def rel(v):
    return v ^ (v >> 1)


ORDER = (0, 1, 3, 2)


def dot(lhs, rhs, dims):
    return lax.dot_general(lhs, rhs, (dims, ((), ())), preferred_element_type=F32)


def solution(mesh):
    n_col, n_row, n_depth = mesh.shape['col'], mesh.shape['row'], mesh.shape['depth']
    assert (n_col, n_row, n_depth) == (4, 2, 4)
    tok_spec = P(('dp', 'depth', 'row'), 'col')
    vec_spec = P('col')
    mat_spec = P('row', 'col')
    grad_vec = P(('dp', 'col'))
    grad_mat = P(('dp', 'row'), 'col')
    near = [(i, i ^ 1) for i in range(4)]
    far = [(i, i ^ 3) for i in range(4)]
    opposite = [(i, i ^ 2) for i in range(4)]
    cross = [(0, 1), (1, 0)]
    tau_of = [rel(c) & 1 for c in range(4)]

    def hop_near(v, axis):
        return lax.ppermute(v, axis, near)

    def hop_far(v, axis):
        return lax.ppermute(v, axis, far)

    def swap(v):
        return lax.ppermute(v, 'row', cross)

    def gather4(block, axis):
        h = block.shape[0] // 2
        b1 = hop_near(block, axis)
        b2 = hop_far(block, axis)
        o0 = hop_near(b2[:h], axis)
        o1 = hop_far(b1[h:], axis)
        return block, b1, b2, o0, o1

    def join4(g):
        return [g[0], g[1], g[2], jnp.concatenate([g[3], g[4]], axis=0)]

    def scatter4(parts, axis):
        h = parts[3].shape[0] // 2
        r1 = hop_near(parts[3][:h], axis)
        r2 = hop_far(parts[3][h:], axis)
        p2 = jnp.concatenate([parts[2][:h] + r1, parts[2][h:]], axis=0)
        p1 = jnp.concatenate([parts[1][:h], parts[1][h:] + r2], axis=0)
        return parts[0] + hop_far(p2, axis) + hop_near(p1, axis)

    def local_pass(x_blk, gamma_blk, beta_blk, w_up_blk, b_up_blk, w_down_blk, b_down_blk, dy_blk):
        tok, hb = x_blk.shape
        fb = w_up_blk.shape[1]
        fh = fb // 2
        width = hb * n_col
        inv_width = 1.0 / width
        c = lax.axis_index('col')
        r = lax.axis_index('row')
        d = lax.axis_index('depth')
        tau = rel(c) & 1
        is_tau = r == tau
        th = tok // 2

        def tokens(block):
            own = gather4(block, 'col')
            oth = [swap(v) for v in own]
            own = jnp.concatenate(join4(own), axis=1)
            oth = jnp.concatenate(join4(oth), axis=1)
            return jnp.where(is_tau, own, oth), jnp.where(is_tau, oth, own)

        x_t, x_n = tokens(x_blk)

        vecs = jnp.stack([gamma_blk, beta_blk, b_down_blk.astype(F32)], axis=0)
        v1, v2 = hop_near(vecs, 'col'), hop_far(vecs, 'col')
        v3 = hop_near(v2, 'col')
        vecs = jnp.concatenate([vecs, v1, v2, v3], axis=1)
        gamma, beta = vecs[0:1], vecs[1:2]
        bd2 = vecs[2:3, :2 * hb]
        b_up_mine = lax.dynamic_slice_in_dim(b_up_blk, r * fh, fh)
        b_up_pair = jnp.concatenate([b_up_mine, hop_near(b_up_mine, 'col')]).astype(F32)[None, :]

        wu = w_up_blk
        wu_keep = lax.dynamic_slice_in_dim(wu, r * fh, fh, axis=1)
        wu_got = swap(lax.dynamic_slice_in_dim(wu, (1 - r) * fh, fh, axis=1))
        wu_abs = jnp.concatenate([jnp.where(r == 0, wu_keep, wu_got), jnp.where(r == 0, wu_got, wu_keep)], axis=0)
        quarter = width // n_depth
        wq = hop_near(lax.dynamic_slice_in_dim(wu_abs, d * quarter, quarter, axis=0), 'col')
        wq = jnp.stack(join4(gather4(wq, 'depth')))
        cat = []
        for p in range(4):
            hb_abs = c ^ ORDER[p]
            mine = lax.dynamic_slice_in_dim(wu_abs, hb_abs * hb, hb, axis=0)
            theirs = lax.dynamic_index_in_dim(wq, rel(d ^ hb_abs), 0, keepdims=False)
            cat.append(jnp.concatenate([mine, theirs], axis=1))
        wu_cat = jnp.concatenate(cat, axis=0)
        wu_mine = wu_cat[:, :fh]

        wd = w_down_blk.reshape(2, 2, fh, hb)
        wd_keep = lax.dynamic_index_in_dim(wd, r, 1, keepdims=False)
        wd_got = swap(lax.dynamic_index_in_dim(wd, 1 - r, 1, keepdims=False))
        v_all = jnp.stack([jnp.where(r == 0, wd_keep, wd_got), jnp.where(r == 0, wd_got, wd_keep)])
        v_all = v_all.reshape(4, fh, hb)
        f = c >> 1
        qf = fh // n_depth
        v_q = lax.dynamic_slice_in_dim(v_all, d * qf, qf, axis=1).reshape(2, 2, qf, hb)
        same = lax.dynamic_index_in_dim(v_q, f, 0, keepdims=False)
        diff = lax.dynamic_index_in_dim(v_q, 1 - f, 0, keepdims=False)
        n1 = hop_near(same, 'col')
        n2 = hop_far(diff, 'col')
        n3 = hop_near(n2, 'col')
        nq = jnp.concatenate([n1, n2, n3], axis=2)
        nq = jnp.stack(join4(gather4(nq, 'depth')))
        rows = []
        for p in range(2):
            q = c ^ p
            own = lax.dynamic_index_in_dim(v_all, q, 0, keepdims=False)
            rest = jnp.concatenate([
                lax.dynamic_slice(nq, (rel(d ^ k), q & 1, 0, 0), (1, 1, qf, 3 * hb)).reshape(qf, 3 * hb)
                for k in range(4)], axis=0)
            rows.append(jnp.concatenate([own, rest], axis=1))
        wd_cat = jnp.concatenate(rows, axis=0)

        dy_t, dy_n = tokens(dy_blk)

        def norm(xv):
            xf = xv.astype(F32)
            mean = jnp.sum(xf, axis=1, keepdims=True) * inv_width
            cen = xf - mean
            inv = lax.rsqrt(jnp.sum(cen * cen, axis=1, keepdims=True) * inv_width + LN_EPS)
            return (cen * inv * gamma + beta).astype(BF16), mean, inv

        xn_t, mean_t, inv_t = norm(x_t)
        xn_n, _, _ = norm(x_n)
        u_t = (dot(xn_t, wu_cat, ((1,), (0,))) + b_up_pair).astype(BF16)
        u_n = (dot(xn_n, wu_mine, ((1,), (0,))) + b_up_pair[:, :fh]).astype(BF16)
        a_t = gelu_tanh(u_t.astype(F32)).astype(BF16)
        a_n = gelu_tanh(u_n.astype(F32)).astype(BF16)

        def pair_sum(lhs, rhs, dims):
            give = lax.dynamic_slice_in_dim(lhs, (1 - r) * th, th, axis=0)
            keep = lax.dynamic_slice_in_dim(lhs, r * th, th, axis=0)
            got = swap(dot(give, rhs, dims))
            return dot(keep, rhs, dims) + got

        x_own = lax.dynamic_slice_in_dim(x_t, r * th, th, axis=0)[:, :2 * hb].astype(F32)
        dy_own = lax.dynamic_slice_in_dim(dy_t, r * th, th, axis=0)[:, :2 * hb].astype(F32)

        def place(v):
            k0 = lax.ppermute(v[:, :hb], ('col', 'row'), [(q * 2 + 1 - tau_of[q], q * 2 + tau_of[q]) for q in range(4)])
            k1 = [lax.ppermute(v[:, hb:], ('col', 'row'), [(q * 2 + s, (q ^ 1) * 2 + tau_of[q]) for q in range(4)]) for s in range(2)]
            mine = v[:, :hb]
            first = jnp.where(is_tau, jnp.where(r == 0, mine, k0), k1[0])
            second = jnp.where(is_tau, jnp.where(r == 0, k0, mine), k1[1])
            return jnp.concatenate([first, second], axis=0)

        y_part = pair_sum(a_t, wd_cat, ((1,), (0,)))
        y_far = hop_far(y_part[:, 2 * hb:], 'col')
        y_blk = place((x_own + (y_part[:, :2 * hb] + y_far) + bd2).astype(BF16))

        def gelu_grad(u, da):
            return jax.vjp(gelu_tanh, u.astype(F32))[1](da)[0].astype(BF16)

        du_t = gelu_grad(u_t, dot(dy_t, wd_cat, ((1,), (1,))))
        du_n = gelu_grad(u_n, dot(dy_n, wd_cat[:fh], ((1,), (1,))))

        dwd = dot(a_t[:, :fh], dy_t, ((0,), (0,))) + dot(a_n, dy_n, ((0,), (0,)))
        dwd = scatter4([lax.dynamic_slice_in_dim(dwd, (d ^ ORDER[p]) * qf, qf, axis=0) for p in range(4)], 'depth').astype(BF16)
        pieces = [dwd[:, p * hb:(p + 1) * hb] for p in range(4)]
        pieces = jnp.stack([pieces[0], hop_near(pieces[1], 'col'), hop_far(pieces[2], 'col'), lax.ppermute(pieces[3], 'col', opposite)])
        pieces = jnp.stack(join4(gather4(pieces, 'depth')), axis=0)

        def hidden_rows(q):
            return jnp.concatenate([lax.dynamic_slice(pieces, (rel(d ^ k), rel(c ^ q), 0, 0), (1, 1, qf, hb)).reshape(qf, hb) for k in range(4)], axis=0)

        keep = [hidden_rows(2 * r + j) for j in range(2)]
        got = swap(jnp.stack([hidden_rows(2 * (1 - r) + j) for j in range(2)]))
        grad_w_down = jnp.concatenate(
            [v for j in range(2) for v in (jnp.where(r == 0, keep[j], got[j]), jnp.where(r == 0, got[j], keep[j]))], axis=0)

        g_part = pair_sum(du_t, wu_cat, ((1,), (1,)))

        dwu = dot(xn_t, du_t[:, :fh], ((0,), (0,))) + dot(xn_n, du_n, ((0,), (0,)))
        dwu = scatter4([lax.dynamic_slice_in_dim(dwu, (d ^ ORDER[p]) * hb, hb, axis=0) for p in range(4)], 'depth').astype(BF16)
        dwu = jnp.stack(join4(gather4(dwu, 'depth')))

        def width_rows(h):
            return lax.dynamic_index_in_dim(dwu, rel(d ^ rel(c ^ h)), 0, keepdims=False)

        keep = jnp.concatenate([width_rows(2 * r), width_rows(2 * r + 1)], axis=0)
        got = swap(jnp.concatenate([width_rows(2 * (1 - r)), width_rows(2 * (1 - r) + 1)], axis=0))
        grad_w_up = jnp.concatenate([jnp.where(r == 0, keep, got), jnp.where(r == 0, got, keep)], axis=1)

        g_far = hop_far(g_part[:, 2 * hb:], 'col')
        x_half = lax.dynamic_slice_in_dim(x_t, r * th, th, axis=0).astype(F32)
        mean_h = lax.dynamic_slice_in_dim(mean_t, r * th, th, axis=0)
        inv_h = lax.dynamic_slice_in_dim(inv_t, r * th, th, axis=0)
        xhat = (x_half - mean_h) * inv_h
        gh = g_part * gamma
        stats = jnp.concatenate([jnp.sum(gh, axis=1)[None], jnp.sum(gh * xhat, axis=1)[None]], axis=0)
        stats = (stats + hop_far(stats, 'col')) * inv_width
        dxn = g_part[:, :2 * hb] + g_far
        xh2 = xhat[:, :2 * hb]
        dx = dy_own + inv_h * (dxn * gamma[:, :2 * hb] - stats[0][:, None] - xh2 * stats[1][:, None])
        dx_blk = place(dx.astype(BF16))

        cols = jnp.concatenate([jnp.sum(dxn * xh2, axis=0)[None], jnp.sum(dxn, axis=0)[None]], axis=0)
        cols = cols[:, :hb] + hop_near(cols[:, hb:], 'col')
        db_up = jnp.sum(du_t[:, :fh].astype(F32), axis=0) + jnp.sum(du_n.astype(F32), axis=0)
        db_up = lax.dynamic_update_slice_in_dim(jnp.zeros((fb,), F32), db_up, r * fh, axis=0)
        db_down = jnp.sum(dy_blk.astype(F32), axis=0)
        sums = lax.psum(jnp.concatenate([cols[0], cols[1], db_up, db_down]), ('depth', 'row'))
        return (y_blk, dx_blk, sums[:hb], sums[hb:2 * hb], grad_w_up, sums[2 * hb:2 * hb + fb], grad_w_down, sums[2 * hb + fb:])

    return jax.shard_map(
        local_pass,
        mesh=mesh,
        in_specs=(tok_spec, vec_spec, vec_spec, mat_spec, vec_spec, mat_spec, vec_spec, tok_spec),
        out_specs=(tok_spec, tok_spec, grad_vec, grad_vec, grad_mat, grad_vec, grad_mat, grad_vec),
        check_vma=False,
    )
```

```python
import functools

import jax
import jax.numpy as jnp
from jax import lax
from jax.experimental import pallas as pl
from jax.experimental.pallas import tpu as pltpu
from jax.sharding import PartitionSpec as P

LN_EPS = 1e-5
F32 = jnp.float32
BF16 = jnp.bfloat16
MESH = pl.DeviceIdType.MESH
GELU_A = 0.7978845608028654
GELU_B = 0.044715
NCH = 4
ROWS = 16

NN = (((1,), (0,)), ((), ()))
NT = (((1,), (1,)), ((), ()))
TN = (((0,), (0,)), ((), ()))

SEMS = {}
for _z in ('x', 'g'):
    for _n in ('near', 'far', 'opp', 'd2d', 'd2o', 's_near', 's_far', 's_rel', 's_d2d'):
        SEMS[_z + _n] = NCH
    SEMS[_z + 'bounce'] = 2
for _p in ('y', 'd'):
    SEMS.update({_p + 's_give': 2, _p + 'got': 2, _p + 's_far': 1, _p + 'keep': 1, _p + 'far': 2, _p + 's_out': 4, _p + 'out': 1, _p + 'loc': 2})
SEMS.update(l_wu=1, s_wu=1, r_wu=1, s_wun=2, r_wun=1, s_wuy=4, r_wuy=4,
            s_wd0=2, s_wdx=4, r_wd=4, s_wdr=2, s_wdy=8, r_wdy=4,
            l_vec=2, s_vec=4, r_vec=2,
            ld=8, st=4, s_st=1, r_st=1,
            d_so=8, d_r=8, d_sa=8, d_p=8, d_sf=4, d_out=1, d_sy=8, d_y=2, d_sr=8, d_o=2,
            u_so=2, u_r=2, u_sa=2, u_p=2, u_sf=3, u_out=3, u_sr=1, u_o=2, l_small=2)
BASE = {}
_at = 0
for _n, _c in SEMS.items():
    BASE[_n] = _at
    _at += _c
N_SEM = _at


def gelu(v):
    return 0.5 * v * (1.0 + jnp.tanh(GELU_A * (v + GELU_B * (v * v * v))))


def gelu_slope(v):
    v2 = v * v
    t = jnp.tanh(GELU_A * (v + GELU_B * (v * v2)))
    return 0.5 * (1.0 + t) + 0.5 * v * (1.0 - t * t) * (GELU_A * (1.0 + 3.0 * GELU_B * v2))


def body(dims, x_ref, dy_ref, wu_ref, wd_ref, vec_ref, bu_ref,
         y_out, dx_out, gwu_out, gwd_out, cs_out, db_out,
         X, DY, XN, U, A, DU, YGOT, YFAR, YKEEP, GGOT, GFAR, GKEEP, PFD, PND, PFU, PNU,
         wu_v, wd_v, accD, accU, r1D, r2D, r1U, r2U, vec_v, bu_v, wb, fb, ob, finD, finU,
         db_v, cs_v, st_v, ms_v, st2_v, sx_v, sr_v, sem):
    TK, HB, FH = dims
    W, HW, TH, BLK, QF = 4 * HB, 2 * HB, TK // 2, TK // NCH, FH // 4
    RH, DQ, QH, DH, FB = W // 2, W // 4, FH // 8, W // 8, 2 * FH
    NTW = HB
    inv_w = 1.0 / W

    c, r, d = lax.axis_index('col'), lax.axis_index('row'), lax.axis_index('depth')
    c_odd, d_odd = lax.rem(c, 2), lax.rem(d, 2)
    cn, cf, co = c + 1 - 2 * c_odd, 3 - c, lax.rem(c + 2, 4)
    dn, df, do = d + 1 - 2 * d_odd, 3 - d, lax.rem(d + 2, 4)
    f, dh = lax.div(c, 2), lax.div(d, 2)
    tau = lax.rem(lax.div(c + 1, 2), 2)
    rp = 1 - r
    o, o2 = c_odd * FH, (1 - c_odd) * FH

    def S(name, i=0):
        return sem.at[BASE[name] + i]

    def ds(start, size):
        return pl.ds(pl.multiple_of(start, size), size)

    def dsm(start, size, mult):
        return pl.ds(pl.multiple_of(start, mult), size)

    def put(src, dst, ssem, rsem, **dev):
        pltpu.make_async_remote_copy(src_ref=src, dst_ref=dst, send_sem=ssem, recv_sem=rsem,
                                     device_id=dev, device_id_type=MESH).start()

    def copy(src, dst, s):
        pltpu.make_async_copy(src, dst, s).start()

    def wait(ref, s):
        pltpu.make_async_copy(ref, ref, s).wait()

    def loop(n, fn):
        def step(i, carry):
            fn(i)
            return carry
        lax.fori_loop(0, n, step, 0)

    bar = pltpu.get_barrier_semaphore()
    for dev in [dict(row=rp)] + [dict(row=h, **q) for h in range(2) for q in
                                 (dict(col=cn), dict(col=cf), dict(col=co), dict(depth=dn), dict(depth=df))]:
        pl.semaphore_signal(bar, inc=1, device_id=dev, device_id_type=MESH)
    pl.semaphore_wait(bar, 11)

    wun_src = lambda h: wu_ref.at[ds(d_odd * DQ, DQ), pl.ds(h * FH, FH)]
    wun_dst = wu_v.at[ds(d * DQ, DQ), ds(o, FH)]

    @pl.when(r == dh)
    def _():
        for h in range(2):
            put(wun_src(h), wun_dst, S('s_wun', h), S('r_wun'), col=cn, row=h)

    def wd_src(s, h):
        return wd_ref.at[dsm((2 * s + h) * FH + d * QF, QF, QF), :]

    def wd_dst(s, col):
        return wd_v.at[dsm(s * FH + d * QF, QF, QF), ds(col * HB, HB)]

    @pl.when(r == f)
    def _():
        for s in range(2):
            for h in range(2):
                put(wd_src(s, h), wd_dst(s, c), S('s_wdx', 2 * s + h), S('r_wd', 1), col=cn, row=h)
            copy(wd_src(s, r), wd_dst(s, c), S('r_wd', 0))
            put(wd_src(s, rp), wd_dst(s, c), S('s_wd0', s), S('r_wd', 0), row=rp)

    @pl.when(r != f)
    def _():
        for s in range(2):
            for h in range(2):
                put(wd_src(s, h), wd_dst(s, c), S('s_wdx', 2 * s + h), S('r_wd', 2), col=cf, row=h)

    copy(wu_ref.at[:, ds(r * FH, FH)], wu_v.at[ds(r * RH, RH), ds(o, FH)], S('l_wu'))
    put(wu_ref.at[:, ds(rp * FH, FH)], wu_v.at[ds(r * RH, RH), ds(o, FH)], S('s_wu'), S('r_wu'), row=rp)

    vec_at = vec_v.at[:, ds(c * HB, HB)]
    copy(vec_ref, vec_at, S('l_vec', 0))
    put(vec_ref, vec_at, S('s_vec', 0), S('r_vec', 0), col=cn)
    put(vec_ref, vec_at, S('s_vec', 1), S('r_vec', 0), col=cf)
    put(vec_ref, vec_at, S('s_vec', 2), S('r_vec', 0), col=co)
    bu_src, bu_at = bu_ref.at[:, ds(r * FH, FH)], bu_v.at[:, ds(o, FH)]
    copy(bu_src, bu_at, S('l_vec', 1))
    put(bu_src, bu_at, S('s_vec', 3), S('r_vec', 1), col=cn)

    def reg(Z, k, col):
        return Z.at[r, ds(k * BLK, BLK), ds(col * HB, HB)]

    def src_of(z_ref, k):
        return z_ref.at[ds(k * BLK, BLK), :]

    def send_own(z, z_ref, Z, which):
        def step(k):
            if 'near' in which:
                put(src_of(z_ref, k), reg(Z, k, c), S(z + 's_near', k), S(z + 'near', k), col=cn)
            if 'far' in which:
                put(src_of(z_ref, k), reg(Z, k, c), S(z + 's_far', k), S(z + 'far', k), col=cf)
            if 'd2d' in which:
                put(src_of(z_ref, k), reg(Z, k, c), S(z + 's_d2d', k), S(z + 'd2d', k), row=rp)
        loop(NCH, step)

    def d2d(z, Z, k, col, s):
        put(reg(Z, k, col), reg(Z, k, col), S(z + 's_d2d', k), S(z + s, k), row=rp)

    send_own('x', x_ref, X, ('near', 'far', 'd2d'))
    send_own('g', dy_ref, DY, ('near', 'd2d'))
    for i, z_ref in enumerate((x_ref, dy_ref)):
        for k in range(NCH):
            copy(z_ref.at[pl.ds(k * BLK, BLK), :], wb.at[i, :, pl.ds(k * HB, HB)], S('xg'[i] + 'bounce', 0))
    for i, Z in enumerate((X, DY)):
        wait(wb.at[i], S('xg'[i] + 'bounce', 0))
        for k in range(NCH):
            copy(wb.at[i, :, pl.ds(k * HB, HB)], reg(Z, k, c), S('xg'[i] + 'bounce', 1))

    db_v[...] = jnp.zeros_like(db_v)
    cs_v[...] = jnp.zeros_like(cs_v)

    for s in range(1):
        wait(wd_v.at[pl.ds(0, 2 * QF), pl.ds(0, HB)], S('r_wd', 2))
    for s in range(2):
        put(wd_dst(s, cf), wd_dst(s, cf), S('s_wdr', s), S('r_wd', 3), col=cn)

    def wuq(dd, half=None):
        if half is None:
            return wu_v.at[ds(dd * DQ, DQ), ds(o2, FH)]
        return wu_v.at[dsm(dd * DQ + half * DH, DH, DH), ds(o2, FH)]

    wait(wuq(d), S('r_wun'))
    put(wuq(d), wuq(d), S('s_wuy', 0), S('r_wuy', 0), depth=dn)
    put(wuq(d), wuq(d), S('s_wuy', 1), S('r_wuy', 1), depth=df)

    def wdq(s, dd, half=None):
        if half is None:
            return wd_v.at[dsm(s * FH + dd * QF, QF, QF), :]
        return wd_v.at[dsm(s * FH + dd * QF + half * QH, QH, QH), :]

    for i in (0, 1, 3):
        wait(wd_v.at[pl.ds(0, 2 * QF), pl.ds(0, HB)], S('r_wd', i))
    for s in range(2):
        put(wdq(s, d), wdq(s, d), S('s_wdy', s), S('r_wdy', 0), depth=dn)
        put(wdq(s, d), wdq(s, d), S('s_wdy', 2 + s), S('r_wdy', 1), depth=df)

    def x_near(k):
        wait(reg(X, k, cn), S('xnear', k))
        put(reg(X, k, cn), reg(X, k, cn), S('xs_rel', k), S('xopp', k), col=cf)
        d2d('x', X, k, cn, 'd2d')

    x_near(0)

    wait(wuq(dn), S('r_wuy', 0))
    put(wuq(dn, 1), wuq(dn, 1), S('s_wuy', 2), S('r_wuy', 3), depth=df)
    wait(wuq(df), S('r_wuy', 1))
    put(wuq(df, 0), wuq(df, 0), S('s_wuy', 3), S('r_wuy', 2), depth=dn)

    for i, Z in enumerate((X, DY)):
        wait(wb.at[i], S('xg'[i] + 'bounce', 1))
    wait(vec_at, S('l_vec', 0))
    wait(vec_v.at[:, pl.ds(0, 3 * HB)], S('r_vec', 0))
    wait(bu_at, S('l_vec', 1))
    wait(bu_at, S('r_vec', 1))
    wait(wu_v.at[ds(r * RH, RH), ds(o, FH)], S('l_wu'))
    wait(wu_v.at[ds(rp * RH, RH), ds(o, FH)], S('r_wu'))

    def norm_rows(buf, rows):
        xf = buf[rows, :].astype(F32)
        mean = jnp.sum(xf, axis=1, keepdims=True) * inv_w
        cen = xf - mean
        inv = lax.rsqrt(jnp.sum(cen * cen, axis=1, keepdims=True) * inv_w + LN_EPS)
        return cen, mean, inv

    def tok_of(s):
        return tau + s * (1 - 2 * tau)

    def w_relay():
        for s in range(1):
            wait(wd_v.at[pl.ds(0, 2 * QF), :], S('r_wdy', 0))
            wait(wd_v.at[pl.ds(0, 2 * QF), :], S('r_wdy', 1))
        for s in range(2):
            put(wdq(s, dn, 1), wdq(s, dn, 1), S('s_wdy', 4 + s), S('r_wdy', 3), depth=df)
            put(wdq(s, df, 0), wdq(s, df, 0), S('s_wdy', 6 + s), S('r_wdy', 2), depth=dn)

    def phase1(k):
        @pl.when(k < NCH - 1)
        def _():
            x_near(k + 1)

        @pl.when(k == 2)
        def _():
            send_own('g', dy_ref, DY, ('far',))
            w_relay()

        wait(reg(X, k, cf), S('xfar', k))
        d2d('x', X, k, cf, 'd2d')
        wait(reg(X, k, co), S('xopp', k))
        d2d('x', X, k, co, 'd2d')
        rows = ds(k * BLK, BLK)
        wait(X.at[rp, rows, :], S('xd2d', k))

        @pl.when(k == 0)
        def _():
            wait(wuq(do, 0), S('r_wuy', 2))
            wait(wuq(do, 1), S('r_wuy', 3))

        @pl.when(k > 0)
        def _():
            for s in range(2):
                wait(wb.at[s], S('st', s))
        for s in range(2):
            copy(X.at[tok_of(s), rows, :], wb.at[s], S('ld', s))

        def half(s):
            wait(wb.at[s], S('ld', s))

            def ln(i):
                rr = ds(i * ROWS, ROWS)
                cen, _, inv = norm_rows(wb.at[s], rr)
                wb[s, rr, :] = (cen * inv * vec_v[0:1, :] + vec_v[1:2, :]).astype(BF16)
            loop(BLK // ROWS, ln)
            copy(wb.at[s], XN.at[s, rows, :], S('st', s))

            @pl.when(k + s > 0)
            def _():
                wait(wb.at[2], S('st', 2))
                wait(wb.at[3], S('st', 3))

            def tile(n):
                cols = ds(s * o + n * NTW, NTW)
                acc = lax.dot_general(wb[s], wu_v[:, cols], NN, preferred_element_type=F32) + bu_v[0:1, cols]
                u = acc.astype(BF16)
                wb[2, :, cols] = u
                wb[3, :, cols] = gelu(u.astype(F32)).astype(BF16)
            loop((2 - s) * (FH // NTW), tile)
            copy(wb.at[2, :, pl.ds(0, FB)], U.at[s, rows, :], S('st', 2))
            copy(wb.at[3, :, pl.ds(0, FB)], A.at[s, rows, :], S('st', 3))
        loop(2, half)
    loop(NCH, phase1)
    for i in range(4):
        wait(wb.at[i], S('st', i))

    def g_near_far(k):
        wait(reg(DY, k, cf), S('gfar', k))
        put(reg(DY, k, cf), reg(DY, k, cf), S('gs_rel', k), S('gopp', k), col=cn)
        d2d('g', DY, k, cf, 'd2d')
        wait(reg(DY, k, cn), S('gnear', k))
        d2d('g', DY, k, cn, 'd2d')

    def g_opp(k):
        wait(reg(DY, k, co), S('gopp', k))
        d2d('g', DY, k, co, 'd2o')
        wait(reg(DY, k, co), S('gd2o', k))

    def tile_y(lhs, col):
        return lax.dot_general(lhs, wd_v[:, dsm(col, NTW, NTW)], NN, preferred_element_type=F32)

    def tile_g(lhs, col):
        return lax.dot_general(lhs, wu_v[dsm(col, NTW, NTW), :], NT, preferred_element_type=F32)

    def give(p, src, tile, GOT):
        def blk(b):
            return src.at[0, dsm(rp * TH + b * BLK, BLK, BLK), :]
        copy(blk(0), wb.at[0, :, pl.ds(0, FB)], S('ld', 0))

        def step(b):
            wait(wb.at[b, :, pl.ds(0, FB)], S('ld', b))

            @pl.when(b == 0)
            def _():
                copy(blk(1), wb.at[1, :, pl.ds(0, FB)], S('ld', 1))

            def half(h):
                @pl.when(b == 1)
                def _():
                    wait(fb.at[h], S(p + 's_give', h))

                def n_tile(n):
                    fb[h, :, ds(n * NTW, NTW)] = tile(wb[b, :, :FB], h * HW + n * NTW)
                loop(HW // NTW, n_tile)
                put(fb.at[h], GOT.at[ds(b * BLK, BLK), ds(h * HW, HW)], S(p + 's_give', h), S(p + 'got', b), row=rp)
            loop(2, half)
        loop(2, step)

    def keep(p, src, tile, GOT, FAR, KEEP):
        def blk(b):
            return src.at[0, dsm(r * TH + b * BLK, BLK, BLK), :]
        copy(blk(0), wb.at[0, :, pl.ds(0, FB)], S('ld', 0))
        for h in range(2):
            wait(fb.at[h], S(p + 's_give', h))

        def step(b):
            brow = ds(b * BLK, BLK)
            wait(GOT.at[brow, :], S(p + 'got', b))
            for h in range(2):
                col0 = (f if h else 1 - f) * HW
                copy(GOT.at[brow, ds(col0, HW)], fb.at[h], S('ld', 2 + h))
            wait(wb.at[b, :, pl.ds(0, FB)], S('ld', b))

            @pl.when(b == 0)
            def _():
                copy(blk(1), wb.at[1, :, pl.ds(0, FB)], S('ld', 1))

            def half(h):
                col0 = (1 - f + h * (2 * f - 1)) * HW

                @pl.when(jnp.logical_and(b == 1, h == 0))
                def _():
                    wait(fb.at[2], S(p + 's_far'))

                @pl.when(jnp.logical_and(b == 1, h == 1))
                def _():
                    wait(fb.at[3], S(p + 'keep'))

                def n_tile(n):
                    fb[2 + h, :, ds(n * NTW, NTW)] = tile(wb[b, :, :FB], col0 + n * NTW)
                loop(HW // NTW, n_tile)
                wait(fb.at[h], S('ld', 2 + h))

                def add(i):
                    rr = ds(i * ROWS, ROWS)
                    fb[2 + h, rr, :] = fb[2 + h, rr, :] + fb[h, rr, :]
                loop(BLK // ROWS, add)

                @pl.when(h == 0)
                def _():
                    put(fb.at[2], FAR.at[brow, :], S(p + 's_far'), S(p + 'far', b), col=cf)

                @pl.when(h == 1)
                def _():
                    copy(fb.at[3], KEEP.at[brow, :], S(p + 'keep'))
            loop(2, half)
        loop(2, step)

    def keep_end(p):
        wait(fb.at[2], S(p + 's_far'))
        wait(fb.at[3], S(p + 'keep'))

    def place(p, out, b):
        dst = out.at[dsm(r * TH + b * BLK, BLK, BLK), :]
        mine, other = ob.at[b, :, ds(c_odd * HB, HB)], ob.at[b, :, ds((1 - c_odd) * HB, HB)]
        put(other, dst, S(p + 's_out', 2 * b), S(p + 'out'), col=cn, row=tau)

        @pl.when(r == tau)
        def _():
            copy(mine, dst, S(p + 'loc', b))

        @pl.when(r != tau)
        def _():
            put(mine, dst, S(p + 's_out', 2 * b + 1), S(p + 'out'), row=rp)

    def place_end(p, b):
        wait(ob.at[b, :, pl.ds(0, HB)], S(p + 's_out', 2 * b))

        @pl.when(r == tau)
        def _():
            wait(ob.at[b, :, pl.ds(0, HB)], S(p + 'loc', b))

        @pl.when(r != tau)
        def _():
            wait(ob.at[b, :, pl.ds(0, HB)], S(p + 's_out', 2 * b + 1))

    fcols = ds(f * HW, HW)

    def y_final(b):
        brow = ds(b * BLK, BLK)
        wait(YFAR.at[brow, :], S('yfar', b))
        copy(YFAR.at[brow, :], fb.at[0], S('ld', 0))
        copy(YKEEP.at[brow, :], fb.at[1], S('ld', 1))
        copy(X.at[tau, dsm(r * TH + b * BLK, BLK, BLK), fcols], wb.at[0, :, pl.ds(0, HW)], S('ld', 2))
        wait(fb.at[0], S('ld', 0))
        wait(fb.at[1], S('ld', 1))
        wait(wb.at[0, :, pl.ds(0, HW)], S('ld', 2))

        def fin(i):
            rr = ds(i * ROWS, ROWS)
            ob[b, rr, :] = (wb[0, rr, :HW].astype(F32) + (fb[0, rr, :] + fb[1, rr, :]) + vec_v[2:3, fcols]).astype(BF16)
        loop(BLK // ROWS, fin)
        place('y', y_out, b)

    def da_block(k, s):
        rows = ds(k * BLK, BLK)
        copy(DY.at[tok_of(s), rows, :], wb.at[0], S('ld', 0))
        copy(U.at[s, rows, :], wb.at[1, :, pl.ds(0, FB)], S('ld', 1))
        wait(wb.at[0], S('ld', 0))
        wait(wb.at[1, :, pl.ds(0, FB)], S('ld', 1))

        @pl.when(k > 0)
        def _():
            wait(wb.at[2, :, pl.ds(0, FB)], S('st', 0))

        def tile(n):
            start = s * o + n * NTW
            cols = ds(start, NTW)
            da = lax.dot_general(wb[0], wd_v[ds(start, NTW), :], NT, preferred_element_type=F32)
            du = (da * gelu_slope(wb[1, :, cols].astype(F32))).astype(BF16)
            wb[2, :, cols] = du
            db_v[s, :, cols] += jnp.sum(du.astype(F32).reshape(BLK // 8, 8, NTW), axis=0)
        loop((2 - s) * (FH // NTW), tile)
        copy(wb.at[2, :, pl.ds(0, FB)], DU.at[s, rows, :], S('st', 0))

    def da_end():
        wait(wb.at[2, :, pl.ds(0, FB)], S('st', 0))

    def rows_of(kb):
        return ds(lax.rem(kb, NCH) * BLK, BLK), lax.div(kb, NCH)

    d_col = (c, cn, cf, co)

    def dwd_pass(js):
        def load(kb, slot):
            rows, s = rows_of(kb)
            copy(A.at[s, rows, ds(o, FH)], wb.at[slot, :, pl.ds(0, FH)], S('ld', slot))
            for i, j in enumerate(js):
                copy(DY.at[tok_of(s), rows, ds(d_col[j] * HB, HB)], wb.at[2 + slot, :, pl.ds(i * HB, HB)], S('ld', 2 + slot))
        for j in js:
            accD[j] = jnp.zeros((FH, HB), F32)
        load(0, 0)

        def step(kb):
            slot = lax.rem(kb, 2)

            @pl.when(kb < 2 * NCH - 1)
            def _():
                load(kb + 1, 1 - slot)
            wait(wb.at[slot, :, pl.ds(0, FH)], S('ld', slot))
            wait(wb.at[2 + slot, :, pl.ds(0, len(js) * HB)], S('ld', 2 + slot))
            for i, j in enumerate(js):
                accD[j] += lax.dot_general(wb[slot, :, :FH], wb[2 + slot, :, i * HB:(i + 1) * HB], TN, preferred_element_type=F32)
        loop(2 * NCH, step)

    def dwd_opp(j):
        put(accD.at[j, dsm(do * QF, QH, QH), :], r1D.at[j], S('d_so', 2 * j), S('d_r', 2 * j), depth=dn)
        put(accD.at[j, dsm(do * QF + QH, QH, QH), :], r2D.at[j], S('d_so', 2 * j + 1), S('d_r', 2 * j + 1), depth=df)

    def dwd_a(j):
        wait(r1D.at[j], S('d_r', 2 * j))
        rr = dsm(df * QF, QH, QH)
        accD[j, rr, :] += r1D[j]
        put(accD.at[j, ds(df * QF, QF), :], PFD.at[j], S('d_sa', 2 * j), S('d_p', 2 * j), depth=df)
        wait(r2D.at[j], S('d_r', 2 * j + 1))
        rr = dsm(dn * QF + QH, QH, QH)
        accD[j, rr, :] += r2D[j]
        put(accD.at[j, ds(dn * QF, QF), :], PND.at[j], S('d_sa', 2 * j + 1), S('d_p', 2 * j + 1), depth=dn)

    def dwd_rows(q, h, dd):
        return dsm((2 * q + h) * FH + dd * QF, QF, QF)

    def dwd_b(j):
        wait(PFD.at[j], S('d_p', 2 * j))
        wait(PND.at[j], S('d_p', 2 * j + 1))
        pf, pn = fb.at[0, pl.ds(0, QF), pl.ds(0, HB)], fb.at[1, pl.ds(0, QF), pl.ds(0, HB)]
        copy(PFD.at[j], pf, S('ld', 6))
        copy(PND.at[j], pn, S('ld', 7))
        wait(pf, S('ld', 6))
        wait(pn, S('ld', 7))
        finD[j] = (accD[j, ds(d * QF, QF), :] + (pf[...] + pn[...])).astype(BF16)
        dst = gwd_out.at[dwd_rows(c_odd, r, d), :]
        if j:
            put(finD.at[j], dst, S('d_sf', j), S('d_out'), col=d_col[j], row=f)
        else:
            @pl.when(r == f)
            def _():
                copy(finD.at[0], dst, S('d_out'))

            @pl.when(r != f)
            def _():
                put(finD.at[0], dst, S('d_sf', 0), S('d_out'), row=rp)

    def gwd(i, dd, half=None):
        if half is None:
            return gwd_out.at[dsm(i * FH + dd * QF, QF, QF), :]
        return gwd_out.at[dsm(i * FH + dd * QF + half * QH, QH, QH), :]

    def gwd_send():
        wait(gwd_out.at[pl.ds(0, 4 * QF), :], S('d_out'))
        for i in range(4):
            put(gwd(i, d), gwd(i, d), S('d_sy', i), S('d_y', 0), depth=dn)
            put(gwd(i, d), gwd(i, d), S('d_sy', 4 + i), S('d_y', 1), depth=df)

    def gwd_relay():
        wait(gwd_out.at[pl.ds(0, 4 * QF), :], S('d_y', 0))
        for i in range(4):
            put(gwd(i, dn, 1), gwd(i, dn, 1), S('d_sr', i), S('d_o', 1), depth=df)
        wait(gwd_out.at[pl.ds(0, 4 * QF), :], S('d_y', 1))
        for i in range(4):
            put(gwd(i, df, 0), gwd(i, df, 0), S('d_sr', 4 + i), S('d_o', 0), depth=dn)

    def dwu_part(dd):
        def load(kb, slot):
            rows, s = rows_of(kb)
            copy(XN.at[s, rows, ds(dd * DQ, DQ)], wb.at[slot, :, pl.ds(0, DQ)], S('ld', slot))
            copy(DU.at[s, rows, ds(o, FH)], wb.at[2 + slot, :, pl.ds(0, FH)], S('ld', 2 + slot))
        accU[dd] = jnp.zeros((DQ, FH), F32)
        load(0, 0)

        def step(kb):
            slot = lax.rem(kb, 2)

            @pl.when(kb < 2 * NCH - 1)
            def _():
                load(kb + 1, 1 - slot)
            wait(wb.at[slot, :, pl.ds(0, DQ)], S('ld', slot))
            wait(wb.at[2 + slot, :, pl.ds(0, FH)], S('ld', 2 + slot))
            accU[dd] += lax.dot_general(wb[slot, :, :DQ], wb[2 + slot, :, :FH], TN, preferred_element_type=F32)
        loop(2 * NCH, step)

    def dwu_opp():
        put(accU.at[do, pl.ds(0, DH), :], r1U, S('u_so', 0), S('u_r', 0), depth=dn)
        put(accU.at[do, pl.ds(DH, DH), :], r2U, S('u_so', 1), S('u_r', 1), depth=df)

    def dwu_a():
        wait(r1U, S('u_r', 0))
        accU[df, :DH, :] += r1U[...]
        put(accU.at[df], PFU, S('u_sa', 0), S('u_p', 0), depth=df)
        wait(r2U, S('u_r', 1))
        accU[dn, DH:, :] += r2U[...]
        put(accU.at[dn], PNU, S('u_sa', 1), S('u_p', 1), depth=dn)

    def dwu_parts(p):
        dd = jnp.where(p == 0, do, jnp.where(p == 1, df, jnp.where(p == 2, dn, d)))
        dwu_part(dd)

        @pl.when(p == 0)
        def _():
            dwu_opp()
            gwd_send()

        @pl.when(p == 2)
        def _():
            dwu_a()
            gwd_relay()

    def dwu_b():
        wait(PFU, S('u_p', 0))
        wait(PNU, S('u_p', 1))
        pf, pn = fb.at[0, :, pl.ds(0, FH)], fb.at[1, :, pl.ds(0, FH)]
        copy(PFU, pf, S('ld', 6))
        copy(PNU, pn, S('ld', 7))
        wait(pf, S('ld', 6))
        wait(pn, S('ld', 7))

        def fin(i):
            rr = ds(i * ROWS, ROWS)
            finU[rr, :] = (accU[d, rr, :] + (fb[0, rr, :FH] + fb[1, rr, :FH])).astype(BF16)
        loop(DQ // ROWS, fin)
        dst = gwu_out.at[ds(d_odd * DQ, DQ), ds(r * FH, FH)]
        put(finU, dst, S('u_sf', 0), S('u_out', 1), depth=dn, row=dh)
        put(finU, dst, S('u_sf', 1), S('u_out', 2), depth=df, row=dh)

        @pl.when(r == dh)
        def _():
            copy(finU, dst, S('u_out', 0))

        @pl.when(r != dh)
        def _():
            put(finU, dst, S('u_sf', 2), S('u_out', 0), row=rp)

    def gwu(start, size):
        return gwu_out.at[dsm(start, size, size), :]

    def gwu_relay():
        @pl.when(r == dh)
        def _():
            wait(gwu(lax.rem(dn, 2) * DQ, DQ), S('u_out', 1))
            part = gwu(lax.rem(dn, 2) * DQ + DH, DH)
            put(part, part, S('u_sr'), S('u_o', 1), depth=df)

        @pl.when(r != dh)
        def _():
            wait(gwu(lax.rem(df, 2) * DQ, DQ), S('u_out', 2))
            part = gwu(lax.rem(df, 2) * DQ, DH)
            put(part, part, S('u_sr'), S('u_o', 0), depth=dn)

    def gwu_end():
        @pl.when(r == dh)
        def _():
            wait(gwu(d_odd * DQ, DQ), S('u_out', 0))

        @pl.when(r != dh)
        def _():
            wait(gwu(0, DH), S('u_o', 0))
            wait(gwu(0, DH), S('u_o', 1))

    lane = lax.broadcasted_iota(jnp.int32, (ROWS, 128), 1)

    def dx_a(b):
        brow = ds(b * BLK, BLK)
        trow = dsm(r * TH + b * BLK, BLK, BLK)
        wait(GFAR.at[brow, :], S('dfar', b))
        copy(GFAR.at[brow, :], fb.at[0], S('ld', 0))
        copy(GKEEP.at[brow, :], fb.at[1], S('ld', 1))
        copy(X.at[tau, trow, :], wb.at[b], S('ld', 2))
        copy(DY.at[tau, trow, fcols], wb.at[2 + b, :, pl.ds(0, HW)], S('ld', 3))
        wait(fb.at[0], S('ld', 0))
        wait(fb.at[1], S('ld', 1))
        wait(wb.at[b], S('ld', 2))
        wait(wb.at[2 + b, :, pl.ds(0, HW)], S('ld', 3))

        def rows_step(i):
            rr = ds(i * ROWS, ROWS)
            _, mean, inv = norm_rows(wb.at[b], rr)
            xhat = (wb[b, rr, fcols].astype(F32) - mean) * inv
            dxn = fb[0, rr, :] + fb[1, rr, :]
            fb[2 + b, rr, :] = dxn
            gh = dxn * vec_v[0:1, fcols]
            s0 = jnp.sum(gh, axis=1, keepdims=True)
            s1 = jnp.sum(gh * xhat, axis=1, keepdims=True)
            srow = dsm(b * BLK + i * ROWS, ROWS, ROWS)
            st_v[srow, :] = jnp.where(lane < 64, s0, s1)
            ms_v[srow, :] = jnp.where(lane < 64, mean, inv)
            p1 = dxn * xhat
            cs_v[0] += jnp.sum(p1.reshape(ROWS // 8, 8, HW), axis=0)
            cs_v[1] += jnp.sum(dxn.reshape(ROWS // 8, 8, HW), axis=0)
        loop(BLK // ROWS, rows_step)

    NS = max(TH // 128, 1)
    SB = TH // NS

    def stats_send():
        for t in range(NS):
            tr = st_v[t * SB:(t + 1) * SB, :].T
            sx_v[t:t + 1, :SB] = tr[0:1, :]
            sx_v[NS + t:NS + t + 1, :SB] = tr[64:65, :]
        put(sx_v, sr_v, S('s_st'), S('r_st'), col=cf)

    def stats_recv():
        wait(sr_v, S('r_st'))
        for t in range(NS):
            for i in range(2):
                row = (sx_v[i * NS + t:i * NS + t + 1, :SB] + sr_v[i * NS + t:i * NS + t + 1, :SB]) * inv_w
                st2_v[i, t * SB:(t + 1) * SB, :] = jnp.broadcast_to(row, (128, SB)).T

    def dx_b(b):
        def rows_step(i):
            rr = ds(i * ROWS, ROWS)
            srow = dsm(b * BLK + i * ROWS, ROWS, ROWS)
            mean, inv = ms_v[srow, 0:1], ms_v[srow, 64:65]
            xhat = (wb[b, rr, fcols].astype(F32) - mean) * inv
            gh = fb[2 + b, rr, :] * vec_v[0:1, fcols]
            dx = wb[2 + b, rr, :HW].astype(F32) + inv * (gh - st2_v[0, srow, 0:1] - xhat * st2_v[1, srow, 0:1])
            ob[b, rr, :] = dx.astype(BF16)
        loop(BLK // ROWS, rows_step)
        place('d', dx_out, b)

    loop(2, g_near_far)
    wait(wd_v.at[pl.ds(0, 2 * QH), :], S('r_wdy', 2))
    wait(wd_v.at[pl.ds(0, 2 * QH), :], S('r_wdy', 3))
    give('y', A, tile_y, YGOT)
    g_near_far(2)
    keep('y', A, tile_y, YGOT, YFAR, YKEEP)
    g_near_far(3)

    def g_ready(k):
        wait(DY.at[rp, ds(k * BLK, BLK), pl.ds(0, 3 * HB)], S('gd2d', k))
    loop(NCH, g_ready)
    dwd_pass((0, 1, 2))
    for j in (0, 1, 2):
        dwd_opp(j)
    for j in (0, 1, 2):
        dwd_a(j)

    def da_t(k):
        g_opp(k)
        da_block(k, 0)
    loop(NCH, da_t)
    da_end()
    keep_end('y')
    for j in (0, 1, 2):
        dwd_b(j)
    dwd_pass((3,))
    dwd_opp(3)
    y_final(0)
    give('d', DU, tile_g, GGOT)
    dwd_a(3)
    keep('d', DU, tile_g, GGOT, GFAR, GKEEP)
    keep_end('d')
    dwd_b(3)
    loop(NCH, lambda k: da_block(k, 1))
    da_end()
    loop(4, dwu_parts)
    y_final(1)
    dwu_b()
    for b in range(2):
        place_end('y', b)
        dx_a(b)
    stats_send()
    stats_recv()
    for b in range(2):
        dx_b(b)
    gwu_relay()
    copy(cs_v, cs_out, S('l_small', 0))
    copy(db_v, db_out, S('l_small', 1))

    gwu_end()
    wait(gwd_out.at[pl.ds(0, 4 * QH), :], S('d_o', 0))
    wait(gwd_out.at[pl.ds(0, 4 * QH), :], S('d_o', 1))
    for p, out in (('y', y_out), ('d', dx_out)):
        @pl.when(r == tau)
        def _():
            wait(out.at[pl.ds(0, TH), :], S(p + 'out'))

        @pl.when(r != tau)
        def _():
            wait(out, S(p + 'out'))
    wait(cs_v, S('l_small', 0))
    wait(db_v, S('l_small', 1))
    for b in range(2):
        place_end('d', b)
    wait(sx_v, S('s_st'))

    @pl.when(r == dh)
    def _():
        for h in range(2):
            wait(wun_dst, S('s_wun', h))

    @pl.when(r == f)
    def _():
        for s in range(2):
            wait(wd_dst(0, c), S('s_wd0', s))
    for i in range(4):
        wait(wd_dst(0, c), S('s_wdx', i))
    wait(wu_v.at[ds(r * RH, RH), ds(o, FH)], S('s_wu'))
    for i in range(3):
        wait(vec_at, S('s_vec', i))
    wait(bu_at, S('s_vec', 3))
    for s in range(2):
        wait(wd_dst(s, cf), S('s_wdr', s))
    for i in range(2):
        wait(wuq(d), S('s_wuy', i))
        wait(wuq(d, 0), S('s_wuy', 2 + i))
    for i in range(4):
        wait(wdq(0, d), S('s_wdy', i))
        wait(wdq(0, d, 0), S('s_wdy', 4 + i))

    def sends(k):
        for z, Z in (('x', X), ('g', DY)):
            for n in ('s_near', 's_far', 's_rel'):
                wait(reg(Z, k, c), S(z + n, k))
            wait(Z.at[r, ds(k * BLK, BLK), :], S(z + 's_d2d', k))
    loop(NCH, sends)
    for i in range(8):
        wait(r1D.at[0], S('d_so', i))
        wait(PFD.at[0], S('d_sa', i))
        wait(gwd(0, d), S('d_sy', i))
        wait(gwd(0, d, 0), S('d_sr', i))
    for j in range(1, 4):
        wait(finD.at[j], S('d_sf', j))

    @pl.when(r != f)
    def _():
        wait(finD.at[0], S('d_sf', 0))
    for i in range(2):
        wait(r1U, S('u_so', i))
        wait(PFU, S('u_sa', i))
        wait(finU, S('u_sf', i))

    @pl.when(r != dh)
    def _():
        wait(finU, S('u_sf', 2))
    wait(gwu(0, DH), S('u_sr'))


def block_kernel(x, dy, wu, wd, vec, bu):
    (TK, HB), FH = x.shape, wu.shape[1] // 2
    W, HW, TH, BLK, QF, FB = 4 * HB, 2 * HB, TK // 2, TK // NCH, FH // 4, 2 * FH
    assert FB <= W and FH <= HW
    sd = jax.ShapeDtypeStruct
    NS = max(TH // 128, 1)
    outs = [sd((TK, HB), BF16), sd((TK, HB), BF16), sd((W // 2, FB), BF16), sd((4 * FH, HB), BF16), sd((2, 8, HW), F32), sd((2, 8, FB), F32)]
    n_out = len(outs)
    outs += [sd((2, TK, W), BF16)] * 3 + [sd((2, TK, FB), BF16)] * 3
    outs += [sd((TH, W), F32), sd((TH, HW), F32), sd((TH, HW), F32)] * 2
    outs += [sd((4, QF, HB), F32)] * 2 + [sd((W // 4, FH), F32)] * 2
    V = pltpu.VMEM
    scratch = [
        V((W, FB), BF16), V((FB, W), BF16), V((4, FH, HB), F32), V((4, W // 4, FH), F32),
        V((4, FH // 8, HB), F32), V((4, FH // 8, HB), F32), V((W // 8, FH), F32), V((W // 8, FH), F32),
        V((8, W), F32), V((8, FB), F32), V((4, BLK, W), BF16), V((4, BLK, HW), F32), V((2, BLK, HW), BF16),
        V((4, QF, HB), BF16), V((W // 4, FH), BF16), V((2, 8, FB), F32), V((2, 8, HW), F32),
        V((TH, 128), F32), V((TH, 128), F32), V((2, TH, 128), F32), V((2 * NS, 128), F32), V((2 * NS, 128), F32),
        pltpu.SemaphoreType.DMA((N_SEM,)),
    ]
    res = pl.pallas_call(
        functools.partial(body, (TK, HB, FH)),
        out_shape=outs,
        in_specs=[pl.BlockSpec(memory_space=pl.ANY)] * 6,
        out_specs=[pl.BlockSpec(memory_space=pl.ANY)] * len(outs),
        scratch_shapes=scratch,
        compiler_params=pltpu.CompilerParams(collective_id=0, has_side_effects=True, vmem_limit_bytes=67043328),
        name='mlp_block',
    )(x, dy, wu, wd, vec, bu)
    return res[:n_out]


def solution(mesh):
    assert (mesh.shape['col'], mesh.shape['row'], mesh.shape['depth']) == (4, 2, 4)
    tok_spec = P(('dp', 'depth', 'row'), 'col')
    vec_spec = P('col')
    mat_spec = P('row', 'col')
    grad_vec = P(('dp', 'col'))
    grad_mat = P(('dp', 'row'), 'col')
    near = [(i, i ^ 1) for i in range(4)]

    def local_pass(x_blk, gamma_blk, beta_blk, w_up_blk, b_up_blk, w_down_blk, b_down_blk, dy_blk):
        hb, fb = x_blk.shape[1], w_up_blk.shape[1]
        fh = fb // 2
        c, r = lax.axis_index('col'), lax.axis_index('row')
        vec = jnp.stack([gamma_blk, beta_blk, b_down_blk.astype(F32)] + [jnp.zeros_like(gamma_blk)] * 5)
        bu = jnp.broadcast_to(b_up_blk.astype(F32)[None], (8, fb))
        db_down = jnp.sum(dy_blk.astype(F32), axis=0)
        y_blk, dx_blk, grad_w_up, grad_w_down, cs, db = block_kernel(x_blk, dy_blk, w_up_blk, w_down_blk, vec, bu)
        cols = jnp.sum(cs, axis=1)
        mine = lax.dynamic_slice_in_dim(cols, (c % 2) * hb, hb, axis=1)
        other = lax.dynamic_slice_in_dim(cols, (1 - c % 2) * hb, hb, axis=1)
        cols = mine + lax.ppermute(other, 'col', near)
        db_up = jnp.sum(lax.dynamic_slice_in_dim(db, (c % 2) * fh, fh, axis=2), axis=(0, 1))
        db_up = lax.dynamic_update_slice_in_dim(jnp.zeros((fb,), F32), db_up, r * fh, axis=0)
        sums = lax.psum(jnp.concatenate([cols[0], cols[1], db_up, db_down]), ('depth', 'row'))
        return (y_blk, dx_blk, sums[:hb], sums[hb:2 * hb], grad_w_up, sums[2 * hb:2 * hb + fb], grad_w_down, sums[2 * hb + fb:])

    return jax.shard_map(
        local_pass,
        mesh=mesh,
        in_specs=(tok_spec, vec_spec, vec_spec, mat_spec, vec_spec, mat_spec, vec_spec, tok_spec),
        out_specs=(tok_spec, tok_spec, grad_vec, grad_vec, grad_mat, grad_vec, grad_mat, grad_vec),
        check_vma=False,
    )
```

```python
import functools

import jax
import jax.numpy as jnp
from jax import lax
from jax.experimental import pallas as pl
from jax.experimental.pallas import tpu as pltpu
from jax.sharding import PartitionSpec as P

LN_EPS = 1e-5
F32 = jnp.float32
BF16 = jnp.bfloat16
MESH = pl.DeviceIdType.MESH
GELU_A = 0.7978845608028654
GELU_B = 0.044715
NCH = 4
ROWS = 16
LROWS = 64

NN = (((1,), (0,)), ((), ()))
NT = (((1,), (1,)), ((), ()))
TN = (((0,), (0,)), ((), ()))

SEMS = {}
for _z in ('x', 'g'):
    for _n in ('near', 'far', 'opp', 'd2d', 'd2o', 's_near', 's_far', 's_rel', 's_d2d'):
        SEMS[_z + _n] = NCH
    SEMS[_z + 'bounce'] = 2
for _p in ('y', 'd'):
    SEMS.update({_p + 's_give': 2, _p + 'got': 2, _p + 's_far': 2, _p + 'keep': 1, _p + 'far': 2, _p + 's_out': 4, _p + 'out': 1, _p + 'loc': 2})
SEMS.update(l_wu=1, s_wu=1, r_wu=1, s_wun=1, r_wun=1, s_wuy=4, r_wuy=4,
            s_wd0=2, s_wdx=4, r_wd=4, s_wdr=2, s_wdy=32, r_wdy=8,
            l_vec=2, s_vec=4, r_vec=2,
            ld=8, st=4, s_st=2, r_st=2, s_sum=4, r_sum=4,
            d_so=8, d_r=8, d_sa=8, d_p=8, d_sf=4, d_out=1, d_sy=8, d_y=2, d_sr=8, d_o=2,
            u_so=2, u_r=2, u_sa=2, u_p=2, u_sf=3, u_out=3, u_sr=1, u_o=2, l_small=2)
BASE = {}
_at = 0
for _n, _c in SEMS.items():
    BASE[_n] = _at
    _at += _c
N_SEM = _at


def gelu(v):
    return 0.5 * v * (1.0 + jnp.tanh(GELU_A * (v + GELU_B * (v * v * v))))


def gelu_slope(v):
    v2 = v * v
    t = jnp.tanh(GELU_A * (v + GELU_B * (v * v2)))
    return 0.5 * (1.0 + t) + 0.5 * v * (1.0 - t * t) * (GELU_A * (1.0 + 3.0 * GELU_B * v2))


def body(dims, x_ref, dy_ref, wu_ref, wd_ref, vec_ref, bu_ref,
         y_out, dx_out, gwu_out, gwd_out, sum_out,
         X, DY, XN, U, A, DU, YGOT, YFAR, YKEEP, GGOT, GFAR, GKEEP, PFD, PND, PFU, PNU,
         wu_v, wd_v, accD, accU, r1D, r2D, r1U, r2U, vec_v, bu_v, wb, fb, ob, finD,
         db_v, cs_v, st_v, ms_v, st2_v, sx_v, sr_v, bd_v, sum_v, sumr_v, sem):
    TK, HB, FH = dims
    W, HW, TH, BLK, QF = 4 * HB, 2 * HB, TK // 2, TK // NCH, FH // 4
    RH, DQ, QH, DH, FB = W // 2, W // 4, FH // 8, W // 8, 2 * FH
    NTW = HB
    inv_w = 1.0 / W
    finU = wb.at[3, pl.ds(0, DQ), pl.ds(HW, FH)]

    c, r, d = lax.axis_index('col'), lax.axis_index('row'), lax.axis_index('depth')
    c_odd, d_odd = lax.rem(c, 2), lax.rem(d, 2)
    cn, cf, co = c + 1 - 2 * c_odd, 3 - c, lax.rem(c + 2, 4)
    dn, df, do = d + 1 - 2 * d_odd, 3 - d, lax.rem(d + 2, 4)
    f, dh = lax.div(c, 2), lax.div(d, 2)
    tau = lax.rem(lax.div(c + 1, 2), 2)
    rp = 1 - r
    o, o2 = c_odd * FH, (1 - c_odd) * FH

    def S(name, i=0):
        return sem.at[BASE[name] + i]

    def ds(start, size):
        return pl.ds(pl.multiple_of(start, size), size)

    def dsm(start, size, mult):
        return pl.ds(pl.multiple_of(start, mult), size)

    def put(src, dst, ssem, rsem, **dev):
        pltpu.make_async_remote_copy(src_ref=src, dst_ref=dst, send_sem=ssem, recv_sem=rsem,
                                     device_id=dev, device_id_type=MESH).start()

    def copy(src, dst, s):
        pltpu.make_async_copy(src, dst, s).start()

    def wait(ref, s):
        pltpu.make_async_copy(ref, ref, s).wait()

    def loop(n, fn):
        def step(i, carry):
            fn(i)
            return carry
        lax.fori_loop(0, n, step, 0)

    bar = pltpu.get_barrier_semaphore()
    for dev in [dict(row=rp)] + [dict(row=h, **q) for h in range(2) for q in
                                 (dict(col=cn), dict(col=cf), dict(col=co), dict(depth=dn), dict(depth=df))]:
        pl.semaphore_signal(bar, inc=1, device_id=dev, device_id_type=MESH)
    pl.semaphore_wait(bar, 11)

    def wd_src(s, h):
        return wd_ref.at[dsm((2 * s + h) * FH + d * QF, QF, QF), :]

    def wd_dst(s, col):
        return wd_v.at[dsm(s * FH + d * QF, QF, QF), ds(col * HB, HB)]

    def reg(Z, k, col):
        return Z.at[r, ds(k * BLK, BLK), ds(col * HB, HB)]

    def send_own(z, z_ref, Z, which, chunks=(0, NCH)):
        def step(k):
            src = z_ref.at[ds(k * BLK, BLK), :]
            if 'near' in which:
                put(src, reg(Z, k, c), S(z + 's_near', k), S(z + 'near', k), col=cn)
            if 'far' in which:
                put(src, reg(Z, k, c), S(z + 's_far', k), S(z + 'far', k), col=cf)
            if 'd2d' in which:
                put(src, reg(Z, k, c), S(z + 's_d2d', k), S(z + 'd2d', k), row=rp)
        for k in range(*chunks):
            step(k)

    def d2d(z, Z, k, col, s):
        put(reg(Z, k, col), reg(Z, k, col), S(z + 's_d2d', k), S(z + s, k), row=rp)

    wu_own = wu_v.at[ds(r * RH, RH), ds(o, FH)]
    put(wu_ref.at[:, ds(rp * FH, FH)], wu_own, S('s_wu'), S('r_wu'), row=rp)
    copy(wu_ref.at[:, ds(r * FH, FH)], wu_own, S('l_wu'))

    @pl.when(r != f)
    def _():
        for s in range(2):
            for h in range(2):
                put(wd_src(s, h), wd_dst(s, c), S('s_wdx', 2 * s + h), S('r_wd', 2), col=cf, row=h)

    @pl.when(r == f)
    def _():
        for s in range(2):
            copy(wd_src(s, r), wd_dst(s, c), S('r_wd', 0))
            put(wd_src(s, rp), wd_dst(s, c), S('s_wd0', s), S('r_wd', 0), row=rp)

    send_own('x', x_ref, X, ('far', 'd2d'))
    send_own('g', dy_ref, DY, ('d2d',))
    for i, z_ref in enumerate((x_ref, dy_ref)):
        for k in range(NCH):
            copy(z_ref.at[pl.ds(k * BLK, BLK), :], wb.at[i, :, pl.ds(k * HB, HB)], S('xg'[i] + 'bounce', 0))

    vec_at = vec_v.at[:, ds(c * HB, HB)]
    copy(vec_ref, vec_at, S('l_vec', 0))
    put(vec_ref, vec_at, S('s_vec', 0), S('r_vec', 0), col=cn)
    put(vec_ref, vec_at, S('s_vec', 1), S('r_vec', 0), col=cf)
    put(vec_ref, vec_at, S('s_vec', 2), S('r_vec', 0), col=co)
    bu_src, bu_at = bu_ref.at[:, ds(r * FH, FH)], bu_v.at[:, ds(o, FH)]
    copy(bu_src, bu_at, S('l_vec', 1))
    put(bu_src, bu_at, S('s_vec', 3), S('r_vec', 1), col=cn)

    with jax.named_scope('wu_own'):
        wait(wu_own, S('l_wu'))
        wait(wu_v.at[ds(rp * RH, RH), ds(o, FH)], S('r_wu'))
    wun = wu_v.at[ds(d * DQ, DQ), ds(o, FH)]
    put(wun, wun, S('s_wun'), S('r_wun'), col=cn)

    @pl.when(r == f)
    def _():
        for s in range(2):
            for h in range(2):
                put(wd_src(s, h), wd_dst(s, c), S('s_wdx', 2 * s + h), S('r_wd', 1), col=cn, row=h)
    send_own('x', x_ref, X, ('near',), (0, 2))

    for i, Z in enumerate((X, DY)):
        wait(wb.at[i], S('xg'[i] + 'bounce', 0))
        for k in range(NCH):
            copy(wb.at[i, :, pl.ds(k * HB, HB)], reg(Z, k, c), S('xg'[i] + 'bounce', 1))

    db_v[...] = jnp.zeros_like(db_v)
    cs_v[...] = jnp.zeros_like(cs_v)
    bd_v[...] = jnp.zeros_like(bd_v)

    def dy_sum(i):
        rr = ds(i * ROWS, ROWS)
        part = jnp.sum(wb[1, rr, :].astype(F32).reshape(ROWS // 8, 8, W), axis=0)
        bd_v[...] += part[:, :HB] + part[:, HB:2 * HB] + part[:, 2 * HB:3 * HB] + part[:, 3 * HB:]
    loop(BLK // ROWS, dy_sum)

    with jax.named_scope('wd_far'):
        wait(wd_v.at[pl.ds(0, 2 * QF), pl.ds(0, HB)], S('r_wd', 2))
    for s in range(2):
        put(wd_dst(s, cf), wd_dst(s, cf), S('s_wdr', s), S('r_wd', 3), col=cn)
    send_own('x', x_ref, X, ('near',), (2, NCH))

    def wuq(dd, half=None):
        if half is None:
            return wu_v.at[ds(dd * DQ, DQ), ds(o2, FH)]
        return wu_v.at[dsm(dd * DQ + half * DH, DH, DH), ds(o2, FH)]

    with jax.named_scope('wu_near'):
        wait(wuq(d), S('r_wun'))
    put(wuq(d), wuq(d), S('s_wuy', 0), S('r_wuy', 0), depth=dn)
    put(wuq(d), wuq(d), S('s_wuy', 1), S('r_wuy', 1), depth=df)

    def wdq(s, dd, col, half=None):
        if half is None:
            return wd_v.at[dsm(s * FH + dd * QF, QF, QF), ds(col * HB, HB)]
        return wd_v.at[dsm(s * FH + dd * QF + half * QH, QH, QH), ds(col * HB, HB)]

    W_GROUPS = (((0, c), (1, cn), (2, cf)), ((3, co),))

    def wd_send(g):
        if g == 0:
            for i in (0, 1):
                wait(wd_v.at[pl.ds(0, 2 * QF), pl.ds(0, HB)], S('r_wd', i))
        else:
            wait(wd_v.at[pl.ds(0, 2 * QF), pl.ds(0, HB)], S('r_wd', 3))
        for i, col in W_GROUPS[g]:
            for s in range(2):
                put(wdq(s, d, col), wdq(s, d, col), S('s_wdy', 4 * i + s), S('r_wdy', 4 * g), depth=dn)
                put(wdq(s, d, col), wdq(s, d, col), S('s_wdy', 4 * i + 2 + s), S('r_wdy', 4 * g + 1), depth=df)

    def wd_bytes(g, rows):
        return wd_v.at[pl.ds(0, 2 * rows), pl.ds(0, len(W_GROUPS[g]) * HB)]

    def wd_relay(g):
        for i in range(2):
            wait(wd_bytes(g, QF), S('r_wdy', 4 * g + i))
        for i, col in W_GROUPS[g]:
            for s in range(2):
                put(wdq(s, dn, col, 1), wdq(s, dn, col, 1), S('s_wdy', 16 + 4 * i + s), S('r_wdy', 4 * g + 3), depth=df)
                put(wdq(s, df, col, 0), wdq(s, df, col, 0), S('s_wdy', 16 + 4 * i + 2 + s), S('r_wdy', 4 * g + 2), depth=dn)

    def x_near(k):
        wait(reg(X, k, cn), S('xnear', k))
        put(reg(X, k, cn), reg(X, k, cn), S('xs_rel', k), S('xopp', k), col=cf)
        d2d('x', X, k, cn, 'd2d')

    with jax.named_scope('x_near'):
        x_near(0)

    with jax.named_scope('wuy0'):
        wait(wuq(dn), S('r_wuy', 0))
    put(wuq(dn, 1), wuq(dn, 1), S('s_wuy', 2), S('r_wuy', 3), depth=df)
    with jax.named_scope('wuy1'):
        wait(wuq(df), S('r_wuy', 1))
    put(wuq(df, 0), wuq(df, 0), S('s_wuy', 3), S('r_wuy', 2), depth=dn)
    with jax.named_scope('wd_send0'):
        wd_send(0)

    for i, Z in enumerate((X, DY)):
        wait(wb.at[i], S('xg'[i] + 'bounce', 1))
    wait(vec_at, S('l_vec', 0))
    wait(vec_v.at[:, pl.ds(0, 3 * HB)], S('r_vec', 0))
    wait(bu_at, S('l_vec', 1))
    wait(bu_at, S('r_vec', 1))

    def norm_rows(buf, rows):
        xf = buf[rows, :].astype(F32)
        mean = jnp.sum(xf, axis=1, keepdims=True) * inv_w
        cen = xf - mean
        inv = lax.rsqrt(jnp.sum(cen * cen, axis=1, keepdims=True) * inv_w + LN_EPS)
        return cen, mean, inv

    def tok_of(s):
        return tau + s * (1 - 2 * tau)

    def phase1(k):
        @pl.when(k < NCH - 1)
        def _():
            with jax.named_scope('x_near'):
                x_near(k + 1)

        @pl.when(k == 1)
        def _():
            with jax.named_scope('wd_send1'):
                wd_send(1)
            send_own('g', dy_ref, DY, ('near',))

        @pl.when(k == 2)
        def _():
            send_own('g', dy_ref, DY, ('far',))

        @pl.when(k == NCH - 1)
        def _():
            with jax.named_scope('wd_relay0'):
                wd_relay(0)

        with jax.named_scope('x_far'):
            wait(reg(X, k, cf), S('xfar', k))
            d2d('x', X, k, cf, 'd2d')
        with jax.named_scope('x_opp'):
            wait(reg(X, k, co), S('xopp', k))
            d2d('x', X, k, co, 'd2d')
        rows = ds(k * BLK, BLK)
        with jax.named_scope('x_d2d'):
            wait(X.at[rp, rows, :], S('xd2d', k))

        @pl.when(k > 0)
        def _():
            for s in range(2):
                wait(wb.at[s], S('st', s))
        for s in range(2):
            copy(X.at[tok_of(s), rows, :], wb.at[s], S('ld', s))

        @pl.when(k == 0)
        def _():
            with jax.named_scope('wuo'):
                wait(wuq(do, 0), S('r_wuy', 2))
                wait(wuq(do, 1), S('r_wuy', 3))

        for s in range(2):
            wait(wb.at[s], S('ld', s))

            def ln(i):
                rr = ds(i * LROWS, LROWS)
                cen, _, inv = norm_rows(wb.at[s], rr)
                wb[s, rr, :] = (cen * inv * vec_v[0:1, :] + vec_v[1:2, :]).astype(BF16)
            with jax.named_scope('ln'):
                loop(BLK // LROWS, ln)
            copy(wb.at[s], XN.at[s, rows, :], S('st', s))

            def stored():
                wait(wb.at[2], S('st', 2))
                wait(wb.at[3], S('st', 3))
            if s:
                stored()
            else:
                pl.when(k > 0)(stored)

            def tile(n):
                cols = ds(s * o + n * NTW, NTW)
                acc = lax.dot_general(wb[s], wu_v[:, cols], NN, preferred_element_type=F32) + bu_v[0:1, cols]
                u = acc.astype(BF16)
                wb[2, :, cols] = u
                wb[3, :, cols] = gelu(u.astype(F32)).astype(BF16)
            with jax.named_scope('u_tiles'):
                loop((2 - s) * (FH // NTW), tile)
            copy(wb.at[2, :, pl.ds(0, FB)], U.at[s, rows, :], S('st', 2))
            copy(wb.at[3, :, pl.ds(0, FB)], A.at[s, rows, :], S('st', 3))
    loop(NCH, phase1)
    for i in range(4):
        wait(wb.at[i], S('st', i))

    def g_near_far(k):
        wait(reg(DY, k, cf), S('gfar', k))
        put(reg(DY, k, cf), reg(DY, k, cf), S('gs_rel', k), S('gopp', k), col=cn)
        d2d('g', DY, k, cf, 'd2d')
        wait(reg(DY, k, cn), S('gnear', k))
        d2d('g', DY, k, cn, 'd2d')

    def g_opp(k):
        wait(reg(DY, k, co), S('gopp', k))
        d2d('g', DY, k, co, 'd2o')
        wait(reg(DY, k, co), S('gd2o', k))

    def tile_y(lhs, col):
        return lax.dot_general(lhs, wd_v[:, dsm(col, NTW, NTW)], NN, preferred_element_type=F32)

    def tile_g(lhs, col):
        return lax.dot_general(lhs, wu_v[dsm(col, NTW, NTW), :], NT, preferred_element_type=F32)

    def give(p, src, tile, GOT):
        def blk(b):
            return src.at[0, dsm(rp * TH + b * BLK, BLK, BLK), :]
        copy(blk(0), wb.at[0, :, pl.ds(0, FB)], S('ld', 0))

        def step(b):
            wait(wb.at[b, :, pl.ds(0, FB)], S('ld', b))

            @pl.when(b == 0)
            def _():
                copy(blk(1), wb.at[1, :, pl.ds(0, FB)], S('ld', 1))

            def half(h):
                @pl.when(b == 1)
                def _():
                    wait(fb.at[h], S(p + 's_give', h))

                def n_tile(n):
                    fb[h, :, ds(n * NTW, NTW)] = tile(wb[b, :, :FB], h * HW + n * NTW)
                loop(HW // NTW, n_tile)
                put(fb.at[h], GOT.at[ds(b * BLK, BLK), ds(h * HW, HW)], S(p + 's_give', h), S(p + 'got', b), row=rp)
            loop(2, half)
        loop(2, step)

    def keep(p, src, tile, GOT, FAR, KEEP):
        def blk(b):
            return src.at[0, dsm(r * TH + b * BLK, BLK, BLK), :]
        copy(blk(0), wb.at[0, :, pl.ds(0, FB)], S('ld', 0))
        copy(blk(1), wb.at[1, :, pl.ds(0, FB)], S('ld', 1))
        for h in range(2):
            wait(fb.at[h], S(p + 's_give', h))

        def part(b, h):
            brow = ds(b * BLK, BLK)
            col0 = (1 - f + h * (2 * f - 1)) * HW
            out = (2 + b) * (1 - h) + h
            copy(GOT.at[brow, ds(col0, HW)], fb.at[0], S('ld', 2))

            @pl.when(jnp.logical_and(b == 1, h == 1))
            def _():
                wait(fb.at[1], S(p + 'keep'))

            def n_tile(n):
                fb[out, :, ds(n * NTW, NTW)] = tile(wb[b, :, :FB], col0 + n * NTW)
            loop(HW // NTW, n_tile)
            wait(fb.at[0], S('ld', 2))

            def add(i):
                rr = ds(i * ROWS, ROWS)
                fb[out, rr, :] = fb[out, rr, :] + fb[0, rr, :]
            loop(BLK // ROWS, add)

            @pl.when(h == 0)
            def _():
                put(fb.at[2 + b], FAR.at[brow, :], S(p + 's_far', b), S(p + 'far', b), col=cf)

            @pl.when(h == 1)
            def _():
                copy(fb.at[1], KEEP.at[brow, :], S(p + 'keep'))

        def step(b):
            with jax.named_scope('got'):
                wait(GOT.at[ds(b * BLK, BLK), :], S(p + 'got', b))
            wait(wb.at[b, :, pl.ds(0, FB)], S('ld', b))
            loop(2, lambda h: part(b, h))
        loop(2, step)
        wait(fb.at[1], S(p + 'keep'))

    def keep_end(p):
        for b in range(2):
            wait(fb.at[2 + b], S(p + 's_far', b))

    def place(p, out, b):
        dst = out.at[dsm(r * TH + b * BLK, BLK, BLK), :]
        mine, other = ob.at[b, :, ds(c_odd * HB, HB)], ob.at[b, :, ds((1 - c_odd) * HB, HB)]
        put(other, dst, S(p + 's_out', 2 * b), S(p + 'out'), col=cn, row=tau)

        @pl.when(r == tau)
        def _():
            copy(mine, dst, S(p + 'loc', b))

        @pl.when(r != tau)
        def _():
            put(mine, dst, S(p + 's_out', 2 * b + 1), S(p + 'out'), row=rp)

    def place_end(p, b):
        wait(ob.at[b, :, pl.ds(0, HB)], S(p + 's_out', 2 * b))

        @pl.when(r == tau)
        def _():
            wait(ob.at[b, :, pl.ds(0, HB)], S(p + 'loc', b))

        @pl.when(r != tau)
        def _():
            wait(ob.at[b, :, pl.ds(0, HB)], S(p + 's_out', 2 * b + 1))

    fcols = ds(f * HW, HW)

    def y_final(b):
        brow = ds(b * BLK, BLK)
        wait(YFAR.at[brow, :], S('yfar', b))
        copy(YFAR.at[brow, :], fb.at[0], S('ld', 0))
        copy(YKEEP.at[brow, :], fb.at[1], S('ld', 1))
        copy(X.at[tau, dsm(r * TH + b * BLK, BLK, BLK), fcols], wb.at[0, :, pl.ds(0, HW)], S('ld', 2))
        wait(fb.at[0], S('ld', 0))
        wait(fb.at[1], S('ld', 1))
        wait(wb.at[0, :, pl.ds(0, HW)], S('ld', 2))

        def fin(i):
            rr = ds(i * ROWS, ROWS)
            ob[b, rr, :] = (wb[0, rr, :HW].astype(F32) + (fb[0, rr, :] + fb[1, rr, :]) + vec_v[2:3, fcols]).astype(BF16)
        loop(BLK // ROWS, fin)
        place('y', y_out, b)

    def da_load(k, s, slot):
        rows = ds(k * BLK, BLK)
        copy(DY.at[tok_of(s), rows, :], wb.at[slot], S('ld', slot))
        copy(U.at[s, rows, :], wb.at[2 + slot, :, pl.ds(0, FB)], S('ld', 2 + slot))

    def da_block(k, s, slot):
        rows = ds(k * BLK, BLK)
        wait(wb.at[slot], S('ld', slot))
        wait(wb.at[2 + slot, :, pl.ds(0, FB)], S('ld', 2 + slot))

        def tile(n):
            cols = ds(s * o + n * NTW, NTW)
            da = lax.dot_general(wb[slot], wd_v[cols, :], NT, preferred_element_type=F32)
            du = (da * gelu_slope(wb[2 + slot, :, cols].astype(F32))).astype(BF16)
            wb[2 + slot, :, cols] = du
            db_v[s, :, cols] += jnp.sum(du.astype(F32).reshape(BLK // 8, 8, NTW), axis=0)
        loop((2 - s) * (FH // NTW), tile)
        copy(wb.at[2 + slot, :, pl.ds(0, FB)], DU.at[s, rows, :], S('st', slot))

    def da_stored(slot):
        wait(wb.at[2 + slot, :, pl.ds(0, FB)], S('st', slot))

    def rows_of(kb):
        return ds(lax.rem(kb, NCH) * BLK, BLK), lax.div(kb, NCH)

    d_col = (c, cn, cf, co)

    NB, NSLOT = 2 * NCH, 4

    def k_loop(load, use, width):
        for kb in range(NSLOT - 1):
            load(kb, kb)

        def step(kb):
            slot = lax.rem(kb, NSLOT)

            @pl.when(kb + NSLOT - 1 < NB)
            def _():
                load(kb + NSLOT - 1, lax.rem(kb + NSLOT - 1, NSLOT))
            wait(wb.at[slot, :, pl.ds(0, width)], S('ld', slot))
            use(slot)
        loop(NB, step)

    def dwd_pass(js):
        def load(kb, slot):
            rows, s = rows_of(kb)
            copy(A.at[s, rows, ds(o, FH)], wb.at[slot, :, pl.ds(0, FH)], S('ld', slot))
            for i, j in enumerate(js):
                copy(DY.at[tok_of(s), rows, ds(d_col[j] * HB, HB)], wb.at[slot, :, pl.ds(FH + i * HB, HB)], S('ld', slot))

        def use(slot):
            for i, j in enumerate(js):
                for m in range(2):
                    mm = slice(m * FH // 2, (m + 1) * FH // 2)
                    accD[j, mm, :] += lax.dot_general(wb[slot, :, mm], wb[slot, :, FH + i * HB:FH + (i + 1) * HB], TN, preferred_element_type=F32)
        for j in js:
            accD[j] = jnp.zeros((FH, HB), F32)
        k_loop(load, use, FH + len(js) * HB)

    def dwd_opp(j):
        put(accD.at[j, dsm(do * QF, QH, QH), :], r1D.at[j], S('d_so', 2 * j), S('d_r', 2 * j), depth=dn)
        put(accD.at[j, dsm(do * QF + QH, QH, QH), :], r2D.at[j], S('d_so', 2 * j + 1), S('d_r', 2 * j + 1), depth=df)

    def dwd_a(j):
        wait(r1D.at[j], S('d_r', 2 * j))
        rr = dsm(df * QF, QH, QH)
        accD[j, rr, :] += r1D[j]
        put(accD.at[j, ds(df * QF, QF), :], PFD.at[j], S('d_sa', 2 * j), S('d_p', 2 * j), depth=df)
        wait(r2D.at[j], S('d_r', 2 * j + 1))
        rr = dsm(dn * QF + QH, QH, QH)
        accD[j, rr, :] += r2D[j]
        put(accD.at[j, ds(dn * QF, QF), :], PND.at[j], S('d_sa', 2 * j + 1), S('d_p', 2 * j + 1), depth=dn)

    def dwd_rows(q, h, dd):
        return dsm((2 * q + h) * FH + dd * QF, QF, QF)

    def dwd_b(j):
        wait(PFD.at[j], S('d_p', 2 * j))
        wait(PND.at[j], S('d_p', 2 * j + 1))
        wait(PFD.at[j], S('d_sa', 2 * j))
        wait(PND.at[j], S('d_sa', 2 * j + 1))
        pf, pn = accD.at[j, ds(df * QF, QF), :], accD.at[j, ds(dn * QF, QF), :]
        copy(PFD.at[j], pf, S('ld', 6))
        copy(PND.at[j], pn, S('ld', 7))
        wait(pf, S('ld', 6))
        wait(pn, S('ld', 7))
        finD[j] = (accD[j, ds(d * QF, QF), :] + (pf[...] + pn[...])).astype(BF16)
        dst = gwd_out.at[dwd_rows(c_odd, r, d), :]
        if j:
            put(finD.at[j], dst, S('d_sf', j), S('d_out'), col=d_col[j], row=f)
        else:
            @pl.when(r == f)
            def _():
                copy(finD.at[0], dst, S('d_out'))

            @pl.when(r != f)
            def _():
                put(finD.at[0], dst, S('d_sf', 0), S('d_out'), row=rp)

    def gwd(i, dd, half=None):
        if half is None:
            return gwd_out.at[dsm(i * FH + dd * QF, QF, QF), :]
        return gwd_out.at[dsm(i * FH + dd * QF + half * QH, QH, QH), :]

    def gwd_send():
        wait(gwd_out.at[pl.ds(0, 4 * QF), :], S('d_out'))
        for i in range(4):
            put(gwd(i, d), gwd(i, d), S('d_sy', i), S('d_y', 0), depth=dn)
            put(gwd(i, d), gwd(i, d), S('d_sy', 4 + i), S('d_y', 1), depth=df)

    def gwd_relay():
        wait(gwd_out.at[pl.ds(0, 4 * QF), :], S('d_y', 0))
        for i in range(4):
            put(gwd(i, dn, 1), gwd(i, dn, 1), S('d_sr', i), S('d_o', 1), depth=df)
        wait(gwd_out.at[pl.ds(0, 4 * QF), :], S('d_y', 1))
        for i in range(4):
            put(gwd(i, df, 0), gwd(i, df, 0), S('d_sr', 4 + i), S('d_o', 0), depth=dn)

    def dwu_pass(dds):
        def load(kb, slot):
            rows, s = rows_of(kb)
            copy(DU.at[s, rows, ds(o, FH)], wb.at[slot, :, pl.ds(0, FH)], S('ld', slot))
            for i, dd in enumerate(dds):
                copy(XN.at[s, rows, ds(dd * DQ, DQ)], wb.at[slot, :, pl.ds(FH + i * DQ, DQ)], S('ld', slot))

        def use(slot):
            for i, dd in enumerate(dds):
                for m in range(2):
                    mm = slice(m * FH // 2, (m + 1) * FH // 2)
                    accU[dd, :, mm] += lax.dot_general(wb[slot, :, FH + i * DQ:FH + (i + 1) * DQ], wb[slot, :, mm], TN, preferred_element_type=F32)
        for dd in dds:
            accU[dd] = jnp.zeros((DQ, FH), F32)
        k_loop(load, use, FH + len(dds) * DQ)

    def dwu_opp():
        put(accU.at[do, pl.ds(0, DH), :], r1U, S('u_so', 0), S('u_r', 0), depth=dn)
        put(accU.at[do, pl.ds(DH, DH), :], r2U, S('u_so', 1), S('u_r', 1), depth=df)

    def dwu_a():
        wait(r1U, S('u_r', 0))
        accU[df, :DH, :] += r1U[...]
        put(accU.at[df], PFU, S('u_sa', 0), S('u_p', 0), depth=df)
        wait(r2U, S('u_r', 1))
        accU[dn, DH:, :] += r2U[...]
        put(accU.at[dn], PNU, S('u_sa', 1), S('u_p', 1), depth=dn)

    def dwu_b():
        wait(PFU, S('u_p', 0))
        wait(PNU, S('u_p', 1))
        pf, pn = fb.at[0, :, pl.ds(0, FH)], fb.at[1, :, pl.ds(0, FH)]
        copy(PFU, pf, S('ld', 6))
        copy(PNU, pn, S('ld', 7))
        wait(pf, S('ld', 6))
        wait(pn, S('ld', 7))

        def fin(i):
            rr = ds(i * ROWS, ROWS)
            wb[3, rr, HW:HW + FH] = (accU[d, rr, :] + (fb[0, rr, :FH] + fb[1, rr, :FH])).astype(BF16)
        loop(DQ // ROWS, fin)
        dst = gwu_out.at[ds(d_odd * DQ, DQ), ds(r * FH, FH)]
        put(finU, dst, S('u_sf', 0), S('u_out', 1), depth=dn, row=dh)
        put(finU, dst, S('u_sf', 1), S('u_out', 2), depth=df, row=dh)

        @pl.when(r == dh)
        def _():
            copy(finU, dst, S('u_out', 0))

        @pl.when(r != dh)
        def _():
            put(finU, dst, S('u_sf', 2), S('u_out', 0), row=rp)

    def gwu(start, size):
        return gwu_out.at[dsm(start, size, size), :]

    def gwu_relay():
        @pl.when(r == dh)
        def _():
            wait(gwu(lax.rem(dn, 2) * DQ, DQ), S('u_out', 1))
            part = gwu(lax.rem(dn, 2) * DQ + DH, DH)
            put(part, part, S('u_sr'), S('u_o', 1), depth=df)

        @pl.when(r != dh)
        def _():
            wait(gwu(lax.rem(df, 2) * DQ, DQ), S('u_out', 2))
            part = gwu(lax.rem(df, 2) * DQ, DH)
            put(part, part, S('u_sr'), S('u_o', 0), depth=dn)

    def gwu_end():
        @pl.when(r == dh)
        def _():
            wait(gwu(d_odd * DQ, DQ), S('u_out', 0))

        @pl.when(r != dh)
        def _():
            wait(gwu(0, DH), S('u_o', 0))
            wait(gwu(0, DH), S('u_o', 1))

    lane = lax.broadcasted_iota(jnp.int32, (LROWS, 128), 1)

    def dx_a(b):
        brow = ds(b * BLK, BLK)
        trow = dsm(r * TH + b * BLK, BLK, BLK)
        wait(GFAR.at[brow, :], S('dfar', b))
        copy(GFAR.at[brow, :], fb.at[0], S('ld', 0))
        copy(GKEEP.at[brow, :], fb.at[1], S('ld', 1))
        copy(X.at[tau, trow, :], wb.at[b], S('ld', 2))
        copy(DY.at[tau, trow, fcols], wb.at[2 + b, :, pl.ds(0, HW)], S('ld', 3))
        wait(fb.at[0], S('ld', 0))
        wait(fb.at[1], S('ld', 1))
        wait(wb.at[b], S('ld', 2))
        wait(wb.at[2 + b, :, pl.ds(0, HW)], S('ld', 3))

        def rows_step(i):
            rr = ds(i * LROWS, LROWS)
            _, mean, inv = norm_rows(wb.at[b], rr)
            xhat = (wb[b, rr, fcols].astype(F32) - mean) * inv
            dxn = fb[0, rr, :] + fb[1, rr, :]
            fb[2 + b, rr, :] = dxn
            gh = dxn * vec_v[0:1, fcols]
            s0 = jnp.sum(gh, axis=1, keepdims=True)
            s1 = jnp.sum(gh * xhat, axis=1, keepdims=True)
            srow = rr
            st_v[srow, :] = jnp.where(lane < 64, s0, s1)
            ms_v[srow, :] = jnp.where(lane < 64, mean, inv)
            p1 = dxn * xhat
            cs_v[0] += jnp.sum(p1.reshape(LROWS // 8, 8, HW), axis=0)
            cs_v[1] += jnp.sum(dxn.reshape(LROWS // 8, 8, HW), axis=0)
        loop(BLK // LROWS, rows_step)

    SB = min(BLK, 128)
    NS = BLK // SB

    def stats_send(b):
        for t in range(NS):
            tr = st_v[t * SB:(t + 1) * SB, :].T
            sx_v[b, t:t + 1, :SB] = tr[0:1, :]
            sx_v[b, NS + t:NS + t + 1, :SB] = tr[64:65, :]
        put(sx_v.at[b], sr_v.at[b], S('s_st', b), S('r_st', b), col=cf)

    def stats_recv(b):
        wait(sr_v.at[b], S('r_st', b))
        for t in range(NS):
            for i in range(2):
                row = (sx_v[b, i * NS + t:i * NS + t + 1, :SB] + sr_v[b, i * NS + t:i * NS + t + 1, :SB]) * inv_w
                st2_v[i, t * SB:(t + 1) * SB, :] = jnp.broadcast_to(row, (128, SB)).T

    def dx_b(b):
        def rows_step(i):
            rr = ds(i * ROWS, ROWS)
            srow = rr
            mean, inv = ms_v[srow, 0:1], ms_v[srow, 64:65]
            xhat = (wb[b, rr, fcols].astype(F32) - mean) * inv
            gh = fb[2 + b, rr, :] * vec_v[0:1, fcols]
            dx = wb[2 + b, rr, :HW].astype(F32) + inv * (gh - st2_v[0, srow, 0:1] - xhat * st2_v[1, srow, 0:1])
            ob[b, rr, :] = dx.astype(BF16)
        loop(BLK // ROWS, rows_step)
        place('d', dx_out, b)

    def sums():
        cw = jnp.sum(cs_v[...], axis=1)
        for i in range(2):
            for q in range(2):
                @pl.when(c_odd == q)
                def _():
                    sum_v[0, :, i * HB:(i + 1) * HB] = cw[i:i + 1, q * HB:(q + 1) * HB]
                    sum_v[1, :, i * HB:(i + 1) * HB] = cw[i:i + 1, (1 - q) * HB:(2 - q) * HB]
        near = sum_v.at[1, :, pl.ds(0, 2 * HB)]
        near_in = sumr_v.at[0, :, pl.ds(0, 2 * HB)]
        put(near, near_in, S('s_sum', 0), S('r_sum', 0), col=cn)
        sum_v[0, :, 2 * HB:2 * HB + FB] = jnp.zeros((1, FB), F32)
        sum_v[0, :, dsm(2 * HB + r * FH, FH, HB)] = jnp.sum(db_v[0, :, ds(o, FH)] + db_v[1, :, ds(o, FH)], axis=0, keepdims=True)
        sum_v[0, :, 2 * HB + FB:] = jnp.sum(bd_v[...], axis=0, keepdims=True)
        wait(near_in, S('r_sum', 0))
        sum_v[2, :, :2 * HB] = sum_v[0, :, :2 * HB] + sumr_v[0, :, :2 * HB]
        sum_v[2, :, 2 * HB:] = sum_v[0, :, 2 * HB:]
        for i, dev in enumerate((dict(row=rp), dict(depth=dn), dict(depth=df))):
            put(sum_v.at[2 + i], sumr_v.at[1 + i], S('s_sum', 1 + i), S('r_sum', 1 + i), **dev)
            wait(sumr_v.at[1 + i], S('r_sum', 1 + i))
            sum_v[3 + i] = sum_v[2 + i] + sumr_v[1 + i]
        copy(sum_v.at[5], sum_out, S('l_small', 0))

    scope = jax.named_scope

    def g_ready(k):
        wait(DY.at[rp, ds(k * BLK, BLK), pl.ds(0, 3 * HB)], S('gd2d', k))

    def da_t(k):
        with scope('g_opp'):
            g_opp(k)
        slot = lax.rem(k, 2)

        @pl.when(k > 1)
        def _():
            da_stored(slot)
        da_load(k, 0, slot)
        with scope('da_t'):
            da_block(k, 0, slot)

    def da_n(k):
        slot = lax.rem(k, 2)

        @pl.when(k < NCH - 1)
        def _():
            @pl.when(k > 0)
            def _():
                da_stored(1 - slot)
            da_load(k + 1, 1, 1 - slot)
        with scope('da_n'):
            da_block(k, 1, slot)

    def da_end():
        da_stored(0)
        da_stored(1)

    with scope('g01'):
        loop(2, g_near_far)
    with scope('wd_relay1'):
        wd_relay(1)
    with scope('wd_wait'):
        for g in range(2):
            for i in range(2, 4):
                wait(wd_bytes(g, QH), S('r_wdy', 4 * g + i))
    with scope('y_give'):
        give('y', A, tile_y, YGOT)
    with scope('g2'):
        g_near_far(2)
    with scope('y_keep'):
        keep('y', A, tile_y, YGOT, YFAR, YKEEP)
    with scope('g3'):
        g_near_far(3)
    with scope('g_ready'):
        loop(NCH, g_ready)
    with scope('dwd_0'):
        dwd_pass((0,))
        dwd_opp(0)
    with scope('dwd_12'):
        dwd_pass((1, 2))
        dwd_opp(1)
        dwd_opp(2)
    with scope('dwd_a0'):
        dwd_a(0)
    loop(NCH, da_t)
    da_end()
    with scope('dwd_a12'):
        dwd_a(1)
        dwd_a(2)
    with scope('dwd_3'):
        dwd_pass((3,))
        dwd_opp(3)
    with scope('dwd_b0'):
        dwd_b(0)
    with scope('d_give'):
        give('d', DU, tile_g, GGOT)
    with scope('dwd_a3'):
        dwd_a(3)
    with scope('da_n_all'):
        da_load(0, 1, 0)
        loop(NCH, da_n)
        da_end()
    with scope('dwd_b12'):
        dwd_b(1)
        dwd_b(2)
    with scope('dwu_01'):
        dwu_pass((do, df))
        dwu_opp()
    with scope('keep_end_y'):
        keep_end('y')
    with scope('d_keep'):
        keep('d', DU, tile_g, GGOT, GFAR, GKEEP)
    with scope('dwd_b3'):
        dwd_b(3)
    with scope('dwu_23'):
        dwu_pass((dn, d))
    with scope('dwu_a'):
        dwu_a()
    with scope('gwd_send'):
        gwd_send()
    for b in range(2):
        with scope('y_final'):
            y_final(b)
    with scope('gwd_relay'):
        gwd_relay()
    with scope('dwu_b'):
        dwu_b()
    with scope('keep_end_d'):
        keep_end('d')
    for b in range(2):
        with scope('place_end_y'):
            place_end('y', b)
        with scope('dx_a'):
            dx_a(b)
        with scope('stats'):
            stats_send(b)
            stats_recv(b)
        with scope('dx_b'):
            dx_b(b)
        if b == 0:
            with scope('gwu_relay'):
                gwu_relay()
    with scope('sums'):
        sums()

    with scope('gwu_end'):
        gwu_end()
    wait(gwd_out.at[pl.ds(0, 4 * QH), :], S('d_o', 0))
    wait(gwd_out.at[pl.ds(0, 4 * QH), :], S('d_o', 1))
    for p, out in (('y', y_out), ('d', dx_out)):
        @pl.when(r == tau)
        def _():
            wait(out.at[pl.ds(0, TH), :], S(p + 'out'))

        @pl.when(r != tau)
        def _():
            wait(out, S(p + 'out'))
    wait(sum_out, S('l_small', 0))
    for b in range(2):
        place_end('d', b)
    for b in range(2):
        wait(sx_v.at[b], S('s_st', b))
    wait(sum_v.at[1, :, pl.ds(0, 2 * HB)], S('s_sum', 0))
    for i in range(3):
        wait(sum_v.at[2 + i], S('s_sum', 1 + i))
    wait(wun, S('s_wun'))

    @pl.when(r == f)
    def _():
        for s in range(2):
            wait(wd_dst(0, c), S('s_wd0', s))
    for i in range(4):
        wait(wd_dst(0, c), S('s_wdx', i))
    wait(wu_own, S('s_wu'))
    for i in range(3):
        wait(vec_at, S('s_vec', i))
    wait(bu_at, S('s_vec', 3))
    for s in range(2):
        wait(wd_dst(s, cf), S('s_wdr', s))
    for i in range(2):
        wait(wuq(d), S('s_wuy', i))
        wait(wuq(d, 0), S('s_wuy', 2 + i))
    for i in range(16):
        wait(wdq(0, d, c), S('s_wdy', i))
        wait(wdq(0, d, c, 0), S('s_wdy', 16 + i))

    def sends(k):
        for z, Z in (('x', X), ('g', DY)):
            for n in ('s_near', 's_far', 's_rel'):
                wait(reg(Z, k, c), S(z + n, k))
            wait(Z.at[r, ds(k * BLK, BLK), :], S(z + 's_d2d', k))
    loop(NCH, sends)
    for i in range(8):
        wait(r1D.at[0], S('d_so', i))
        wait(gwd(0, d), S('d_sy', i))
        wait(gwd(0, d, 0), S('d_sr', i))
    for j in range(1, 4):
        wait(finD.at[j], S('d_sf', j))

    @pl.when(r != f)
    def _():
        wait(finD.at[0], S('d_sf', 0))
    for i in range(2):
        wait(r1U, S('u_so', i))
        wait(PFU, S('u_sa', i))
        wait(finU, S('u_sf', i))

    @pl.when(r != dh)
    def _():
        wait(finU, S('u_sf', 2))
    wait(gwu(0, DH), S('u_sr'))


def block_kernel(x, dy, wu, wd, vec, bu):
    (TK, HB), FH = x.shape, wu.shape[1] // 2
    W, HW, TH, BLK, QF, FB = 4 * HB, 2 * HB, TK // 2, TK // NCH, FH // 4, 2 * FH
    assert FB <= W and FH <= HW and W // 4 <= BLK and QF <= BLK
    sd = jax.ShapeDtypeStruct
    NS = BLK // min(BLK, 128)
    outs = [sd((TK, HB), BF16), sd((TK, HB), BF16), sd((W // 2, FB), BF16), sd((4 * FH, HB), BF16), sd((1, 3 * HB + FB), F32)]
    n_out = len(outs)
    outs += [sd((2, TK, W), BF16)] * 3 + [sd((2, TK, FB), BF16)] * 3
    outs += [sd((TH, W), F32), sd((TH, HW), F32), sd((TH, HW), F32)] * 2
    outs += [sd((4, QF, HB), F32)] * 2 + [sd((W // 4, FH), F32)] * 2
    V = pltpu.VMEM
    scratch = [
        V((W, FB), BF16), V((FB, W), BF16), V((4, FH, HB), F32), V((4, W // 4, FH), F32),
        V((4, FH // 8, HB), F32), V((4, FH // 8, HB), F32), V((W // 8, FH), F32), V((W // 8, FH), F32),
        V((8, W), F32), V((8, FB), F32), V((4, BLK, W), BF16), V((4, BLK, HW), F32), V((2, BLK, HW), BF16),
        V((4, QF, HB), BF16), V((2, 8, FB), F32), V((2, 8, HW), F32),
        V((BLK, 128), F32), V((BLK, 128), F32), V((2, BLK, 128), F32), V((2, 2 * NS, 128), F32), V((2, 2 * NS, 128), F32),
        V((8, HB), F32), V((6, 1, 3 * HB + FB), F32), V((4, 1, 3 * HB + FB), F32),
        pltpu.SemaphoreType.DMA((N_SEM,)),
    ]
    res = pl.pallas_call(
        functools.partial(body, (TK, HB, FH)),
        out_shape=outs,
        in_specs=[pl.BlockSpec(memory_space=pl.ANY)] * 6,
        out_specs=[pl.BlockSpec(memory_space=pl.ANY)] * len(outs),
        scratch_shapes=scratch,
        compiler_params=pltpu.CompilerParams(collective_id=0, has_side_effects=True, vmem_limit_bytes=67043328),
        name='mlp_block',
    )(x, dy, wu, wd, vec, bu)
    return res[:n_out]


def solution(mesh):
    assert (mesh.shape['col'], mesh.shape['row'], mesh.shape['depth']) == (4, 2, 4)
    tok_spec = P(('dp', 'depth', 'row'), 'col')
    vec_spec = P('col')
    mat_spec = P('row', 'col')
    grad_vec = P(('dp', 'col'))
    grad_mat = P(('dp', 'row'), 'col')
    def local_pass(x_blk, gamma_blk, beta_blk, w_up_blk, b_up_blk, w_down_blk, b_down_blk, dy_blk):
        hb, fb = x_blk.shape[1], w_up_blk.shape[1]
        vec = jnp.stack([gamma_blk, beta_blk, b_down_blk.astype(F32)] + [jnp.zeros_like(gamma_blk)] * 5)
        bu = jnp.broadcast_to(b_up_blk.astype(F32)[None], (8, fb))
        y_blk, dx_blk, grad_w_up, grad_w_down, sums = block_kernel(x_blk, dy_blk, w_up_blk, w_down_blk, vec, bu)
        sums = sums[0]
        return (y_blk, dx_blk, sums[:hb], sums[hb:2 * hb], grad_w_up, sums[2 * hb:2 * hb + fb], grad_w_down, sums[2 * hb + fb:])

    return jax.shard_map(
        local_pass,
        mesh=mesh,
        in_specs=(tok_spec, vec_spec, vec_spec, mat_spec, vec_spec, mat_spec, vec_spec, tok_spec),
        out_specs=(tok_spec, tok_spec, grad_vec, grad_vec, grad_mat, grad_vec, grad_mat, grad_vec),
        check_vma=False,
    )
```

```python
import functools

import jax
import jax.numpy as jnp
from jax import lax
from jax.experimental import pallas as pl
from jax.experimental.pallas import tpu as pltpu
from jax.sharding import PartitionSpec as P

LN_EPS = 1e-5
F32 = jnp.float32
BF16 = jnp.bfloat16
MESH = pl.DeviceIdType.MESH
GELU_A = 0.7978845608028654
GELU_B = 0.044715
NCH = 4
ROWS = 16
LROWS = 64

NN = (((1,), (0,)), ((), ()))
NT = (((1,), (1,)), ((), ()))
TN = (((0,), (0,)), ((), ()))

SEMS = {}
for _z in ('x', 'g'):
    for _n in ('near', 'far', 'opp', 'd2d', 'd2w', 'd2o', 's_near', 's_far', 's_rel', 's_d2d'):
        SEMS[_z + _n] = NCH
    SEMS[_z + 'bounce'] = 2
for _p in ('y', 'd'):
    SEMS.update({_p + 's_give': 2, _p + 'got': 2, _p + 's_far': 2, _p + 'keep': 1, _p + 'far': 2, _p + 's_out': 4, _p + 'out': 1, _p + 'loc': 2})
SEMS.update(l_wu=1, s_wu=1, r_wu=1, s_wun=1, r_wun=1, s_wuy=4, r_wuy=4,
            s_wd0=2, s_wdx=4, r_wd=4, s_wdr=2, s_wdy=24, r_wdy=8,
            l_vec=2, s_vec=4, r_vec=2,
            ld=8, st=6, s_st=2, r_st=2, s_sum=4, r_sum=4,
            d_so=8, d_r=8, d_sa=8, d_p=8, d_sf=4, d_out=1, d_sy=8, d_y=2, d_sr=8, d_o=2,
            u_so=2, u_r=2, u_sa=2, u_p=2, u_sf=3, u_out=3, u_sr=1, u_o=2, l_small=2)
BASE = {}
_at = 0
for _n, _c in SEMS.items():
    BASE[_n] = _at
    _at += _c
N_SEM = _at


def gelu(v):
    return 0.5 * v * (1.0 + jnp.tanh(GELU_A * (v + GELU_B * (v * v * v))))


def gelu_slope(v):
    v2 = v * v
    t = jnp.tanh(v * (GELU_A + (GELU_A * GELU_B) * v2))
    q = (1.0 - t) * (GELU_A + (3.0 * GELU_A * GELU_B) * v2)
    return 0.5 * ((1.0 + t) * (1.0 + v * q))


def body(dims, x_ref, dy_ref, wu_ref, wd_ref, vec_ref, bu_ref,
         y_out, dx_out, gwu_out, gwd_out, sum_out,
         X, DY, XN, U, A, DU, YGOT, YFAR, YKEEP, GGOT, GFAR, GKEEP, PFD, PND, PFU, PNU,
         wu_v, wd_v, accD, accU, r1D, r2D, r1U, r2U, vec_v, bu_v, wx, wo, f0, f1, fs, ob, finD,
         db_v, cs_v, st_v, ms_v, st2_v, sx_v, sr_v, bd_v, sum_v, sumr_v, sem):
    TK, HB, FH = dims
    W, HW, TH, BLK, QF = 4 * HB, 2 * HB, TK // 2, TK // NCH, FH // 4
    RH, DQ, QH, DH, FB = W // 2, W // 4, FH // 8, W // 8, 2 * FH
    NTW = HB
    inv_w = 1.0 / W
    finU = wo.at[1, pl.ds(0, DQ), pl.ds(HW, FH)]
    fg = (f0, f1)
    own2 = (pl.ds(0, FH), pl.ds(FH, FH))

    c, r, d = lax.axis_index('col'), lax.axis_index('row'), lax.axis_index('depth')
    c_odd, d_odd = lax.rem(c, 2), lax.rem(d, 2)
    cn, cf, co = c + 1 - 2 * c_odd, 3 - c, lax.rem(c + 2, 4)
    dn, df, do = d + 1 - 2 * d_odd, 3 - d, lax.rem(d + 2, 4)
    f, dh = lax.div(c, 2), lax.div(d, 2)
    tau = lax.rem(lax.div(c + 1, 2), 2)
    rp = 1 - r
    o, o2 = c_odd * FH, (1 - c_odd) * FH

    def S(name, i=0):
        return sem.at[BASE[name] + i]

    def ds(start, size):
        return pl.ds(pl.multiple_of(start, size), size)

    def dsm(start, size, mult):
        return pl.ds(pl.multiple_of(start, mult), size)

    def put(src, dst, ssem, rsem, **dev):
        pltpu.make_async_remote_copy(src_ref=src, dst_ref=dst, send_sem=ssem, recv_sem=rsem,
                                     device_id=dev, device_id_type=MESH).start()

    def copy(src, dst, s):
        pltpu.make_async_copy(src, dst, s).start()

    def wait(ref, s):
        pltpu.make_async_copy(ref, ref, s).wait()

    def loop(n, fn):
        def step(i, carry):
            fn(i)
            return carry
        lax.fori_loop(0, n, step, 0)

    bar = pltpu.get_barrier_semaphore()
    for dev in [dict(row=rp)] + [dict(row=h, **q) for h in range(2) for q in
                                 (dict(col=cn), dict(col=cf), dict(col=co), dict(depth=dn), dict(depth=df))]:
        pl.semaphore_signal(bar, inc=1, device_id=dev, device_id_type=MESH)
    pl.semaphore_wait(bar, 11)

    def wd_src(s, h):
        return wd_ref.at[dsm((2 * s + h) * FH + d * QF, QF, QF), :]

    def wd_dst(s, col):
        return wd_v.at[dsm(s * FH + d * QF, QF, QF), ds(col * HB, HB)]

    def reg(Z, k, col):
        return Z.at[r, ds(k * BLK, BLK), ds(col * HB, HB)]

    def send_own(z, z_ref, Z, which, chunks=(0, NCH)):
        def step(k):
            src = z_ref.at[ds(k * BLK, BLK), :]
            if 'near' in which:
                put(src, reg(Z, k, c), S(z + 's_near', k), S(z + 'near', k), col=cn)
            if 'far' in which:
                put(src, reg(Z, k, c), S(z + 's_far', k), S(z + 'far', k), col=cf)
            if 'd2d' in which:
                put(src, reg(Z, k, c), S(z + 's_d2d', k), S(z + ('d2d' if z == 'x' else 'd2w'), k), row=rp)
        for k in range(*chunks):
            step(k)

    def d2d(z, Z, k, col, s):
        put(reg(Z, k, col), reg(Z, k, col), S(z + 's_d2d', k), S(z + s, k), row=rp)

    wu_own = wu_v.at[ds(r * RH, RH), ds(o, FH)]
    wd_own = lambda s: wd_v.at[pl.ds(s * FH, FH), ds(c * HB, HB)]

    @pl.when(r != f)
    def _():
        for s in range(2):
            for h in range(2):
                put(wd_src(s, h), wd_dst(s, c), S('s_wdx', 2 * s + h), S('r_wd', 2), col=cf, row=h)

    @pl.when(r == f)
    def _():
        for s in range(2):
            for h in range(2):
                put(wd_src(s, h), wd_dst(s, c), S('s_wdx', 2 * s + h), S('r_wd', 1), col=cn, row=h)
    send_own('x', x_ref, X, ('far',), (0, 2))
    send_own('x', x_ref, X, ('near',), (0, 1))
    put(wu_ref.at[:, ds(rp * FH, FH)], wu_own, S('s_wu'), S('r_wu'), row=rp)
    copy(wu_ref.at[:, ds(r * FH, FH)], wu_own, S('l_wu'))
    send_own('x', x_ref, X, ('d2d',))
    send_own('g', dy_ref, DY, ('d2d',))
    for i, z_ref in enumerate((x_ref, dy_ref)):
        for k in range(NCH):
            copy(z_ref.at[pl.ds(k * BLK, BLK), :], wx.at[i, :, pl.ds(k * HB, HB)], S('xg'[i] + 'bounce', 0))

    vec_at = vec_v.at[:, ds(c * HB, HB)]
    copy(vec_ref, vec_at, S('l_vec', 0))
    put(vec_ref, vec_at, S('s_vec', 0), S('r_vec', 0), col=cn)
    put(vec_ref, vec_at, S('s_vec', 1), S('r_vec', 0), col=cf)
    put(vec_ref, vec_at, S('s_vec', 2), S('r_vec', 0), col=co)
    bu_src, bu_at = bu_ref.at[:, ds(r * FH, FH)], bu_v.at[:, ds(o, FH)]
    copy(bu_src, bu_at, S('l_vec', 1))
    put(bu_src, bu_at, S('s_vec', 3), S('r_vec', 1), col=cn)

    @pl.when(r == f)
    def _():
        for s in range(2):
            copy(wd_ref.at[dsm((2 * s + r) * FH, FH, FH), :], wd_own(s), S('r_wd', 0))
            put(wd_ref.at[dsm((2 * s + rp) * FH, FH, FH), :], wd_own(s), S('s_wd0', s), S('r_wd', 0), row=rp)

    for i, Z in enumerate((X, DY)):
        wait(wx.at[i], S('xg'[i] + 'bounce', 0))
        for k in range(NCH):
            copy(wx.at[i, :, pl.ds(k * HB, HB)], reg(Z, k, c), S('xg'[i] + 'bounce', 1))

    with jax.named_scope('wd_far'):
        wait(wd_v.at[pl.ds(0, 2 * QF), pl.ds(0, HB)], S('r_wd', 2))
    for s in range(2):
        put(wd_dst(s, cf), wd_dst(s, cf), S('s_wdr', s), S('r_wd', 3), col=cn)
    send_own('x', x_ref, X, ('near',), (1, NCH))

    with jax.named_scope('wu_own'):
        wait(wu_own, S('l_wu'))
        wait(wu_v.at[ds(rp * RH, RH), ds(o, FH)], S('r_wu'))
    wun = wu_v.at[ds(d * DQ, DQ), ds(o, FH)]
    put(wun, wun, S('s_wun'), S('r_wun'), col=cn)

    db_v[...] = jnp.zeros_like(db_v)
    cs_v[...] = jnp.zeros_like(cs_v)
    bd_v[...] = jnp.zeros_like(bd_v)

    def dy_sum(i):
        rr = ds(i * ROWS, ROWS)
        part = jnp.sum(wx[1, rr, :].astype(F32).reshape(ROWS // 8, 8, W), axis=0)
        bd_v[...] += part[:, :HB] + part[:, HB:2 * HB] + part[:, 2 * HB:3 * HB] + part[:, 3 * HB:]
    with jax.named_scope('dy_sum'):
        loop(BLK // ROWS, dy_sum)

    def wuq(dd, half=None):
        if half is None:
            return wu_v.at[ds(dd * DQ, DQ), ds(o2, FH)]
        return wu_v.at[dsm(dd * DQ + half * DH, DH, DH), ds(o2, FH)]

    def wu_send():
        with jax.named_scope('wu_near'):
            wait(wuq(d), S('r_wun'))
        put(wuq(d), wuq(d), S('s_wuy', 0), S('r_wuy', 0), depth=dn)
        put(wuq(d), wuq(d), S('s_wuy', 1), S('r_wuy', 1), depth=df)

    def wu_relay():
        with jax.named_scope('wuy'):
            wait(wuq(dn), S('r_wuy', 0))
            wait(wuq(df), S('r_wuy', 1))
        put(wuq(dn, 1), wuq(dn, 1), S('s_wuy', 2), S('r_wuy', 3), depth=df)
        put(wuq(df, 0), wuq(df, 0), S('s_wuy', 3), S('r_wuy', 2), depth=dn)

    def wdq(s, dd, col, half=None):
        if half is None:
            return wd_v.at[dsm(s * FH + dd * QF, QF, QF), ds(col * HB, HB)]
        return wd_v.at[dsm(s * FH + dd * QF + half * QH, QH, QH), ds(col * HB, HB)]

    W_GROUPS = (((0, cn), (1, cf)), ((2, co),))

    def wd_send(g):
        if g == 0:
            wait(wd_v.at[pl.ds(0, 2 * QF), pl.ds(0, HB)], S('r_wd', 1))
        else:
            wait(wd_v.at[pl.ds(0, 2 * QF), pl.ds(0, HB)], S('r_wd', 3))
        for i, col in W_GROUPS[g]:
            for s in range(2):
                put(wdq(s, d, col), wdq(s, d, col), S('s_wdy', 4 * i + s), S('r_wdy', 4 * g), depth=dn)
                put(wdq(s, d, col), wdq(s, d, col), S('s_wdy', 4 * i + 2 + s), S('r_wdy', 4 * g + 1), depth=df)

    def wd_bytes(g, rows):
        return wd_v.at[pl.ds(0, 2 * rows), pl.ds(0, len(W_GROUPS[g]) * HB)]

    def wd_relay(g):
        for i in range(2):
            wait(wd_bytes(g, QF), S('r_wdy', 4 * g + i))
        for i, col in W_GROUPS[g]:
            for s in range(2):
                put(wdq(s, dn, col, 1), wdq(s, dn, col, 1), S('s_wdy', 12 + 4 * i + s), S('r_wdy', 4 * g + 3), depth=df)
                put(wdq(s, df, col, 0), wdq(s, df, col, 0), S('s_wdy', 12 + 4 * i + 2 + s), S('r_wdy', 4 * g + 2), depth=dn)

    def x_near(k):
        wait(reg(X, k, cn), S('xnear', k))
        put(reg(X, k, cn), reg(X, k, cn), S('xs_rel', k), S('xopp', k), col=cf)
        d2d('x', X, k, cn, 'd2d')

    with jax.named_scope('wd_send0'):
        wd_send(0)
    with jax.named_scope('x_near'):
        x_near(0)
    send_own('x', x_ref, X, ('far',), (2, 3))

    for i, Z in enumerate((X, DY)):
        wait(wx.at[i], S('xg'[i] + 'bounce', 1))
    wait(vec_at, S('l_vec', 0))
    wait(vec_v.at[:, pl.ds(0, 3 * HB)], S('r_vec', 0))
    wait(bu_at, S('l_vec', 1))
    wait(bu_at, S('r_vec', 1))

    def norm_rows(buf, rows):
        xf = buf[rows, :].astype(F32)
        mean = jnp.sum(xf, axis=1, keepdims=True) * inv_w
        cen = xf - mean
        inv = lax.rsqrt(jnp.sum(cen * cen, axis=1, keepdims=True) * inv_w + LN_EPS)
        return cen, mean, inv

    def tok_of(s):
        return tau + s * (1 - 2 * tau)

    def chain(tiles, half_done=None):
        for i, (product, _) in enumerate(tiles):
            if i:
                tiles[i - 1][1](fg[(i - 1) % 2])
            fg[i % 2][:, :NTW] = product()
            if half_done and i == N_T:
                half_done()
        tiles[-1][1](fg[(len(tiles) - 1) % 2])

    N_T = FH // NTW

    def u_tile(i, n, start):
        cols = ds(start + n * NTW, NTW)
        at = pl.ds((i * N_T + n) * NTW, NTW)

        def product():
            return lax.dot_general(wx[i], wu_v[:, cols], NN, preferred_element_type=F32)

        def epilogue(acc):
            u = (acc[:, :NTW] + bu_v[0:1, cols]).astype(BF16)
            wo[0, :, at] = u
            wo[1, :, at] = gelu(u.astype(F32)).astype(BF16)
        return product, epilogue

    def u_store(i, s, rows, start):
        copy(wo.at[0, :, own2[i]], U.at[s, rows, ds(start, FH)], S('st', 2 + i))
        copy(wo.at[1, :, own2[i]], A.at[s, rows, ds(start, FH)], S('st', 4 + i))

    def u_stored():
        for i in range(2):
            wait(wo.at[0, :, own2[i]], S('st', 2 + i))
            wait(wo.at[1, :, own2[i]], S('st', 4 + i))

    def phase1(k):
        @pl.when(k < NCH - 1)
        def _():
            with jax.named_scope('x_near'):
                x_near(k + 1)

        @pl.when(k == 0)
        def _():
            send_own('x', x_ref, X, ('far',), (3, 4))
            with jax.named_scope('wd_send1'):
                wd_send(1)

        @pl.when(k == 1)
        def _():
            with jax.named_scope('wd_relay0'):
                wd_relay(0)
            send_own('g', dy_ref, DY, ('near',))

        @pl.when(k == 2)
        def _():
            send_own('g', dy_ref, DY, ('far',))
            with jax.named_scope('wd_relay1'):
                wd_relay(1)

        with jax.named_scope('x_far'):
            wait(reg(X, k, cf), S('xfar', k))
            d2d('x', X, k, cf, 'd2d')
        with jax.named_scope('x_opp'):
            wait(reg(X, k, co), S('xopp', k))
            d2d('x', X, k, co, 'd2d')

        @pl.when(k == NCH - 1)
        def _():
            wu_send()
        rows = ds(k * BLK, BLK)
        with jax.named_scope('x_d2d'):
            wait(X.at[rp, rows, :], S('xd2d', k))

        @pl.when(k > 0)
        def _():
            for s in range(2):
                wait(wx.at[s], S('st', s))
        for s in range(2):
            copy(X.at[tok_of(s), rows, :], wx.at[s], S('ld', s))
        for s in range(2):
            wait(wx.at[s], S('ld', s))

            def ln(i):
                rr = ds(i * LROWS, LROWS)
                cen, _, inv = norm_rows(wx.at[s], rr)
                wx[s, rr, :] = (cen * inv * vec_v[0:1, :] + vec_v[1:2, :]).astype(BF16)
            with jax.named_scope('ln'):
                loop(BLK // LROWS, ln)
            copy(wx.at[s], XN.at[s, rows, :], S('st', s))
        pl.when(k > 0)(u_stored)
        with jax.named_scope('u_own'):
            chain([u_tile(i, n, o) for i in range(2) for n in range(N_T)])
        for s in range(2):
            u_store(s, s, rows, o)
    loop(NCH, phase1)
    for s in range(2):
        wait(wx.at[s], S('st', s))
    u_stored()

    def u_near(kp):
        rows = [ds((2 * kp + i) * BLK, BLK) for i in range(2)]
        for i in range(2):
            copy(XN.at[0, rows[i], :], wx.at[i], S('ld', i))
        for i in range(2):
            wait(wx.at[i], S('ld', i))
        pl.when(kp > 0)(u_stored)
        chain([u_tile(i, n, o2) for i in range(2) for n in range(N_T)])
        for i in range(2):
            u_store(i, 0, rows[i], o2)

    def g_near_far(k):
        wait(reg(DY, k, cf), S('gfar', k))
        put(reg(DY, k, cf), reg(DY, k, cf), S('gs_rel', k), S('gopp', k), col=cn)
        d2d('g', DY, k, cf, 'd2d')
        wait(reg(DY, k, cn), S('gnear', k))
        d2d('g', DY, k, cn, 'd2d')

    def g_opp(k):
        wait(reg(DY, k, co), S('gopp', k))
        d2d('g', DY, k, co, 'd2o')
        wait(reg(DY, k, co), S('gd2o', k))

    def tile_y(lhs, col):
        return lax.dot_general(lhs, wd_v[:, dsm(col, NTW, NTW)], NN, preferred_element_type=F32)

    def tile_g(lhs, col):
        return lax.dot_general(lhs, wu_v[dsm(col, NTW, NTW), :], NT, preferred_element_type=F32)

    def give(p, src, tile, GOT):
        def blk(b):
            return src.at[0, dsm(rp * TH + b * BLK, BLK, BLK), :]
        for b in range(2):
            copy(blk(b), wx.at[b, :, pl.ds(0, FB)], S('ld', b))

        def step(b):
            wait(wx.at[b, :, pl.ds(0, FB)], S('ld', b))
            for h in range(2):
                @pl.when(b == 1)
                def _():
                    wait(fg[h], S(p + 's_give', h))

                def n_tile(n):
                    fg[h][:, ds(n * NTW, NTW)] = tile(wx[b, :, :FB], h * HW + n * NTW)
                loop(HW // NTW, n_tile)
                put(fg[h], GOT.at[ds(b * BLK, BLK), pl.ds(h * HW, HW)], S(p + 's_give', h), S(p + 'got', b), row=rp)
        loop(2, step)

    def keep(p, src, tile, GOT, FAR, KEEP):
        def blk(b):
            return src.at[0, dsm(r * TH + b * BLK, BLK, BLK), :]
        for b in range(2):
            copy(blk(b), wx.at[b, :, pl.ds(0, FB)], S('ld', b))
        for h in range(2):
            wait(fg[h], S(p + 's_give', h))

        def part(b, h):
            brow = ds(b * BLK, BLK)
            col0 = (1 - f + h * (2 * f - 1)) * HW
            out = f1 if h else fs.at[b]
            copy(GOT.at[brow, ds(col0, HW)], f0, S('ld', 2))
            if h:
                @pl.when(b == 1)
                def _():
                    wait(f1, S(p + 'keep'))

            def n_tile(n):
                out[:, ds(n * NTW, NTW)] = tile(wx[b, :, :FB], col0 + n * NTW)
            loop(HW // NTW, n_tile)
            wait(f0, S('ld', 2))

            def add(i):
                rr = ds(i * LROWS, LROWS)
                out[rr, :] = out[rr, :] + f0[rr, :]
            loop(BLK // LROWS, add)
            if h:
                copy(f1, KEEP.at[brow, :], S(p + 'keep'))
            else:
                put(fs.at[b], FAR.at[brow, :], S(p + 's_far', b), S(p + 'far', b), col=cf)

        def step(b):
            with jax.named_scope('got'):
                wait(GOT.at[ds(b * BLK, BLK), :], S(p + 'got', b))
            wait(wx.at[b, :, pl.ds(0, FB)], S('ld', b))
            for h in range(2):
                part(b, h)
        loop(2, step)
        wait(f1, S(p + 'keep'))

    def keep_end(p):
        for b in range(2):
            wait(fs.at[b], S(p + 's_far', b))

    def place(p, out, b):
        dst = out.at[dsm(r * TH + b * BLK, BLK, BLK), :]
        mine, other = ob.at[b, :, ds(c_odd * HB, HB)], ob.at[b, :, ds((1 - c_odd) * HB, HB)]
        put(other, dst, S(p + 's_out', 2 * b), S(p + 'out'), col=cn, row=tau)

        @pl.when(r == tau)
        def _():
            copy(mine, dst, S(p + 'loc', b))

        @pl.when(r != tau)
        def _():
            put(mine, dst, S(p + 's_out', 2 * b + 1), S(p + 'out'), row=rp)

    def place_end(p, b):
        wait(ob.at[b, :, pl.ds(0, HB)], S(p + 's_out', 2 * b))

        @pl.when(r == tau)
        def _():
            wait(ob.at[b, :, pl.ds(0, HB)], S(p + 'loc', b))

        @pl.when(r != tau)
        def _():
            wait(ob.at[b, :, pl.ds(0, HB)], S(p + 's_out', 2 * b + 1))

    fcols = ds(f * HW, HW)

    def y_final(b):
        brow = ds(b * BLK, BLK)
        wait(YFAR.at[brow, :], S('yfar', b))
        copy(YFAR.at[brow, :], f0, S('ld', 0))
        copy(YKEEP.at[brow, :], f1, S('ld', 1))
        copy(X.at[tau, dsm(r * TH + b * BLK, BLK, BLK), fcols], wx.at[0, :, pl.ds(0, HW)], S('ld', 2))
        wait(f0, S('ld', 0))
        wait(f1, S('ld', 1))
        wait(wx.at[0, :, pl.ds(0, HW)], S('ld', 2))

        def fin(i):
            rr = ds(i * ROWS, ROWS)
            ob[b, rr, :] = (wx[0, rr, :HW].astype(F32) + (f0[rr, :] + f1[rr, :]) + vec_v[2:3, fcols]).astype(BF16)
        loop(BLK // ROWS, fin)
        place('y', y_out, b)

    def da_tile(i, n, start, s):
        cols = ds(start + n * NTW, NTW)
        at = pl.ds((i * N_T + n) * NTW, NTW)

        def product():
            return lax.dot_general(wx[i], wd_v[cols, :], NT, preferred_element_type=F32)

        def epilogue(acc):
            du = (acc[:, :NTW] * gelu_slope(wo[0, :, at].astype(F32))).astype(BF16)
            wo[1, :, at] = du
            if s is not None:
                db_v[s, :, n * NTW:(n + 1) * NTW] += jnp.sum(du.astype(F32).reshape(BLK // 8, 8, NTW), axis=0)
        return product, epilogue

    def du_stored():
        for i in range(2):
            wait(wo.at[1, :, own2[i]], S('st', 4 + i))

    def da_pass(parts, start, with_sum):
        def load(k, i):
            t, s, kk = parts(k)[i]
            rows = ds(kk * BLK, BLK)
            copy(DY.at[t, rows, :], wx.at[i], S('ld', i))
            copy(U.at[s, rows, ds(start, FH)], wo.at[0, :, own2[i]], S('ld', 2 + i))

        def store(k, i):
            t, s, kk = parts(k)[i]
            copy(wo.at[1, :, own2[i]], DU.at[s, ds(kk * BLK, BLK), ds(start, FH)], S('st', 4 + i))

        def step(k, n_steps):
            tiles = [da_tile(i, n, start, i if with_sum else None) for i in range(2) for n in range(N_T)]
            for i in range(2):
                wait(wx.at[i], S('ld', i))
                wait(wo.at[0, :, own2[i]], S('ld', 2 + i))
            pl.when(k > 0)(du_stored)
            def done(i):
                store(k, i)

                @pl.when(k < n_steps - 1)
                def _():
                    load(k + 1, i)
            chain(tiles, lambda: done(0))
            done(1)
        for i in range(2):
            load(0, i)
        return step

    def rows_of(kb):
        return ds(lax.rem(kb, NCH) * BLK, BLK), lax.div(kb, NCH)

    d_col = (c, cn, cf, co)

    NB = 2 * NCH
    rings = (wx, wo)

    def k_loop(load, use, width):
        for kb in range(3):
            load(kb, rings[kb % 2].at[kb // 2], S('ld', kb))

        def step(i):
            p = lax.rem(i, 2)
            for q in range(2):
                kb = 2 * i + q
                np_ = lax.rem(i + 1 + q, 2)

                @pl.when(kb + 3 < NB)
                def _():
                    load(kb + 3, rings[1 - q].at[np_], S('ld', (1 - q) + 2 * np_))
                buf = rings[q].at[p]
                wait(buf.at[:, pl.ds(0, width)], S('ld', q + 2 * p))
                use(buf)
        loop(NB // 2, step)

    def dwd_pass(js):
        def load(kb, buf, s_):
            rows, s = rows_of(kb)
            copy(A.at[s, rows, ds(o, FH)], buf.at[:, pl.ds(0, FH)], s_)
            for i, j in enumerate(js):
                copy(DY.at[tok_of(s), rows, ds(d_col[j] * HB, HB)], buf.at[:, pl.ds(FH + i * HB, HB)], s_)

        def use(buf):
            for i, j in enumerate(js):
                for m in range(2):
                    mm = slice(m * FH // 2, (m + 1) * FH // 2)
                    accD[j, mm, :] += lax.dot_general(buf[:, mm], buf[:, FH + i * HB:FH + (i + 1) * HB], TN, preferred_element_type=F32)
        for j in js:
            accD[j] = jnp.zeros((FH, HB), F32)
        k_loop(load, use, FH + len(js) * HB)

    def dwd_opp(j):
        put(accD.at[j, dsm(do * QF, QH, QH), :], r1D.at[j], S('d_so', 2 * j), S('d_r', 2 * j), depth=dn)
        put(accD.at[j, dsm(do * QF + QH, QH, QH), :], r2D.at[j], S('d_so', 2 * j + 1), S('d_r', 2 * j + 1), depth=df)

    def dwd_a(j):
        wait(r1D.at[j], S('d_r', 2 * j))
        rr = dsm(df * QF, QH, QH)
        accD[j, rr, :] += r1D[j]
        put(accD.at[j, ds(df * QF, QF), :], PFD.at[j], S('d_sa', 2 * j), S('d_p', 2 * j), depth=df)
        wait(r2D.at[j], S('d_r', 2 * j + 1))
        rr = dsm(dn * QF + QH, QH, QH)
        accD[j, rr, :] += r2D[j]
        put(accD.at[j, ds(dn * QF, QF), :], PND.at[j], S('d_sa', 2 * j + 1), S('d_p', 2 * j + 1), depth=dn)

    def dwd_rows(q, h, dd):
        return dsm((2 * q + h) * FH + dd * QF, QF, QF)

    def dwd_b(j):
        wait(PFD.at[j], S('d_p', 2 * j))
        wait(PND.at[j], S('d_p', 2 * j + 1))
        wait(PFD.at[j], S('d_sa', 2 * j))
        wait(PND.at[j], S('d_sa', 2 * j + 1))
        pf, pn = accD.at[j, ds(df * QF, QF), :], accD.at[j, ds(dn * QF, QF), :]
        copy(PFD.at[j], pf, S('ld', 6))
        copy(PND.at[j], pn, S('ld', 7))
        wait(pf, S('ld', 6))
        wait(pn, S('ld', 7))
        finD[j] = (accD[j, ds(d * QF, QF), :] + (pf[...] + pn[...])).astype(BF16)
        dst = gwd_out.at[dwd_rows(c_odd, r, d), :]
        if j:
            put(finD.at[j], dst, S('d_sf', j), S('d_out'), col=d_col[j], row=f)
        else:
            @pl.when(r == f)
            def _():
                copy(finD.at[0], dst, S('d_out'))

            @pl.when(r != f)
            def _():
                put(finD.at[0], dst, S('d_sf', 0), S('d_out'), row=rp)

    def gwd(i, dd, half=None):
        if half is None:
            return gwd_out.at[dsm(i * FH + dd * QF, QF, QF), :]
        return gwd_out.at[dsm(i * FH + dd * QF + half * QH, QH, QH), :]

    def gwd_send():
        wait(gwd_out.at[pl.ds(0, 4 * QF), :], S('d_out'))
        for i in range(4):
            put(gwd(i, d), gwd(i, d), S('d_sy', i), S('d_y', 0), depth=dn)
            put(gwd(i, d), gwd(i, d), S('d_sy', 4 + i), S('d_y', 1), depth=df)

    def gwd_relay():
        wait(gwd_out.at[pl.ds(0, 4 * QF), :], S('d_y', 0))
        for i in range(4):
            put(gwd(i, dn, 1), gwd(i, dn, 1), S('d_sr', i), S('d_o', 1), depth=df)
        wait(gwd_out.at[pl.ds(0, 4 * QF), :], S('d_y', 1))
        for i in range(4):
            put(gwd(i, df, 0), gwd(i, df, 0), S('d_sr', 4 + i), S('d_o', 0), depth=dn)

    def dwu_pass(dds):
        def load(kb, buf, s_):
            rows, s = rows_of(kb)
            copy(DU.at[s, rows, ds(o, FH)], buf.at[:, pl.ds(0, FH)], s_)
            for i, dd in enumerate(dds):
                copy(XN.at[s, rows, ds(dd * DQ, DQ)], buf.at[:, pl.ds(FH + i * DQ, DQ)], s_)

        def use(buf):
            for i, dd in enumerate(dds):
                for m in range(2):
                    mm = slice(m * FH // 2, (m + 1) * FH // 2)
                    accU[dd, :, mm] += lax.dot_general(buf[:, FH + i * DQ:FH + (i + 1) * DQ], buf[:, mm], TN, preferred_element_type=F32)
        for dd in dds:
            accU[dd] = jnp.zeros((DQ, FH), F32)
        k_loop(load, use, FH + len(dds) * DQ)

    def dwu_opp():
        put(accU.at[do, pl.ds(0, DH), :], r1U, S('u_so', 0), S('u_r', 0), depth=dn)
        put(accU.at[do, pl.ds(DH, DH), :], r2U, S('u_so', 1), S('u_r', 1), depth=df)

    def dwu_a():
        wait(r1U, S('u_r', 0))
        accU[df, :DH, :] += r1U[...]
        put(accU.at[df], PFU, S('u_sa', 0), S('u_p', 0), depth=df)
        wait(r2U, S('u_r', 1))
        accU[dn, DH:, :] += r2U[...]
        put(accU.at[dn], PNU, S('u_sa', 1), S('u_p', 1), depth=dn)

    def dwu_b():
        wait(PFU, S('u_p', 0))
        wait(PNU, S('u_p', 1))
        pf, pn = f0.at[pl.ds(0, DQ), pl.ds(0, FH)], f1.at[pl.ds(0, DQ), pl.ds(0, FH)]
        copy(PFU, pf, S('ld', 6))
        copy(PNU, pn, S('ld', 7))
        wait(pf, S('ld', 6))
        wait(pn, S('ld', 7))

        def fin(i):
            rr = ds(i * ROWS, ROWS)
            wo[1, rr, HW:HW + FH] = (accU[d, rr, :] + (f0[rr, :FH] + f1[rr, :FH])).astype(BF16)
        loop(DQ // ROWS, fin)
        dst = gwu_out.at[ds(d_odd * DQ, DQ), ds(r * FH, FH)]
        put(finU, dst, S('u_sf', 0), S('u_out', 1), depth=dn, row=dh)
        put(finU, dst, S('u_sf', 1), S('u_out', 2), depth=df, row=dh)

        @pl.when(r == dh)
        def _():
            copy(finU, dst, S('u_out', 0))

        @pl.when(r != dh)
        def _():
            put(finU, dst, S('u_sf', 2), S('u_out', 0), row=rp)

    def gwu(start, size):
        return gwu_out.at[dsm(start, size, size), :]

    def gwu_relay():
        @pl.when(r == dh)
        def _():
            wait(gwu(lax.rem(dn, 2) * DQ, DQ), S('u_out', 1))
            part = gwu(lax.rem(dn, 2) * DQ + DH, DH)
            put(part, part, S('u_sr'), S('u_o', 1), depth=df)

        @pl.when(r != dh)
        def _():
            wait(gwu(lax.rem(df, 2) * DQ, DQ), S('u_out', 2))
            part = gwu(lax.rem(df, 2) * DQ, DH)
            put(part, part, S('u_sr'), S('u_o', 0), depth=dn)

    def gwu_end():
        @pl.when(r == dh)
        def _():
            wait(gwu(d_odd * DQ, DQ), S('u_out', 0))

        @pl.when(r != dh)
        def _():
            wait(gwu(0, DH), S('u_o', 0))
            wait(gwu(0, DH), S('u_o', 1))

    lane = lax.broadcasted_iota(jnp.int32, (LROWS, 128), 1)

    def dx_a(b):
        brow = ds(b * BLK, BLK)
        trow = dsm(r * TH + b * BLK, BLK, BLK)
        wait(GFAR.at[brow, :], S('dfar', b))
        copy(GFAR.at[brow, :], f0, S('ld', 0))
        copy(GKEEP.at[brow, :], f1, S('ld', 1))
        copy(X.at[tau, trow, :], wx.at[b], S('ld', 2))
        copy(DY.at[tau, trow, fcols], wo.at[b, :, pl.ds(0, HW)], S('ld', 3))
        wait(f0, S('ld', 0))
        wait(f1, S('ld', 1))
        wait(wx.at[b], S('ld', 2))
        wait(wo.at[b, :, pl.ds(0, HW)], S('ld', 3))

        def rows_step(i):
            rr = ds(i * LROWS, LROWS)
            _, mean, inv = norm_rows(wx.at[b], rr)
            xhat = (wx[b, rr, fcols].astype(F32) - mean) * inv
            dxn = f0[rr, :] + f1[rr, :]
            fs[b, rr, :] = dxn
            gh = dxn * vec_v[0:1, fcols]
            s0 = jnp.sum(gh, axis=1, keepdims=True)
            s1 = jnp.sum(gh * xhat, axis=1, keepdims=True)
            srow = rr
            st_v[srow, :] = jnp.where(lane < 64, s0, s1)
            ms_v[srow, :] = jnp.where(lane < 64, mean, inv)
            p1 = dxn * xhat
            cs_v[0] += jnp.sum(p1.reshape(LROWS // 8, 8, HW), axis=0)
            cs_v[1] += jnp.sum(dxn.reshape(LROWS // 8, 8, HW), axis=0)
        loop(BLK // LROWS, rows_step)

    SB = min(BLK, 128)
    NS = BLK // SB

    def stats_send(b):
        for t in range(NS):
            tr = st_v[t * SB:(t + 1) * SB, :].T
            sx_v[b, t:t + 1, :SB] = tr[0:1, :]
            sx_v[b, NS + t:NS + t + 1, :SB] = tr[64:65, :]
        put(sx_v.at[b], sr_v.at[b], S('s_st', b), S('r_st', b), col=cf)

    def stats_recv(b):
        wait(sr_v.at[b], S('r_st', b))
        for t in range(NS):
            for i in range(2):
                row = (sx_v[b, i * NS + t:i * NS + t + 1, :SB] + sr_v[b, i * NS + t:i * NS + t + 1, :SB]) * inv_w
                st2_v[i, t * SB:(t + 1) * SB, :] = jnp.broadcast_to(row, (128, SB)).T

    def dx_b(b):
        def rows_step(i):
            rr = ds(i * ROWS, ROWS)
            srow = rr
            mean, inv = ms_v[srow, 0:1], ms_v[srow, 64:65]
            xhat = (wx[b, rr, fcols].astype(F32) - mean) * inv
            gh = fs[b, rr, :] * vec_v[0:1, fcols]
            dx = wo[b, rr, :HW].astype(F32) + inv * (gh - st2_v[0, srow, 0:1] - xhat * st2_v[1, srow, 0:1])
            ob[b, rr, :] = dx.astype(BF16)
        loop(BLK // ROWS, rows_step)
        place('d', dx_out, b)

    def sums():
        cw = jnp.sum(cs_v[...], axis=1)
        for i in range(2):
            for q in range(2):
                @pl.when(c_odd == q)
                def _():
                    sum_v[0, :, i * HB:(i + 1) * HB] = cw[i:i + 1, q * HB:(q + 1) * HB]
                    sum_v[1, :, i * HB:(i + 1) * HB] = cw[i:i + 1, (1 - q) * HB:(2 - q) * HB]
        near = sum_v.at[1, :, pl.ds(0, 2 * HB)]
        near_in = sumr_v.at[0, :, pl.ds(0, 2 * HB)]
        put(near, near_in, S('s_sum', 0), S('r_sum', 0), col=cn)
        sum_v[0, :, 2 * HB:2 * HB + FB] = jnp.zeros((1, FB), F32)
        sum_v[0, :, dsm(2 * HB + r * FH, FH, HB)] = jnp.sum(db_v[0] + db_v[1], axis=0, keepdims=True)
        sum_v[0, :, 2 * HB + FB:] = jnp.sum(bd_v[...], axis=0, keepdims=True)
        wait(near_in, S('r_sum', 0))
        sum_v[2, :, :2 * HB] = sum_v[0, :, :2 * HB] + sumr_v[0, :, :2 * HB]
        sum_v[2, :, 2 * HB:] = sum_v[0, :, 2 * HB:]
        for i, dev in enumerate((dict(row=rp), dict(depth=dn), dict(depth=df))):
            put(sum_v.at[2 + i], sumr_v.at[1 + i], S('s_sum', 1 + i), S('r_sum', 1 + i), **dev)
            wait(sumr_v.at[1 + i], S('r_sum', 1 + i))
            sum_v[3 + i] = sum_v[2 + i] + sumr_v[1 + i]
        copy(sum_v.at[5], sum_out, S('l_small', 0))

    scope = jax.named_scope

    def g_ready(k):
        wait(DY.at[rp, ds(k * BLK, BLK), pl.ds(0, 2 * HB)], S('gd2d', k))

    def g_own(k):
        wait(reg(DY, k, c), S('gd2w', k))

    with scope('g0'):
        g_near_far(0)
    with scope('wu_relay'):
        wu_relay()
    with scope('g_own'):
        loop(NCH, g_own)
    with scope('dwd_0'):
        dwd_pass((0,))
        dwd_opp(0)
    with scope('g1'):
        g_near_far(1)
    with scope('wuo'):
        wait(wuq(do, 0), S('r_wuy', 2))
        wait(wuq(do, 1), S('r_wuy', 3))
    with scope('u_near'):
        loop(2, u_near)
        u_stored()
    with scope('g2'):
        g_near_far(2)
    with scope('wd_wait'):
        wait(wd_v.at[pl.ds(0, 2 * FH), pl.ds(0, HB)], S('r_wd', 0))
        for g in range(2):
            for i in range(2, 4):
                wait(wd_bytes(g, QH), S('r_wdy', 4 * g + i))
    with scope('y_give'):
        give('y', A, tile_y, YGOT)
    with scope('dwd_a0'):
        dwd_a(0)
    with scope('g3'):
        g_near_far(3)
    with scope('y_keep'):
        keep('y', A, tile_y, YGOT, YFAR, YKEEP)
    with scope('g_ready'):
        loop(NCH, g_ready)
    with scope('dwd_12'):
        dwd_pass((1, 2))
        dwd_opp(1)
        dwd_opp(2)
    with scope('dwd_b0'):
        dwd_b(0)
    with scope('g_opp'):
        loop(NCH, g_opp)
    with scope('dwd_3'):
        dwd_pass((3,))
        dwd_opp(3)
    with scope('dwd_a12'):
        dwd_a(1)
        dwd_a(2)

    def own_parts(k):
        return (tau, 0, k), (1 - tau, 1, k)

    def near_parts(k):
        return (tau, 0, 2 * k), (tau, 0, 2 * k + 1)

    with scope('da_own'):
        step = da_pass(own_parts, o, True)
        loop(NCH, lambda k: step(k, NCH))
        du_stored()
    with scope('dwd_a3'):
        dwd_a(3)
    with scope('dwu_01'):
        dwu_pass((do, df))
        dwu_opp()
    with scope('dwd_b12'):
        dwd_b(1)
        dwd_b(2)
    with scope('dwu_23'):
        dwu_pass((dn, d))
    with scope('dwu_a'):
        dwu_a()
    with scope('dwd_b3'):
        dwd_b(3)
    with scope('da_near'):
        step2 = da_pass(near_parts, o2, False)
        loop(2, lambda k: step2(k, 2))
        du_stored()
    with scope('gwd_send'):
        gwd_send()
    with scope('d_give'):
        give('d', DU, tile_g, GGOT)
    with scope('keep_end_y'):
        keep_end('y')
    with scope('d_keep'):
        keep('d', DU, tile_g, GGOT, GFAR, GKEEP)
    for b in range(2):
        with scope('y_final'):
            y_final(b)
    with scope('dwu_b'):
        dwu_b()
    with scope('gwd_relay'):
        gwd_relay()
    with scope('keep_end_d'):
        keep_end('d')
    for b in range(2):
        with scope('place_end_y'):
            place_end('y', b)
        with scope('dx_a'):
            dx_a(b)
        with scope('stats'):
            stats_send(b)
            stats_recv(b)
        with scope('dx_b'):
            dx_b(b)
        if b == 0:
            with scope('gwu_relay'):
                gwu_relay()
    with scope('sums'):
        sums()

    with scope('gwu_end'):
        gwu_end()
    wait(gwd_out.at[pl.ds(0, 4 * QH), :], S('d_o', 0))
    wait(gwd_out.at[pl.ds(0, 4 * QH), :], S('d_o', 1))
    for p, out in (('y', y_out), ('d', dx_out)):
        @pl.when(r == tau)
        def _():
            wait(out.at[pl.ds(0, TH), :], S(p + 'out'))

        @pl.when(r != tau)
        def _():
            wait(out, S(p + 'out'))
    wait(sum_out, S('l_small', 0))
    for b in range(2):
        place_end('d', b)
    for b in range(2):
        wait(sx_v.at[b], S('s_st', b))
    wait(sum_v.at[1, :, pl.ds(0, 2 * HB)], S('s_sum', 0))
    for i in range(3):
        wait(sum_v.at[2 + i], S('s_sum', 1 + i))
    wait(wun, S('s_wun'))

    @pl.when(r == f)
    def _():
        for s in range(2):
            wait(wd_own(s), S('s_wd0', s))
    for i in range(4):
        wait(wd_dst(0, c), S('s_wdx', i))
    wait(wu_own, S('s_wu'))
    for i in range(3):
        wait(vec_at, S('s_vec', i))
    wait(bu_at, S('s_vec', 3))
    for s in range(2):
        wait(wd_dst(s, cf), S('s_wdr', s))
    for i in range(2):
        wait(wuq(d), S('s_wuy', i))
        wait(wuq(d, 0), S('s_wuy', 2 + i))
    for i in range(12):
        wait(wdq(0, d, c), S('s_wdy', i))
        wait(wdq(0, d, c, 0), S('s_wdy', 12 + i))

    def sends(k):
        for z, Z in (('x', X), ('g', DY)):
            for n in ('s_near', 's_far', 's_rel'):
                wait(reg(Z, k, c), S(z + n, k))
            wait(Z.at[r, ds(k * BLK, BLK), :], S(z + 's_d2d', k))
    loop(NCH, sends)
    for i in range(8):
        wait(r1D.at[0], S('d_so', i))
        wait(gwd(0, d), S('d_sy', i))
        wait(gwd(0, d, 0), S('d_sr', i))
    for j in range(1, 4):
        wait(finD.at[j], S('d_sf', j))

    @pl.when(r != f)
    def _():
        wait(finD.at[0], S('d_sf', 0))
    for i in range(2):
        wait(r1U, S('u_so', i))
        wait(PFU, S('u_sa', i))
        wait(finU, S('u_sf', i))

    @pl.when(r != dh)
    def _():
        wait(finU, S('u_sf', 2))
    wait(gwu(0, DH), S('u_sr'))


def block_kernel(x, dy, wu, wd, vec, bu):
    (TK, HB), FH = x.shape, wu.shape[1] // 2
    W, HW, TH, BLK, QF, FB = 4 * HB, 2 * HB, TK // 2, TK // NCH, FH // 4, 2 * FH
    assert FB <= W and FH <= HW and W // 4 <= BLK and QF <= BLK
    sd = jax.ShapeDtypeStruct
    NS = BLK // min(BLK, 128)
    outs = [sd((TK, HB), BF16), sd((TK, HB), BF16), sd((W // 2, FB), BF16), sd((4 * FH, HB), BF16), sd((1, 3 * HB + FB), F32)]
    n_out = len(outs)
    outs += [sd((2, TK, W), BF16)] * 3 + [sd((2, TK, FB), BF16)] * 3
    outs += [sd((TH, W), F32), sd((TH, HW), F32), sd((TH, HW), F32)] * 2
    outs += [sd((4, QF, HB), F32)] * 2 + [sd((W // 4, FH), F32)] * 2
    V = pltpu.VMEM
    scratch = [
        V((W, FB), BF16), V((FB, W), BF16), V((4, FH, HB), F32), V((4, W // 4, FH), F32),
        V((4, FH // 8, HB), F32), V((4, FH // 8, HB), F32), V((W // 8, FH), F32), V((W // 8, FH), F32),
        V((8, W), F32), V((8, FB), F32), V((2, BLK, W), BF16), V((2, BLK, W), BF16), V((BLK, HW), F32), V((BLK, HW), F32), V((2, BLK, HW), F32), V((2, BLK, HW), BF16),
        V((4, QF, HB), BF16), V((2, 8, FH), F32), V((2, 8, HW), F32),
        V((BLK, 128), F32), V((BLK, 128), F32), V((2, BLK, 128), F32), V((2, 2 * NS, 128), F32), V((2, 2 * NS, 128), F32),
        V((8, HB), F32), V((6, 1, 3 * HB + FB), F32), V((4, 1, 3 * HB + FB), F32),
        pltpu.SemaphoreType.DMA((N_SEM,)),
    ]
    res = pl.pallas_call(
        functools.partial(body, (TK, HB, FH)),
        out_shape=outs,
        in_specs=[pl.BlockSpec(memory_space=pl.ANY)] * 6,
        out_specs=[pl.BlockSpec(memory_space=pl.ANY)] * len(outs),
        scratch_shapes=scratch,
        compiler_params=pltpu.CompilerParams(collective_id=0, has_side_effects=True, vmem_limit_bytes=67043328),
        name='mlp_block',
    )(x, dy, wu, wd, vec, bu)
    return res[:n_out]


def solution(mesh):
    assert (mesh.shape['col'], mesh.shape['row'], mesh.shape['depth']) == (4, 2, 4)
    tok_spec = P(('dp', 'depth', 'row'), 'col')
    vec_spec = P('col')
    mat_spec = P('row', 'col')
    grad_vec = P(('dp', 'col'))
    grad_mat = P(('dp', 'row'), 'col')
    def local_pass(x_blk, gamma_blk, beta_blk, w_up_blk, b_up_blk, w_down_blk, b_down_blk, dy_blk):
        hb, fb = x_blk.shape[1], w_up_blk.shape[1]
        vec = jnp.stack([gamma_blk, beta_blk, b_down_blk.astype(F32)] + [jnp.zeros_like(gamma_blk)] * 5)
        bu = jnp.broadcast_to(b_up_blk.astype(F32)[None], (8, fb))
        y_blk, dx_blk, grad_w_up, grad_w_down, sums = block_kernel(x_blk, dy_blk, w_up_blk, w_down_blk, vec, bu)
        sums = sums[0]
        return (y_blk, dx_blk, sums[:hb], sums[hb:2 * hb], grad_w_up, sums[2 * hb:2 * hb + fb], grad_w_down, sums[2 * hb + fb:])

    return jax.shard_map(
        local_pass,
        mesh=mesh,
        in_specs=(tok_spec, vec_spec, vec_spec, mat_spec, vec_spec, mat_spec, vec_spec, tok_spec),
        out_specs=(tok_spec, tok_spec, grad_vec, grad_vec, grad_mat, grad_vec, grad_mat, grad_vec),
        check_vma=False,
    )
```

```python
import functools

import jax
import jax.numpy as jnp
from jax import lax
from jax.experimental import pallas as pl
from jax.experimental.pallas import tpu as pltpu
from jax.sharding import PartitionSpec as P

LN_EPS = 1e-5
F32 = jnp.float32
BF16 = jnp.bfloat16
MESH = pl.DeviceIdType.MESH
GELU_A = 0.7978845608028654
GELU_B = 0.044715
NCH = 4
ROWS = 16
LROWS = 64

NN = (((1,), (0,)), ((), ()))
NT = (((1,), (1,)), ((), ()))
TN = (((0,), (0,)), ((), ()))

SEMS = {}
for _z in ('x', 'g'):
    for _n in ('near', 'far', 'opp', 'd2d', 'd2w', 'd2o', 's_near', 's_far', 's_rel', 's_d2d'):
        SEMS[_z + _n] = NCH
    SEMS[_z + 'bounce'] = 2
for _p in ('y', 'd'):
    SEMS.update({_p + 's_give': 2, _p + 'got': 2, _p + 's_far': 2, _p + 'keep': 2, _p + 'far': 2, _p + 's_out': 4, _p + 'out': 1, _p + 'loc': 2})
SEMS.update(l_wu=1, s_wu=1, r_wu=1, s_wun=1, r_wun=1, s_wuy=4, r_wuy=4,
            s_wd0=2, s_wdx=4, r_wd=4, s_wdr=2, s_wdy=24, r_wdy=8,
            l_vec=2, s_vec=4, r_vec=2,
            ld=8, st=6, s_st=2, r_st=2, s_sum=8, r_sum=2,
            d_so=8, d_r=8, d_sa=8, d_p=8, d_sf=4, d_out=1, d_sy=8, d_y=2, d_sr=8, d_o=2,
            u_so=2, u_r=2, u_sa=2, u_p=2, u_sf=3, u_out=3, u_sr=1, u_o=2, l_small=2)
BASE = {}
_at = 0
for _n, _c in SEMS.items():
    BASE[_n] = _at
    _at += _c
N_SEM = _at


def gelu(v):
    return 0.5 * v * (1.0 + jnp.tanh(GELU_A * (v + GELU_B * (v * v * v))))


def gelu_slope(v):
    v2 = v * v
    t = jnp.tanh(v * (GELU_A + (GELU_A * GELU_B) * v2))
    q = (1.0 - t) * (GELU_A + (3.0 * GELU_A * GELU_B) * v2)
    return 0.5 * ((1.0 + t) * (1.0 + v * q))


def body(dims, x_ref, dy_ref, wu_ref, wd_ref, vec_ref, bu_ref,
         y_out, dx_out, gwu_out, gwd_out, sum_out,
         X, DY, XN, U, A, DU, YGOT, YFAR, YKEEP, GGOT, GFAR, GKEEP, PFD, PND, PFU, PNU,
         wu_v, wd_v, accD, accU, r1D, r2D, r1U, r2U, vec_v, bu_v, wx, wo, F4, ob, finD,
         db_v, cs_v, st_v, ms_v, st2_v, sx_v, sr_v, bd_v, sum_v, sumr_v, sem):
    TK, HB, FH = dims
    W, HW, TH, BLK, QF = 4 * HB, 2 * HB, TK // 2, TK // NCH, FH // 4
    RH, DQ, QH, DH, FB = W // 2, W // 4, FH // 8, W // 8, 2 * FH
    NTW = HB
    inv_w = 1.0 / W
    finU = wo.at[1, pl.ds(0, DQ), pl.ds(HW, FH)]
    f0, f1 = F4.at[0], F4.at[1]
    own2 = (pl.ds(0, FH), pl.ds(FH, FH))

    c, r, d = lax.axis_index('col'), lax.axis_index('row'), lax.axis_index('depth')
    c_odd, d_odd = lax.rem(c, 2), lax.rem(d, 2)
    cn, cf, co = c + 1 - 2 * c_odd, 3 - c, lax.rem(c + 2, 4)
    dn, df, do = d + 1 - 2 * d_odd, 3 - d, lax.rem(d + 2, 4)
    f, dh = lax.div(c, 2), lax.div(d, 2)
    tau = lax.rem(lax.div(c + 1, 2), 2)
    rp = 1 - r
    o, o2 = c_odd * FH, (1 - c_odd) * FH

    def S(name, i=0):
        return sem.at[BASE[name] + i]

    def ds(start, size):
        return pl.ds(pl.multiple_of(start, size), size)

    def dsm(start, size, mult):
        return pl.ds(pl.multiple_of(start, mult), size)

    def put(src, dst, ssem, rsem, **dev):
        pltpu.make_async_remote_copy(src_ref=src, dst_ref=dst, send_sem=ssem, recv_sem=rsem,
                                     device_id=dev, device_id_type=MESH).start()

    def copy(src, dst, s):
        pltpu.make_async_copy(src, dst, s).start()

    def wait(ref, s):
        pltpu.make_async_copy(ref, ref, s).wait()

    def loop(n, fn):
        def step(i, carry):
            fn(i)
            return carry
        lax.fori_loop(0, n, step, 0)

    bar = pltpu.get_barrier_semaphore()
    for dev in [dict(row=rp)] + [dict(row=h, **q) for h in range(2) for q in
                                 (dict(col=cn), dict(col=cf), dict(col=co), dict(depth=dn), dict(depth=df), dict(depth=do))]:
        pl.semaphore_signal(bar, inc=1, device_id=dev, device_id_type=MESH)
    pl.semaphore_wait(bar, 13)

    def wd_src(s, h):
        return wd_ref.at[dsm((2 * s + h) * FH + d * QF, QF, QF), :]

    def wd_dst(s, col):
        return wd_v.at[dsm(s * FH + d * QF, QF, QF), ds(col * HB, HB)]

    def reg(Z, k, col):
        return Z.at[r, ds(k * BLK, BLK), ds(col * HB, HB)]

    def send_own(z, z_ref, Z, which, chunks=(0, NCH)):
        def step(k):
            src = z_ref.at[ds(k * BLK, BLK), :]
            if 'near' in which:
                put(src, reg(Z, k, c), S(z + 's_near', k), S(z + 'near', k), col=cn)
            if 'far' in which:
                put(src, reg(Z, k, c), S(z + 's_far', k), S(z + 'far', k), col=cf)
            if 'd2d' in which:
                put(src, reg(Z, k, c), S(z + 's_d2d', k), S(z + ('d2d' if z == 'x' else 'd2w'), k), row=rp)
        for k in range(*chunks):
            step(k)

    def d2d(z, Z, k, col, s):
        put(reg(Z, k, col), reg(Z, k, col), S(z + 's_d2d', k), S(z + s, k), row=rp)

    vec_at = vec_v.at[:, ds(c * HB, HB)]
    copy(vec_ref, vec_at, S('l_vec', 0))
    put(vec_ref, vec_at, S('s_vec', 0), S('r_vec', 0), col=cn)
    put(vec_ref, vec_at, S('s_vec', 1), S('r_vec', 0), col=cf)
    put(vec_ref, vec_at, S('s_vec', 2), S('r_vec', 0), col=co)
    bu_src, bu_at = bu_ref.at[:, ds(r * FH, FH)], bu_v.at[:, ds(o, FH)]
    copy(bu_src, bu_at, S('l_vec', 1))
    put(bu_src, bu_at, S('s_vec', 3), S('r_vec', 1), col=cn)

    wu_own = wu_v.at[ds(r * RH, RH), ds(o, FH)]
    wd_own = lambda s: wd_v.at[pl.ds(s * FH, FH), ds(c * HB, HB)]

    @pl.when(r != f)
    def _():
        for s in range(2):
            for h in range(2):
                put(wd_src(s, h), wd_dst(s, c), S('s_wdx', 2 * s + h), S('r_wd', 2), col=cf, row=h)

    @pl.when(r == f)
    def _():
        for s in range(2):
            for h in range(2):
                put(wd_src(s, h), wd_dst(s, c), S('s_wdx', 2 * s + h), S('r_wd', 1), col=cn, row=h)
    send_own('x', x_ref, X, ('far',), (0, 2))
    send_own('x', x_ref, X, ('near',), (0, 1))
    put(wu_ref.at[:, ds(rp * FH, FH)], wu_own, S('s_wu'), S('r_wu'), row=rp)
    copy(wu_ref.at[:, ds(r * FH, FH)], wu_own, S('l_wu'))
    send_own('x', x_ref, X, ('d2d',))
    send_own('g', dy_ref, DY, ('d2d',))
    for i, z_ref in enumerate((x_ref, dy_ref)):
        for k in range(NCH):
            copy(z_ref.at[pl.ds(k * BLK, BLK), :], wx.at[i, :, pl.ds(k * HB, HB)], S('xg'[i] + 'bounce', 0))

    @pl.when(r == f)
    def _():
        for s in range(2):
            copy(wd_ref.at[dsm((2 * s + r) * FH, FH, FH), :], wd_own(s), S('r_wd', 0))
            put(wd_ref.at[dsm((2 * s + rp) * FH, FH, FH), :], wd_own(s), S('s_wd0', s), S('r_wd', 0), row=rp)

    for i, Z in enumerate((X, DY)):
        wait(wx.at[i], S('xg'[i] + 'bounce', 0))
        for k in range(NCH):
            copy(wx.at[i, :, pl.ds(k * HB, HB)], reg(Z, k, c), S('xg'[i] + 'bounce', 1))

    with jax.named_scope('wd_far'):
        wait(wd_v.at[pl.ds(0, 2 * QF), pl.ds(0, HB)], S('r_wd', 2))
    for s in range(2):
        put(wd_dst(s, cf), wd_dst(s, cf), S('s_wdr', s), S('r_wd', 3), col=cn)
    send_own('x', x_ref, X, ('near',), (1, NCH - 1))

    with jax.named_scope('wu_own'):
        wait(wu_own, S('l_wu'))
        wait(wu_v.at[ds(rp * RH, RH), ds(o, FH)], S('r_wu'))
    wun = wu_v.at[ds(d * DQ, DQ), ds(o, FH)]
    put(wun, wun, S('s_wun'), S('r_wun'), col=cn)
    send_own('x', x_ref, X, ('near',), (NCH - 1, NCH))

    db_v[...] = jnp.zeros_like(db_v)
    cs_v[...] = jnp.zeros_like(cs_v)
    bd_v[...] = jnp.zeros_like(bd_v)

    def dy_sum(i):
        rr = ds(i * ROWS, ROWS)
        part = jnp.sum(wx[1, rr, :].astype(F32).reshape(ROWS // 8, 8, W), axis=0)
        bd_v[...] += part[:, :HB] + part[:, HB:2 * HB] + part[:, 2 * HB:3 * HB] + part[:, 3 * HB:]
    with jax.named_scope('dy_sum'):
        loop(BLK // ROWS, dy_sum)

    def wuq(dd, half=None):
        if half is None:
            return wu_v.at[ds(dd * DQ, DQ), ds(o2, FH)]
        return wu_v.at[dsm(dd * DQ + half * DH, DH, DH), ds(o2, FH)]

    def wu_send():
        with jax.named_scope('wu_near'):
            wait(wuq(d), S('r_wun'))
        put(wuq(d), wuq(d), S('s_wuy', 0), S('r_wuy', 0), depth=dn)
        put(wuq(d), wuq(d), S('s_wuy', 1), S('r_wuy', 1), depth=df)

    def wu_relay():
        with jax.named_scope('wuy'):
            wait(wuq(dn), S('r_wuy', 0))
            wait(wuq(df), S('r_wuy', 1))
        put(wuq(dn, 1), wuq(dn, 1), S('s_wuy', 2), S('r_wuy', 3), depth=df)
        put(wuq(df, 0), wuq(df, 0), S('s_wuy', 3), S('r_wuy', 2), depth=dn)

    def wdq(s, dd, col, half=None):
        if half is None:
            return wd_v.at[dsm(s * FH + dd * QF, QF, QF), ds(col * HB, HB)]
        return wd_v.at[dsm(s * FH + dd * QF + half * QH, QH, QH), ds(col * HB, HB)]

    W_GROUPS = (((0, cn), (1, cf)), ((2, co),))

    def wd_send(g):
        if g == 0:
            wait(wd_v.at[pl.ds(0, 2 * QF), pl.ds(0, HB)], S('r_wd', 1))
        else:
            wait(wd_v.at[pl.ds(0, 2 * QF), pl.ds(0, HB)], S('r_wd', 3))
        for i, col in W_GROUPS[g]:
            for s in range(2):
                put(wdq(s, d, col), wdq(s, d, col), S('s_wdy', 4 * i + s), S('r_wdy', 4 * g), depth=dn)
                put(wdq(s, d, col), wdq(s, d, col), S('s_wdy', 4 * i + 2 + s), S('r_wdy', 4 * g + 1), depth=df)

    def wd_bytes(g, rows):
        return wd_v.at[pl.ds(0, 2 * rows), pl.ds(0, len(W_GROUPS[g]) * HB)]

    def wd_relay(g):
        for i in range(2):
            wait(wd_bytes(g, QF), S('r_wdy', 4 * g + i))
        for i, col in W_GROUPS[g]:
            for s in range(2):
                put(wdq(s, dn, col, 1), wdq(s, dn, col, 1), S('s_wdy', 12 + 4 * i + s), S('r_wdy', 4 * g + 3), depth=df)
                put(wdq(s, df, col, 0), wdq(s, df, col, 0), S('s_wdy', 12 + 4 * i + 2 + s), S('r_wdy', 4 * g + 2), depth=dn)

    def x_near(k):
        wait(reg(X, k, cn), S('xnear', k))
        put(reg(X, k, cn), reg(X, k, cn), S('xs_rel', k), S('xopp', k), col=cf)
        d2d('x', X, k, cn, 'd2d')

    with jax.named_scope('wd_send0'):
        wd_send(0)
    with jax.named_scope('x_near'):
        x_near(0)
    send_own('x', x_ref, X, ('far',), (2, 3))

    for i, Z in enumerate((X, DY)):
        wait(wx.at[i], S('xg'[i] + 'bounce', 1))
    wait(vec_at, S('l_vec', 0))
    wait(vec_v.at[:, pl.ds(0, 3 * HB)], S('r_vec', 0))
    wait(bu_at, S('l_vec', 1))
    wait(bu_at, S('r_vec', 1))

    def norm_rows(buf, rows):
        xf = buf[rows, :].astype(F32)
        mean = jnp.sum(xf, axis=1, keepdims=True) * inv_w
        cen = xf - mean
        inv = lax.rsqrt(jnp.sum(cen * cen, axis=1, keepdims=True) * inv_w + LN_EPS)
        return cen, mean, inv

    def tok_of(s):
        return tau + s * (1 - 2 * tau)

    N_T = FH // NTW

    def chain(tiles, hooks=None):
        hooks = hooks or {}

        def hook(what, i):
            for fn in hooks.get((what, i), ()):
                fn()
        for i, (product, _) in enumerate(tiles):
            hook('before', i)
            if i:
                tiles[i - 1][1](F4.at[(i - 1) % 2])
            F4[i % 2, :, :NTW] = product()
            hook('product', i)
            if i:
                hook('epilogue', i - 1)
        tiles[-1][1](F4.at[(len(tiles) - 1) % 2])
        hook('epilogue', len(tiles) - 1)

    def u_tile(i, n, start):
        cols = ds(start + n * NTW, NTW)
        at = pl.ds((i * N_T + n) * NTW, NTW)

        def product():
            return lax.dot_general(wx[i], wu_v[:, cols], NN, preferred_element_type=F32)

        def epilogue(acc):
            u = (acc[:, :NTW] + bu_v[0:1, cols]).astype(BF16)
            wo[0, :, at] = u
            wo[1, :, at] = gelu(u.astype(F32)).astype(BF16)
        return product, epilogue

    def u_store(i, s, rows, start):
        copy(wo.at[0, :, own2[i]], U.at[s, rows, ds(start, FH)], S('st', 2 + i))
        copy(wo.at[1, :, own2[i]], A.at[s, rows, ds(start, FH)], S('st', 4 + i))

    def u_stored():
        for i in range(2):
            wait(wo.at[0, :, own2[i]], S('st', 2 + i))
            wait(wo.at[1, :, own2[i]], S('st', 4 + i))

    def phase1(k):
        @pl.when(k < NCH - 1)
        def _():
            with jax.named_scope('x_near'):
                x_near(k + 1)

        @pl.when(k == 0)
        def _():
            send_own('x', x_ref, X, ('far',), (3, 4))
            with jax.named_scope('wd_send1'):
                wd_send(1)

        @pl.when(k == 1)
        def _():
            with jax.named_scope('wd_relay0'):
                wd_relay(0)
            send_own('g', dy_ref, DY, ('near',))

        @pl.when(k == 2)
        def _():
            send_own('g', dy_ref, DY, ('far',))
            with jax.named_scope('wd_relay1'):
                wd_relay(1)
            wu_send()

        @pl.when(k == NCH - 1)
        def _():
            wu_relay()

        with jax.named_scope('x_far'):
            wait(reg(X, k, cf), S('xfar', k))
            d2d('x', X, k, cf, 'd2d')
        with jax.named_scope('x_opp'):
            wait(reg(X, k, co), S('xopp', k))
            d2d('x', X, k, co, 'd2d')

        rows = ds(k * BLK, BLK)
        with jax.named_scope('x_d2d'):
            wait(X.at[rp, rows, :], S('xd2d', k))

        @pl.when(k > 0)
        def _():
            for s in range(2):
                wait(wx.at[s], S('st', s))
        for s in range(2):
            copy(X.at[tok_of(s), rows, :], wx.at[s], S('ld', s))
        for s in range(2):
            wait(wx.at[s], S('ld', s))

            def ln(i):
                rr = ds(i * LROWS, LROWS)
                cen, _, inv = norm_rows(wx.at[s], rr)
                wx[s, rr, :] = (cen * inv * vec_v[0:1, :] + vec_v[1:2, :]).astype(BF16)
            with jax.named_scope('ln'):
                loop(BLK // LROWS, ln)
            copy(wx.at[s], XN.at[s, rows, :], S('st', s))
        pl.when(k > 0)(u_stored)
        with jax.named_scope('u_own'):
            chain([u_tile(i, n, o) for i in range(2) for n in range(N_T)])
        for s in range(2):
            u_store(s, s, rows, o)
    loop(NCH, phase1)
    for s in range(2):
        wait(wx.at[s], S('st', s))
    u_stored()

    def u_near():
        def load(kp, i):
            copy(XN.at[0, ds((2 * kp + i) * BLK, BLK), :], wx.at[i], S('ld', i))

        def step(kp):
            def more(i):
                @pl.when(kp == 0)
                def _():
                    load(1, i)
            wait(wx.at[0], S('ld', 0))
            pl.when(kp > 0)(u_stored)
            chain([u_tile(i, n, o2) for i in range(2) for n in range(N_T)],
                  {('before', N_T): [lambda: wait(wx.at[1], S('ld', 1))],
                   ('product', N_T - 1): [lambda: more(0)],
                   ('product', 2 * N_T - 1): [lambda: more(1)],
                   ('epilogue', N_T - 1): [lambda: u_store(0, 0, ds(2 * kp * BLK, BLK), o2)],
                   ('epilogue', 2 * N_T - 1): [lambda: u_store(1, 0, ds((2 * kp + 1) * BLK, BLK), o2)]})
        for i in range(2):
            load(0, i)
        loop(2, step)
        u_stored()

    def g_near_far(k):
        wait(reg(DY, k, cf), S('gfar', k))
        put(reg(DY, k, cf), reg(DY, k, cf), S('gs_rel', k), S('gopp', k), col=cn)
        d2d('g', DY, k, cf, 'd2d')
        wait(reg(DY, k, cn), S('gnear', k))
        d2d('g', DY, k, cn, 'd2d')

    def g_opp(k):
        wait(reg(DY, k, co), S('gopp', k))
        d2d('g', DY, k, co, 'd2o')
        wait(reg(DY, k, co), S('gd2o', k))

    def tile_y(lhs, col):
        return lax.dot_general(lhs, wd_v[:, dsm(col, NTW, NTW)], NN, preferred_element_type=F32)

    def tile_g(lhs, col):
        return lax.dot_general(lhs, wu_v[dsm(col, NTW, NTW), :], NT, preferred_element_type=F32)

    def give(p, src, tile, GOT):
        def blk(b):
            return src.at[0, dsm(rp * TH + b * BLK, BLK, BLK), :]
        for b in range(2):
            copy(blk(b), wx.at[b, :, pl.ds(0, FB)], S('ld', b))

        def step(b):
            wait(wx.at[b, :, pl.ds(0, FB)], S('ld', b))

            def half(h):
                @pl.when(b == 1)
                def _():
                    wait(F4.at[h], S(p + 's_give', h))

                def n_tile(n):
                    F4[h, :, ds(n * NTW, NTW)] = tile(wx[b, :, :FB], h * HW + n * NTW)
                loop(HW // NTW, n_tile)
                put(F4.at[h], GOT.at[ds(b * BLK, BLK), ds(h * HW, HW)], S(p + 's_give', h), S(p + 'got', b), row=rp)
            loop(2, half)
        loop(2, step)

    def keep(p, src, tile, GOT, FAR, KEEP):
        def blk(b):
            return src.at[0, dsm(r * TH + b * BLK, BLK, BLK), :]

        def col_of(h):
            return (1 - f + h * (2 * f - 1)) * HW

        def out_of(b, h):
            return (2 + b) * (1 - h) + (1 - b) * h
        for b in range(2):
            copy(blk(b), wx.at[b, :, pl.ds(0, FB)], S('ld', b))
        for h in range(2):
            wait(F4.at[h], S(p + 's_give', h))

        def fetch(b):
            with jax.named_scope('got'):
                wait(GOT.at[ds(b * BLK, BLK), :], S(p + 'got', b))
            for h in range(2):
                copy(GOT.at[ds(b * BLK, BLK), ds(col_of(h), HW)], F4.at[out_of(b, h)], S('ld', 4 + h))
        fetch(0)

        def step(b):
            brow = ds(b * BLK, BLK)
            wait(wx.at[b, :, pl.ds(0, FB)], S('ld', b))

            def half(h):
                out = out_of(b, h)
                wait(F4.at[out], S('ld', 4 + h))

                def n_tile(n):
                    at = ds(n * NTW, NTW)
                    F4[out, :, at] = F4[out, :, at] + tile(wx[b, :, :FB], col_of(h) + n * NTW)
                loop(HW // NTW, n_tile)

                @pl.when(h == 0)
                def _():
                    put(F4.at[2 + b], FAR.at[brow, :], S(p + 's_far', b), S(p + 'far', b), col=cf)

                @pl.when(h == 1)
                def _():
                    copy(F4.at[1 - b], KEEP.at[brow, :], S(p + 'keep', b))

                @pl.when(jnp.logical_and(b == 0, h == 1))
                def _():
                    fetch(1)
            loop(2, half)
        loop(2, step)
        for b in range(2):
            wait(F4.at[b], S(p + 'keep', b))

    def keep_end(p):
        for b in range(2):
            wait(F4.at[2 + b], S(p + 's_far', b))

    def place(p, out, b):
        dst = out.at[dsm(r * TH + b * BLK, BLK, BLK), :]
        mine, other = ob.at[b, :, ds(c_odd * HB, HB)], ob.at[b, :, ds((1 - c_odd) * HB, HB)]
        put(other, dst, S(p + 's_out', 2 * b), S(p + 'out'), col=cn, row=tau)

        @pl.when(r == tau)
        def _():
            copy(mine, dst, S(p + 'loc', b))

        @pl.when(r != tau)
        def _():
            put(mine, dst, S(p + 's_out', 2 * b + 1), S(p + 'out'), row=rp)

    def place_end(p, b):
        wait(ob.at[b, :, pl.ds(0, HB)], S(p + 's_out', 2 * b))

        @pl.when(r == tau)
        def _():
            wait(ob.at[b, :, pl.ds(0, HB)], S(p + 'loc', b))

        @pl.when(r != tau)
        def _():
            wait(ob.at[b, :, pl.ds(0, HB)], S(p + 's_out', 2 * b + 1))

    fcols = ds(f * HW, HW)

    def y_final(b):
        brow = ds(b * BLK, BLK)
        wait(YFAR.at[brow, :], S('yfar', b))
        copy(YFAR.at[brow, :], f0, S('ld', 0))
        copy(YKEEP.at[brow, :], f1, S('ld', 1))
        copy(X.at[tau, dsm(r * TH + b * BLK, BLK, BLK), fcols], wx.at[0, :, pl.ds(0, HW)], S('ld', 2))
        wait(f0, S('ld', 0))
        wait(f1, S('ld', 1))
        wait(wx.at[0, :, pl.ds(0, HW)], S('ld', 2))

        def fin(i):
            rr = ds(i * ROWS, ROWS)
            ob[b, rr, :] = (wx[0, rr, :HW].astype(F32) + (f0[rr, :] + f1[rr, :]) + vec_v[2:3, fcols]).astype(BF16)
        loop(BLK // ROWS, fin)
        place('y', y_out, b)

    def da_all():
        def part(t, i):
            near = lax.div(t, NCH)
            tok = tau + i * (1 - near) * (1 - 2 * tau)
            chunk = t * (1 - near) + near * (2 * (t - NCH) + i)
            return near, tok, i * (1 - near), ds(chunk * BLK, BLK), near * o2 + (1 - near) * o

        def load_dy(t, i):
            _, tok, _, rows, _ = part(t, i)
            copy(DY.at[tok, rows, :], wx.at[i], S('ld', i))

        def load_u(t, i):
            _, _, us, rows, start = part(t, i)
            copy(U.at[us, rows, ds(start, FH)], wo.at[0, :, own2[i]], S('ld', 2 + i))

        def store(t, i):
            _, _, us, rows, start = part(t, i)
            copy(wo.at[1, :, own2[i]], DU.at[us, rows, ds(start, FH)], S('st', 4 + i))

        def stored(i):
            wait(wo.at[1, :, own2[i]], S('st', 4 + i))

        n_steps = NCH + NCH // 2

        def step(t):
            near, _, _, _, start = part(t, 0)

            def tile(i, n):
                cols = ds(start + n * NTW, NTW)
                at = pl.ds((i * N_T + n) * NTW, NTW)

                def product():
                    return lax.dot_general(wx[i], wd_v[cols, :], NT, preferred_element_type=F32)

                def epilogue(acc):
                    du = (acc[:, :NTW] * gelu_slope(wo[0, :, at].astype(F32))).astype(BF16)
                    wo[1, :, at] = du
                    db_v[near, :, n * NTW:(n + 1) * NTW] += jnp.sum(du.astype(F32).reshape(BLK // 8, 8, NTW), axis=0)
                return product, epilogue

            def arrive(i):
                wait(wx.at[i], S('ld', i))
                wait(wo.at[0, :, own2[i]], S('ld', 2 + i))
                pl.when(t > 0)(lambda: stored(i))

            def more(fn, i):
                @pl.when(t < n_steps - 1)
                def _():
                    fn(t + 1, i)

            def finish(i):
                store(t, i)
                more(load_u, i)
            arrive(0)
            chain([tile(i, n) for i in range(2) for n in range(N_T)],
                  {('before', N_T): [lambda: arrive(1)],
                   ('product', N_T - 1): [lambda: more(load_dy, 0)],
                   ('product', 2 * N_T - 1): [lambda: more(load_dy, 1)],
                   ('epilogue', N_T - 1): [lambda: finish(0)],
                   ('epilogue', 2 * N_T - 1): [lambda: finish(1)]})
        for i in range(2):
            load_dy(0, i)
            load_u(0, i)
        loop(n_steps, step)
        for i in range(2):
            stored(i)

    def rows_of(kb):
        return ds(lax.rem(kb, NCH) * BLK, BLK), lax.div(kb, NCH)

    d_col = (c, cn, cf, co)

    NB = 2 * NCH
    rings = (wx, wo)

    def k_loop(load, use, width):
        for kb in range(3):
            load(kb, rings[kb % 2].at[kb // 2], S('ld', kb))

        def step(i):
            p = lax.rem(i, 2)
            for q in range(2):
                kb = 2 * i + q
                np_ = lax.rem(i + 1 + q, 2)

                @pl.when(kb + 3 < NB)
                def _():
                    load(kb + 3, rings[1 - q].at[np_], S('ld', (1 - q) + 2 * np_))
                buf = rings[q].at[p]
                wait(buf.at[:, pl.ds(0, width)], S('ld', q + 2 * p))
                use(buf)
        loop(NB // 2, step)

    def dwd_pass(js):
        def load(kb, buf, s_):
            rows, s = rows_of(kb)
            copy(A.at[s, rows, ds(o, FH)], buf.at[:, pl.ds(0, FH)], s_)
            for i, j in enumerate(js):
                copy(DY.at[tok_of(s), rows, ds(d_col[j] * HB, HB)], buf.at[:, pl.ds(FH + i * HB, HB)], s_)

        def use(buf):
            for i, j in enumerate(js):
                for m in range(2):
                    mm = slice(m * FH // 2, (m + 1) * FH // 2)
                    accD[j, mm, :] += lax.dot_general(buf[:, mm], buf[:, FH + i * HB:FH + (i + 1) * HB], TN, preferred_element_type=F32)
        for j in js:
            accD[j] = jnp.zeros((FH, HB), F32)
        k_loop(load, use, FH + len(js) * HB)

    def dwd_opp(j):
        put(accD.at[j, dsm(do * QF, QH, QH), :], r1D.at[j], S('d_so', 2 * j), S('d_r', 2 * j), depth=dn)
        put(accD.at[j, dsm(do * QF + QH, QH, QH), :], r2D.at[j], S('d_so', 2 * j + 1), S('d_r', 2 * j + 1), depth=df)

    def dwd_a(j):
        wait(r1D.at[j], S('d_r', 2 * j))
        rr = dsm(df * QF, QH, QH)
        accD[j, rr, :] += r1D[j]
        put(accD.at[j, ds(df * QF, QF), :], PFD.at[j], S('d_sa', 2 * j), S('d_p', 2 * j), depth=df)
        wait(r2D.at[j], S('d_r', 2 * j + 1))
        rr = dsm(dn * QF + QH, QH, QH)
        accD[j, rr, :] += r2D[j]
        put(accD.at[j, ds(dn * QF, QF), :], PND.at[j], S('d_sa', 2 * j + 1), S('d_p', 2 * j + 1), depth=dn)

    def dwd_rows(q, h, dd):
        return dsm((2 * q + h) * FH + dd * QF, QF, QF)

    def dwd_b(j):
        wait(PFD.at[j], S('d_p', 2 * j))
        wait(PND.at[j], S('d_p', 2 * j + 1))
        wait(PFD.at[j], S('d_sa', 2 * j))
        wait(PND.at[j], S('d_sa', 2 * j + 1))
        pf, pn = accD.at[j, ds(df * QF, QF), :], accD.at[j, ds(dn * QF, QF), :]
        copy(PFD.at[j], pf, S('ld', 6))
        copy(PND.at[j], pn, S('ld', 7))
        wait(pf, S('ld', 6))
        wait(pn, S('ld', 7))
        finD[j] = (accD[j, ds(d * QF, QF), :] + (pf[...] + pn[...])).astype(BF16)
        dst = gwd_out.at[dwd_rows(c_odd, r, d), :]
        if j:
            put(finD.at[j], dst, S('d_sf', j), S('d_out'), col=d_col[j], row=f)
        else:
            @pl.when(r == f)
            def _():
                copy(finD.at[0], dst, S('d_out'))

            @pl.when(r != f)
            def _():
                put(finD.at[0], dst, S('d_sf', 0), S('d_out'), row=rp)

    def gwd(i, dd, half=None):
        if half is None:
            return gwd_out.at[dsm(i * FH + dd * QF, QF, QF), :]
        return gwd_out.at[dsm(i * FH + dd * QF + half * QH, QH, QH), :]

    def gwd_send():
        wait(gwd_out.at[pl.ds(0, 4 * QF), :], S('d_out'))
        for i in range(4):
            put(gwd(i, d), gwd(i, d), S('d_sy', i), S('d_y', 0), depth=dn)
            put(gwd(i, d), gwd(i, d), S('d_sy', 4 + i), S('d_y', 1), depth=df)

    def gwd_relay():
        wait(gwd_out.at[pl.ds(0, 4 * QF), :], S('d_y', 0))
        for i in range(4):
            put(gwd(i, dn, 1), gwd(i, dn, 1), S('d_sr', i), S('d_o', 1), depth=df)
        wait(gwd_out.at[pl.ds(0, 4 * QF), :], S('d_y', 1))
        for i in range(4):
            put(gwd(i, df, 0), gwd(i, df, 0), S('d_sr', 4 + i), S('d_o', 0), depth=dn)

    def dwu_pass(dds):
        def load(kb, buf, s_):
            rows, s = rows_of(kb)
            copy(DU.at[s, rows, ds(o, FH)], buf.at[:, pl.ds(0, FH)], s_)
            for i, dd in enumerate(dds):
                copy(XN.at[s, rows, ds(dd * DQ, DQ)], buf.at[:, pl.ds(FH + i * DQ, DQ)], s_)

        def use(buf):
            for i, dd in enumerate(dds):
                for m in range(2):
                    mm = slice(m * FH // 2, (m + 1) * FH // 2)
                    accU[dd, :, mm] += lax.dot_general(buf[:, FH + i * DQ:FH + (i + 1) * DQ], buf[:, mm], TN, preferred_element_type=F32)
        for dd in dds:
            accU[dd] = jnp.zeros((DQ, FH), F32)
        k_loop(load, use, FH + len(dds) * DQ)

    def dwu_opp():
        put(accU.at[do, pl.ds(0, DH), :], r1U, S('u_so', 0), S('u_r', 0), depth=dn)
        put(accU.at[do, pl.ds(DH, DH), :], r2U, S('u_so', 1), S('u_r', 1), depth=df)

    def dwu_a():
        wait(r1U, S('u_r', 0))
        accU[df, :DH, :] += r1U[...]
        put(accU.at[df], PFU, S('u_sa', 0), S('u_p', 0), depth=df)
        wait(r2U, S('u_r', 1))
        accU[dn, DH:, :] += r2U[...]
        put(accU.at[dn], PNU, S('u_sa', 1), S('u_p', 1), depth=dn)

    def dwu_b():
        wait(PFU, S('u_p', 0))
        wait(PNU, S('u_p', 1))
        pf, pn = f0.at[pl.ds(0, DQ), pl.ds(0, FH)], f1.at[pl.ds(0, DQ), pl.ds(0, FH)]
        copy(PFU, pf, S('ld', 6))
        copy(PNU, pn, S('ld', 7))
        wait(pf, S('ld', 6))
        wait(pn, S('ld', 7))

        def fin(i):
            rr = ds(i * ROWS, ROWS)
            wo[1, rr, HW:HW + FH] = (accU[d, rr, :] + (f0[rr, :FH] + f1[rr, :FH])).astype(BF16)
        loop(DQ // ROWS, fin)
        dst = gwu_out.at[ds(d_odd * DQ, DQ), ds(r * FH, FH)]
        put(finU, dst, S('u_sf', 0), S('u_out', 1), depth=dn, row=dh)
        put(finU, dst, S('u_sf', 1), S('u_out', 2), depth=df, row=dh)

        @pl.when(r == dh)
        def _():
            copy(finU, dst, S('u_out', 0))

        @pl.when(r != dh)
        def _():
            put(finU, dst, S('u_sf', 2), S('u_out', 0), row=rp)

    def gwu(start, size):
        return gwu_out.at[dsm(start, size, size), :]

    def gwu_relay():
        @pl.when(r == dh)
        def _():
            wait(gwu(lax.rem(dn, 2) * DQ, DQ), S('u_out', 1))
            part = gwu(lax.rem(dn, 2) * DQ + DH, DH)
            put(part, part, S('u_sr'), S('u_o', 1), depth=df)

        @pl.when(r != dh)
        def _():
            wait(gwu(lax.rem(df, 2) * DQ, DQ), S('u_out', 2))
            part = gwu(lax.rem(df, 2) * DQ, DH)
            put(part, part, S('u_sr'), S('u_o', 0), depth=dn)

    def gwu_end():
        @pl.when(r == dh)
        def _():
            wait(gwu(d_odd * DQ, DQ), S('u_out', 0))

        @pl.when(r != dh)
        def _():
            wait(gwu(0, DH), S('u_o', 0))
            wait(gwu(0, DH), S('u_o', 1))

    lane = lax.broadcasted_iota(jnp.int32, (LROWS, 128), 1)

    def dx_a(b):
        brow = ds(b * BLK, BLK)
        trow = dsm(r * TH + b * BLK, BLK, BLK)
        wait(GFAR.at[brow, :], S('dfar', b))
        copy(GFAR.at[brow, :], f0, S('ld', 0))
        copy(GKEEP.at[brow, :], f1, S('ld', 1))
        copy(X.at[tau, trow, :], wx.at[b], S('ld', 2))
        copy(DY.at[tau, trow, fcols], wo.at[b, :, pl.ds(0, HW)], S('ld', 3))
        wait(f0, S('ld', 0))
        wait(f1, S('ld', 1))
        wait(wx.at[b], S('ld', 2))
        wait(wo.at[b, :, pl.ds(0, HW)], S('ld', 3))

        def rows_step(i):
            rr = ds(i * LROWS, LROWS)
            _, mean, inv = norm_rows(wx.at[b], rr)
            xhat = (wx[b, rr, fcols].astype(F32) - mean) * inv
            dxn = f0[rr, :] + f1[rr, :]
            F4[2 + b, rr, :] = dxn
            gh = dxn * vec_v[0:1, fcols]
            s0 = jnp.sum(gh, axis=1, keepdims=True)
            s1 = jnp.sum(gh * xhat, axis=1, keepdims=True)
            srow = rr
            st_v[srow, :] = jnp.where(lane < 64, s0, s1)
            ms_v[srow, :] = jnp.where(lane < 64, mean, inv)
            p1 = dxn * xhat
            cs_v[0] += jnp.sum(p1.reshape(LROWS // 8, 8, HW), axis=0)
            cs_v[1] += jnp.sum(dxn.reshape(LROWS // 8, 8, HW), axis=0)
        loop(BLK // LROWS, rows_step)

    SB = min(BLK, 128)
    NS = BLK // SB

    def stats_send(b):
        for t in range(NS):
            tr = st_v[t * SB:(t + 1) * SB, :].T
            sx_v[b, t:t + 1, :SB] = tr[0:1, :]
            sx_v[b, NS + t:NS + t + 1, :SB] = tr[64:65, :]
        put(sx_v.at[b], sr_v.at[b], S('s_st', b), S('r_st', b), col=cf)

    def stats_recv(b):
        wait(sr_v.at[b], S('r_st', b))
        for t in range(NS):
            for i in range(2):
                row = (sx_v[b, i * NS + t:i * NS + t + 1, :SB] + sr_v[b, i * NS + t:i * NS + t + 1, :SB]) * inv_w
                st2_v[i, t * SB:(t + 1) * SB, :] = jnp.broadcast_to(row, (128, SB)).T

    def dx_b(b):
        def rows_step(i):
            rr = ds(i * ROWS, ROWS)
            srow = rr
            mean, inv = ms_v[srow, 0:1], ms_v[srow, 64:65]
            xhat = (wx[b, rr, fcols].astype(F32) - mean) * inv
            gh = F4[2 + b, rr, :] * vec_v[0:1, fcols]
            dx = wo[b, rr, :HW].astype(F32) + inv * (gh - st2_v[0, srow, 0:1] - xhat * st2_v[1, srow, 0:1])
            ob[b, rr, :] = dx.astype(BF16)
        loop(BLK // ROWS, rows_step)
        place('d', dx_out, b)

    me = 2 * d + r
    peers = [dict(row=rp)] + [dict(depth=q, row=h) for q in (dn, df, do) for h in range(2)]
    near_in = sumr_v.at[8, :, pl.ds(0, 2 * HB)]

    def sums_1():
        cw = jnp.sum(cs_v[...], axis=1)
        for i in range(2):
            for q in range(2):
                @pl.when(c_odd == q)
                def _():
                    sum_v[0, :, i * HB:(i + 1) * HB] = cw[i:i + 1, q * HB:(q + 1) * HB]
                    sum_v[1, :, i * HB:(i + 1) * HB] = cw[i:i + 1, (1 - q) * HB:(2 - q) * HB]
        put(sum_v.at[1, :, pl.ds(0, 2 * HB)], near_in, S('s_sum', 0), S('r_sum', 0), col=cn)
        sum_v[0, :, 2 * HB:2 * HB + FB] = jnp.zeros((1, FB), F32)
        sum_v[0, :, dsm(2 * HB + r * FH, FH, HB)] = jnp.sum(db_v[0], axis=0, keepdims=True)
        sum_v[0, :, 2 * HB + FB:] = jnp.sum(bd_v[...], axis=0, keepdims=True)

    def sums_2():
        wait(near_in, S('r_sum', 0))
        sumr_v[me, :, :2 * HB] = sum_v[0, :, :2 * HB] + sumr_v[8, :, :2 * HB]
        sumr_v[me, :, 2 * HB:] = sum_v[0, :, 2 * HB:]
        for i, dev in enumerate(peers):
            put(sumr_v.at[me], sumr_v.at[me], S('s_sum', 1 + i), S('r_sum', 1), **dev)

    def sums_3():
        wait(sumr_v.at[pl.ds(0, 7)], S('r_sum', 1))
        total = sumr_v[0]
        for i in range(1, 8):
            total = total + sumr_v[i]
        sum_v[0] = total
        copy(sum_v.at[0], sum_out, S('l_small', 0))

    scope = jax.named_scope

    def g_ready(k):
        wait(DY.at[rp, ds(k * BLK, BLK), pl.ds(0, 2 * HB)], S('gd2d', k))

    def g_own(k):
        wait(reg(DY, k, c), S('gd2w', k))

    with scope('g0'):
        g_near_far(0)
    with scope('g_own'):
        loop(NCH, g_own)
    with scope('dwd_0'):
        dwd_pass((0,))
        dwd_opp(0)
    with scope('g1'):
        g_near_far(1)
    with scope('wuo'):
        wait(wuq(do, 0), S('r_wuy', 2))
        wait(wuq(do, 1), S('r_wuy', 3))
    with scope('u_near'):
        u_near()
    with scope('g2'):
        g_near_far(2)
    with scope('wd_wait'):
        wait(wd_v.at[pl.ds(0, 2 * FH), pl.ds(0, HB)], S('r_wd', 0))
        for g in range(2):
            for i in range(2, 4):
                wait(wd_bytes(g, QH), S('r_wdy', 4 * g + i))
    with scope('y_give'):
        give('y', A, tile_y, YGOT)
    with scope('dwd_a0'):
        dwd_a(0)
    with scope('g3'):
        g_near_far(3)
    with scope('y_keep'):
        keep('y', A, tile_y, YGOT, YFAR, YKEEP)
    with scope('g_ready'):
        loop(NCH, g_ready)
    with scope('dwd_12'):
        dwd_pass((1, 2))
        dwd_opp(1)
        dwd_opp(2)
    with scope('dwd_b0'):
        dwd_b(0)
    with scope('g_opp'):
        loop(NCH, g_opp)
    with scope('dwd_3'):
        dwd_pass((3,))
        dwd_opp(3)
    with scope('dwd_a12'):
        dwd_a(1)
        dwd_a(2)
    with scope('da'):
        da_all()
    with scope('dwd_a3'):
        dwd_a(3)
    with scope('dwd_b12'):
        dwd_b(1)
        dwd_b(2)
    with scope('d_give'):
        give('d', DU, tile_g, GGOT)
    with scope('dwd_b3'):
        dwd_b(3)
    with scope('keep_end_y'):
        keep_end('y')
    with scope('d_keep'):
        keep('d', DU, tile_g, GGOT, GFAR, GKEEP)
    with scope('gwd_send'):
        gwd_send()
    with scope('dwu_01'):
        dwu_pass((do, df))
        dwu_opp()
    with scope('dwu_23'):
        dwu_pass((dn, d))
    with scope('dwu_a'):
        dwu_a()
    for b in range(2):
        with scope('y_final'):
            y_final(b)
    with scope('gwd_relay'):
        gwd_relay()
    with scope('keep_end_d'):
        keep_end('d')
    for b in range(2):
        with scope('place_end_y'):
            place_end('y', b)
        with scope('dx_a'):
            dx_a(b)
        if b:
            with scope('sums_1'):
                sums_1()
        with scope('stats'):
            stats_send(b)
            stats_recv(b)
        if b:
            with scope('sums_2'):
                sums_2()
        with scope('dx_b'):
            dx_b(b)
        if b == 0:
            with scope('dwu_b'):
                dwu_b()
    with scope('sums_3'):
        sums_3()
    with scope('gwu_relay'):
        gwu_relay()

    with scope('gwu_end'):
        gwu_end()
    wait(gwd_out.at[pl.ds(0, 4 * QH), :], S('d_o', 0))
    wait(gwd_out.at[pl.ds(0, 4 * QH), :], S('d_o', 1))
    for p, out in (('y', y_out), ('d', dx_out)):
        @pl.when(r == tau)
        def _():
            wait(out.at[pl.ds(0, TH), :], S(p + 'out'))

        @pl.when(r != tau)
        def _():
            wait(out, S(p + 'out'))
    wait(sum_out, S('l_small', 0))
    for b in range(2):
        place_end('d', b)
    for b in range(2):
        wait(sx_v.at[b], S('s_st', b))
    wait(sum_v.at[1, :, pl.ds(0, 2 * HB)], S('s_sum', 0))
    for i in range(7):
        wait(sumr_v.at[0], S('s_sum', 1 + i))
    wait(wun, S('s_wun'))

    @pl.when(r == f)
    def _():
        for s in range(2):
            wait(wd_own(s), S('s_wd0', s))
    for i in range(4):
        wait(wd_dst(0, c), S('s_wdx', i))
    wait(wu_own, S('s_wu'))
    for i in range(3):
        wait(vec_at, S('s_vec', i))
    wait(bu_at, S('s_vec', 3))
    for s in range(2):
        wait(wd_dst(s, cf), S('s_wdr', s))
    for i in range(2):
        wait(wuq(d), S('s_wuy', i))
        wait(wuq(d, 0), S('s_wuy', 2 + i))
    for i in range(12):
        wait(wdq(0, d, c), S('s_wdy', i))
        wait(wdq(0, d, c, 0), S('s_wdy', 12 + i))

    def sends(k):
        for z, Z in (('x', X), ('g', DY)):
            for n in ('s_near', 's_far', 's_rel'):
                wait(reg(Z, k, c), S(z + n, k))
            wait(Z.at[r, ds(k * BLK, BLK), :], S(z + 's_d2d', k))
    loop(NCH, sends)
    for i in range(8):
        wait(r1D.at[0], S('d_so', i))
        wait(gwd(0, d), S('d_sy', i))
        wait(gwd(0, d, 0), S('d_sr', i))
    for j in range(1, 4):
        wait(finD.at[j], S('d_sf', j))

    @pl.when(r != f)
    def _():
        wait(finD.at[0], S('d_sf', 0))
    for i in range(2):
        wait(r1U, S('u_so', i))
        wait(PFU, S('u_sa', i))
        wait(finU, S('u_sf', i))

    @pl.when(r != dh)
    def _():
        wait(finU, S('u_sf', 2))
    wait(gwu(0, DH), S('u_sr'))


def block_kernel(x, dy, wu, wd, vec, bu):
    (TK, HB), FH = x.shape, wu.shape[1] // 2
    W, HW, TH, BLK, QF, FB = 4 * HB, 2 * HB, TK // 2, TK // NCH, FH // 4, 2 * FH
    assert FB <= W and FH <= HW and W // 4 <= BLK and QF <= BLK
    sd = jax.ShapeDtypeStruct
    NS = BLK // min(BLK, 128)
    outs = [sd((TK, HB), BF16), sd((TK, HB), BF16), sd((W // 2, FB), BF16), sd((4 * FH, HB), BF16), sd((1, 3 * HB + FB), F32)]
    n_out = len(outs)
    outs += [sd((2, TK, W), BF16)] * 3 + [sd((2, TK, FB), BF16)] * 3
    outs += [sd((TH, W), F32), sd((TH, HW), F32), sd((TH, HW), F32)] * 2
    outs += [sd((4, QF, HB), F32)] * 2 + [sd((W // 4, FH), F32)] * 2
    V = pltpu.VMEM
    scratch = [
        V((W, FB), BF16), V((FB, W), BF16), V((4, FH, HB), F32), V((4, W // 4, FH), F32),
        V((4, FH // 8, HB), F32), V((4, FH // 8, HB), F32), V((W // 8, FH), F32), V((W // 8, FH), F32),
        V((8, W), F32), V((8, FB), F32), V((2, BLK, W), BF16), V((2, BLK, W), BF16), V((4, BLK, HW), F32), V((2, BLK, HW), BF16),
        V((4, QF, HB), BF16), V((2, 8, FH), F32), V((2, 8, HW), F32),
        V((BLK, 128), F32), V((BLK, 128), F32), V((2, BLK, 128), F32), V((2, 2 * NS, 128), F32), V((2, 2 * NS, 128), F32),
        V((8, HB), F32), V((2, 1, 3 * HB + FB), F32), V((9, 1, 3 * HB + FB), F32),
        pltpu.SemaphoreType.DMA((N_SEM,)),
    ]
    res = pl.pallas_call(
        functools.partial(body, (TK, HB, FH)),
        out_shape=outs,
        in_specs=[pl.BlockSpec(memory_space=pl.ANY)] * 6,
        out_specs=[pl.BlockSpec(memory_space=pl.ANY)] * len(outs),
        scratch_shapes=scratch,
        compiler_params=pltpu.CompilerParams(collective_id=0, has_side_effects=True, vmem_limit_bytes=67043328),
        name='mlp_block',
    )(x, dy, wu, wd, vec, bu)
    return res[:n_out]


def solution(mesh):
    assert (mesh.shape['col'], mesh.shape['row'], mesh.shape['depth']) == (4, 2, 4)
    tok_spec = P(('dp', 'depth', 'row'), 'col')
    vec_spec = P('col')
    mat_spec = P('row', 'col')
    grad_vec = P(('dp', 'col'))
    grad_mat = P(('dp', 'row'), 'col')
    def local_pass(x_blk, gamma_blk, beta_blk, w_up_blk, b_up_blk, w_down_blk, b_down_blk, dy_blk):
        hb, fb = x_blk.shape[1], w_up_blk.shape[1]
        vec = jnp.stack([gamma_blk, beta_blk, b_down_blk.astype(F32)] + [jnp.zeros_like(gamma_blk)] * 5)
        bu = jnp.broadcast_to(b_up_blk.astype(F32)[None], (8, fb))
        y_blk, dx_blk, grad_w_up, grad_w_down, sums = block_kernel(x_blk, dy_blk, w_up_blk, w_down_blk, vec, bu)
        sums = sums[0]
        return (y_blk, dx_blk, sums[:hb], sums[hb:2 * hb], grad_w_up, sums[2 * hb:2 * hb + fb], grad_w_down, sums[2 * hb + fb:])

    return jax.shard_map(
        local_pass,
        mesh=mesh,
        in_specs=(tok_spec, vec_spec, vec_spec, mat_spec, vec_spec, mat_spec, vec_spec, tok_spec),
        out_specs=(tok_spec, tok_spec, grad_vec, grad_vec, grad_mat, grad_vec, grad_mat, grad_vec),
        check_vma=False,
    )
```

```python
import functools

import jax
import jax.numpy as jnp
from jax import lax
from jax.experimental import pallas as pl
from jax.experimental.pallas import tpu as pltpu
from jax.sharding import PartitionSpec as P

LN_EPS = 1e-5
F32 = jnp.float32
BF16 = jnp.bfloat16
MESH = pl.DeviceIdType.MESH
GELU_A = 0.7978845608028654
GELU_B = 0.044715
NCH = 4
ROWS = 16
LROWS = 64

NN = (((1,), (0,)), ((), ()))
NT = (((1,), (1,)), ((), ()))
TN = (((0,), (0,)), ((), ()))

SEMS = {}
for _z in ('x', 'g'):
    for _n in ('near', 'far', 'opp', 'd2d', 'd2w', 'd2o', 's_near', 's_far', 's_rel', 's_d2d'):
        SEMS[_z + _n] = NCH
    SEMS[_z + 'bounce'] = 2
for _p in ('y', 'd'):
    SEMS.update({_p + 's_give': 2, _p + 'got': 2, _p + 's_far': 2, _p + 'keep': 2, _p + 'far': 2, _p + 's_out': 4, _p + 'out': 1, _p + 'loc': 2})
SEMS.update(l_wu=1, s_wu=1, r_wu=1, s_wun=1, r_wun=1, s_wuy=4, r_wuy=4,
            s_wd0=2, s_wdx=4, r_wd=4, s_wdr=2, s_wdy=24, r_wdy=8,
            l_vec=2, s_vec=4, r_vec=2,
            ld=8, st=6, s_st=2, r_st=2, s_sum=8, r_sum=2,
            d_so=8, d_r=8, d_sa=8, d_p=8, d_sf=4, d_out=1, d_sy=8, d_y=2, d_sr=8, d_o=2,
            u_so=2, u_r=2, u_sa=2, u_p=2, u_sf=3, u_out=3, u_sr=1, u_o=2, l_small=2)
BASE = {}
_at = 0
for _n, _c in SEMS.items():
    BASE[_n] = _at
    _at += _c
N_SEM = _at


def gelu(v):
    return 0.5 * v * (1.0 + jnp.tanh(GELU_A * (v + GELU_B * (v * v * v))))


def gelu_slope(v):
    v2 = v * v
    t = jnp.tanh(v * (GELU_A + (GELU_A * GELU_B) * v2))
    q = (1.0 - t) * (GELU_A + (3.0 * GELU_A * GELU_B) * v2)
    return 0.5 * ((1.0 + t) * (1.0 + v * q))


def body(dims, x_ref, dy_ref, wu_ref, wd_ref, vec_ref, bu_ref,
         y_out, dx_out, gwu_out, gwd_out, sum_out,
         X, DY, XN, U, A, DU, YGOT, YFAR, YKEEP, GGOT, GFAR, GKEEP, PFD, PND, PFU, PNU,
         wu_v, wd_v, accD, accU, r1D, r2D, r1U, r2U, vec_v, bu_v, wx, wo, F4, ob, finD,
         db_v, cs_v, st_v, ms_v, st2_v, sx_v, sr_v, bd_v, sum_v, sumr_v, sem):
    TK, HB, FH = dims
    W, HW, TH, BLK, QF = 4 * HB, 2 * HB, TK // 2, TK // NCH, FH // 4
    RH, DQ, QH, DH, FB = W // 2, W // 4, FH // 8, W // 8, 2 * FH
    NTW = HB
    inv_w = 1.0 / W
    finU = wo.at[1, pl.ds(0, DQ), pl.ds(HW, FH)]
    f0, f1 = F4.at[0], F4.at[1]
    own2 = (pl.ds(0, FH), pl.ds(FH, FH))

    c, r, d = lax.axis_index('col'), lax.axis_index('row'), lax.axis_index('depth')
    c_odd, d_odd = lax.rem(c, 2), lax.rem(d, 2)
    cn, cf, co = c + 1 - 2 * c_odd, 3 - c, lax.rem(c + 2, 4)
    dn, df, do = d + 1 - 2 * d_odd, 3 - d, lax.rem(d + 2, 4)
    f, dh = lax.div(c, 2), lax.div(d, 2)
    tau = lax.rem(lax.div(c + 1, 2), 2)
    rp = 1 - r
    o, o2 = c_odd * FH, (1 - c_odd) * FH

    def S(name, i=0):
        return sem.at[BASE[name] + i]

    def ds(start, size):
        return pl.ds(pl.multiple_of(start, size), size)

    def dsm(start, size, mult):
        return pl.ds(pl.multiple_of(start, mult), size)

    def put(src, dst, ssem, rsem, **dev):
        pltpu.make_async_remote_copy(src_ref=src, dst_ref=dst, send_sem=ssem, recv_sem=rsem,
                                     device_id=dev, device_id_type=MESH).start()

    def copy(src, dst, s):
        pltpu.make_async_copy(src, dst, s).start()

    def wait(ref, s):
        pltpu.make_async_copy(ref, ref, s).wait()

    def loop(n, fn):
        def step(i, carry):
            fn(i)
            return carry
        lax.fori_loop(0, n, step, 0)

    bar = pltpu.get_barrier_semaphore()
    for dev in [dict(row=rp)] + [dict(row=h, **q) for h in range(2) for q in
                                 (dict(col=cn), dict(col=cf), dict(col=co), dict(depth=dn), dict(depth=df), dict(depth=do))]:
        pl.semaphore_signal(bar, inc=1, device_id=dev, device_id_type=MESH)
    pl.semaphore_wait(bar, 13)

    def wd_src(s, h):
        return wd_ref.at[dsm((2 * s + h) * FH + d * QF, QF, QF), :]

    def wd_dst(s, col):
        return wd_v.at[dsm(s * FH + d * QF, QF, QF), ds(col * HB, HB)]

    def reg(Z, k, col):
        return Z.at[r, ds(k * BLK, BLK), ds(col * HB, HB)]

    def send_own(z, z_ref, Z, which, chunks=(0, NCH)):
        def step(k):
            src = z_ref.at[ds(k * BLK, BLK), :]
            if 'near' in which:
                put(src, reg(Z, k, c), S(z + 's_near', k), S(z + 'near', k), col=cn)
            if 'far' in which:
                put(src, reg(Z, k, c), S(z + 's_far', k), S(z + 'far', k), col=cf)
            if 'd2d' in which:
                put(src, reg(Z, k, c), S(z + 's_d2d', k), S(z + ('d2d' if z == 'x' else 'd2w'), k), row=rp)
        for k in range(*chunks):
            step(k)

    def d2d(z, Z, k, col, s):
        put(reg(Z, k, col), reg(Z, k, col), S(z + 's_d2d', k), S(z + s, k), row=rp)

    vec_at = vec_v.at[:, ds(c * HB, HB)]
    copy(vec_ref, vec_at, S('l_vec', 0))
    put(vec_ref, vec_at, S('s_vec', 0), S('r_vec', 0), col=cn)
    put(vec_ref, vec_at, S('s_vec', 1), S('r_vec', 0), col=cf)
    put(vec_ref, vec_at, S('s_vec', 2), S('r_vec', 0), col=co)
    bu_src, bu_at = bu_ref.at[:, ds(r * FH, FH)], bu_v.at[:, ds(o, FH)]
    copy(bu_src, bu_at, S('l_vec', 1))
    put(bu_src, bu_at, S('s_vec', 3), S('r_vec', 1), col=cn)

    wu_own = wu_v.at[ds(r * RH, RH), ds(o, FH)]
    wd_own = lambda s: wd_v.at[pl.ds(s * FH, FH), ds(c * HB, HB)]

    @pl.when(r != f)
    def _():
        for s in range(2):
            for h in range(2):
                put(wd_src(s, h), wd_dst(s, c), S('s_wdx', 2 * s + h), S('r_wd', 2), col=cf, row=h)

    @pl.when(r == f)
    def _():
        for s in range(2):
            for h in range(2):
                put(wd_src(s, h), wd_dst(s, c), S('s_wdx', 2 * s + h), S('r_wd', 1), col=cn, row=h)
    send_own('x', x_ref, X, ('far',), (0, 2))
    send_own('x', x_ref, X, ('near',), (0, 1))
    put(wu_ref.at[:, ds(rp * FH, FH)], wu_own, S('s_wu'), S('r_wu'), row=rp)
    copy(wu_ref.at[:, ds(r * FH, FH)], wu_own, S('l_wu'))
    send_own('x', x_ref, X, ('d2d',))
    send_own('g', dy_ref, DY, ('d2d',))
    for i, z_ref in enumerate((x_ref, dy_ref)):
        for k in range(NCH):
            copy(z_ref.at[pl.ds(k * BLK, BLK), :], wx.at[i, :, pl.ds(k * HB, HB)], S('xg'[i] + 'bounce', 0))

    @pl.when(r == f)
    def _():
        for s in range(2):
            copy(wd_ref.at[dsm((2 * s + r) * FH, FH, FH), :], wd_own(s), S('r_wd', 0))
            put(wd_ref.at[dsm((2 * s + rp) * FH, FH, FH), :], wd_own(s), S('s_wd0', s), S('r_wd', 0), row=rp)

    for i, Z in enumerate((X, DY)):
        wait(wx.at[i], S('xg'[i] + 'bounce', 0))
        for k in range(NCH):
            copy(wx.at[i, :, pl.ds(k * HB, HB)], reg(Z, k, c), S('xg'[i] + 'bounce', 1))

    with jax.named_scope('wd_far'):
        wait(wd_v.at[pl.ds(0, 2 * QF), pl.ds(0, HB)], S('r_wd', 2))
    for s in range(2):
        put(wd_dst(s, cf), wd_dst(s, cf), S('s_wdr', s), S('r_wd', 3), col=cn)
    send_own('x', x_ref, X, ('near',), (1, NCH - 1))

    with jax.named_scope('wu_own'):
        wait(wu_own, S('l_wu'))
        wait(wu_v.at[ds(rp * RH, RH), ds(o, FH)], S('r_wu'))
    wun = wu_v.at[ds(d * DQ, DQ), ds(o, FH)]
    put(wun, wun, S('s_wun'), S('r_wun'), col=cn)
    send_own('x', x_ref, X, ('near',), (NCH - 1, NCH))

    db_v[...] = jnp.zeros_like(db_v)
    cs_v[...] = jnp.zeros_like(cs_v)
    bd_v[...] = jnp.zeros_like(bd_v)

    def dy_sum(i):
        rr = ds(i * ROWS, ROWS)
        part = jnp.sum(wx[1, rr, :].astype(F32).reshape(ROWS // 8, 8, W), axis=0)
        bd_v[...] += part[:, :HB] + part[:, HB:2 * HB] + part[:, 2 * HB:3 * HB] + part[:, 3 * HB:]
    with jax.named_scope('dy_sum'):
        loop(BLK // ROWS, dy_sum)

    def wuq(dd, half=None):
        if half is None:
            return wu_v.at[ds(dd * DQ, DQ), ds(o2, FH)]
        return wu_v.at[dsm(dd * DQ + half * DH, DH, DH), ds(o2, FH)]

    def wu_send():
        with jax.named_scope('wu_near'):
            wait(wuq(d), S('r_wun'))
        put(wuq(d), wuq(d), S('s_wuy', 0), S('r_wuy', 0), depth=dn)
        put(wuq(d), wuq(d), S('s_wuy', 1), S('r_wuy', 1), depth=df)

    def wu_relay():
        with jax.named_scope('wuy'):
            wait(wuq(dn), S('r_wuy', 0))
            wait(wuq(df), S('r_wuy', 1))
        put(wuq(dn, 1), wuq(dn, 1), S('s_wuy', 2), S('r_wuy', 3), depth=df)
        put(wuq(df, 0), wuq(df, 0), S('s_wuy', 3), S('r_wuy', 2), depth=dn)

    def wdq(s, dd, col, half=None):
        if half is None:
            return wd_v.at[dsm(s * FH + dd * QF, QF, QF), ds(col * HB, HB)]
        return wd_v.at[dsm(s * FH + dd * QF + half * QH, QH, QH), ds(col * HB, HB)]

    W_GROUPS = (((0, cn), (1, cf)), ((2, co),))

    def wd_send(g):
        if g == 0:
            wait(wd_v.at[pl.ds(0, 2 * QF), pl.ds(0, HB)], S('r_wd', 1))
        else:
            wait(wd_v.at[pl.ds(0, 2 * QF), pl.ds(0, HB)], S('r_wd', 3))
        for i, col in W_GROUPS[g]:
            for s in range(2):
                put(wdq(s, d, col), wdq(s, d, col), S('s_wdy', 4 * i + s), S('r_wdy', 4 * g), depth=dn)
                put(wdq(s, d, col), wdq(s, d, col), S('s_wdy', 4 * i + 2 + s), S('r_wdy', 4 * g + 1), depth=df)

    def wd_bytes(g, rows):
        return wd_v.at[pl.ds(0, 2 * rows), pl.ds(0, len(W_GROUPS[g]) * HB)]

    def wd_relay(g):
        for i in range(2):
            wait(wd_bytes(g, QF), S('r_wdy', 4 * g + i))
        for i, col in W_GROUPS[g]:
            for s in range(2):
                put(wdq(s, dn, col, 1), wdq(s, dn, col, 1), S('s_wdy', 12 + 4 * i + s), S('r_wdy', 4 * g + 3), depth=df)
                put(wdq(s, df, col, 0), wdq(s, df, col, 0), S('s_wdy', 12 + 4 * i + 2 + s), S('r_wdy', 4 * g + 2), depth=dn)

    def x_near(k):
        wait(reg(X, k, cn), S('xnear', k))
        put(reg(X, k, cn), reg(X, k, cn), S('xs_rel', k), S('xopp', k), col=cf)
        d2d('x', X, k, cn, 'd2d')

    with jax.named_scope('wd_send0'):
        wd_send(0)
    with jax.named_scope('x_near'):
        x_near(0)
    send_own('x', x_ref, X, ('far',), (2, 3))

    for i, Z in enumerate((X, DY)):
        wait(wx.at[i], S('xg'[i] + 'bounce', 1))
    wait(vec_at, S('l_vec', 0))
    wait(vec_v.at[:, pl.ds(0, 3 * HB)], S('r_vec', 0))
    wait(bu_at, S('l_vec', 1))
    wait(bu_at, S('r_vec', 1))

    def norm_rows(buf, rows):
        xf = buf[rows, :].astype(F32)
        mean = jnp.sum(xf, axis=1, keepdims=True) * inv_w
        cen = xf - mean
        inv = lax.rsqrt(jnp.sum(cen * cen, axis=1, keepdims=True) * inv_w + LN_EPS)
        return cen, mean, inv

    def tok_of(s):
        return tau + s * (1 - 2 * tau)

    N_T = FH // NTW

    def chain(tiles, hooks=None):
        hooks = hooks or {}

        def hook(what, i):
            for fn in hooks.get((what, i), ()):
                fn()
        for i, (product, _) in enumerate(tiles):
            hook('before', i)
            if i:
                tiles[i - 1][1](F4.at[(i - 1) % 2])
            F4[i % 2, :, :NTW] = product()
            hook('product', i)
            if i:
                hook('epilogue', i - 1)
        tiles[-1][1](F4.at[(len(tiles) - 1) % 2])
        hook('epilogue', len(tiles) - 1)

    def u_tile(i, n, start):
        cols = ds(start + n * NTW, NTW)
        at = pl.ds((i * N_T + n) * NTW, NTW)

        def product():
            return lax.dot_general(wx[i], wu_v[:, cols], NN, preferred_element_type=F32)

        def epilogue(acc):
            u = (acc[:, :NTW] + bu_v[0:1, cols]).astype(BF16)
            wo[0, :, at] = u
            wo[1, :, at] = gelu(u.astype(F32)).astype(BF16)
        return product, epilogue

    def u_store(i, s, rows, start):
        copy(wo.at[0, :, own2[i]], U.at[s, rows, ds(start, FH)], S('st', 2 + i))
        copy(wo.at[1, :, own2[i]], A.at[s, rows, ds(start, FH)], S('st', 4 + i))

    def u_stored():
        for i in range(2):
            wait(wo.at[0, :, own2[i]], S('st', 2 + i))
            wait(wo.at[1, :, own2[i]], S('st', 4 + i))

    def phase1(k):
        @pl.when(k < NCH - 1)
        def _():
            with jax.named_scope('x_near'):
                x_near(k + 1)

        @pl.when(k == 0)
        def _():
            send_own('x', x_ref, X, ('far',), (3, 4))
            with jax.named_scope('wd_send1'):
                wd_send(1)

        @pl.when(k == 1)
        def _():
            with jax.named_scope('wd_relay0'):
                wd_relay(0)
            send_own('g', dy_ref, DY, ('near',))

        @pl.when(k == 2)
        def _():
            send_own('g', dy_ref, DY, ('far',))
            with jax.named_scope('wd_relay1'):
                wd_relay(1)
            wu_send()

        with jax.named_scope('x_far'):
            wait(reg(X, k, cf), S('xfar', k))
            d2d('x', X, k, cf, 'd2d')
        with jax.named_scope('x_opp'):
            wait(reg(X, k, co), S('xopp', k))
            d2d('x', X, k, co, 'd2d')

        rows = ds(k * BLK, BLK)
        with jax.named_scope('x_d2d'):
            wait(X.at[rp, rows, :], S('xd2d', k))

        @pl.when(k > 0)
        def _():
            for s in range(2):
                wait(wx.at[s], S('st', s))
        for s in range(2):
            copy(X.at[tok_of(s), rows, :], wx.at[s], S('ld', s))
        for s in range(2):
            wait(wx.at[s], S('ld', s))

            def ln(i):
                rr = ds(i * LROWS, LROWS)
                cen, _, inv = norm_rows(wx.at[s], rr)
                wx[s, rr, :] = (cen * inv * vec_v[0:1, :] + vec_v[1:2, :]).astype(BF16)
            with jax.named_scope('ln'):
                loop(BLK // LROWS, ln)
            copy(wx.at[s], XN.at[s, rows, :], S('st', s))
        pl.when(k > 0)(u_stored)
        with jax.named_scope('u_own'):
            chain([u_tile(i, n, o) for i in range(2) for n in range(N_T)])
        for s in range(2):
            u_store(s, s, rows, o)
    loop(NCH, phase1)
    for s in range(2):
        wait(wx.at[s], S('st', s))
    u_stored()

    def u_near():
        def load(kp, i):
            copy(XN.at[0, ds((2 * kp + i) * BLK, BLK), :], wx.at[i], S('ld', i))

        def step(kp):
            def more(i):
                load(1, i)
            wait(wx.at[0], S('ld', 0))
            pl.when(kp > 0)(u_stored)
            chain([u_tile(i, n, o2) for i in range(2) for n in range(N_T)],
                  {('before', N_T): [lambda: wait(wx.at[1], S('ld', 1))],
                   ('product', N_T - 1): [lambda: more(0)],
                   ('product', 2 * N_T - 1): [lambda: more(1)],
                   ('epilogue', N_T - 1): [lambda: u_store(0, 0, ds(2 * kp * BLK, BLK), o2)],
                   ('epilogue', 2 * N_T - 1): [lambda: u_store(1, 0, ds((2 * kp + 1) * BLK, BLK), o2)]})
        for i in range(2):
            load(0, i)
        loop(2, step)
        u_stored()
        for i in range(2):
            wait(wx.at[i], S('ld', i))

    def g_near_far(k):
        wait(reg(DY, k, cf), S('gfar', k))
        put(reg(DY, k, cf), reg(DY, k, cf), S('gs_rel', k), S('gopp', k), col=cn)
        d2d('g', DY, k, cf, 'd2d')
        wait(reg(DY, k, cn), S('gnear', k))
        d2d('g', DY, k, cn, 'd2d')

    def g_opp(k):
        wait(reg(DY, k, co), S('gopp', k))
        d2d('g', DY, k, co, 'd2o')
        wait(reg(DY, k, co), S('gd2o', k))

    def tile_y(lhs, col):
        return lax.dot_general(lhs, wd_v[:, dsm(col, NTW, NTW)], NN, preferred_element_type=F32)

    def tile_g(lhs, col):
        return lax.dot_general(lhs, wu_v[dsm(col, NTW, NTW), :], NT, preferred_element_type=F32)

    def give(p, src, tile, GOT):
        def blk(b):
            return src.at[0, dsm(rp * TH + b * BLK, BLK, BLK), :]
        for b in range(2):
            copy(blk(b), wx.at[b, :, pl.ds(0, FB)], S('ld', b))

        def step(b):
            wait(wx.at[b, :, pl.ds(0, FB)], S('ld', b))

            def half(h):
                @pl.when(b == 1)
                def _():
                    wait(F4.at[h], S(p + 's_give', h))

                def n_tile(n):
                    F4[h, :, ds(n * NTW, NTW)] = tile(wx[b, :, :FB], h * HW + n * NTW)
                loop(HW // NTW, n_tile)
                put(F4.at[h], GOT.at[ds(b * BLK, BLK), ds(h * HW, HW)], S(p + 's_give', h), S(p + 'got', b), row=rp)
            loop(2, half)
        loop(2, step)

    def keep(p, src, tile, GOT, FAR, KEEP):
        def blk(b):
            return src.at[0, dsm(r * TH + b * BLK, BLK, BLK), :]

        def col_of(h):
            return (1 - f + h * (2 * f - 1)) * HW

        def out_of(b, h):
            return (2 + b) * (1 - h) + (1 - b) * h
        for b in range(2):
            copy(blk(b), wx.at[b, :, pl.ds(0, FB)], S('ld', b))
        for h in range(2):
            wait(F4.at[h], S(p + 's_give', h))

        def fetch(b):
            with jax.named_scope('got'):
                wait(GOT.at[ds(b * BLK, BLK), :], S(p + 'got', b))
            for h in range(2):
                copy(GOT.at[ds(b * BLK, BLK), ds(col_of(h), HW)], F4.at[out_of(b, h)], S('ld', 4 + 2 * b + h))
        fetch(0)

        def step(b):
            brow = ds(b * BLK, BLK)
            wait(wx.at[b, :, pl.ds(0, FB)], S('ld', b))

            def half(h):
                out = out_of(b, h)
                wait(F4.at[out], S('ld', 4 + 2 * b + h))

                def n_tile(n):
                    at = ds(n * NTW, NTW)
                    F4[out, :, at] = F4[out, :, at] + tile(wx[b, :, :FB], col_of(h) + n * NTW)
                loop(HW // NTW, n_tile)

                @pl.when(h == 0)
                def _():
                    put(F4.at[2 + b], FAR.at[brow, :], S(p + 's_far', b), S(p + 'far', b), col=cf)

                @pl.when(h == 1)
                def _():
                    copy(F4.at[1 - b], KEEP.at[brow, :], S(p + 'keep', b))

                @pl.when(jnp.logical_and(b == 0, h == 0))
                def _():
                    fetch(1)
            loop(2, half)
        loop(2, step)
        for b in range(2):
            wait(F4.at[b], S(p + 'keep', b))

    def keep_end(p):
        for b in range(2):
            wait(F4.at[2 + b], S(p + 's_far', b))

    def place(p, out, b):
        dst = out.at[dsm(r * TH + b * BLK, BLK, BLK), :]
        mine, other = ob.at[b, :, ds(c_odd * HB, HB)], ob.at[b, :, ds((1 - c_odd) * HB, HB)]
        put(other, dst, S(p + 's_out', 2 * b), S(p + 'out'), col=cn, row=tau)

        @pl.when(r == tau)
        def _():
            copy(mine, dst, S(p + 'loc', b))

        @pl.when(r != tau)
        def _():
            put(mine, dst, S(p + 's_out', 2 * b + 1), S(p + 'out'), row=rp)

    def place_end(p, b):
        wait(ob.at[b, :, pl.ds(0, HB)], S(p + 's_out', 2 * b))

        @pl.when(r == tau)
        def _():
            wait(ob.at[b, :, pl.ds(0, HB)], S(p + 'loc', b))

        @pl.when(r != tau)
        def _():
            wait(ob.at[b, :, pl.ds(0, HB)], S(p + 's_out', 2 * b + 1))

    fcols = ds(f * HW, HW)

    def y_final(b):
        brow = ds(b * BLK, BLK)
        wait(YFAR.at[brow, :], S('yfar', b))
        copy(YFAR.at[brow, :], f0, S('ld', 0))
        copy(YKEEP.at[brow, :], f1, S('ld', 1))
        copy(X.at[tau, dsm(r * TH + b * BLK, BLK, BLK), fcols], wx.at[0, :, pl.ds(0, HW)], S('ld', 2))
        wait(f0, S('ld', 0))
        wait(f1, S('ld', 1))
        wait(wx.at[0, :, pl.ds(0, HW)], S('ld', 2))

        def fin(i):
            rr = ds(i * ROWS, ROWS)
            ob[b, rr, :] = (wx[0, rr, :HW].astype(F32) + (f0[rr, :] + f1[rr, :]) + vec_v[2:3, fcols]).astype(BF16)
        loop(BLK // ROWS, fin)
        place('y', y_out, b)

    def services(t):
        @pl.when(t == 3)
        def _():
            with jax.named_scope('dwd_b1'):
                dwd_b(1)

        @pl.when(t == 4)
        def _():
            with jax.named_scope('dwd_a3b2'):
                dwd_a(3)
                dwd_b(2)

    def da_all():
        def part(t, i):
            near = lax.div(t, NCH)
            tok = tau + i * (1 - near) * (1 - 2 * tau)
            chunk = t * (1 - near) + near * (2 * (t - NCH) + i)
            return near, tok, i * (1 - near), ds(chunk * BLK, BLK), near * o2 + (1 - near) * o

        def load_dy(t, i):
            _, tok, _, rows, _ = part(t, i)
            copy(DY.at[tok, rows, :], wx.at[i], S('ld', i))

        def load_u(t, i):
            _, _, us, rows, start = part(t, i)
            copy(U.at[us, rows, ds(start, FH)], wo.at[0, :, own2[i]], S('ld', 2 + i))

        def store(t, i):
            _, _, us, rows, start = part(t, i)
            copy(wo.at[1, :, own2[i]], DU.at[us, rows, ds(start, FH)], S('st', 4 + i))

        def stored(i):
            wait(wo.at[1, :, own2[i]], S('st', 4 + i))

        n_steps = NCH + NCH // 2

        def step(t):
            near, _, _, _, start = part(t, 0)
            services(t)

            def tile(i, n):
                cols = ds(start + n * NTW, NTW)
                at = pl.ds((i * N_T + n) * NTW, NTW)

                def product():
                    return lax.dot_general(wx[i], wd_v[cols, :], NT, preferred_element_type=F32)

                def epilogue(acc):
                    du = (acc[:, :NTW] * gelu_slope(wo[0, :, at].astype(F32))).astype(BF16)
                    wo[1, :, at] = du
                    db_v[near, :, n * NTW:(n + 1) * NTW] += jnp.sum(du.astype(F32).reshape(BLK // 8, 8, NTW), axis=0)
                return product, epilogue

            def arrive(i):
                wait(wx.at[i], S('ld', i))
                wait(wo.at[0, :, own2[i]], S('ld', 2 + i))
                stored(i)

            def more(fn, i):
                fn(jnp.minimum(t + 1, n_steps - 1), i)

            def finish(i):
                store(t, i)
                more(load_u, i)
            arrive(0)
            chain([tile(i, n) for i in range(2) for n in range(N_T)],
                  {('before', N_T): [lambda: arrive(1)],
                   ('product', N_T - 1): [lambda: more(load_dy, 0)],
                   ('product', 2 * N_T - 1): [lambda: more(load_dy, 1)],
                   ('epilogue', N_T - 1): [lambda: finish(0)],
                   ('epilogue', 2 * N_T - 1): [lambda: finish(1)]})
        for i in range(2):
            load_dy(0, i)
            load_u(0, i)
            store(0, i)
        loop(n_steps, step)
        for i in range(2):
            stored(i)
            wait(wx.at[i], S('ld', i))
            wait(wo.at[0, :, own2[i]], S('ld', 2 + i))

    def rows_of(kb):
        return ds(lax.rem(kb, NCH) * BLK, BLK), lax.div(kb, NCH)

    d_col = (c, cn, cf, co)

    NB = 2 * NCH
    rings = (wx, wo)

    def k_loop(load, use, width):
        for kb in range(3):
            load(kb, rings[kb % 2].at[kb // 2], S('ld', kb))

        def step(i):
            p = lax.rem(i, 2)
            for q in range(2):
                kb = 2 * i + q
                np_ = lax.rem(i + 1 + q, 2)

                @pl.when(kb + 3 < NB)
                def _():
                    load(kb + 3, rings[1 - q].at[np_], S('ld', (1 - q) + 2 * np_))
                buf = rings[q].at[p]
                wait(buf.at[:, pl.ds(0, width)], S('ld', q + 2 * p))
                use(buf)
        loop(NB // 2, step)

    def dwd_pass(js):
        def load(kb, buf, s_):
            rows, s = rows_of(kb)
            copy(A.at[s, rows, ds(o, FH)], buf.at[:, pl.ds(0, FH)], s_)
            for i, j in enumerate(js):
                copy(DY.at[tok_of(s), rows, ds(d_col[j] * HB, HB)], buf.at[:, pl.ds(FH + i * HB, HB)], s_)

        def use(buf):
            for i, j in enumerate(js):
                for m in range(2):
                    mm = slice(m * FH // 2, (m + 1) * FH // 2)
                    accD[j, mm, :] += lax.dot_general(buf[:, mm], buf[:, FH + i * HB:FH + (i + 1) * HB], TN, preferred_element_type=F32)
        for j in js:
            accD[j] = jnp.zeros((FH, HB), F32)
        k_loop(load, use, FH + len(js) * HB)

    def dwd_opp(j):
        put(accD.at[j, dsm(do * QF, QH, QH), :], r1D.at[j], S('d_so', 2 * j), S('d_r', 2 * j), depth=dn)
        put(accD.at[j, dsm(do * QF + QH, QH, QH), :], r2D.at[j], S('d_so', 2 * j + 1), S('d_r', 2 * j + 1), depth=df)

    def dwd_a(j):
        wait(r1D.at[j], S('d_r', 2 * j))
        rr = dsm(df * QF, QH, QH)
        accD[j, rr, :] += r1D[j]
        put(accD.at[j, ds(df * QF, QF), :], PFD.at[j], S('d_sa', 2 * j), S('d_p', 2 * j), depth=df)
        wait(r2D.at[j], S('d_r', 2 * j + 1))
        rr = dsm(dn * QF + QH, QH, QH)
        accD[j, rr, :] += r2D[j]
        put(accD.at[j, ds(dn * QF, QF), :], PND.at[j], S('d_sa', 2 * j + 1), S('d_p', 2 * j + 1), depth=dn)

    def dwd_rows(q, h, dd):
        return dsm((2 * q + h) * FH + dd * QF, QF, QF)

    def dwd_b(j):
        wait(PFD.at[j], S('d_p', 2 * j))
        wait(PND.at[j], S('d_p', 2 * j + 1))
        wait(PFD.at[j], S('d_sa', 2 * j))
        wait(PND.at[j], S('d_sa', 2 * j + 1))
        pf, pn = accD.at[j, ds(df * QF, QF), :], accD.at[j, ds(dn * QF, QF), :]
        copy(PFD.at[j], pf, S('ld', 6))
        copy(PND.at[j], pn, S('ld', 7))
        wait(pf, S('ld', 6))
        wait(pn, S('ld', 7))
        finD[j] = (accD[j, ds(d * QF, QF), :] + (pf[...] + pn[...])).astype(BF16)
        dst = gwd_out.at[dwd_rows(c_odd, r, d), :]
        if j:
            put(finD.at[j], dst, S('d_sf', j), S('d_out'), col=d_col[j], row=f)
        else:
            @pl.when(r == f)
            def _():
                copy(finD.at[0], dst, S('d_out'))

            @pl.when(r != f)
            def _():
                put(finD.at[0], dst, S('d_sf', 0), S('d_out'), row=rp)

    def gwd(i, dd, half=None):
        if half is None:
            return gwd_out.at[dsm(i * FH + dd * QF, QF, QF), :]
        return gwd_out.at[dsm(i * FH + dd * QF + half * QH, QH, QH), :]

    def gwd_send():
        wait(gwd_out.at[pl.ds(0, 4 * QF), :], S('d_out'))
        for i in range(4):
            put(gwd(i, d), gwd(i, d), S('d_sy', i), S('d_y', 0), depth=dn)
            put(gwd(i, d), gwd(i, d), S('d_sy', 4 + i), S('d_y', 1), depth=df)

    def gwd_relay():
        wait(gwd_out.at[pl.ds(0, 4 * QF), :], S('d_y', 0))
        for i in range(4):
            put(gwd(i, dn, 1), gwd(i, dn, 1), S('d_sr', i), S('d_o', 1), depth=df)
        wait(gwd_out.at[pl.ds(0, 4 * QF), :], S('d_y', 1))
        for i in range(4):
            put(gwd(i, df, 0), gwd(i, df, 0), S('d_sr', 4 + i), S('d_o', 0), depth=dn)

    def dwu_pass(dds):
        def load(kb, buf, s_):
            rows, s = rows_of(kb)
            copy(DU.at[s, rows, ds(o, FH)], buf.at[:, pl.ds(0, FH)], s_)
            for i, dd in enumerate(dds):
                copy(XN.at[s, rows, ds(dd * DQ, DQ)], buf.at[:, pl.ds(FH + i * DQ, DQ)], s_)

        def use(buf):
            for i, dd in enumerate(dds):
                for m in range(2):
                    mm = slice(m * FH // 2, (m + 1) * FH // 2)
                    accU[dd, :, mm] += lax.dot_general(buf[:, FH + i * DQ:FH + (i + 1) * DQ], buf[:, mm], TN, preferred_element_type=F32)
        for dd in dds:
            accU[dd] = jnp.zeros((DQ, FH), F32)
        k_loop(load, use, FH + len(dds) * DQ)

    def dwu_opp():
        put(accU.at[do, pl.ds(0, DH), :], r1U, S('u_so', 0), S('u_r', 0), depth=dn)
        put(accU.at[do, pl.ds(DH, DH), :], r2U, S('u_so', 1), S('u_r', 1), depth=df)

    def dwu_a():
        wait(r1U, S('u_r', 0))
        accU[df, :DH, :] += r1U[...]
        put(accU.at[df], PFU, S('u_sa', 0), S('u_p', 0), depth=df)
        wait(r2U, S('u_r', 1))
        accU[dn, DH:, :] += r2U[...]
        put(accU.at[dn], PNU, S('u_sa', 1), S('u_p', 1), depth=dn)

    def dwu_b():
        wait(PFU, S('u_p', 0))
        wait(PNU, S('u_p', 1))
        pf, pn = f0.at[pl.ds(0, DQ), pl.ds(0, FH)], f1.at[pl.ds(0, DQ), pl.ds(0, FH)]
        copy(PFU, pf, S('ld', 6))
        copy(PNU, pn, S('ld', 7))
        wait(pf, S('ld', 6))
        wait(pn, S('ld', 7))

        def fin(i):
            rr = ds(i * ROWS, ROWS)
            wo[1, rr, HW:HW + FH] = (accU[d, rr, :] + (f0[rr, :FH] + f1[rr, :FH])).astype(BF16)
        loop(DQ // ROWS, fin)
        dst = gwu_out.at[ds(d_odd * DQ, DQ), ds(r * FH, FH)]
        put(finU, dst, S('u_sf', 0), S('u_out', 1), depth=dn, row=dh)
        put(finU, dst, S('u_sf', 1), S('u_out', 2), depth=df, row=dh)

        @pl.when(r == dh)
        def _():
            copy(finU, dst, S('u_out', 0))

        @pl.when(r != dh)
        def _():
            put(finU, dst, S('u_sf', 2), S('u_out', 0), row=rp)

    def gwu(start, size):
        return gwu_out.at[dsm(start, size, size), :]

    def gwu_relay():
        @pl.when(r == dh)
        def _():
            wait(gwu(lax.rem(dn, 2) * DQ, DQ), S('u_out', 1))
            part = gwu(lax.rem(dn, 2) * DQ + DH, DH)
            put(part, part, S('u_sr'), S('u_o', 1), depth=df)

        @pl.when(r != dh)
        def _():
            wait(gwu(lax.rem(df, 2) * DQ, DQ), S('u_out', 2))
            part = gwu(lax.rem(df, 2) * DQ, DH)
            put(part, part, S('u_sr'), S('u_o', 0), depth=dn)

    def gwu_end():
        @pl.when(r == dh)
        def _():
            wait(gwu(d_odd * DQ, DQ), S('u_out', 0))

        @pl.when(r != dh)
        def _():
            wait(gwu(0, DH), S('u_o', 0))
            wait(gwu(0, DH), S('u_o', 1))

    lane = lax.broadcasted_iota(jnp.int32, (LROWS, 128), 1)

    def dx_a(b):
        brow = ds(b * BLK, BLK)
        trow = dsm(r * TH + b * BLK, BLK, BLK)
        wait(GFAR.at[brow, :], S('dfar', b))
        copy(GFAR.at[brow, :], f0, S('ld', 0))
        copy(GKEEP.at[brow, :], f1, S('ld', 1))
        copy(X.at[tau, trow, :], wx.at[b], S('ld', 2))
        copy(DY.at[tau, trow, fcols], wo.at[b, :, pl.ds(0, HW)], S('ld', 3))
        wait(f0, S('ld', 0))
        wait(f1, S('ld', 1))
        wait(wx.at[b], S('ld', 2))
        wait(wo.at[b, :, pl.ds(0, HW)], S('ld', 3))

        def rows_step(i):
            rr = ds(i * LROWS, LROWS)
            _, mean, inv = norm_rows(wx.at[b], rr)
            xhat = (wx[b, rr, fcols].astype(F32) - mean) * inv
            dxn = f0[rr, :] + f1[rr, :]
            F4[2 + b, rr, :] = dxn
            gh = dxn * vec_v[0:1, fcols]
            s0 = jnp.sum(gh, axis=1, keepdims=True)
            s1 = jnp.sum(gh * xhat, axis=1, keepdims=True)
            srow = rr
            st_v[srow, :] = jnp.where(lane < 64, s0, s1)
            ms_v[srow, :] = jnp.where(lane < 64, mean, inv)
            p1 = dxn * xhat
            cs_v[0] += jnp.sum(p1.reshape(LROWS // 8, 8, HW), axis=0)
            cs_v[1] += jnp.sum(dxn.reshape(LROWS // 8, 8, HW), axis=0)
        loop(BLK // LROWS, rows_step)

    SB = min(BLK, 128)
    NS = BLK // SB

    def stats_send(b):
        for t in range(NS):
            tr = st_v[t * SB:(t + 1) * SB, :].T
            sx_v[b, t:t + 1, :SB] = tr[0:1, :]
            sx_v[b, NS + t:NS + t + 1, :SB] = tr[64:65, :]
        put(sx_v.at[b], sr_v.at[b], S('s_st', b), S('r_st', b), col=cf)

    def stats_recv(b):
        wait(sr_v.at[b], S('r_st', b))
        for t in range(NS):
            for i in range(2):
                row = (sx_v[b, i * NS + t:i * NS + t + 1, :SB] + sr_v[b, i * NS + t:i * NS + t + 1, :SB]) * inv_w
                st2_v[i, t * SB:(t + 1) * SB, :] = jnp.broadcast_to(row, (128, SB)).T

    def dx_b(b):
        def rows_step(i):
            rr = ds(i * ROWS, ROWS)
            srow = rr
            mean, inv = ms_v[srow, 0:1], ms_v[srow, 64:65]
            xhat = (wx[b, rr, fcols].astype(F32) - mean) * inv
            gh = F4[2 + b, rr, :] * vec_v[0:1, fcols]
            dx = wo[b, rr, :HW].astype(F32) + inv * (gh - st2_v[0, srow, 0:1] - xhat * st2_v[1, srow, 0:1])
            ob[b, rr, :] = dx.astype(BF16)
        loop(BLK // ROWS, rows_step)
        place('d', dx_out, b)

    me = 2 * d + r
    peers = [dict(row=rp)] + [dict(depth=q, row=h) for q in (dn, df, do) for h in range(2)]
    near_in = sumr_v.at[8, :, pl.ds(0, 2 * HB)]

    def sums_1():
        cw = jnp.sum(cs_v[...], axis=1)
        for i in range(2):
            for q in range(2):
                @pl.when(c_odd == q)
                def _():
                    sum_v[0, :, i * HB:(i + 1) * HB] = cw[i:i + 1, q * HB:(q + 1) * HB]
                    sum_v[1, :, i * HB:(i + 1) * HB] = cw[i:i + 1, (1 - q) * HB:(2 - q) * HB]
        put(sum_v.at[1, :, pl.ds(0, 2 * HB)], near_in, S('s_sum', 0), S('r_sum', 0), col=cn)
        sum_v[0, :, 2 * HB:2 * HB + FB] = jnp.zeros((1, FB), F32)
        sum_v[0, :, dsm(2 * HB + r * FH, FH, HB)] = jnp.sum(db_v[0], axis=0, keepdims=True)
        sum_v[0, :, 2 * HB + FB:] = jnp.sum(bd_v[...], axis=0, keepdims=True)

    def sums_2():
        wait(near_in, S('r_sum', 0))
        sumr_v[me, :, :2 * HB] = sum_v[0, :, :2 * HB] + sumr_v[8, :, :2 * HB]
        sumr_v[me, :, 2 * HB:] = sum_v[0, :, 2 * HB:]
        for i, dev in enumerate(peers):
            put(sumr_v.at[me], sumr_v.at[me], S('s_sum', 1 + i), S('r_sum', 1), **dev)

    def sums_3():
        wait(sumr_v.at[pl.ds(0, 7)], S('r_sum', 1))
        total = sumr_v[0]
        for i in range(1, 8):
            total = total + sumr_v[i]
        sum_v[0] = total
        copy(sum_v.at[0], sum_out, S('l_small', 0))

    scope = jax.named_scope

    def g_ready(k):
        wait(DY.at[rp, ds(k * BLK, BLK), pl.ds(0, 2 * HB)], S('gd2d', k))

    def g_own(k):
        wait(reg(DY, k, c), S('gd2w', k))

    wu_relay()
    with scope('g0'):
        g_near_far(0)
    with scope('g_own'):
        loop(NCH, g_own)
    with scope('dwd_0'):
        dwd_pass((0,))
        dwd_opp(0)
    with scope('g1'):
        g_near_far(1)
    with scope('wuo'):
        wait(wuq(do, 0), S('r_wuy', 2))
        wait(wuq(do, 1), S('r_wuy', 3))
    with scope('u_near'):
        u_near()
    with scope('g2'):
        g_near_far(2)
    with scope('wd_wait'):
        wait(wd_v.at[pl.ds(0, 2 * FH), pl.ds(0, HB)], S('r_wd', 0))
        for g in range(2):
            for i in range(2, 4):
                wait(wd_bytes(g, QH), S('r_wdy', 4 * g + i))
    with scope('y_give'):
        give('y', A, tile_y, YGOT)
    with scope('dwd_a0'):
        dwd_a(0)
    with scope('g3'):
        g_near_far(3)
    with scope('y_keep'):
        keep('y', A, tile_y, YGOT, YFAR, YKEEP)
    with scope('g_ready'):
        loop(NCH, g_ready)
    with scope('dwd_12'):
        dwd_pass((1, 2))
        dwd_opp(1)
        dwd_opp(2)
    with scope('dwd_b0'):
        dwd_b(0)
    with scope('g_opp'):
        loop(NCH, g_opp)
    with scope('dwd_3'):
        dwd_pass((3,))
        dwd_opp(3)
    with scope('dwd_a12'):
        dwd_a(1)
        dwd_a(2)
    with scope('da'):
        da_all()
    with scope('d_give'):
        give('d', DU, tile_g, GGOT)
    with scope('dwd_b3'):
        dwd_b(3)
    with scope('gwd_send'):
        gwd_send()
    with scope('keep_end_y'):
        keep_end('y')
    with scope('d_keep'):
        keep('d', DU, tile_g, GGOT, GFAR, GKEEP)
    with scope('dwu_01'):
        dwu_pass((do, df))
        dwu_opp()
    with scope('dwu_23'):
        dwu_pass((dn, d))
    with scope('dwu_a'):
        dwu_a()
    with scope('gwd_relay'):
        gwd_relay()
    for b in range(2):
        with scope('y_final'):
            y_final(b)
    with scope('keep_end_d'):
        keep_end('d')
    for b in range(2):
        with scope('place_end_y'):
            place_end('y', b)
        with scope('dx_a'):
            dx_a(b)
        if b:
            with scope('sums_1'):
                sums_1()
        with scope('stats'):
            stats_send(b)
            stats_recv(b)
        if b:
            with scope('sums_2'):
                sums_2()
        with scope('dx_b'):
            dx_b(b)
        if b == 0:
            with scope('dwu_b'):
                dwu_b()
    with scope('sums_3'):
        sums_3()
    with scope('gwu_relay'):
        gwu_relay()

    with scope('gwu_end'):
        gwu_end()
    with scope('gwd_end'):
        wait(gwd_out.at[pl.ds(0, 4 * QH), :], S('d_o', 0))
    wait(gwd_out.at[pl.ds(0, 4 * QH), :], S('d_o', 1))
    for p, out in (('y', y_out), ('d', dx_out)):
        @pl.when(r == tau)
        def _():
            with scope('out_end'):
                wait(out.at[pl.ds(0, TH), :], S(p + 'out'))

        @pl.when(r != tau)
        def _():
            with scope('out_end'):
                wait(out, S(p + 'out'))
    wait(sum_out, S('l_small', 0))
    for b in range(2):
        place_end('d', b)
    for b in range(2):
        wait(sx_v.at[b], S('s_st', b))
    wait(sum_v.at[1, :, pl.ds(0, 2 * HB)], S('s_sum', 0))
    for i in range(7):
        wait(sumr_v.at[0], S('s_sum', 1 + i))
    wait(wun, S('s_wun'))

    @pl.when(r == f)
    def _():
        for s in range(2):
            wait(wd_own(s), S('s_wd0', s))
    for i in range(4):
        wait(wd_dst(0, c), S('s_wdx', i))
    wait(wu_own, S('s_wu'))
    for i in range(3):
        wait(vec_at, S('s_vec', i))
    wait(bu_at, S('s_vec', 3))
    for s in range(2):
        wait(wd_dst(s, cf), S('s_wdr', s))
    for i in range(2):
        wait(wuq(d), S('s_wuy', i))
        wait(wuq(d, 0), S('s_wuy', 2 + i))
    for i in range(12):
        wait(wdq(0, d, c), S('s_wdy', i))
        wait(wdq(0, d, c, 0), S('s_wdy', 12 + i))

    def sends(k):
        for z, Z in (('x', X), ('g', DY)):
            for n in ('s_near', 's_far', 's_rel'):
                wait(reg(Z, k, c), S(z + n, k))
            wait(Z.at[r, ds(k * BLK, BLK), :], S(z + 's_d2d', k))
    loop(NCH, sends)
    for i in range(8):
        wait(r1D.at[0], S('d_so', i))
        wait(gwd(0, d), S('d_sy', i))
        wait(gwd(0, d, 0), S('d_sr', i))
    for j in range(1, 4):
        wait(finD.at[j], S('d_sf', j))

    @pl.when(r != f)
    def _():
        wait(finD.at[0], S('d_sf', 0))
    for i in range(2):
        wait(r1U, S('u_so', i))
        wait(PFU, S('u_sa', i))
        wait(finU, S('u_sf', i))

    @pl.when(r != dh)
    def _():
        wait(finU, S('u_sf', 2))
    wait(gwu(0, DH), S('u_sr'))


def block_kernel(x, dy, wu, wd, vec, bu):
    (TK, HB), FH = x.shape, wu.shape[1] // 2
    W, HW, TH, BLK, QF, FB = 4 * HB, 2 * HB, TK // 2, TK // NCH, FH // 4, 2 * FH
    assert FB <= W and FH <= HW and W // 4 <= BLK and QF <= BLK
    sd = jax.ShapeDtypeStruct
    NS = BLK // min(BLK, 128)
    outs = [sd((TK, HB), BF16), sd((TK, HB), BF16), sd((W // 2, FB), BF16), sd((4 * FH, HB), BF16), sd((1, 3 * HB + FB), F32)]
    n_out = len(outs)
    outs += [sd((2, TK, W), BF16)] * 3 + [sd((2, TK, FB), BF16)] * 3
    outs += [sd((TH, W), F32), sd((TH, HW), F32), sd((TH, HW), F32)] * 2
    outs += [sd((4, QF, HB), F32)] * 2 + [sd((W // 4, FH), F32)] * 2
    V = pltpu.VMEM
    scratch = [
        V((W, FB), BF16), V((FB, W), BF16), V((4, FH, HB), F32), V((4, W // 4, FH), F32),
        V((4, FH // 8, HB), F32), V((4, FH // 8, HB), F32), V((W // 8, FH), F32), V((W // 8, FH), F32),
        V((8, W), F32), V((8, FB), F32), V((2, BLK, W), BF16), V((2, BLK, W), BF16), V((4, BLK, HW), F32), V((2, BLK, HW), BF16),
        V((4, QF, HB), BF16), V((2, 8, FH), F32), V((2, 8, HW), F32),
        V((BLK, 128), F32), V((BLK, 128), F32), V((2, BLK, 128), F32), V((2, 2 * NS, 128), F32), V((2, 2 * NS, 128), F32),
        V((8, HB), F32), V((2, 1, 3 * HB + FB), F32), V((9, 1, 3 * HB + FB), F32),
        pltpu.SemaphoreType.DMA((N_SEM,)),
    ]
    res = pl.pallas_call(
        functools.partial(body, (TK, HB, FH)),
        out_shape=outs,
        in_specs=[pl.BlockSpec(memory_space=pl.ANY)] * 6,
        out_specs=[pl.BlockSpec(memory_space=pl.ANY)] * len(outs),
        scratch_shapes=scratch,
        compiler_params=pltpu.CompilerParams(collective_id=0, has_side_effects=True, vmem_limit_bytes=67043328),
        name='mlp_block',
    )(x, dy, wu, wd, vec, bu)
    return res[:n_out]


def solution(mesh):
    assert (mesh.shape['col'], mesh.shape['row'], mesh.shape['depth']) == (4, 2, 4)
    tok_spec = P(('dp', 'depth', 'row'), 'col')
    vec_spec = P('col')
    mat_spec = P('row', 'col')
    grad_vec = P(('dp', 'col'))
    grad_mat = P(('dp', 'row'), 'col')
    def local_pass(x_blk, gamma_blk, beta_blk, w_up_blk, b_up_blk, w_down_blk, b_down_blk, dy_blk):
        hb, fb = x_blk.shape[1], w_up_blk.shape[1]
        vec = jnp.stack([gamma_blk, beta_blk, b_down_blk.astype(F32)] + [jnp.zeros_like(gamma_blk)] * 5)
        bu = jnp.broadcast_to(b_up_blk.astype(F32)[None], (8, fb))
        y_blk, dx_blk, grad_w_up, grad_w_down, sums = block_kernel(x_blk, dy_blk, w_up_blk, w_down_blk, vec, bu)
        sums = sums[0]
        return (y_blk, dx_blk, sums[:hb], sums[hb:2 * hb], grad_w_up, sums[2 * hb:2 * hb + fb], grad_w_down, sums[2 * hb + fb:])

    return jax.shard_map(
        local_pass,
        mesh=mesh,
        in_specs=(tok_spec, vec_spec, vec_spec, mat_spec, vec_spec, mat_spec, vec_spec, tok_spec),
        out_specs=(tok_spec, tok_spec, grad_vec, grad_vec, grad_mat, grad_vec, grad_mat, grad_vec),
        check_vma=False,
    )
```

```python
import functools

import jax
import jax.numpy as jnp
from jax import lax
from jax.experimental import pallas as pl
from jax.experimental.pallas import tpu as pltpu
from jax.sharding import PartitionSpec as P

LN_EPS = 1e-5
F32 = jnp.float32
BF16 = jnp.bfloat16
MESH = pl.DeviceIdType.MESH
GELU_A = 0.7978845608028654
GELU_B = 0.044715
NCH = 4
ROWS = 16
LROWS = 64

NN = (((1,), (0,)), ((), ()))
NT = (((1,), (1,)), ((), ()))
TN = (((0,), (0,)), ((), ()))

SEMS = {}
for _z in ('x', 'g'):
    for _n in ('near', 'far', 'opp', 'd2d', 'd2w', 'd2o', 's_near', 's_far', 's_rel', 's_d2d'):
        SEMS[_z + _n] = NCH
    SEMS[_z + 'bounce'] = 2
for _p in ('y', 'd'):
    SEMS.update({_p + 's_give': 2, _p + 'got': 2, _p + 's_far': 2, _p + 'keep': 2, _p + 'far': 2, _p + 's_out': 4, _p + 'out': 1, _p + 'loc': 2})
SEMS.update(l_wu=1, s_wu=1, r_wu=1, s_wun=1, r_wun=1, s_wuy=4, r_wuy=4,
            s_wd0=2, s_wdx=4, r_wd=4, s_wdr=2, s_wdy=24, r_wdy=8,
            l_vec=2, s_vec=4, r_vec=2,
            ld=8, ldb=2, st=6, s_st=2, r_st=2, s_sum=8, r_sum=2,
            d_so=8, d_r=8, d_sa=8, d_p=8, d_sf=4, d_out=1, d_sy=8, d_y=2, d_sr=8, d_o=2,
            u_so=2, u_r=2, u_sa=2, u_p=2, u_sf=3, u_out=3, u_sr=1, u_o=2, l_small=2)
BASE = {}
_at = 0
for _n, _c in SEMS.items():
    BASE[_n] = _at
    _at += _c
N_SEM = _at


def gelu_and_slope(v):
    v2 = v * v
    t = jnp.tanh(v * (GELU_A + (GELU_A * GELU_B) * v2))
    q = (1.0 - t) * (GELU_A + (3.0 * GELU_A * GELU_B) * v2)
    return 0.5 * v * (1.0 + t), 0.5 * ((1.0 + t) * (1.0 + v * q))


def body(dims, x_ref, dy_ref, wu_ref, wd_ref, vec_ref, bu_ref,
         y_out, dx_out, gwu_out, gwd_out, sum_out,
         X, DY, XN, A, DU, SL, YGOT, YFAR, YKEEP, GGOT, GFAR, GKEEP, PFD, PND, PFU, PNU,
         wu_v, wd_v, accD, accU, r1D, r2D, r1U, r2U, vec_v, bu_v, wx, F4, ob, finD,
         db_v, cs_v, st_v, ms_v, st2_v, sx_v, sr_v, bd_v, sum_v, sumr_v, sem):
    TK, HB, FH = dims
    W, HW, TH, BLK, QF = 4 * HB, 2 * HB, TK // 2, TK // NCH, FH // 4
    RH, DQ, QH, DH, FB = W // 2, W // 4, FH // 8, W // 8, 2 * FH
    NTW = HB
    inv_w = 1.0 / W
    finU = wx.at[3, pl.ds(0, DQ), pl.ds(HW, FH)]
    f0, f1 = F4.at[0], F4.at[1]

    c, r, d = lax.axis_index('col'), lax.axis_index('row'), lax.axis_index('depth')
    c_odd, d_odd = lax.rem(c, 2), lax.rem(d, 2)
    cn, cf, co = c + 1 - 2 * c_odd, 3 - c, lax.rem(c + 2, 4)
    dn, df, do = d + 1 - 2 * d_odd, 3 - d, lax.rem(d + 2, 4)
    f, dh = lax.div(c, 2), lax.div(d, 2)
    tau = lax.rem(lax.div(c + 1, 2), 2)
    rp = 1 - r
    o, o2 = c_odd * FH, (1 - c_odd) * FH

    def S(name, i=0):
        return sem.at[BASE[name] + i]

    def ds(start, size):
        return pl.ds(pl.multiple_of(start, size), size)

    def dsm(start, size, mult):
        return pl.ds(pl.multiple_of(start, mult), size)

    def put(src, dst, ssem, rsem, **dev):
        pltpu.make_async_remote_copy(src_ref=src, dst_ref=dst, send_sem=ssem, recv_sem=rsem,
                                     device_id=dev, device_id_type=MESH).start()

    def copy(src, dst, s):
        pltpu.make_async_copy(src, dst, s).start()

    def wait(ref, s):
        pltpu.make_async_copy(ref, ref, s).wait()

    def loop(n, fn):
        def step(i, carry):
            fn(i)
            return carry
        lax.fori_loop(0, n, step, 0)

    bar = pltpu.get_barrier_semaphore()
    for dev in [dict(row=rp)] + [dict(row=h, **q) for h in range(2) for q in
                                 (dict(col=cn), dict(col=cf), dict(col=co), dict(depth=dn), dict(depth=df), dict(depth=do))]:
        pl.semaphore_signal(bar, inc=1, device_id=dev, device_id_type=MESH)
    pl.semaphore_wait(bar, 13)

    def wd_src(s, h):
        return wd_ref.at[dsm((2 * s + h) * FH + d * QF, QF, QF), :]

    def wd_dst(s, col):
        return wd_v.at[dsm(s * FH + d * QF, QF, QF), ds(col * HB, HB)]

    def reg(Z, k, col):
        return Z.at[r, ds(k * BLK, BLK), ds(col * HB, HB)]

    def send_own(z, z_ref, Z, which, chunks=(0, NCH)):
        def step(k):
            src = z_ref.at[ds(k * BLK, BLK), :]
            if 'near' in which:
                put(src, reg(Z, k, c), S(z + 's_near', k), S(z + 'near', k), col=cn)
            if 'far' in which:
                put(src, reg(Z, k, c), S(z + 's_far', k), S(z + 'far', k), col=cf)
            if 'd2d' in which:
                put(src, reg(Z, k, c), S(z + 's_d2d', k), S(z + ('d2d' if z == 'x' else 'd2w'), k), row=rp)
        for k in range(*chunks):
            step(k)

    def d2d(z, Z, k, col, s):
        put(reg(Z, k, col), reg(Z, k, col), S(z + 's_d2d', k), S(z + s, k), row=rp)

    vec_at = vec_v.at[:, ds(c * HB, HB)]
    copy(vec_ref, vec_at, S('l_vec', 0))
    put(vec_ref, vec_at, S('s_vec', 0), S('r_vec', 0), col=cn)
    put(vec_ref, vec_at, S('s_vec', 1), S('r_vec', 0), col=cf)
    put(vec_ref, vec_at, S('s_vec', 2), S('r_vec', 0), col=co)
    bu_src, bu_at = bu_ref.at[:, ds(r * FH, FH)], bu_v.at[:, ds(o, FH)]
    copy(bu_src, bu_at, S('l_vec', 1))
    put(bu_src, bu_at, S('s_vec', 3), S('r_vec', 1), col=cn)

    wu_own = wu_v.at[ds(r * RH, RH), ds(o, FH)]
    wd_own = lambda s: wd_v.at[pl.ds(s * FH, FH), ds(c * HB, HB)]

    @pl.when(r != f)
    def _():
        for s in range(2):
            for h in range(2):
                put(wd_src(s, h), wd_dst(s, c), S('s_wdx', 2 * s + h), S('r_wd', 2), col=cf, row=h)

    @pl.when(r == f)
    def _():
        for s in range(2):
            for h in range(2):
                put(wd_src(s, h), wd_dst(s, c), S('s_wdx', 2 * s + h), S('r_wd', 1), col=cn, row=h)
    send_own('x', x_ref, X, ('far',), (0, 2))
    send_own('x', x_ref, X, ('near',), (0, 1))
    put(wu_ref.at[:, ds(rp * FH, FH)], wu_own, S('s_wu'), S('r_wu'), row=rp)
    copy(wu_ref.at[:, ds(r * FH, FH)], wu_own, S('l_wu'))
    send_own('x', x_ref, X, ('d2d',))
    send_own('g', dy_ref, DY, ('d2d',))
    for i, z_ref in enumerate((x_ref, dy_ref)):
        for k in range(NCH):
            copy(z_ref.at[pl.ds(k * BLK, BLK), :], wx.at[i, :, pl.ds(k * HB, HB)], S('xg'[i] + 'bounce', 0))

    @pl.when(r == f)
    def _():
        for s in range(2):
            copy(wd_ref.at[dsm((2 * s + r) * FH, FH, FH), :], wd_own(s), S('r_wd', 0))
            put(wd_ref.at[dsm((2 * s + rp) * FH, FH, FH), :], wd_own(s), S('s_wd0', s), S('r_wd', 0), row=rp)

    for i, Z in enumerate((X, DY)):
        wait(wx.at[i], S('xg'[i] + 'bounce', 0))
        for k in range(NCH):
            copy(wx.at[i, :, pl.ds(k * HB, HB)], reg(Z, k, c), S('xg'[i] + 'bounce', 1))

    with jax.named_scope('wd_far'):
        wait(wd_v.at[pl.ds(0, 2 * QF), pl.ds(0, HB)], S('r_wd', 2))
    for s in range(2):
        put(wd_dst(s, cf), wd_dst(s, cf), S('s_wdr', s), S('r_wd', 3), col=cn)
    send_own('x', x_ref, X, ('near',), (1, NCH - 1))

    with jax.named_scope('wu_own'):
        wait(wu_own, S('l_wu'))
        wait(wu_v.at[ds(rp * RH, RH), ds(o, FH)], S('r_wu'))
    wun = wu_v.at[ds(d * DQ, DQ), ds(o, FH)]
    put(wun, wun, S('s_wun'), S('r_wun'), col=cn)
    send_own('x', x_ref, X, ('near',), (NCH - 1, NCH))

    db_v[...] = jnp.zeros_like(db_v)
    cs_v[...] = jnp.zeros_like(cs_v)
    bd_v[...] = jnp.zeros_like(bd_v)

    def dy_sum(i):
        rr = ds(i * ROWS, ROWS)
        part = jnp.sum(wx[1, rr, :].astype(F32).reshape(ROWS // 8, 8, W), axis=0)
        bd_v[...] += part[:, :HB] + part[:, HB:2 * HB] + part[:, 2 * HB:3 * HB] + part[:, 3 * HB:]
    with jax.named_scope('dy_sum'):
        loop(BLK // ROWS, dy_sum)

    def wuq(dd, half=None):
        if half is None:
            return wu_v.at[ds(dd * DQ, DQ), ds(o2, FH)]
        return wu_v.at[dsm(dd * DQ + half * DH, DH, DH), ds(o2, FH)]

    def wu_send():
        with jax.named_scope('wu_near'):
            wait(wuq(d), S('r_wun'))
        put(wuq(d), wuq(d), S('s_wuy', 0), S('r_wuy', 0), depth=dn)
        put(wuq(d), wuq(d), S('s_wuy', 1), S('r_wuy', 1), depth=df)

    def wu_relay():
        with jax.named_scope('wuy'):
            wait(wuq(dn), S('r_wuy', 0))
            wait(wuq(df), S('r_wuy', 1))
        put(wuq(dn, 1), wuq(dn, 1), S('s_wuy', 2), S('r_wuy', 3), depth=df)
        put(wuq(df, 0), wuq(df, 0), S('s_wuy', 3), S('r_wuy', 2), depth=dn)

    def wdq(s, dd, col, half=None):
        if half is None:
            return wd_v.at[dsm(s * FH + dd * QF, QF, QF), ds(col * HB, HB)]
        return wd_v.at[dsm(s * FH + dd * QF + half * QH, QH, QH), ds(col * HB, HB)]

    W_GROUPS = (((0, cn), (1, cf)), ((2, co),))

    def wd_send(g):
        if g == 0:
            wait(wd_v.at[pl.ds(0, 2 * QF), pl.ds(0, HB)], S('r_wd', 1))
        else:
            wait(wd_v.at[pl.ds(0, 2 * QF), pl.ds(0, HB)], S('r_wd', 3))
        for i, col in W_GROUPS[g]:
            for s in range(2):
                put(wdq(s, d, col), wdq(s, d, col), S('s_wdy', 4 * i + s), S('r_wdy', 4 * g), depth=dn)
                put(wdq(s, d, col), wdq(s, d, col), S('s_wdy', 4 * i + 2 + s), S('r_wdy', 4 * g + 1), depth=df)

    def wd_bytes(g, rows):
        return wd_v.at[pl.ds(0, 2 * rows), pl.ds(0, len(W_GROUPS[g]) * HB)]

    def wd_relay(g):
        for i in range(2):
            wait(wd_bytes(g, QF), S('r_wdy', 4 * g + i))
        for i, col in W_GROUPS[g]:
            for s in range(2):
                put(wdq(s, dn, col, 1), wdq(s, dn, col, 1), S('s_wdy', 12 + 4 * i + s), S('r_wdy', 4 * g + 3), depth=df)
                put(wdq(s, df, col, 0), wdq(s, df, col, 0), S('s_wdy', 12 + 4 * i + 2 + s), S('r_wdy', 4 * g + 2), depth=dn)

    def x_near(k):
        wait(reg(X, k, cn), S('xnear', k))
        put(reg(X, k, cn), reg(X, k, cn), S('xs_rel', k), S('xopp', k), col=cf)
        d2d('x', X, k, cn, 'd2d')

    with jax.named_scope('wd_send0'):
        wd_send(0)
    with jax.named_scope('x_near'):
        x_near(0)
    send_own('x', x_ref, X, ('far',), (2, 3))

    for i, Z in enumerate((X, DY)):
        wait(wx.at[i], S('xg'[i] + 'bounce', 1))
    wait(vec_at, S('l_vec', 0))
    wait(vec_v.at[:, pl.ds(0, 3 * HB)], S('r_vec', 0))
    wait(bu_at, S('l_vec', 1))
    wait(bu_at, S('r_vec', 1))

    def norm_rows(buf, rows):
        xf = buf[rows, :].astype(F32)
        mean = jnp.sum(xf, axis=1, keepdims=True) * inv_w
        cen = xf - mean
        inv = lax.rsqrt(jnp.sum(cen * cen, axis=1, keepdims=True) * inv_w + LN_EPS)
        return cen, mean, inv

    def tok_of(s):
        return tau + s * (1 - 2 * tau)

    N_T = FH // NTW

    def chain(tiles, hooks=None):
        hooks = hooks or {}

        def hook(what, i):
            for fn in hooks.get((what, i), ()):
                fn()
        for i, (product, _) in enumerate(tiles):
            hook('before', i)
            if i:
                tiles[i - 1][1](F4.at[(i - 1) % 2])
            F4[i % 2, :, :NTW] = product()
            hook('product', i)
            if i:
                hook('epilogue', i - 1)
        tiles[-1][1](F4.at[(len(tiles) - 1) % 2])
        hook('epilogue', len(tiles) - 1)

    def u_tile(src, i, n, start):
        cols = ds(start + n * NTW, NTW)
        at = pl.ds(n * NTW, NTW)

        def product():
            return lax.dot_general(wx[src], wu_v[:, cols], NN, preferred_element_type=F32)

        def epilogue(acc):
            u = (acc[:, :NTW] + bu_v[0:1, cols]).astype(BF16)
            a, slope = gelu_and_slope(u.astype(F32))
            ob[i, :, at] = a.astype(BF16)
            F4[2 + i, :, at] = slope
        return product, epilogue

    def u_store(i, s, rows, start):
        copy(ob.at[i], A.at[s, rows, ds(start, FH)], S('st', 2 + i))
        copy(F4.at[2 + i], SL.at[s, rows, ds(start, FH)], S('st', 4 + i))

    def u_stored():
        for i in range(2):
            wait(ob.at[i], S('st', 2 + i))
            wait(F4.at[2 + i], S('st', 4 + i))

    def phase1(k):
        @pl.when(k < NCH - 1)
        def _():
            with jax.named_scope('x_near'):
                x_near(k + 1)

        @pl.when(k == 0)
        def _():
            send_own('x', x_ref, X, ('far',), (3, 4))
            with jax.named_scope('wd_send1'):
                wd_send(1)

        @pl.when(k == 1)
        def _():
            with jax.named_scope('wd_relay0'):
                wd_relay(0)
            send_own('g', dy_ref, DY, ('near',))

        @pl.when(k == 2)
        def _():
            send_own('g', dy_ref, DY, ('far',))
            with jax.named_scope('wd_relay1'):
                wd_relay(1)
            wu_send()

        with jax.named_scope('x_far'):
            wait(reg(X, k, cf), S('xfar', k))
            d2d('x', X, k, cf, 'd2d')
        with jax.named_scope('x_opp'):
            wait(reg(X, k, co), S('xopp', k))
            d2d('x', X, k, co, 'd2d')

        rows = ds(k * BLK, BLK)
        with jax.named_scope('x_d2d'):
            wait(X.at[rp, rows, :], S('xd2d', k))

        @pl.when(k > 0)
        def _():
            for s in range(2):
                wait(wx.at[s], S('st', s))
        for s in range(2):
            copy(X.at[tok_of(s), rows, :], wx.at[s], S('ld', s))
        for s in range(2):
            wait(wx.at[s], S('ld', s))

            def ln(i):
                rr = ds(i * LROWS, LROWS)
                cen, _, inv = norm_rows(wx.at[s], rr)
                wx[s, rr, :] = (cen * inv * vec_v[0:1, :] + vec_v[1:2, :]).astype(BF16)
            with jax.named_scope('ln'):
                loop(BLK // LROWS, ln)
            copy(wx.at[s], XN.at[s, rows, :], S('st', s))
        pl.when(k > 0)(u_stored)
        with jax.named_scope('u_own'):
            chain([u_tile(i, i, n, o) for i in range(2) for n in range(N_T)])
        for s in range(2):
            u_store(s, s, rows, o)
    loop(NCH, phase1)
    for s in range(2):
        wait(wx.at[s], S('st', s))
    u_stored()

    def u_near():
        for b in range(NCH):
            copy(XN.at[0, pl.ds(b * BLK, BLK), :], wx.at[b], S('ld', b))

        def step(kp):
            for i in range(2):
                wait(wx.at[2 * kp + i], S('ld', 2 * kp + i))
            chain([u_tile(2 * kp + i, i, n, o2) for i in range(2) for n in range(N_T)], {('before', 1): [lambda: pl.when(kp > 0)(u_stored)]})
            for i in range(2):
                u_store(i, 0, ds((2 * kp + i) * BLK, BLK), o2)
        loop(NCH // 2, step)
        u_stored()

    def g_near_far(k):
        wait(reg(DY, k, cf), S('gfar', k))
        put(reg(DY, k, cf), reg(DY, k, cf), S('gs_rel', k), S('gopp', k), col=cn)
        d2d('g', DY, k, cf, 'd2d')
        wait(reg(DY, k, cn), S('gnear', k))
        d2d('g', DY, k, cn, 'd2d')

    def g_opp(k):
        wait(reg(DY, k, co), S('gopp', k))
        d2d('g', DY, k, co, 'd2o')

    def g_opp_got(k):
        wait(reg(DY, k, co), S('gd2o', k))

    def tile_y(lhs, col):
        return lax.dot_general(lhs, wd_v[:, dsm(col, NTW, NTW)], NN, preferred_element_type=F32)

    def tile_g(lhs, col):
        return lax.dot_general(lhs, wu_v[dsm(col, NTW, NTW), :], NT, preferred_element_type=F32)

    def give(p, src, tile, GOT):
        def blk(b):
            return src.at[0, dsm(rp * TH + b * BLK, BLK, BLK), :]
        for b in range(2):
            copy(blk(b), wx.at[b, :, pl.ds(0, FB)], S('ld', b))
        for b in range(2):
            copy(src.at[0, dsm(r * TH + b * BLK, BLK, BLK), :], wx.at[2 + b, :, pl.ds(0, FB)], S('ld', 2 + b))

        def step(b):
            wait(wx.at[b, :, pl.ds(0, FB)], S('ld', b))

            def half(h):
                @pl.when(b == 1)
                def _():
                    wait(F4.at[h], S(p + 's_give', h))

                def n_tile(n):
                    F4[h, :, ds(n * NTW, NTW)] = tile(wx[b, :, :FB], h * HW + n * NTW)
                loop(HW // NTW, n_tile)
                put(F4.at[h], GOT.at[ds(b * BLK, BLK), ds(h * HW, HW)], S(p + 's_give', h), S(p + 'got', b), row=rp)
            loop(2, half)
        loop(2, step)

    def keep(p, src, tile, GOT, FAR, KEEP):
        def col_of(h):
            return (1 - f + h * (2 * f - 1)) * HW

        def out_of(b, h):
            return (2 + b) * (1 - h) + (1 - b) * h
        for h in range(2):
            wait(F4.at[h], S(p + 's_give', h))

        def fetch(b):
            with jax.named_scope('got'):
                wait(GOT.at[ds(b * BLK, BLK), :], S(p + 'got', b))
            for h in range(2):
                copy(GOT.at[ds(b * BLK, BLK), ds(col_of(h), HW)], F4.at[out_of(b, h)], S('ld', 4 + 2 * b + h))
        fetch(0)

        def step(b):
            brow = ds(b * BLK, BLK)
            wait(wx.at[2 + b, :, pl.ds(0, FB)], S('ld', 2 + b))

            def half(h):
                out = out_of(b, h)
                wait(F4.at[out], S('ld', 4 + 2 * b + h))

                def n_tile(n):
                    at = ds(n * NTW, NTW)
                    F4[out, :, at] = F4[out, :, at] + tile(wx[2 + b, :, :FB], col_of(h) + n * NTW)
                loop(HW // NTW, n_tile)

                @pl.when(h == 0)
                def _():
                    put(F4.at[2 + b], FAR.at[brow, :], S(p + 's_far', b), S(p + 'far', b), col=cf)

                @pl.when(h == 1)
                def _():
                    copy(F4.at[1 - b], KEEP.at[brow, :], S(p + 'keep', b))

                @pl.when(jnp.logical_and(b == 0, h == 0))
                def _():
                    fetch(1)
            loop(2, half)
        loop(2, step)
        for b in range(2):
            wait(F4.at[b], S(p + 'keep', b))

    def keep_end(p):
        for b in range(2):
            wait(F4.at[2 + b], S(p + 's_far', b))

    def place(p, out, b):
        dst = out.at[dsm(r * TH + b * BLK, BLK, BLK), :]
        mine, other = ob.at[b, :, ds(c_odd * HB, HB)], ob.at[b, :, ds((1 - c_odd) * HB, HB)]
        put(other, dst, S(p + 's_out', 2 * b), S(p + 'out'), col=cn, row=tau)

        @pl.when(r == tau)
        def _():
            copy(mine, dst, S(p + 'loc', b))

        @pl.when(r != tau)
        def _():
            put(mine, dst, S(p + 's_out', 2 * b + 1), S(p + 'out'), row=rp)

    def place_end(p, b):
        wait(ob.at[b, :, pl.ds(0, HB)], S(p + 's_out', 2 * b))

        @pl.when(r == tau)
        def _():
            wait(ob.at[b, :, pl.ds(0, HB)], S(p + 'loc', b))

        @pl.when(r != tau)
        def _():
            wait(ob.at[b, :, pl.ds(0, HB)], S(p + 's_out', 2 * b + 1))

    fcols = ds(f * HW, HW)

    def y_final(b):
        brow = ds(b * BLK, BLK)
        wait(YFAR.at[brow, :], S('yfar', b))
        copy(YFAR.at[brow, :], f0, S('ld', 0))
        copy(YKEEP.at[brow, :], f1, S('ld', 1))
        copy(X.at[tau, dsm(r * TH + b * BLK, BLK, BLK), fcols], wx.at[0, :, pl.ds(0, HW)], S('ld', 2))
        wait(f0, S('ld', 0))
        wait(f1, S('ld', 1))
        wait(wx.at[0, :, pl.ds(0, HW)], S('ld', 2))

        def fin(i):
            rr = ds(i * ROWS, ROWS)
            ob[b, rr, :] = (wx[0, rr, :HW].astype(F32) + (f0[rr, :] + f1[rr, :]) + vec_v[2:3, fcols]).astype(BF16)
        loop(BLK // ROWS, fin)
        place('y', y_out, b)

    def services(t):
        @pl.when(t == 3)
        def _():
            with jax.named_scope('dwd_b1'):
                dwd_b(1)

        @pl.when(t == 4)
        def _():
            with jax.named_scope('dwd_a3b2'):
                dwd_a(3)
                dwd_b(2)

    def da_all():
        def part(t, i):
            near = lax.div(t, NCH)
            tok = tau + i * (1 - near) * (1 - 2 * tau)
            chunk = t * (1 - near) + near * (2 * (t - NCH) + i)
            return near, tok, i * (1 - near), ds(chunk * BLK, BLK), near * o2 + (1 - near) * o

        def load(t, p):
            for i in range(2):
                _, tok, us, rows, start = part(t, i)
                copy(DY.at[tok, rows, :], wx.at[2 * p + i], S('ld', 2 * p + i))
                copy(SL.at[us, rows, ds(start, FH)], accU.at[2 * p + i], S('ld', 4 + 2 * p + i))

        def store(t, i):
            _, _, us, rows, start = part(t, i)
            copy(ob.at[i], DU.at[us, rows, ds(start, FH)], S('st', 4 + i))

        def stored():
            for i in range(2):
                wait(ob.at[i], S('st', 4 + i))

        n_steps = NCH + NCH // 2

        def step(t):
            near, _, _, _, start = part(t, 0)
            p = lax.rem(t, 2)
            services(t)
            for i in range(2):
                wait(wx.at[2 * p + i], S('ld', 2 * p + i))
                wait(accU.at[2 * p + i], S('ld', 4 + 2 * p + i))

            @pl.when(t < n_steps - 1)
            def _():
                load(t + 1, 1 - p)

            def tile(i, n):
                cols = ds(start + n * NTW, NTW)
                at = pl.ds(n * NTW, NTW)

                def product():
                    return lax.dot_general(wx[2 * p + i], wd_v[cols, :], NT, preferred_element_type=F32)

                def epilogue(acc):
                    du = (acc[:, :NTW] * accU[2 * p + i, :, at]).astype(BF16)
                    ob[i, :, at] = du
                    db_v[near, :, at] += jnp.sum(du.astype(F32).reshape(BLK // 8, 8, NTW), axis=0)
                return product, epilogue
            chain([tile(i, n) for i in range(2) for n in range(N_T)], {('before', 1): [lambda: pl.when(t > 0)(stored)]})
            for i in range(2):
                store(t, i)
        load(0, 0)
        loop(n_steps, step)
        stored()

    def rows_of(kb):
        return ds(lax.rem(kb, NCH) * BLK, BLK), lax.div(kb, NCH)

    d_col = (c, cn, cf, co)

    NB, NSLOT = 2 * NCH, 4

    def k_loop(load, use, width):
        for kb in range(NSLOT - 1):
            load(kb, wx.at[kb], S('ld', kb))

        def step(kb):
            slot = lax.rem(kb, NSLOT)

            @pl.when(kb + NSLOT - 1 < NB)
            def _():
                nxt = lax.rem(kb + NSLOT - 1, NSLOT)
                load(kb + NSLOT - 1, wx.at[nxt], S('ld', nxt))
            buf = wx.at[slot]
            wait(buf.at[:, pl.ds(0, width)], S('ld', slot))
            use(buf)
        loop(NB, step)

    def dwd_pass(js):
        def load(kb, buf, s_):
            rows, s = rows_of(kb)
            copy(A.at[s, rows, ds(o, FH)], buf.at[:, pl.ds(0, FH)], s_)
            for i, j in enumerate(js):
                copy(DY.at[tok_of(s), rows, ds(d_col[j] * HB, HB)], buf.at[:, pl.ds(FH + i * HB, HB)], s_)

        def use(buf):
            for i, j in enumerate(js):
                for m in range(2):
                    mm = slice(m * FH // 2, (m + 1) * FH // 2)
                    accD[j, mm, :] += lax.dot_general(buf[:, mm], buf[:, FH + i * HB:FH + (i + 1) * HB], TN, preferred_element_type=F32)
        for j in js:
            accD[j] = jnp.zeros((FH, HB), F32)
        k_loop(load, use, FH + len(js) * HB)

    def dwd_opp(j):
        put(accD.at[j, dsm(do * QF, QH, QH), :], r1D.at[j], S('d_so', 2 * j), S('d_r', 2 * j), depth=dn)
        put(accD.at[j, dsm(do * QF + QH, QH, QH), :], r2D.at[j], S('d_so', 2 * j + 1), S('d_r', 2 * j + 1), depth=df)

    def dwd_a(j):
        wait(r1D.at[j], S('d_r', 2 * j))
        rr = dsm(df * QF, QH, QH)
        accD[j, rr, :] += r1D[j]
        put(accD.at[j, ds(df * QF, QF), :], PFD.at[j], S('d_sa', 2 * j), S('d_p', 2 * j), depth=df)
        wait(r2D.at[j], S('d_r', 2 * j + 1))
        rr = dsm(dn * QF + QH, QH, QH)
        accD[j, rr, :] += r2D[j]
        put(accD.at[j, ds(dn * QF, QF), :], PND.at[j], S('d_sa', 2 * j + 1), S('d_p', 2 * j + 1), depth=dn)

    def dwd_rows(q, h, dd):
        return dsm((2 * q + h) * FH + dd * QF, QF, QF)

    def dwd_b(j):
        wait(PFD.at[j], S('d_p', 2 * j))
        wait(PND.at[j], S('d_p', 2 * j + 1))
        wait(PFD.at[j], S('d_sa', 2 * j))
        wait(PND.at[j], S('d_sa', 2 * j + 1))
        pf, pn = accD.at[j, ds(df * QF, QF), :], accD.at[j, ds(dn * QF, QF), :]
        copy(PFD.at[j], pf, S('ldb', 0))
        copy(PND.at[j], pn, S('ldb', 1))
        wait(pf, S('ldb', 0))
        wait(pn, S('ldb', 1))
        finD[j] = (accD[j, ds(d * QF, QF), :] + (pf[...] + pn[...])).astype(BF16)
        dst = gwd_out.at[dwd_rows(c_odd, r, d), :]
        if j:
            put(finD.at[j], dst, S('d_sf', j), S('d_out'), col=d_col[j], row=f)
        else:
            @pl.when(r == f)
            def _():
                copy(finD.at[0], dst, S('d_out'))

            @pl.when(r != f)
            def _():
                put(finD.at[0], dst, S('d_sf', 0), S('d_out'), row=rp)

    def gwd(i, dd, half=None):
        if half is None:
            return gwd_out.at[dsm(i * FH + dd * QF, QF, QF), :]
        return gwd_out.at[dsm(i * FH + dd * QF + half * QH, QH, QH), :]

    def gwd_send():
        wait(gwd_out.at[pl.ds(0, 4 * QF), :], S('d_out'))
        for i in range(4):
            put(gwd(i, d), gwd(i, d), S('d_sy', i), S('d_y', 0), depth=dn)
            put(gwd(i, d), gwd(i, d), S('d_sy', 4 + i), S('d_y', 1), depth=df)

    def gwd_relay():
        wait(gwd_out.at[pl.ds(0, 4 * QF), :], S('d_y', 0))
        for i in range(4):
            put(gwd(i, dn, 1), gwd(i, dn, 1), S('d_sr', i), S('d_o', 1), depth=df)
        wait(gwd_out.at[pl.ds(0, 4 * QF), :], S('d_y', 1))
        for i in range(4):
            put(gwd(i, df, 0), gwd(i, df, 0), S('d_sr', 4 + i), S('d_o', 0), depth=dn)

    def dwu_pass(dds):
        def load(kb, buf, s_):
            rows, s = rows_of(kb)
            copy(DU.at[s, rows, ds(o, FH)], buf.at[:, pl.ds(0, FH)], s_)
            for i, dd in enumerate(dds):
                copy(XN.at[s, rows, ds(dd * DQ, DQ)], buf.at[:, pl.ds(FH + i * DQ, DQ)], s_)

        def use(buf):
            for i, dd in enumerate(dds):
                for m in range(2):
                    mm = slice(m * FH // 2, (m + 1) * FH // 2)
                    accU[dd, :, mm] += lax.dot_general(buf[:, FH + i * DQ:FH + (i + 1) * DQ], buf[:, mm], TN, preferred_element_type=F32)
        for dd in dds:
            accU[dd] = jnp.zeros((DQ, FH), F32)
        k_loop(load, use, FH + len(dds) * DQ)

    def dwu_opp():
        put(accU.at[do, pl.ds(0, DH), :], r1U, S('u_so', 0), S('u_r', 0), depth=dn)
        put(accU.at[do, pl.ds(DH, DH), :], r2U, S('u_so', 1), S('u_r', 1), depth=df)

    def dwu_a():
        wait(r1U, S('u_r', 0))
        accU[df, :DH, :] += r1U[...]
        put(accU.at[df], PFU, S('u_sa', 0), S('u_p', 0), depth=df)
        wait(r2U, S('u_r', 1))
        accU[dn, DH:, :] += r2U[...]
        put(accU.at[dn], PNU, S('u_sa', 1), S('u_p', 1), depth=dn)

    def dwu_b():
        wait(PFU, S('u_p', 0))
        wait(PNU, S('u_p', 1))
        pf, pn = f0.at[pl.ds(0, DQ), pl.ds(0, FH)], f1.at[pl.ds(0, DQ), pl.ds(0, FH)]
        copy(PFU, pf, S('ldb', 0))
        copy(PNU, pn, S('ldb', 1))
        wait(pf, S('ldb', 0))
        wait(pn, S('ldb', 1))

        def fin(i):
            rr = ds(i * ROWS, ROWS)
            wx[3, rr, HW:HW + FH] = (accU[d, rr, :] + (f0[rr, :FH] + f1[rr, :FH])).astype(BF16)
        loop(DQ // ROWS, fin)
        dst = gwu_out.at[ds(d_odd * DQ, DQ), ds(r * FH, FH)]
        put(finU, dst, S('u_sf', 0), S('u_out', 1), depth=dn, row=dh)
        put(finU, dst, S('u_sf', 1), S('u_out', 2), depth=df, row=dh)

        @pl.when(r == dh)
        def _():
            copy(finU, dst, S('u_out', 0))

        @pl.when(r != dh)
        def _():
            put(finU, dst, S('u_sf', 2), S('u_out', 0), row=rp)

    def gwu(start, size):
        return gwu_out.at[dsm(start, size, size), :]

    def gwu_relay():
        @pl.when(r == dh)
        def _():
            wait(gwu(lax.rem(dn, 2) * DQ, DQ), S('u_out', 1))
            part = gwu(lax.rem(dn, 2) * DQ + DH, DH)
            put(part, part, S('u_sr'), S('u_o', 1), depth=df)

        @pl.when(r != dh)
        def _():
            wait(gwu(lax.rem(df, 2) * DQ, DQ), S('u_out', 2))
            part = gwu(lax.rem(df, 2) * DQ, DH)
            put(part, part, S('u_sr'), S('u_o', 0), depth=dn)

    def gwu_end():
        @pl.when(r == dh)
        def _():
            wait(gwu(d_odd * DQ, DQ), S('u_out', 0))

        @pl.when(r != dh)
        def _():
            wait(gwu(0, DH), S('u_o', 0))
            wait(gwu(0, DH), S('u_o', 1))

    lane = lax.broadcasted_iota(jnp.int32, (LROWS, 128), 1)

    def dx_a(b):
        brow = ds(b * BLK, BLK)
        trow = dsm(r * TH + b * BLK, BLK, BLK)
        copy(GFAR.at[brow, :], f0, S('ld', 0))
        copy(GKEEP.at[brow, :], f1, S('ld', 1))
        copy(X.at[tau, trow, :], wx.at[b], S('ld', 2))
        copy(DY.at[tau, trow, fcols], wx.at[2 + b, :, pl.ds(0, HW)], S('ld', 3))
        wait(f0, S('ld', 0))
        wait(f1, S('ld', 1))
        wait(wx.at[b], S('ld', 2))
        wait(wx.at[2 + b, :, pl.ds(0, HW)], S('ld', 3))

        def rows_step(i):
            rr = ds(i * LROWS, LROWS)
            _, mean, inv = norm_rows(wx.at[b], rr)
            xhat = (wx[b, rr, fcols].astype(F32) - mean) * inv
            dxn = f0[rr, :] + f1[rr, :]
            F4[2 + b, rr, :] = dxn
            gh = dxn * vec_v[0:1, fcols]
            s0 = jnp.sum(gh, axis=1, keepdims=True)
            s1 = jnp.sum(gh * xhat, axis=1, keepdims=True)
            srow = rr
            st_v[srow, :] = jnp.where(lane < 64, s0, s1)
            ms_v[srow, :] = jnp.where(lane < 64, mean, inv)
            p1 = dxn * xhat
            cs_v[0] += jnp.sum(p1.reshape(LROWS // 8, 8, HW), axis=0)
            cs_v[1] += jnp.sum(dxn.reshape(LROWS // 8, 8, HW), axis=0)
        loop(BLK // LROWS, rows_step)

    SB = min(BLK, 128)
    NS = BLK // SB

    def stats_send(b):
        for t in range(NS):
            tr = st_v[t * SB:(t + 1) * SB, :].T
            sx_v[b, t:t + 1, :SB] = tr[0:1, :]
            sx_v[b, NS + t:NS + t + 1, :SB] = tr[64:65, :]
        put(sx_v.at[b], sr_v.at[b], S('s_st', b), S('r_st', b), col=cf)

    def stats_recv(b):
        wait(sr_v.at[b], S('r_st', b))
        for t in range(NS):
            for i in range(2):
                row = (sx_v[b, i * NS + t:i * NS + t + 1, :SB] + sr_v[b, i * NS + t:i * NS + t + 1, :SB]) * inv_w
                st2_v[i, t * SB:(t + 1) * SB, :] = jnp.broadcast_to(row, (128, SB)).T

    def dx_b(b):
        def rows_step(i):
            rr = ds(i * ROWS, ROWS)
            srow = rr
            mean, inv = ms_v[srow, 0:1], ms_v[srow, 64:65]
            xhat = (wx[b, rr, fcols].astype(F32) - mean) * inv
            gh = F4[2 + b, rr, :] * vec_v[0:1, fcols]
            dx = wx[2 + b, rr, :HW].astype(F32) + inv * (gh - st2_v[0, srow, 0:1] - xhat * st2_v[1, srow, 0:1])
            ob[b, rr, :] = dx.astype(BF16)
        loop(BLK // ROWS, rows_step)
        place('d', dx_out, b)

    me = 2 * d + r
    peers = [dict(row=rp)] + [dict(depth=q, row=h) for q in (dn, df, do) for h in range(2)]
    near_in = sumr_v.at[8, :, pl.ds(0, 2 * HB)]

    def sums_1():
        cw = jnp.sum(cs_v[...], axis=1)
        for i in range(2):
            for q in range(2):
                @pl.when(c_odd == q)
                def _():
                    sum_v[0, :, i * HB:(i + 1) * HB] = cw[i:i + 1, q * HB:(q + 1) * HB]
                    sum_v[1, :, i * HB:(i + 1) * HB] = cw[i:i + 1, (1 - q) * HB:(2 - q) * HB]
        put(sum_v.at[1, :, pl.ds(0, 2 * HB)], near_in, S('s_sum', 0), S('r_sum', 0), col=cn)
        sum_v[0, :, 2 * HB:2 * HB + FB] = jnp.zeros((1, FB), F32)
        sum_v[0, :, dsm(2 * HB + r * FH, FH, HB)] = jnp.sum(db_v[0], axis=0, keepdims=True)
        sum_v[0, :, 2 * HB + FB:] = jnp.sum(bd_v[...], axis=0, keepdims=True)

    def sums_2():
        wait(near_in, S('r_sum', 0))
        sumr_v[me, :, :2 * HB] = sum_v[0, :, :2 * HB] + sumr_v[8, :, :2 * HB]
        sumr_v[me, :, 2 * HB:] = sum_v[0, :, 2 * HB:]
        for i, dev in enumerate(peers):
            put(sumr_v.at[me], sumr_v.at[me], S('s_sum', 1 + i), S('r_sum', 1), **dev)

    def sums_3():
        wait(sumr_v.at[pl.ds(0, 7)], S('r_sum', 1))
        total = sumr_v[0]
        for i in range(1, 8):
            total = total + sumr_v[i]
        sum_v[0] = total
        copy(sum_v.at[0], sum_out, S('l_small', 0))

    scope = jax.named_scope

    def g_ready(k):
        wait(DY.at[rp, ds(k * BLK, BLK), pl.ds(0, 2 * HB)], S('gd2d', k))

    def g_own(k):
        wait(reg(DY, k, c), S('gd2w', k))

    wu_relay()
    with scope('g0'):
        g_near_far(0)
    with scope('g_own'):
        loop(NCH, g_own)
    with scope('dwd_0'):
        dwd_pass((0,))
        dwd_opp(0)
    with scope('g1'):
        g_near_far(1)
    with scope('wuo'):
        wait(wuq(do, 0), S('r_wuy', 2))
        wait(wuq(do, 1), S('r_wuy', 3))
    with scope('u_near'):
        u_near()
    with scope('g2'):
        g_near_far(2)
    with scope('wd_wait'):
        wait(wd_v.at[pl.ds(0, 2 * FH), pl.ds(0, HB)], S('r_wd', 0))
        for g in range(2):
            for i in range(2, 4):
                wait(wd_bytes(g, QH), S('r_wdy', 4 * g + i))
    with scope('y_give'):
        give('y', A, tile_y, YGOT)
    with scope('dwd_a0'):
        dwd_a(0)
    with scope('g3'):
        g_near_far(3)
    with scope('y_keep'):
        keep('y', A, tile_y, YGOT, YFAR, YKEEP)
    with scope('g_ready'):
        loop(NCH, g_ready)
    with scope('dwd_12'):
        dwd_pass((1, 2))
        dwd_opp(1)
        dwd_opp(2)
    with scope('dwd_b0'):
        dwd_b(0)
    with scope('g_opp'):
        loop(NCH, g_opp)
        loop(NCH, g_opp_got)
    with scope('dwd_3'):
        dwd_pass((3,))
        dwd_opp(3)
    with scope('dwd_a12'):
        dwd_a(1)
        dwd_a(2)
    with scope('da'):
        da_all()
    with scope('d_give'):
        give('d', DU, tile_g, GGOT)
    with scope('dwd_b3'):
        dwd_b(3)
    with scope('gwd_send'):
        gwd_send()
    with scope('keep_end_y'):
        keep_end('y')
    with scope('d_keep'):
        keep('d', DU, tile_g, GGOT, GFAR, GKEEP)
    with scope('dwu_01'):
        dwu_pass((do, df))
        dwu_opp()
    with scope('dwu_23'):
        dwu_pass((dn, d))
    with scope('dwu_a'):
        dwu_a()
    with scope('gwd_relay'):
        gwd_relay()
    for b in range(2):
        with scope('y_final'):
            y_final(b)
    for b in range(2):
        with scope('place_end_y'):
            place_end('y', b)
        with scope('d_far'):
            wait(F4.at[2 + b], S('ds_far', b))
            wait(GFAR.at[ds(b * BLK, BLK), :], S('dfar', b))
        with scope('dx_a'):
            dx_a(b)
        if b:
            with scope('sums_1'):
                sums_1()
        with scope('stats'):
            stats_send(b)
            stats_recv(b)
        if b:
            with scope('sums_2'):
                sums_2()
        with scope('dx_b'):
            dx_b(b)
        if b == 0:
            with scope('dwu_b'):
                dwu_b()
    with scope('sums_3'):
        sums_3()
    with scope('gwu_relay'):
        gwu_relay()

    with scope('gwu_end'):
        gwu_end()
    with scope('gwd_end'):
        wait(gwd_out.at[pl.ds(0, 4 * QH), :], S('d_o', 0))
    wait(gwd_out.at[pl.ds(0, 4 * QH), :], S('d_o', 1))
    for p, out in (('y', y_out), ('d', dx_out)):
        @pl.when(r == tau)
        def _():
            with scope('out_end'):
                wait(out.at[pl.ds(0, TH), :], S(p + 'out'))

        @pl.when(r != tau)
        def _():
            with scope('out_end'):
                wait(out, S(p + 'out'))
    wait(sum_out, S('l_small', 0))
    for b in range(2):
        place_end('d', b)
    for b in range(2):
        wait(sx_v.at[b], S('s_st', b))
    wait(sum_v.at[1, :, pl.ds(0, 2 * HB)], S('s_sum', 0))
    for i in range(7):
        wait(sumr_v.at[0], S('s_sum', 1 + i))
    wait(wun, S('s_wun'))

    @pl.when(r == f)
    def _():
        for s in range(2):
            wait(wd_own(s), S('s_wd0', s))
    for i in range(4):
        wait(wd_dst(0, c), S('s_wdx', i))
    wait(wu_own, S('s_wu'))
    for i in range(3):
        wait(vec_at, S('s_vec', i))
    wait(bu_at, S('s_vec', 3))
    for s in range(2):
        wait(wd_dst(s, cf), S('s_wdr', s))
    for i in range(2):
        wait(wuq(d), S('s_wuy', i))
        wait(wuq(d, 0), S('s_wuy', 2 + i))
    for i in range(12):
        wait(wdq(0, d, c), S('s_wdy', i))
        wait(wdq(0, d, c, 0), S('s_wdy', 12 + i))

    def sends(k):
        for z, Z in (('x', X), ('g', DY)):
            for n in ('s_near', 's_far', 's_rel'):
                wait(reg(Z, k, c), S(z + n, k))
            wait(Z.at[r, ds(k * BLK, BLK), :], S(z + 's_d2d', k))
    loop(NCH, sends)
    for i in range(8):
        wait(r1D.at[0], S('d_so', i))
        wait(gwd(0, d), S('d_sy', i))
        wait(gwd(0, d, 0), S('d_sr', i))
    for j in range(1, 4):
        wait(finD.at[j], S('d_sf', j))

    @pl.when(r != f)
    def _():
        wait(finD.at[0], S('d_sf', 0))
    for i in range(2):
        wait(r1U, S('u_so', i))
        wait(PFU, S('u_sa', i))
        wait(finU, S('u_sf', i))

    @pl.when(r != dh)
    def _():
        wait(finU, S('u_sf', 2))
    wait(gwu(0, DH), S('u_sr'))


def block_kernel(x, dy, wu, wd, vec, bu):
    (TK, HB), FH = x.shape, wu.shape[1] // 2
    W, HW, TH, BLK, QF, FB = 4 * HB, 2 * HB, TK // 2, TK // NCH, FH // 4, 2 * FH
    assert FB <= W and FH <= HW and W // 4 == BLK and QF <= BLK and FH == HW
    sd = jax.ShapeDtypeStruct
    NS = BLK // min(BLK, 128)
    outs = [sd((TK, HB), BF16), sd((TK, HB), BF16), sd((W // 2, FB), BF16), sd((4 * FH, HB), BF16), sd((1, 3 * HB + FB), F32)]
    n_out = len(outs)
    outs += [sd((2, TK, W), BF16)] * 3 + [sd((2, TK, FB), BF16)] * 2 + [sd((2, TK, FB), F32)]
    outs += [sd((TH, W), F32), sd((TH, HW), F32), sd((TH, HW), F32)] * 2
    outs += [sd((4, QF, HB), F32)] * 2 + [sd((W // 4, FH), F32)] * 2
    V = pltpu.VMEM
    scratch = [
        V((W, FB), BF16), V((FB, W), BF16), V((4, FH, HB), F32), V((4, W // 4, FH), F32),
        V((4, FH // 8, HB), F32), V((4, FH // 8, HB), F32), V((W // 8, FH), F32), V((W // 8, FH), F32),
        V((8, W), F32), V((8, FB), F32), V((4, BLK, W), BF16), V((4, BLK, HW), F32), V((2, BLK, HW), BF16),
        V((4, QF, HB), BF16), V((2, 8, FH), F32), V((2, 8, HW), F32),
        V((BLK, 128), F32), V((BLK, 128), F32), V((2, BLK, 128), F32), V((2, 2 * NS, 128), F32), V((2, 2 * NS, 128), F32),
        V((8, HB), F32), V((2, 1, 3 * HB + FB), F32), V((9, 1, 3 * HB + FB), F32),
        pltpu.SemaphoreType.DMA((N_SEM,)),
    ]
    res = pl.pallas_call(
        functools.partial(body, (TK, HB, FH)),
        out_shape=outs,
        in_specs=[pl.BlockSpec(memory_space=pl.ANY)] * 6,
        out_specs=[pl.BlockSpec(memory_space=pl.ANY)] * len(outs),
        scratch_shapes=scratch,
        compiler_params=pltpu.CompilerParams(collective_id=0, has_side_effects=True, vmem_limit_bytes=67043328),
        name='mlp_block',
    )(x, dy, wu, wd, vec, bu)
    return res[:n_out]


def solution(mesh):
    assert (mesh.shape['col'], mesh.shape['row'], mesh.shape['depth']) == (4, 2, 4)
    tok_spec = P(('dp', 'depth', 'row'), 'col')
    vec_spec = P('col')
    mat_spec = P('row', 'col')
    grad_vec = P(('dp', 'col'))
    grad_mat = P(('dp', 'row'), 'col')
    def local_pass(x_blk, gamma_blk, beta_blk, w_up_blk, b_up_blk, w_down_blk, b_down_blk, dy_blk):
        hb, fb = x_blk.shape[1], w_up_blk.shape[1]
        vec = jnp.stack([gamma_blk, beta_blk, b_down_blk.astype(F32)] + [jnp.zeros_like(gamma_blk)] * 5)
        bu = jnp.broadcast_to(b_up_blk.astype(F32)[None], (8, fb))
        y_blk, dx_blk, grad_w_up, grad_w_down, sums = block_kernel(x_blk, dy_blk, w_up_blk, w_down_blk, vec, bu)
        sums = sums[0]
        return (y_blk, dx_blk, sums[:hb], sums[hb:2 * hb], grad_w_up, sums[2 * hb:2 * hb + fb], grad_w_down, sums[2 * hb + fb:])

    return jax.shard_map(
        local_pass,
        mesh=mesh,
        in_specs=(tok_spec, vec_spec, vec_spec, mat_spec, vec_spec, mat_spec, vec_spec, tok_spec),
        out_specs=(tok_spec, tok_spec, grad_vec, grad_vec, grad_mat, grad_vec, grad_mat, grad_vec),
        check_vma=False,
    )
```

```python
import functools

import jax
import jax.numpy as jnp
from jax import lax
from jax.experimental import pallas as pl
from jax.experimental.pallas import tpu as pltpu
from jax.sharding import PartitionSpec as P

LN_EPS = 1e-5
F32 = jnp.float32
BF16 = jnp.bfloat16
MESH = pl.DeviceIdType.MESH
GELU_A = 0.7978845608028654
GELU_B = 0.044715
NCH = 4
ROWS = 16
LROWS = 64
XROWS = 32

NN = (((1,), (0,)), ((), ()))
NT = (((1,), (1,)), ((), ()))
TN = (((0,), (0,)), ((), ()))

SEMS = {}
for _z in ('x', 'g'):
    for _n in ('near', 'far', 'opp', 'd2d', 'd2w', 'd2o', 's_near', 's_far', 's_rel', 's_d2d'):
        SEMS[_z + _n] = NCH
    SEMS[_z + 'bounce'] = 2
for _p in ('y', 'd'):
    SEMS.update({_p + 's_give': 2, _p + 'got': 2, _p + 's_far': 4, _p + 'keep': 2, _p + 'far': 4, _p + 's_out': 8, _p + 'out': 1, _p + 'loc': 4})
SEMS.update(l_wu=1, s_wu=1, r_wu=1, s_wun=1, r_wun=1, s_wuy=4, r_wuy=4,
            s_wd0=2, s_wdx=4, r_wd=4, s_wdr=2, s_wdy=24, r_wdy=8,
            l_vec=2, s_vec=4, r_vec=2,
            ld=8, ldb=2, st=6, s_st=2, r_st=2, s_sum=8, r_sum=2,
            d_so=8, d_r=8, d_sa=8, d_p=8, d_sf=4, d_out=1, d_sy=8, d_y=2, d_sr=8, d_o=2,
            u_so=2, u_r=2, u_sa=2, u_p=2, u_sf=3, u_out=3, u_sr=1, u_o=2, l_small=2)
BASE = {}
_at = 0
for _n, _c in SEMS.items():
    BASE[_n] = _at
    _at += _c
N_SEM = _at


def gelu_and_slope(v):
    v2 = v * v
    t = jnp.tanh(v * (GELU_A + (GELU_A * GELU_B) * v2))
    q = (1.0 - t) * (GELU_A + (3.0 * GELU_A * GELU_B) * v2)
    return 0.5 * v * (1.0 + t), 0.5 * ((1.0 + t) * (1.0 + v * q))


def body(dims, x_ref, dy_ref, wu_ref, wd_ref, vec_ref, bu_ref,
         y_out, dx_out, gwu_out, gwd_out, sum_out,
         X, DY, XN, A, DU, SL, YGOT, YFAR, YKEEP, GGOT, GFAR, GKEEP, PFD, PND, PFU, PNU,
         wu_v, wd_v, accD, accU, r1D, r2D, r1U, r2U, vec_v, bu_v, wx, F4, ob, finD,
         db_v, cs_v, st_v, ms_v, st2_v, sx_v, sr_v, bd_v, sum_v, sumr_v, sem):
    TK, HB, FH = dims
    W, HW, TH, BLK, QF = 4 * HB, 2 * HB, TK // 2, TK // NCH, FH // 4
    RH, DQ, QH, DH, FB = W // 2, W // 4, FH // 8, W // 8, 2 * FH
    NTW = HB
    inv_w = 1.0 / W
    finU = wx.at[3, pl.ds(0, DQ), pl.ds(HW, FH)]
    f0, f1 = F4.at[0], F4.at[1]

    c, r, d = lax.axis_index('col'), lax.axis_index('row'), lax.axis_index('depth')
    c_odd, d_odd = lax.rem(c, 2), lax.rem(d, 2)
    cn, cf, co = c + 1 - 2 * c_odd, 3 - c, lax.rem(c + 2, 4)
    dn, df, do = d + 1 - 2 * d_odd, 3 - d, lax.rem(d + 2, 4)
    f, dh = lax.div(c, 2), lax.div(d, 2)
    tau = lax.rem(lax.div(c + 1, 2), 2)
    rp = 1 - r
    o, o2 = c_odd * FH, (1 - c_odd) * FH

    def S(name, i=0):
        return sem.at[BASE[name] + i]

    def ds(start, size):
        return pl.ds(pl.multiple_of(start, size), size)

    def dsm(start, size, mult):
        return pl.ds(pl.multiple_of(start, mult), size)

    def put(src, dst, ssem, rsem, **dev):
        pltpu.make_async_remote_copy(src_ref=src, dst_ref=dst, send_sem=ssem, recv_sem=rsem,
                                     device_id=dev, device_id_type=MESH).start()

    def copy(src, dst, s):
        pltpu.make_async_copy(src, dst, s).start()

    def wait(ref, s):
        pltpu.make_async_copy(ref, ref, s).wait()

    def loop(n, fn):
        def step(i, carry):
            fn(i)
            return carry
        lax.fori_loop(0, n, step, 0)

    bar = pltpu.get_barrier_semaphore()
    for dev in [dict(row=rp)] + [dict(row=h, **q) for h in range(2) for q in
                                 (dict(col=cn), dict(col=cf), dict(col=co), dict(depth=dn), dict(depth=df), dict(depth=do))]:
        pl.semaphore_signal(bar, inc=1, device_id=dev, device_id_type=MESH)
    pl.semaphore_wait(bar, 13)

    def wd_src(s, h):
        return wd_ref.at[dsm((2 * s + h) * FH + d * QF, QF, QF), :]

    def wd_dst(s, col):
        return wd_v.at[dsm(s * FH + d * QF, QF, QF), ds(col * HB, HB)]

    def reg(Z, k, col):
        return Z.at[r, ds(k * BLK, BLK), ds(col * HB, HB)]

    def send_own(z, z_ref, Z, which, chunks=(0, NCH)):
        def step(k):
            src = z_ref.at[ds(k * BLK, BLK), :]
            if 'near' in which:
                put(src, reg(Z, k, c), S(z + 's_near', k), S(z + 'near', k), col=cn)
            if 'far' in which:
                put(src, reg(Z, k, c), S(z + 's_far', k), S(z + 'far', k), col=cf)
            if 'd2d' in which:
                put(src, reg(Z, k, c), S(z + 's_d2d', k), S(z + ('d2d' if z == 'x' else 'd2w'), k), row=rp)
        for k in range(*chunks):
            step(k)

    def d2d(z, Z, k, col, s):
        put(reg(Z, k, col), reg(Z, k, col), S(z + 's_d2d', k), S(z + s, k), row=rp)

    vec_at = vec_v.at[:, ds(c * HB, HB)]
    copy(vec_ref, vec_at, S('l_vec', 0))
    put(vec_ref, vec_at, S('s_vec', 0), S('r_vec', 0), col=cn)
    put(vec_ref, vec_at, S('s_vec', 1), S('r_vec', 0), col=cf)
    put(vec_ref, vec_at, S('s_vec', 2), S('r_vec', 0), col=co)
    bu_src, bu_at = bu_ref.at[:, ds(r * FH, FH)], bu_v.at[:, ds(o, FH)]
    copy(bu_src, bu_at, S('l_vec', 1))
    put(bu_src, bu_at, S('s_vec', 3), S('r_vec', 1), col=cn)

    wu_own = wu_v.at[ds(r * RH, RH), ds(o, FH)]
    wd_own = lambda s: wd_v.at[pl.ds(s * FH, FH), ds(c * HB, HB)]

    @pl.when(r != f)
    def _():
        for s in range(2):
            for h in range(2):
                put(wd_src(s, h), wd_dst(s, c), S('s_wdx', 2 * s + h), S('r_wd', 2), col=cf, row=h)

    @pl.when(r == f)
    def _():
        for s in range(2):
            for h in range(2):
                put(wd_src(s, h), wd_dst(s, c), S('s_wdx', 2 * s + h), S('r_wd', 1), col=cn, row=h)
    send_own('x', x_ref, X, ('far',), (0, 2))
    send_own('x', x_ref, X, ('near',), (0, 1))
    put(wu_ref.at[:, ds(rp * FH, FH)], wu_own, S('s_wu'), S('r_wu'), row=rp)
    copy(wu_ref.at[:, ds(r * FH, FH)], wu_own, S('l_wu'))
    send_own('x', x_ref, X, ('d2d',))
    send_own('g', dy_ref, DY, ('d2d',))
    for i, z_ref in enumerate((x_ref, dy_ref)):
        for k in range(NCH):
            copy(z_ref.at[pl.ds(k * BLK, BLK), :], wx.at[i, :, pl.ds(k * HB, HB)], S('xg'[i] + 'bounce', 0))

    @pl.when(r == f)
    def _():
        for s in range(2):
            copy(wd_ref.at[dsm((2 * s + r) * FH, FH, FH), :], wd_own(s), S('r_wd', 0))
            put(wd_ref.at[dsm((2 * s + rp) * FH, FH, FH), :], wd_own(s), S('s_wd0', s), S('r_wd', 0), row=rp)

    for i, Z in enumerate((X, DY)):
        wait(wx.at[i], S('xg'[i] + 'bounce', 0))
        for k in range(NCH):
            copy(wx.at[i, :, pl.ds(k * HB, HB)], reg(Z, k, c), S('xg'[i] + 'bounce', 1))

    with jax.named_scope('wd_far'):
        wait(wd_v.at[pl.ds(0, 2 * QF), pl.ds(0, HB)], S('r_wd', 2))
    for s in range(2):
        put(wd_dst(s, cf), wd_dst(s, cf), S('s_wdr', s), S('r_wd', 3), col=cn)
    send_own('x', x_ref, X, ('near',), (1, NCH - 1))

    with jax.named_scope('wu_own'):
        wait(wu_own, S('l_wu'))
        wait(wu_v.at[ds(rp * RH, RH), ds(o, FH)], S('r_wu'))
    wun = wu_v.at[ds(d * DQ, DQ), ds(o, FH)]
    put(wun, wun, S('s_wun'), S('r_wun'), col=cn)
    send_own('x', x_ref, X, ('near',), (NCH - 1, NCH))

    db_v[...] = jnp.zeros_like(db_v)
    cs_v[...] = jnp.zeros_like(cs_v)
    bd_v[...] = jnp.zeros_like(bd_v)

    def dy_sum(i):
        rr = ds(i * ROWS, ROWS)
        part = jnp.sum(wx[1, rr, :].astype(F32).reshape(ROWS // 8, 8, W), axis=0)
        bd_v[...] += part[:, :HB] + part[:, HB:2 * HB] + part[:, 2 * HB:3 * HB] + part[:, 3 * HB:]
    with jax.named_scope('dy_sum'):
        loop(BLK // ROWS, dy_sum)

    def wuq(dd, half=None):
        if half is None:
            return wu_v.at[ds(dd * DQ, DQ), ds(o2, FH)]
        return wu_v.at[dsm(dd * DQ + half * DH, DH, DH), ds(o2, FH)]

    def wu_send():
        with jax.named_scope('wu_near'):
            wait(wuq(d), S('r_wun'))
        put(wuq(d), wuq(d), S('s_wuy', 0), S('r_wuy', 0), depth=dn)
        put(wuq(d), wuq(d), S('s_wuy', 1), S('r_wuy', 1), depth=df)

    def wu_relay():
        with jax.named_scope('wuy'):
            wait(wuq(dn), S('r_wuy', 0))
            wait(wuq(df), S('r_wuy', 1))
        put(wuq(dn, 1), wuq(dn, 1), S('s_wuy', 2), S('r_wuy', 3), depth=df)
        put(wuq(df, 0), wuq(df, 0), S('s_wuy', 3), S('r_wuy', 2), depth=dn)

    def wdq(s, dd, col, half=None):
        if half is None:
            return wd_v.at[dsm(s * FH + dd * QF, QF, QF), ds(col * HB, HB)]
        return wd_v.at[dsm(s * FH + dd * QF + half * QH, QH, QH), ds(col * HB, HB)]

    W_GROUPS = (((0, cn), (1, cf)), ((2, co),))

    def wd_send(g):
        if g == 0:
            wait(wd_v.at[pl.ds(0, 2 * QF), pl.ds(0, HB)], S('r_wd', 1))
        else:
            wait(wd_v.at[pl.ds(0, 2 * QF), pl.ds(0, HB)], S('r_wd', 3))
        for i, col in W_GROUPS[g]:
            for s in range(2):
                put(wdq(s, d, col), wdq(s, d, col), S('s_wdy', 4 * i + s), S('r_wdy', 4 * g), depth=dn)
                put(wdq(s, d, col), wdq(s, d, col), S('s_wdy', 4 * i + 2 + s), S('r_wdy', 4 * g + 1), depth=df)

    def wd_bytes(g, rows):
        return wd_v.at[pl.ds(0, 2 * rows), pl.ds(0, len(W_GROUPS[g]) * HB)]

    def wd_relay(g):
        for i in range(2):
            wait(wd_bytes(g, QF), S('r_wdy', 4 * g + i))
        for i, col in W_GROUPS[g]:
            for s in range(2):
                put(wdq(s, dn, col, 1), wdq(s, dn, col, 1), S('s_wdy', 12 + 4 * i + s), S('r_wdy', 4 * g + 3), depth=df)
                put(wdq(s, df, col, 0), wdq(s, df, col, 0), S('s_wdy', 12 + 4 * i + 2 + s), S('r_wdy', 4 * g + 2), depth=dn)

    def x_near(k):
        wait(reg(X, k, cn), S('xnear', k))
        put(reg(X, k, cn), reg(X, k, cn), S('xs_rel', k), S('xopp', k), col=cf)
        d2d('x', X, k, cn, 'd2d')

    with jax.named_scope('wd_send0'):
        wd_send(0)
    with jax.named_scope('x_near'):
        x_near(0)
    send_own('x', x_ref, X, ('far',), (2, 3))

    for i, Z in enumerate((X, DY)):
        wait(wx.at[i], S('xg'[i] + 'bounce', 1))
    wait(vec_at, S('l_vec', 0))
    wait(vec_v.at[:, pl.ds(0, 3 * HB)], S('r_vec', 0))
    wait(bu_at, S('l_vec', 1))
    wait(bu_at, S('r_vec', 1))

    def norm_rows(buf, rows):
        xf = buf[rows, :].astype(F32)
        mean = jnp.sum(xf, axis=1, keepdims=True) * inv_w
        cen = xf - mean
        inv = lax.rsqrt(jnp.sum(cen * cen, axis=1, keepdims=True) * inv_w + LN_EPS)
        return cen, mean, inv

    def tok_of(s):
        return tau + s * (1 - 2 * tau)

    N_T = FH // NTW

    def chain(tiles, hooks=None):
        hooks = hooks or {}

        def hook(what, i):
            for fn in hooks.get((what, i), ()):
                fn()
        for i, (product, _) in enumerate(tiles):
            hook('before', i)
            if i:
                tiles[i - 1][1](F4.at[(i - 1) % 2])
            F4[i % 2, :, :NTW] = product()
            hook('product', i)
            if i:
                hook('epilogue', i - 1)
        tiles[-1][1](F4.at[(len(tiles) - 1) % 2])
        hook('epilogue', len(tiles) - 1)

    def u_tile(src, i, n, start):
        cols = ds(start + n * NTW, NTW)
        at = pl.ds(n * NTW, NTW)

        def product():
            return lax.dot_general(wx[src], wu_v[:, cols], NN, preferred_element_type=F32)

        def epilogue(acc):
            u = (acc[:, :NTW] + bu_v[0:1, cols]).astype(BF16)
            a, slope = gelu_and_slope(u.astype(F32))
            ob[i, :, at] = a.astype(BF16)
            F4[2 + i, :, at] = slope
        return product, epilogue

    def u_store(i, s, rows, start):
        copy(ob.at[i], A.at[s, rows, ds(start, FH)], S('st', 2 + i))
        copy(F4.at[2 + i], SL.at[s, rows, ds(start, FH)], S('st', 4 + i))

    def u_stored():
        for i in range(2):
            wait(ob.at[i], S('st', 2 + i))
            wait(F4.at[2 + i], S('st', 4 + i))

    def phase1(k):
        @pl.when(k < NCH - 1)
        def _():
            with jax.named_scope('x_near'):
                x_near(k + 1)

        @pl.when(k == 0)
        def _():
            send_own('x', x_ref, X, ('far',), (3, 4))
            with jax.named_scope('wd_send1'):
                wd_send(1)

        @pl.when(k == 1)
        def _():
            with jax.named_scope('wd_relay0'):
                wd_relay(0)
            send_own('g', dy_ref, DY, ('near',))

        @pl.when(k == 2)
        def _():
            send_own('g', dy_ref, DY, ('far',))
            wu_send()
            with jax.named_scope('wd_relay1'):
                wd_relay(1)

        with jax.named_scope('x_far'):
            wait(reg(X, k, cf), S('xfar', k))
            d2d('x', X, k, cf, 'd2d')
        with jax.named_scope('x_opp'):
            wait(reg(X, k, co), S('xopp', k))
            d2d('x', X, k, co, 'd2d')

        rows = ds(k * BLK, BLK)
        with jax.named_scope('x_d2d'):
            wait(X.at[rp, rows, :], S('xd2d', k))

        @pl.when(k == NCH - 1)
        def _():
            wu_relay()
            for b in range(2):
                copy(XN.at[0, pl.ds(b * BLK, BLK), :], wx.at[2 + b], S('ld', 2 + b))

        @pl.when(k > 0)
        def _():
            for s in range(2):
                wait(wx.at[s], S('st', s))
        for s in range(2):
            copy(X.at[tok_of(s), rows, :], wx.at[s], S('ld', s))
        for s in range(2):
            wait(wx.at[s], S('ld', s))

            def ln(i):
                rr = ds(i * LROWS, LROWS)
                cen, _, inv = norm_rows(wx.at[s], rr)
                wx[s, rr, :] = (cen * inv * vec_v[0:1, :] + vec_v[1:2, :]).astype(BF16)
            with jax.named_scope('ln'):
                loop(BLK // LROWS, ln)
            copy(wx.at[s], XN.at[s, rows, :], S('st', s))
        pl.when(k > 0)(u_stored)
        with jax.named_scope('u_own'):
            chain([u_tile(i, i, n, o) for i in range(2) for n in range(N_T)])
        for s in range(2):
            u_store(s, s, rows, o)
    loop(NCH, phase1)
    for s in range(2):
        wait(wx.at[s], S('st', s))
    u_stored()

    def u_near():
        copy(XN.at[0, pl.ds(2 * BLK, BLK), :], wx.at[1], S('ld', 1))

        def step(kp):
            @pl.when(kp == 0)
            def _():
                for i in (2, 3):
                    wait(wx.at[i], S('ld', i))

            @pl.when(kp > 0)
            def _():
                wait(wx.at[1], S('ld', 1))
            chain([u_tile((2 + i) * (1 - kp) + kp * (1 - i), i, n, o2) for i in range(2) for n in range(N_T)],
                  {('before', 1): [lambda: pl.when(kp > 0)(u_stored)]})
            for i in range(2):
                u_store(i, 0, ds((2 * kp + i) * BLK, BLK), o2)
        loop(2, step)
        u_stored()

    def g_near_far(k):
        wait(reg(DY, k, cf), S('gfar', k))
        put(reg(DY, k, cf), reg(DY, k, cf), S('gs_rel', k), S('gopp', k), col=cn)
        d2d('g', DY, k, cf, 'd2d')
        wait(reg(DY, k, cn), S('gnear', k))
        d2d('g', DY, k, cn, 'd2d')

    def g_opp(k):
        wait(reg(DY, k, co), S('gopp', k))
        d2d('g', DY, k, co, 'd2o')

    def g_opp_got(k):
        wait(reg(DY, k, co), S('gd2o', k))

    def tile_y(lhs, col):
        return lax.dot_general(lhs, wd_v[:, dsm(col, NTW, NTW)], NN, preferred_element_type=F32)

    def tile_g(lhs, col):
        return lax.dot_general(lhs, wu_v[dsm(col, NTW, NTW), :], NT, preferred_element_type=F32)

    def give(p, src, tile, GOT):
        def blk(b):
            return src.at[0, dsm(rp * TH + b * BLK, BLK, BLK), :]
        for b in range(2):
            copy(blk(b), wx.at[b, :, pl.ds(0, FB)], S('ld', b))
        keep_load(src)

        def step(b):
            wait(wx.at[b, :, pl.ds(0, FB)], S('ld', b))

            def half(h):
                @pl.when(b == 1)
                def _():
                    wait(F4.at[h], S(p + 's_give', h))

                def n_tile(n):
                    F4[h, :, ds(n * NTW, NTW)] = tile(wx[b, :, :FB], h * HW + n * NTW)
                loop(HW // NTW, n_tile)
                put(F4.at[h], GOT.at[ds(b * BLK, BLK), ds(h * HW, HW)], S(p + 's_give', h), S(p + 'got', b), row=rp)
            loop(2, half)
        loop(2, step)

    HB2 = BLK // 2

    def keep_load(src):
        for b in range(2):
            copy(src.at[0, dsm(r * TH + b * BLK, BLK, BLK), :], wx.at[2 + b, :, pl.ds(0, FB)], S('ld', 2 + b))

    def got_load(GOT, b, col0, out, s_):
        copy(GOT.at[ds(b * BLK, BLK), ds(col0, HW)], F4.at[out], s_)

    def add_tiles(b, out, tile, col0):
        def n_tile(n):
            at = ds(n * NTW, NTW)
            F4[out, :, at] = F4[out, :, at] + tile(wx[2 + b, :, :FB], col0 + n * NTW)
        loop(HW // NTW, n_tile)

    def far_put(p, FAR, b, q):
        put(F4.at[2 + b, ds(q * HB2, HB2), :], FAR.at[ds(b * BLK + q * HB2, HB2), :], S(p + 's_far', 2 * b + q), S(p + 'far', 2 * b + q), col=cf)

    def keep_far(p, tile, GOT, FAR, held):
        for b in range(2):
            with jax.named_scope('got'):
                wait(GOT.at[ds(b * BLK, BLK), :], S(p + 'got', b))
            got_load(GOT, b, (1 - f) * HW, 2 + b, S('ld', 4 + b))

        def step(b):
            wait(wx.at[2 + b, :, pl.ds(0, FB)], S('ld', 2 + b))
            wait(F4.at[2 + b], S('ld', 4 + b))
            add_tiles(b, 2 + b, tile, (1 - f) * HW)
            far_put(p, FAR, b, 0)
            if held:
                pl.when(b == 0)(lambda: far_put(p, FAR, b, 1))
            else:
                far_put(p, FAR, b, 1)
        loop(2, step)

    def keep_own(p, tile, GOT, KEEP, after=None):
        for h in range(2):
            wait(F4.at[h], S(p + 's_give', h))
        for b in range(2):
            got_load(GOT, b, f * HW, 1 - b, S('ld', 4 + b))

        def step(b):
            if after:
                wait(wx.at[2 + b, :, pl.ds(0, FB)], S('ld', 2 + b))
            wait(F4.at[1 - b], S('ld', 4 + b))
            add_tiles(b, 1 - b, tile, f * HW)
            copy(F4.at[1 - b], KEEP.at[ds(b * BLK, BLK), :], S(p + 'keep', b))
            if after:
                after(b)
        loop(2, step)
        for b in range(2):
            wait(F4.at[b], S(p + 'keep', b))

    def far_end(p, b, q):
        wait(F4.at[2 + b, ds(q * HB2, HB2), :], S(p + 's_far', 2 * b + q))

    def place(p, out, b, q, nq):
        nr = BLK // nq
        rr = ds(q * nr, nr)
        dst = out.at[dsm(r * TH + b * BLK + q * nr, nr, nr), :]
        mine, other = ob.at[b, rr, ds(c_odd * HB, HB)], ob.at[b, rr, ds((1 - c_odd) * HB, HB)]
        put(other, dst, S(p + 's_out', 4 * b + 2 * q), S(p + 'out'), col=cn, row=tau)

        @pl.when(r == tau)
        def _():
            copy(mine, dst, S(p + 'loc', 2 * b + q))

        @pl.when(r != tau)
        def _():
            put(mine, dst, S(p + 's_out', 4 * b + 2 * q + 1), S(p + 'out'), row=rp)

    def place_end(p, b, q, nq):
        part = ob.at[b, pl.ds(0, BLK // nq), pl.ds(0, HB)]
        wait(part, S(p + 's_out', 4 * b + 2 * q))

        @pl.when(r == tau)
        def _():
            wait(part, S(p + 'loc', 2 * b + q))

        @pl.when(r != tau)
        def _():
            wait(part, S(p + 's_out', 4 * b + 2 * q + 1))

    fcols = ds(f * HW, HW)

    def y_final(b):
        brow = ds(b * BLK, BLK)
        for q in range(2):
            wait(YFAR.at[ds(b * BLK + q * HB2, HB2), :], S('yfar', 2 * b + q))
        copy(YFAR.at[brow, :], f0, S('ld', 0))
        copy(YKEEP.at[brow, :], f1, S('ld', 1))
        copy(X.at[tau, dsm(r * TH + b * BLK, BLK, BLK), fcols], wx.at[0, :, pl.ds(0, HW)], S('ld', 2))
        wait(f0, S('ld', 0))
        wait(f1, S('ld', 1))
        wait(wx.at[0, :, pl.ds(0, HW)], S('ld', 2))

        def fin(i):
            rr = ds(i * ROWS, ROWS)
            ob[b, rr, :] = (wx[0, rr, :HW].astype(F32) + (f0[rr, :] + f1[rr, :]) + vec_v[2:3, fcols]).astype(BF16)
        loop(BLK // ROWS, fin)
        place('y', y_out, b, 0, 1)

    def services(t):
        @pl.when(t == 2)
        def _():
            with jax.named_scope('dwd_a3b0'):
                dwd_b(0)
                dwd_a(3)

        @pl.when(t == 4)
        def _():
            with jax.named_scope('dwd_b12'):
                dwd_b(1)
                dwd_b(2)

    def da_all():
        def part(t, i):
            near = lax.div(t, NCH)
            tok = tau + i * (1 - near) * (1 - 2 * tau)
            chunk = t * (1 - near) + near * (2 * (t - NCH) + i)
            return near, tok, i * (1 - near), ds(chunk * BLK, BLK), near * o2 + (1 - near) * o

        def load(t, p):
            for i in range(2):
                _, tok, us, rows, start = part(t, i)
                copy(DY.at[tok, rows, :], wx.at[2 * p + i], S('ld', 2 * p + i))
                copy(SL.at[us, rows, ds(start, FH)], accU.at[2 * p + i], S('ld', 4 + 2 * p + i))

        def store(t, i):
            _, _, us, rows, start = part(t, i)
            copy(ob.at[i], DU.at[us, rows, ds(start, FH)], S('st', 4 + i))

        def stored():
            for i in range(2):
                wait(ob.at[i], S('st', 4 + i))

        n_steps = NCH + NCH // 2

        def step(t):
            near, _, _, _, start = part(t, 0)
            p = lax.rem(t, 2)
            services(t)
            for i in range(2):
                wait(wx.at[2 * p + i], S('ld', 2 * p + i))
                wait(accU.at[2 * p + i], S('ld', 4 + 2 * p + i))

            @pl.when(t < n_steps - 1)
            def _():
                load(t + 1, 1 - p)

            def tile(i, n):
                cols = ds(start + n * NTW, NTW)
                at = pl.ds(n * NTW, NTW)

                def product():
                    return lax.dot_general(wx[2 * p + i], wd_v[cols, :], NT, preferred_element_type=F32)

                def epilogue(acc):
                    du = (acc[:, :NTW] * accU[2 * p + i, :, at]).astype(BF16)
                    ob[i, :, at] = du
                    db_v[near, :, at] += jnp.sum(du.astype(F32).reshape(BLK // 8, 8, NTW), axis=0)
                return product, epilogue
            chain([tile(i, n) for i in range(2) for n in range(N_T)], {('before', 1): [lambda: pl.when(t > 0)(stored)]})
            for i in range(2):
                store(t, i)
        load(0, 0)
        loop(n_steps, step)
        stored()

    def rows_of(kb):
        return ds(lax.rem(kb, NCH) * BLK, BLK), lax.div(kb, NCH)

    d_col = (c, cn, cf, co)

    NB, NSLOT = 2 * NCH, 4

    def k_loop(load, use, width):
        for kb in range(NSLOT - 1):
            load(kb, wx.at[kb], S('ld', kb))

        def step(kb):
            slot = lax.rem(kb, NSLOT)

            @pl.when(kb + NSLOT - 1 < NB)
            def _():
                nxt = lax.rem(kb + NSLOT - 1, NSLOT)
                load(kb + NSLOT - 1, wx.at[nxt], S('ld', nxt))
            buf = wx.at[slot]
            wait(buf.at[:, pl.ds(0, width)], S('ld', slot))
            use(buf)
        loop(NB, step)

    def dwd_pass(js):
        def load(kb, buf, s_):
            rows, s = rows_of(kb)
            copy(A.at[s, rows, ds(o, FH)], buf.at[:, pl.ds(0, FH)], s_)
            for i, j in enumerate(js):
                copy(DY.at[tok_of(s), rows, ds(d_col[j] * HB, HB)], buf.at[:, pl.ds(FH + i * HB, HB)], s_)

        def use(buf):
            for i, j in enumerate(js):
                for m in range(2):
                    mm = slice(m * FH // 2, (m + 1) * FH // 2)
                    accD[j, mm, :] += lax.dot_general(buf[:, mm], buf[:, FH + i * HB:FH + (i + 1) * HB], TN, preferred_element_type=F32)
        for j in js:
            accD[j] = jnp.zeros((FH, HB), F32)
        k_loop(load, use, FH + len(js) * HB)

    def dwd_opp(j):
        put(accD.at[j, dsm(do * QF, QH, QH), :], r1D.at[j], S('d_so', 2 * j), S('d_r', 2 * j), depth=dn)
        put(accD.at[j, dsm(do * QF + QH, QH, QH), :], r2D.at[j], S('d_so', 2 * j + 1), S('d_r', 2 * j + 1), depth=df)

    def dwd_a(j):
        wait(r1D.at[j], S('d_r', 2 * j))
        rr = dsm(df * QF, QH, QH)
        accD[j, rr, :] += r1D[j]
        put(accD.at[j, ds(df * QF, QF), :], PFD.at[j], S('d_sa', 2 * j), S('d_p', 2 * j), depth=df)
        wait(r2D.at[j], S('d_r', 2 * j + 1))
        rr = dsm(dn * QF + QH, QH, QH)
        accD[j, rr, :] += r2D[j]
        put(accD.at[j, ds(dn * QF, QF), :], PND.at[j], S('d_sa', 2 * j + 1), S('d_p', 2 * j + 1), depth=dn)

    def dwd_rows(q, h, dd):
        return dsm((2 * q + h) * FH + dd * QF, QF, QF)

    def dwd_b(j):
        wait(PFD.at[j], S('d_p', 2 * j))
        wait(PND.at[j], S('d_p', 2 * j + 1))
        wait(PFD.at[j], S('d_sa', 2 * j))
        wait(PND.at[j], S('d_sa', 2 * j + 1))
        pf, pn = accD.at[j, ds(df * QF, QF), :], accD.at[j, ds(dn * QF, QF), :]
        copy(PFD.at[j], pf, S('ldb', 0))
        copy(PND.at[j], pn, S('ldb', 1))
        wait(pf, S('ldb', 0))
        wait(pn, S('ldb', 1))
        finD[j] = (accD[j, ds(d * QF, QF), :] + (pf[...] + pn[...])).astype(BF16)
        dst = gwd_out.at[dwd_rows(c_odd, r, d), :]
        if j:
            put(finD.at[j], dst, S('d_sf', j), S('d_out'), col=d_col[j], row=f)
        else:
            @pl.when(r == f)
            def _():
                copy(finD.at[0], dst, S('d_out'))

            @pl.when(r != f)
            def _():
                put(finD.at[0], dst, S('d_sf', 0), S('d_out'), row=rp)

    def gwd(i, dd, half=None):
        if half is None:
            return gwd_out.at[dsm(i * FH + dd * QF, QF, QF), :]
        return gwd_out.at[dsm(i * FH + dd * QF + half * QH, QH, QH), :]

    def gwd_send():
        wait(gwd_out.at[pl.ds(0, 4 * QF), :], S('d_out'))
        for i in range(4):
            put(gwd(i, d), gwd(i, d), S('d_sy', i), S('d_y', 0), depth=dn)
            put(gwd(i, d), gwd(i, d), S('d_sy', 4 + i), S('d_y', 1), depth=df)

    def gwd_relay():
        wait(gwd_out.at[pl.ds(0, 4 * QF), :], S('d_y', 0))
        for i in range(4):
            put(gwd(i, dn, 1), gwd(i, dn, 1), S('d_sr', i), S('d_o', 1), depth=df)
        wait(gwd_out.at[pl.ds(0, 4 * QF), :], S('d_y', 1))
        for i in range(4):
            put(gwd(i, df, 0), gwd(i, df, 0), S('d_sr', 4 + i), S('d_o', 0), depth=dn)

    def dwu_pass(dds):
        def load(kb, buf, s_):
            rows, s = rows_of(kb)
            copy(DU.at[s, rows, ds(o, FH)], buf.at[:, pl.ds(0, FH)], s_)
            for i, dd in enumerate(dds):
                copy(XN.at[s, rows, ds(dd * DQ, DQ)], buf.at[:, pl.ds(FH + i * DQ, DQ)], s_)

        def use(buf):
            for i, dd in enumerate(dds):
                for m in range(2):
                    mm = slice(m * FH // 2, (m + 1) * FH // 2)
                    accU[dd, :, mm] += lax.dot_general(buf[:, FH + i * DQ:FH + (i + 1) * DQ], buf[:, mm], TN, preferred_element_type=F32)
        for dd in dds:
            accU[dd] = jnp.zeros((DQ, FH), F32)
        k_loop(load, use, FH + len(dds) * DQ)

    def dwu_opp():
        put(accU.at[do, pl.ds(0, DH), :], r1U, S('u_so', 0), S('u_r', 0), depth=dn)
        put(accU.at[do, pl.ds(DH, DH), :], r2U, S('u_so', 1), S('u_r', 1), depth=df)

    def dwu_a():
        wait(r1U, S('u_r', 0))
        accU[df, :DH, :] += r1U[...]
        put(accU.at[df], PFU, S('u_sa', 0), S('u_p', 0), depth=df)
        wait(r2U, S('u_r', 1))
        accU[dn, DH:, :] += r2U[...]
        put(accU.at[dn], PNU, S('u_sa', 1), S('u_p', 1), depth=dn)

    def dwu_b():
        wait(PFU, S('u_p', 0))
        wait(PNU, S('u_p', 1))
        pf, pn = f0.at[pl.ds(0, DQ), pl.ds(0, FH)], f1.at[pl.ds(0, DQ), pl.ds(0, FH)]
        copy(PFU, pf, S('ldb', 0))
        copy(PNU, pn, S('ldb', 1))
        wait(pf, S('ldb', 0))
        wait(pn, S('ldb', 1))

        def fin(i):
            rr = ds(i * ROWS, ROWS)
            wx[3, rr, HW:HW + FH] = (accU[d, rr, :] + (f0[rr, :FH] + f1[rr, :FH])).astype(BF16)
        loop(DQ // ROWS, fin)
        dst = gwu_out.at[ds(d_odd * DQ, DQ), ds(r * FH, FH)]
        put(finU, dst, S('u_sf', 0), S('u_out', 1), depth=dn, row=dh)
        put(finU, dst, S('u_sf', 1), S('u_out', 2), depth=df, row=dh)

        @pl.when(r == dh)
        def _():
            copy(finU, dst, S('u_out', 0))

        @pl.when(r != dh)
        def _():
            put(finU, dst, S('u_sf', 2), S('u_out', 0), row=rp)

    def gwu(start, size):
        return gwu_out.at[dsm(start, size, size), :]

    def gwu_relay():
        @pl.when(r == dh)
        def _():
            wait(gwu(lax.rem(dn, 2) * DQ, DQ), S('u_out', 1))
            part = gwu(lax.rem(dn, 2) * DQ + DH, DH)
            put(part, part, S('u_sr'), S('u_o', 1), depth=df)

        @pl.when(r != dh)
        def _():
            wait(gwu(lax.rem(df, 2) * DQ, DQ), S('u_out', 2))
            part = gwu(lax.rem(df, 2) * DQ, DH)
            put(part, part, S('u_sr'), S('u_o', 0), depth=dn)

    def gwu_end():
        @pl.when(r == dh)
        def _():
            wait(gwu(d_odd * DQ, DQ), S('u_out', 0))

        @pl.when(r != dh)
        def _():
            wait(gwu(0, DH), S('u_o', 0))
            wait(gwu(0, DH), S('u_o', 1))

    lane = lax.broadcasted_iota(jnp.int32, (LROWS, 128), 1)

    SB = min(BLK, 128)
    NS = BLK // SB

    def stats_load():
        for b in range(2):
            copy(X.at[tau, dsm(r * TH + b * BLK, BLK, BLK), :], wx.at[b], S('ld', b))

    def stats_part(b):
        wait(wx.at[b], S('ld', b))

        def rows_step(i):
            rr = ds(i * LROWS, LROWS)
            _, mean, inv = norm_rows(wx.at[b], rr)
            s0, s1 = jnp.zeros((LROWS, 1), F32), jnp.zeros((LROWS, 1), F32)
            for col0, slot in ((f * HW, 1 - b), ((1 - f) * HW, 2 + b)):
                cols = ds(col0, HW)
                gh = F4[slot, rr, :] * vec_v[0:1, cols]
                s0 = s0 + jnp.sum(gh, axis=1, keepdims=True)
                s1 = s1 + jnp.sum(gh * ((wx[b, rr, cols].astype(F32) - mean) * inv), axis=1, keepdims=True)
            st_v[rr, :] = jnp.where(lane < 64, s0, s1)
            ms_v[b, rr, :] = jnp.where(lane < 64, mean, inv)
        loop(BLK // LROWS, rows_step)
        for t in range(NS):
            tr = st_v[t * SB:(t + 1) * SB, :].T
            sx_v[b, t:t + 1, :SB] = tr[0:1, :]
            sx_v[b, NS + t:NS + t + 1, :SB] = tr[64:65, :]
        put(sx_v.at[b], sr_v.at[b], S('s_st', b), S('r_st', b), col=cf)

    def stats_recv(b):
        wait(sr_v.at[b], S('r_st', b))
        for t in range(NS):
            for i in range(2):
                row = (sx_v[b, i * NS + t:i * NS + t + 1, :SB] + sr_v[b, i * NS + t:i * NS + t + 1, :SB]) * inv_w
                st2_v[i, t * SB:(t + 1) * SB, :] = jnp.broadcast_to(row, (128, SB)).T

    def dx_final(b, q):
        sub = ds(q * HB2, HB2)
        brow = ds(b * BLK + q * HB2, HB2)
        trow = dsm(r * TH + b * BLK + q * HB2, HB2, HB2)
        xb, gb = wx.at[b, sub, pl.ds(0, HW)], wx.at[2 + b, sub, pl.ds(0, HW)]
        copy(GKEEP.at[brow, :], F4.at[1, sub, :], S('ld', 1))
        copy(X.at[tau, trow, fcols], xb, S('ld', 2))
        copy(DY.at[tau, trow, fcols], gb, S('ld', 3))
        with jax.named_scope('d_far'):
            wait(GFAR.at[brow, :], S('dfar', 2 * b + q))
        copy(GFAR.at[brow, :], F4.at[0, sub, :], S('ld', 0))
        wait(F4.at[1, sub, :], S('ld', 1))
        wait(xb, S('ld', 2))
        wait(gb, S('ld', 3))
        wait(F4.at[0, sub, :], S('ld', 0))

        def rows_step(i):
            rr = dsm(q * HB2 + i * XROWS, XROWS, XROWS)
            mean, inv = ms_v[b, rr, 0:1], ms_v[b, rr, 64:65]
            xhat = (wx[b, rr, :HW].astype(F32) - mean) * inv
            dxn = F4[0, rr, :] + F4[1, rr, :]
            gh = dxn * vec_v[0:1, fcols]
            dx = wx[2 + b, rr, :HW].astype(F32) + inv * (gh - st2_v[0, rr, 0:1] - xhat * st2_v[1, rr, 0:1])
            ob[b, rr, :] = dx.astype(BF16)
            cs_v[0] += jnp.sum((dxn * xhat).reshape(XROWS // 8, 8, HW), axis=0)
            cs_v[1] += jnp.sum(dxn.reshape(XROWS // 8, 8, HW), axis=0)
        loop(HB2 // XROWS, rows_step)
        place('d', dx_out, b, q, 2)

    me = 2 * d + r
    peers = [dict(row=rp)] + [dict(depth=q, row=h) for q in (dn, df, do) for h in range(2)]
    near_in = sumr_v.at[8, :, pl.ds(0, 2 * HB)]

    def sums_1():
        cw = jnp.sum(cs_v[...], axis=1)
        for i in range(2):
            for q in range(2):
                @pl.when(c_odd == q)
                def _():
                    sum_v[0, :, i * HB:(i + 1) * HB] = cw[i:i + 1, q * HB:(q + 1) * HB]
                    sum_v[1, :, i * HB:(i + 1) * HB] = cw[i:i + 1, (1 - q) * HB:(2 - q) * HB]
        put(sum_v.at[1, :, pl.ds(0, 2 * HB)], near_in, S('s_sum', 0), S('r_sum', 0), col=cn)
        sum_v[0, :, 2 * HB:2 * HB + FB] = jnp.zeros((1, FB), F32)
        sum_v[0, :, dsm(2 * HB + r * FH, FH, HB)] = jnp.sum(db_v[0], axis=0, keepdims=True)
        sum_v[0, :, 2 * HB + FB:] = jnp.sum(bd_v[...], axis=0, keepdims=True)

    def sums_2():
        wait(near_in, S('r_sum', 0))
        sumr_v[me, :, :2 * HB] = sum_v[0, :, :2 * HB] + sumr_v[8, :, :2 * HB]
        sumr_v[me, :, 2 * HB:] = sum_v[0, :, 2 * HB:]
        for i, dev in enumerate(peers):
            put(sumr_v.at[me], sumr_v.at[me], S('s_sum', 1 + i), S('r_sum', 1), **dev)

    def sums_3():
        wait(sumr_v.at[pl.ds(0, 7)], S('r_sum', 1))
        total = sumr_v[0]
        for i in range(1, 8):
            total = total + sumr_v[i]
        sum_v[0] = total
        copy(sum_v.at[0], sum_out, S('l_small', 0))

    scope = jax.named_scope

    def g_ready(k):
        wait(DY.at[rp, ds(k * BLK, BLK), pl.ds(0, 2 * HB)], S('gd2d', k))

    def g_own(k):
        wait(reg(DY, k, c), S('gd2w', k))

    with scope('g0'):
        g_near_far(0)
    with scope('wuo'):
        wait(wuq(do, 0), S('r_wuy', 2))
        wait(wuq(do, 1), S('r_wuy', 3))
    with scope('u_near'):
        u_near()
    with scope('g12'):
        g_near_far(1)
        g_near_far(2)
    with scope('wd_wait'):
        wait(wd_v.at[pl.ds(0, 2 * FH), pl.ds(0, HB)], S('r_wd', 0))
        for g in range(2):
            for i in range(2, 4):
                wait(wd_bytes(g, QH), S('r_wdy', 4 * g + i))
    with scope('y_give'):
        give('y', A, tile_y, YGOT)
    with scope('g3'):
        g_near_far(3)
    with scope('y_keep'):
        keep_far('y', tile_y, YGOT, YFAR, False)
        keep_own('y', tile_y, YGOT, YKEEP)
    with scope('g_own'):
        loop(NCH, g_own)
    with scope('dwd_0'):
        dwd_pass((0,))
        dwd_opp(0)
    with scope('g_ready'):
        loop(NCH, g_ready)
    with scope('dwd_12'):
        dwd_pass((1, 2))
        dwd_opp(1)
        dwd_opp(2)
    with scope('dwd_a0'):
        dwd_a(0)
    with scope('g_opp'):
        loop(NCH, g_opp)
        loop(NCH, g_opp_got)
    with scope('dwd_3'):
        dwd_pass((3,))
        dwd_opp(3)
    with scope('dwd_a12'):
        dwd_a(1)
        dwd_a(2)
    with scope('da'):
        da_all()
    with scope('d_give'):
        give('d', DU, tile_g, GGOT)
    with scope('dwd_b3'):
        dwd_b(3)
    with scope('gwd_send'):
        gwd_send()
    with scope('far_end_y'):
        for b in range(2):
            for q in range(2):
                far_end('y', b, q)
    with scope('d_keep_far'):
        keep_far('d', tile_g, GGOT, GFAR, True)
    with scope('dwu_01'):
        dwu_pass((do, df))
        dwu_opp()
    with scope('dwu_23'):
        dwu_pass((dn, d))
    with scope('dwu_a'):
        dwu_a()
    with scope('d_keep_own'):
        keep_load(DU)
        stats_load()
        keep_own('d', tile_g, GGOT, GKEEP, stats_part)
        far_put('d', GFAR, 1, 1)
    with scope('gwd_relay'):
        gwd_relay()
    for b in range(2):
        with scope('y_final'):
            y_final(b)
    for b in range(2):
        with scope('place_end_y'):
            place_end('y', b, 0, 1)
        with scope('stats'):
            stats_recv(b)
        for q in range(2):
            if b and q:
                with scope('dwu_b'):
                    dwu_b()
            with scope('dx'):
                dx_final(b, q)
    with scope('sums_1'):
        sums_1()
    with scope('gwu_relay'):
        gwu_relay()
    with scope('sums_2'):
        sums_2()
    with scope('sums_3'):
        sums_3()

    with scope('gwu_end'):
        gwu_end()
    with scope('gwd_end'):
        wait(gwd_out.at[pl.ds(0, 4 * QH), :], S('d_o', 0))
    wait(gwd_out.at[pl.ds(0, 4 * QH), :], S('d_o', 1))
    for p, out in (('y', y_out), ('d', dx_out)):
        @pl.when(r == tau)
        def _():
            with scope('out_end'):
                wait(out.at[pl.ds(0, TH), :], S(p + 'out'))

        @pl.when(r != tau)
        def _():
            with scope('out_end'):
                wait(out, S(p + 'out'))
    wait(sum_out, S('l_small', 0))
    for b in range(2):
        for q in range(2):
            place_end('d', b, q, 2)
            far_end('d', b, q)
    for b in range(2):
        wait(sx_v.at[b], S('s_st', b))
    wait(sum_v.at[1, :, pl.ds(0, 2 * HB)], S('s_sum', 0))
    for i in range(7):
        wait(sumr_v.at[0], S('s_sum', 1 + i))
    wait(wun, S('s_wun'))

    @pl.when(r == f)
    def _():
        for s in range(2):
            wait(wd_own(s), S('s_wd0', s))
    for i in range(4):
        wait(wd_dst(0, c), S('s_wdx', i))
    wait(wu_own, S('s_wu'))
    for i in range(3):
        wait(vec_at, S('s_vec', i))
    wait(bu_at, S('s_vec', 3))
    for s in range(2):
        wait(wd_dst(s, cf), S('s_wdr', s))
    for i in range(2):
        wait(wuq(d), S('s_wuy', i))
        wait(wuq(d, 0), S('s_wuy', 2 + i))
    for i in range(12):
        wait(wdq(0, d, c), S('s_wdy', i))
        wait(wdq(0, d, c, 0), S('s_wdy', 12 + i))

    def sends(k):
        for z, Z in (('x', X), ('g', DY)):
            for n in ('s_near', 's_far', 's_rel'):
                wait(reg(Z, k, c), S(z + n, k))
            wait(Z.at[r, ds(k * BLK, BLK), :], S(z + 's_d2d', k))
    loop(NCH, sends)
    for i in range(8):
        wait(r1D.at[0], S('d_so', i))
        wait(gwd(0, d), S('d_sy', i))
        wait(gwd(0, d, 0), S('d_sr', i))
    for j in range(1, 4):
        wait(finD.at[j], S('d_sf', j))

    @pl.when(r != f)
    def _():
        wait(finD.at[0], S('d_sf', 0))
    for i in range(2):
        wait(r1U, S('u_so', i))
        wait(PFU, S('u_sa', i))
        wait(finU, S('u_sf', i))

    @pl.when(r != dh)
    def _():
        wait(finU, S('u_sf', 2))
    wait(gwu(0, DH), S('u_sr'))


def block_kernel(x, dy, wu, wd, vec, bu):
    (TK, HB), FH = x.shape, wu.shape[1] // 2
    W, HW, TH, BLK, QF, FB = 4 * HB, 2 * HB, TK // 2, TK // NCH, FH // 4, 2 * FH
    assert FB <= W and FH <= HW and W // 4 == BLK and QF <= BLK and FH == HW
    sd = jax.ShapeDtypeStruct
    NS = BLK // min(BLK, 128)
    outs = [sd((TK, HB), BF16), sd((TK, HB), BF16), sd((W // 2, FB), BF16), sd((4 * FH, HB), BF16), sd((1, 3 * HB + FB), F32)]
    n_out = len(outs)
    outs += [sd((2, TK, W), BF16)] * 3 + [sd((2, TK, FB), BF16)] * 2 + [sd((2, TK, FB), F32)]
    outs += [sd((TH, W), F32), sd((TH, HW), F32), sd((TH, HW), F32)] * 2
    outs += [sd((4, QF, HB), F32)] * 2 + [sd((W // 4, FH), F32)] * 2
    V = pltpu.VMEM
    scratch = [
        V((W, FB), BF16), V((FB, W), BF16), V((4, FH, HB), F32), V((4, W // 4, FH), F32),
        V((4, FH // 8, HB), F32), V((4, FH // 8, HB), F32), V((W // 8, FH), F32), V((W // 8, FH), F32),
        V((8, W), F32), V((8, FB), F32), V((4, BLK, W), BF16), V((4, BLK, HW), F32), V((2, BLK, HW), BF16),
        V((4, QF, HB), BF16), V((2, 8, FH), F32), V((2, 8, HW), F32),
        V((BLK, 128), F32), V((2, BLK, 128), F32), V((2, BLK, 128), F32), V((2, 2 * NS, 128), F32), V((2, 2 * NS, 128), F32),
        V((8, HB), F32), V((2, 1, 3 * HB + FB), F32), V((9, 1, 3 * HB + FB), F32),
        pltpu.SemaphoreType.DMA((N_SEM,)),
    ]
    res = pl.pallas_call(
        functools.partial(body, (TK, HB, FH)),
        out_shape=outs,
        in_specs=[pl.BlockSpec(memory_space=pl.ANY)] * 6,
        out_specs=[pl.BlockSpec(memory_space=pl.ANY)] * len(outs),
        scratch_shapes=scratch,
        compiler_params=pltpu.CompilerParams(collective_id=0, has_side_effects=True, vmem_limit_bytes=67043328),
        name='mlp_block',
    )(x, dy, wu, wd, vec, bu)
    return res[:n_out]


def solution(mesh):
    assert (mesh.shape['col'], mesh.shape['row'], mesh.shape['depth']) == (4, 2, 4)
    tok_spec = P(('dp', 'depth', 'row'), 'col')
    vec_spec = P('col')
    mat_spec = P('row', 'col')
    grad_vec = P(('dp', 'col'))
    grad_mat = P(('dp', 'row'), 'col')
    def local_pass(x_blk, gamma_blk, beta_blk, w_up_blk, b_up_blk, w_down_blk, b_down_blk, dy_blk):
        hb, fb = x_blk.shape[1], w_up_blk.shape[1]
        vec = jnp.stack([gamma_blk, beta_blk, b_down_blk.astype(F32)] + [jnp.zeros_like(gamma_blk)] * 5)
        bu = jnp.broadcast_to(b_up_blk.astype(F32)[None], (8, fb))
        y_blk, dx_blk, grad_w_up, grad_w_down, sums = block_kernel(x_blk, dy_blk, w_up_blk, w_down_blk, vec, bu)
        sums = sums[0]
        return (y_blk, dx_blk, sums[:hb], sums[hb:2 * hb], grad_w_up, sums[2 * hb:2 * hb + fb], grad_w_down, sums[2 * hb + fb:])

    return jax.shard_map(
        local_pass,
        mesh=mesh,
        in_specs=(tok_spec, vec_spec, vec_spec, mat_spec, vec_spec, mat_spec, vec_spec, tok_spec),
        out_specs=(tok_spec, tok_spec, grad_vec, grad_vec, grad_mat, grad_vec, grad_mat, grad_vec),
        check_vma=False,
    )
```

```python
import functools

import jax
import jax.numpy as jnp
from jax import lax
from jax.experimental import pallas as pl
from jax.experimental.pallas import tpu as pltpu
from jax.sharding import PartitionSpec as P

LN_EPS = 1e-5
F32 = jnp.float32
BF16 = jnp.bfloat16
MESH = pl.DeviceIdType.MESH
GELU_A = 0.7978845608028654
GELU_B = 0.044715
NCH = 4
ROWS = 16
LROWS = 64
XROWS = 32

NN = (((1,), (0,)), ((), ()))
NT = (((1,), (1,)), ((), ()))
TN = (((0,), (0,)), ((), ()))

SEMS = {}
for _z in ('x', 'g'):
    for _n in ('near', 'far', 'opp', 'd2d', 'd2w', 'd2o', 's_near', 's_far', 's_rel', 's_d2d'):
        SEMS[_z + _n] = NCH
    SEMS[_z + 'bounce'] = 2
for _p in ('y', 'd'):
    SEMS.update({_p + 's_give': 2, _p + 'got': 2, _p + 's_far': 4, _p + 'keep': 2, _p + 'far': 4, _p + 's_out': 8, _p + 'out': 1, _p + 'loc': 4})
SEMS.update(l_wu=1, s_wu=1, r_wu=1, s_wun=1, r_wun=1, s_wuy=4, r_wuy=4,
            s_wd0=2, s_wdx=4, r_wd=4, s_wdr=2, s_wdy=24, r_wdy=8,
            l_vec=2, s_vec=4, r_vec=2,
            ld=8, ldb=2, st=6, s_st=2, r_st=2, s_sum=8, r_sum=2,
            d_so=8, d_r=8, d_sa=8, d_p=8, d_sf=4, d_out=1, d_sy=8, d_y=2, d_sr=8, d_o=2,
            u_so=2, u_r=2, u_sa=2, u_p=2, u_sf=3, u_out=3, u_sr=1, u_o=2, l_small=2)
BASE = {}
_at = 0
for _n, _c in SEMS.items():
    BASE[_n] = _at
    _at += _c
N_SEM = _at


def gelu_and_slope(v):
    v2 = v * v
    t = jnp.tanh(v * (GELU_A + (GELU_A * GELU_B) * v2))
    q = (1.0 - t) * (GELU_A + (3.0 * GELU_A * GELU_B) * v2)
    return 0.5 * v * (1.0 + t), 0.5 * ((1.0 + t) * (1.0 + v * q))


def body(dims, x_ref, dy_ref, wu_ref, wd_ref, vec_ref, bu_ref,
         y_out, dx_out, gwu_out, gwd_out, sum_out,
         X, DY, XN, A, DU, SL, YGOT, YFAR, YKEEP, GGOT, GFAR, GKEEP, PFD, PND, PFU, PNU,
         wu_v, wd_v, accD, accU, r1D, r2D, r1U, r2U, vec_v, bu_v, wx, F4, ob, finD,
         db_v, cs_v, st_v, ms_v, st2_v, sx_v, sr_v, bd_v, sum_v, sumr_v, sem):
    TK, HB, FH = dims
    W, HW, TH, BLK, QF = 4 * HB, 2 * HB, TK // 2, TK // NCH, FH // 4
    RH, DQ, QH, DH, FB = W // 2, W // 4, FH // 8, W // 8, 2 * FH
    NTW = HB
    inv_w = 1.0 / W
    finU = wx.at[3, pl.ds(0, DQ), pl.ds(HW, FH)]
    f0, f1 = F4.at[0], F4.at[1]

    c, r, d = lax.axis_index('col'), lax.axis_index('row'), lax.axis_index('depth')
    c_odd, d_odd = lax.rem(c, 2), lax.rem(d, 2)
    cn, cf, co = c + 1 - 2 * c_odd, 3 - c, lax.rem(c + 2, 4)
    dn, df, do = d + 1 - 2 * d_odd, 3 - d, lax.rem(d + 2, 4)
    f, dh = lax.div(c, 2), lax.div(d, 2)
    tau = lax.rem(lax.div(c + 1, 2), 2)
    rp = 1 - r
    o, o2 = c_odd * FH, (1 - c_odd) * FH

    def S(name, i=0):
        return sem.at[BASE[name] + i]

    def ds(start, size):
        return pl.ds(pl.multiple_of(start, size), size)

    def dsm(start, size, mult):
        return pl.ds(pl.multiple_of(start, mult), size)

    def put(src, dst, ssem, rsem, **dev):
        pltpu.make_async_remote_copy(src_ref=src, dst_ref=dst, send_sem=ssem, recv_sem=rsem,
                                     device_id=dev, device_id_type=MESH).start()

    def copy(src, dst, s):
        pltpu.make_async_copy(src, dst, s).start()

    def wait(ref, s):
        pltpu.make_async_copy(ref, ref, s).wait()

    def loop(n, fn):
        def step(i, carry):
            fn(i)
            return carry
        lax.fori_loop(0, n, step, 0)

    bar = pltpu.get_barrier_semaphore()
    for dev in [dict(row=rp)] + [dict(row=h, **q) for h in range(2) for q in
                                 (dict(col=cn), dict(col=cf), dict(col=co), dict(depth=dn), dict(depth=df), dict(depth=do))]:
        pl.semaphore_signal(bar, inc=1, device_id=dev, device_id_type=MESH)
    pl.semaphore_wait(bar, 13)

    def wd_src(s, h):
        return wd_ref.at[dsm((2 * s + h) * FH + d * QF, QF, QF), :]

    def wd_dst(s, col):
        return wd_v.at[dsm(s * FH + d * QF, QF, QF), ds(col * HB, HB)]

    def reg(Z, k, col):
        return Z.at[r, ds(k * BLK, BLK), ds(col * HB, HB)]

    def send_own(z, z_ref, Z, which, chunks=(0, NCH)):
        def step(k):
            src = z_ref.at[ds(k * BLK, BLK), :]
            if 'near' in which:
                put(src, reg(Z, k, c), S(z + 's_near', k), S(z + 'near', k), col=cn)
            if 'far' in which:
                put(src, reg(Z, k, c), S(z + 's_far', k), S(z + 'far', k), col=cf)
            if 'd2d' in which:
                put(src, reg(Z, k, c), S(z + 's_d2d', k), S(z + ('d2d' if z == 'x' else 'd2w'), k), row=rp)
        for k in range(*chunks):
            step(k)

    def d2d(z, Z, k, col, s):
        put(reg(Z, k, col), reg(Z, k, col), S(z + 's_d2d', k), S(z + s, k), row=rp)

    vec_at = vec_v.at[:, ds(c * HB, HB)]
    copy(vec_ref, vec_at, S('l_vec', 0))
    put(vec_ref, vec_at, S('s_vec', 0), S('r_vec', 0), col=cn)
    put(vec_ref, vec_at, S('s_vec', 1), S('r_vec', 0), col=cf)
    put(vec_ref, vec_at, S('s_vec', 2), S('r_vec', 0), col=co)
    bu_src, bu_at = bu_ref.at[:, ds(r * FH, FH)], bu_v.at[:, ds(o, FH)]
    copy(bu_src, bu_at, S('l_vec', 1))
    put(bu_src, bu_at, S('s_vec', 3), S('r_vec', 1), col=cn)

    wu_own = wu_v.at[ds(r * RH, RH), ds(o, FH)]
    wd_own = lambda s: wd_v.at[pl.ds(s * FH, FH), ds(c * HB, HB)]

    @pl.when(r != f)
    def _():
        for s in range(2):
            for h in range(2):
                put(wd_src(s, h), wd_dst(s, c), S('s_wdx', 2 * s + h), S('r_wd', 2), col=cf, row=h)

    @pl.when(r == f)
    def _():
        for s in range(2):
            for h in range(2):
                put(wd_src(s, h), wd_dst(s, c), S('s_wdx', 2 * s + h), S('r_wd', 1), col=cn, row=h)
    send_own('x', x_ref, X, ('far',), (0, 2))
    send_own('x', x_ref, X, ('near',), (0, 1))
    put(wu_ref.at[:, ds(rp * FH, FH)], wu_own, S('s_wu'), S('r_wu'), row=rp)
    copy(wu_ref.at[:, ds(r * FH, FH)], wu_own, S('l_wu'))
    send_own('x', x_ref, X, ('d2d',))
    send_own('g', dy_ref, DY, ('d2d',))
    for i, z_ref in enumerate((x_ref, dy_ref)):
        for k in range(NCH):
            copy(z_ref.at[pl.ds(k * BLK, BLK), :], wx.at[i, :, pl.ds(k * HB, HB)], S('xg'[i] + 'bounce', 0))

    @pl.when(r == f)
    def _():
        for s in range(2):
            copy(wd_ref.at[dsm((2 * s + r) * FH, FH, FH), :], wd_own(s), S('r_wd', 0))
            put(wd_ref.at[dsm((2 * s + rp) * FH, FH, FH), :], wd_own(s), S('s_wd0', s), S('r_wd', 0), row=rp)

    for i, Z in enumerate((X, DY)):
        wait(wx.at[i], S('xg'[i] + 'bounce', 0))
        for k in range(NCH):
            copy(wx.at[i, :, pl.ds(k * HB, HB)], reg(Z, k, c), S('xg'[i] + 'bounce', 1))

    with jax.named_scope('wd_far'):
        wait(wd_v.at[pl.ds(0, 2 * QF), pl.ds(0, HB)], S('r_wd', 2))
    for s in range(2):
        put(wd_dst(s, cf), wd_dst(s, cf), S('s_wdr', s), S('r_wd', 3), col=cn)
    send_own('x', x_ref, X, ('near',), (1, NCH - 1))

    with jax.named_scope('wu_own'):
        wait(wu_own, S('l_wu'))
        wait(wu_v.at[ds(rp * RH, RH), ds(o, FH)], S('r_wu'))
    wun = wu_v.at[ds(d * DQ, DQ), ds(o, FH)]
    put(wun, wun, S('s_wun'), S('r_wun'), col=cn)
    send_own('x', x_ref, X, ('near',), (NCH - 1, NCH))

    db_v[...] = jnp.zeros_like(db_v)
    cs_v[...] = jnp.zeros_like(cs_v)
    bd_v[...] = jnp.zeros_like(bd_v)

    def dy_sum(i):
        rr = ds(i * ROWS, ROWS)
        part = jnp.sum(wx[1, rr, :].astype(F32).reshape(ROWS // 8, 8, W), axis=0)
        bd_v[...] += part[:, :HB] + part[:, HB:2 * HB] + part[:, 2 * HB:3 * HB] + part[:, 3 * HB:]
    with jax.named_scope('dy_sum'):
        loop(BLK // ROWS, dy_sum)

    def wuq(dd, half=None):
        if half is None:
            return wu_v.at[ds(dd * DQ, DQ), ds(o2, FH)]
        return wu_v.at[dsm(dd * DQ + half * DH, DH, DH), ds(o2, FH)]

    def wu_send():
        with jax.named_scope('wu_near'):
            wait(wuq(d), S('r_wun'))
        put(wuq(d), wuq(d), S('s_wuy', 0), S('r_wuy', 0), depth=dn)
        put(wuq(d), wuq(d), S('s_wuy', 1), S('r_wuy', 1), depth=df)

    def wu_relay():
        with jax.named_scope('wuy'):
            wait(wuq(dn), S('r_wuy', 0))
            wait(wuq(df), S('r_wuy', 1))
        put(wuq(dn, 1), wuq(dn, 1), S('s_wuy', 2), S('r_wuy', 3), depth=df)
        put(wuq(df, 0), wuq(df, 0), S('s_wuy', 3), S('r_wuy', 2), depth=dn)

    def wdq(s, dd, col, half=None):
        if half is None:
            return wd_v.at[dsm(s * FH + dd * QF, QF, QF), ds(col * HB, HB)]
        return wd_v.at[dsm(s * FH + dd * QF + half * QH, QH, QH), ds(col * HB, HB)]

    W_GROUPS = (((0, cn), (1, cf)), ((2, co),))

    def wd_send(g):
        if g == 0:
            wait(wd_v.at[pl.ds(0, 2 * QF), pl.ds(0, HB)], S('r_wd', 1))
        else:
            wait(wd_v.at[pl.ds(0, 2 * QF), pl.ds(0, HB)], S('r_wd', 3))
        for i, col in W_GROUPS[g]:
            for s in range(2):
                put(wdq(s, d, col), wdq(s, d, col), S('s_wdy', 4 * i + s), S('r_wdy', 4 * g), depth=dn)
                put(wdq(s, d, col), wdq(s, d, col), S('s_wdy', 4 * i + 2 + s), S('r_wdy', 4 * g + 1), depth=df)

    def wd_bytes(g, rows):
        return wd_v.at[pl.ds(0, 2 * rows), pl.ds(0, len(W_GROUPS[g]) * HB)]

    def wd_relay(g):
        for i in range(2):
            wait(wd_bytes(g, QF), S('r_wdy', 4 * g + i))
        for i, col in W_GROUPS[g]:
            for s in range(2):
                put(wdq(s, dn, col, 1), wdq(s, dn, col, 1), S('s_wdy', 12 + 4 * i + s), S('r_wdy', 4 * g + 3), depth=df)
                put(wdq(s, df, col, 0), wdq(s, df, col, 0), S('s_wdy', 12 + 4 * i + 2 + s), S('r_wdy', 4 * g + 2), depth=dn)

    def x_near(k):
        wait(reg(X, k, cn), S('xnear', k))
        put(reg(X, k, cn), reg(X, k, cn), S('xs_rel', k), S('xopp', k), col=cf)
        d2d('x', X, k, cn, 'd2d')

    with jax.named_scope('wd_send0'):
        wd_send(0)
    with jax.named_scope('x_near'):
        x_near(0)
    send_own('x', x_ref, X, ('far',), (2, 3))

    for i, Z in enumerate((X, DY)):
        wait(wx.at[i], S('xg'[i] + 'bounce', 1))
    wait(vec_at, S('l_vec', 0))
    wait(vec_v.at[:, pl.ds(0, 3 * HB)], S('r_vec', 0))
    wait(bu_at, S('l_vec', 1))
    wait(bu_at, S('r_vec', 1))

    def norm_rows(buf, rows):
        xf = buf[rows, :].astype(F32)
        mean = jnp.sum(xf, axis=1, keepdims=True) * inv_w
        cen = xf - mean
        inv = lax.rsqrt(jnp.sum(cen * cen, axis=1, keepdims=True) * inv_w + LN_EPS)
        return cen, mean, inv

    def tok_of(s):
        return tau + s * (1 - 2 * tau)

    N_T = FH // NTW

    def chain(tiles, hooks=None):
        hooks = hooks or {}

        def hook(what, i):
            for fn in hooks.get((what, i), ()):
                fn()
        for i, (product, _) in enumerate(tiles):
            hook('before', i)
            if i:
                tiles[i - 1][1](F4.at[(i - 1) % 2])
            F4[i % 2, :, :NTW] = product()
            hook('product', i)
            if i:
                hook('epilogue', i - 1)
        tiles[-1][1](F4.at[(len(tiles) - 1) % 2])
        hook('epilogue', len(tiles) - 1)

    def u_tile(src, i, n, start):
        cols = ds(start + n * NTW, NTW)
        at = pl.ds(n * NTW, NTW)

        def product():
            return lax.dot_general(wx[src], wu_v[:, cols], NN, preferred_element_type=F32)

        def epilogue(acc):
            u = (acc[:, :NTW] + bu_v[0:1, cols]).astype(BF16)
            a, slope = gelu_and_slope(u.astype(F32))
            ob[i, :, at] = a.astype(BF16)
            F4[2 + i, :, at] = slope
        return product, epilogue

    def u_store(i, s, rows, start):
        copy(ob.at[i], A.at[s, rows, ds(start, FH)], S('st', 2 + i))
        copy(F4.at[2 + i], SL.at[s, rows, ds(start, FH)], S('st', 4 + i))

    def u_stored():
        for i in range(2):
            wait(ob.at[i], S('st', 2 + i))
            wait(F4.at[2 + i], S('st', 4 + i))

    def phase1(k):
        @pl.when(k < NCH - 1)
        def _():
            with jax.named_scope('x_near'):
                x_near(k + 1)

        @pl.when(k == 0)
        def _():
            send_own('x', x_ref, X, ('far',), (3, 4))
            with jax.named_scope('wd_send1'):
                wd_send(1)

        @pl.when(k == 1)
        def _():
            with jax.named_scope('wd_relay0'):
                wd_relay(0)
            send_own('g', dy_ref, DY, ('near',))

        @pl.when(k == 2)
        def _():
            send_own('g', dy_ref, DY, ('far',))
            wu_send()
            with jax.named_scope('wd_relay1'):
                wd_relay(1)

        with jax.named_scope('x_far'):
            wait(reg(X, k, cf), S('xfar', k))
            d2d('x', X, k, cf, 'd2d')
        with jax.named_scope('x_opp'):
            wait(reg(X, k, co), S('xopp', k))
            d2d('x', X, k, co, 'd2d')

        rows = ds(k * BLK, BLK)
        with jax.named_scope('x_d2d'):
            wait(X.at[rp, rows, :], S('xd2d', k))

        @pl.when(k == NCH - 1)
        def _():
            wu_relay()

        @pl.when(k > 0)
        def _():
            for s in range(2):
                wait(wx.at[s], S('st', s))
        for s in range(2):
            copy(X.at[tok_of(s), rows, :], wx.at[s], S('ld', s))
        for s in range(2):
            wait(wx.at[s], S('ld', s))

            def ln(i):
                rr = ds(i * LROWS, LROWS)
                cen, _, inv = norm_rows(wx.at[s], rr)
                wx[s, rr, :] = (cen * inv * vec_v[0:1, :] + vec_v[1:2, :]).astype(BF16)
            with jax.named_scope('ln'):
                loop(BLK // LROWS, ln)
            copy(wx.at[s], XN.at[s, rows, :], S('st', s))
        pl.when(k > 0)(u_stored)
        with jax.named_scope('u_own'):
            chain([u_tile(i, i, n, o) for i in range(2) for n in range(N_T)])
        for s in range(2):
            u_store(s, s, rows, o)
    loop(NCH, phase1)
    for s in range(2):
        wait(wx.at[s], S('st', s))
    u_stored()

    def u_near_load():
        for b in range(NCH):
            copy(XN.at[0, pl.ds(b * BLK, BLK), :], wx.at[b], S('ld', b))

    def u_near():
        def step(kp):
            for i in range(2):
                wait(wx.at[2 * kp + i], S('ld', 2 * kp + i))
            chain([u_tile(2 * kp + i, i, n, o2) for i in range(2) for n in range(N_T)],
                  {('before', 1): [lambda: pl.when(kp > 0)(u_stored)]})
            for i in range(2):
                u_store(i, 0, ds((2 * kp + i) * BLK, BLK), o2)
        loop(NCH // 2, step)
        u_stored()

    def g_near_far(k):
        wait(reg(DY, k, cf), S('gfar', k))
        put(reg(DY, k, cf), reg(DY, k, cf), S('gs_rel', k), S('gopp', k), col=cn)
        d2d('g', DY, k, cf, 'd2d')
        wait(reg(DY, k, cn), S('gnear', k))
        d2d('g', DY, k, cn, 'd2d')

    def g_opp(k):
        wait(reg(DY, k, co), S('gopp', k))
        d2d('g', DY, k, co, 'd2o')

    def g_opp_got(k):
        wait(reg(DY, k, co), S('gd2o', k))

    def tile_y(lhs, col):
        return lax.dot_general(lhs, wd_v[:, dsm(col, NTW, NTW)], NN, preferred_element_type=F32)

    def tile_g(lhs, col):
        return lax.dot_general(lhs, wu_v[dsm(col, NTW, NTW), :], NT, preferred_element_type=F32)

    def give(p, src, tile, GOT):
        def blk(b):
            return src.at[0, dsm(rp * TH + b * BLK, BLK, BLK), :]
        for b in range(2):
            copy(blk(b), wx.at[b, :, pl.ds(0, FB)], S('ld', b))
        keep_load(src)

        def step(b):
            wait(wx.at[b, :, pl.ds(0, FB)], S('ld', b))

            def half(h):
                @pl.when(b == 1)
                def _():
                    wait(F4.at[h], S(p + 's_give', h))

                def n_tile(n):
                    F4[h, :, ds(n * NTW, NTW)] = tile(wx[b, :, :FB], h * HW + n * NTW)
                loop(HW // NTW, n_tile)
                put(F4.at[h], GOT.at[ds(b * BLK, BLK), ds(h * HW, HW)], S(p + 's_give', h), S(p + 'got', b), row=rp)
            loop(2, half)
        loop(2, step)

    HB2 = BLK // 2

    def keep_load(src):
        for b in range(2):
            copy(src.at[0, dsm(r * TH + b * BLK, BLK, BLK), :], wx.at[2 + b, :, pl.ds(0, FB)], S('ld', 2 + b))

    def got_load(GOT, b, col0, out, s_):
        copy(GOT.at[ds(b * BLK, BLK), ds(col0, HW)], F4.at[out], s_)

    def add_tiles(b, out, tile, col0):
        def n_tile(n):
            at = ds(n * NTW, NTW)
            F4[out, :, at] = F4[out, :, at] + tile(wx[2 + b, :, :FB], col0 + n * NTW)
        loop(HW // NTW, n_tile)

    def far_put(p, FAR, b, q):
        put(F4.at[2 + b, ds(q * HB2, HB2), :], FAR.at[ds(b * BLK + q * HB2, HB2), :], S(p + 's_far', 2 * b + q), S(p + 'far', 2 * b + q), col=cf)

    def give_end(p):
        for h in range(2):
            wait(F4.at[h], S(p + 's_give', h))

    def keep_far(p, tile, GOT, FAR, b, pieces):
        with jax.named_scope('got'):
            wait(GOT.at[ds(b * BLK, BLK), :], S(p + 'got', b))
        got_load(GOT, b, (1 - f) * HW, 2 + b, S('ld', 4 + b))
        wait(wx.at[2 + b, :, pl.ds(0, FB)], S('ld', 2 + b))
        wait(F4.at[2 + b], S('ld', 4 + b))
        add_tiles(b, 2 + b, tile, (1 - f) * HW)
        for q in range(pieces):
            far_put(p, FAR, b, q)

    def keep_own(p, src, tile, GOT, KEEP, after=None):
        keep_load(src)
        for b in range(2):
            got_load(GOT, b, f * HW, 1 - b, S('ld', 4 + b))

        def step(b):
            wait(wx.at[2 + b, :, pl.ds(0, FB)], S('ld', 2 + b))
            wait(F4.at[1 - b], S('ld', 4 + b))
            add_tiles(b, 1 - b, tile, f * HW)
            copy(F4.at[1 - b], KEEP.at[ds(b * BLK, BLK), :], S(p + 'keep', b))
            if after:
                after(b)
        loop(2, step)
        for b in range(2):
            wait(F4.at[b], S(p + 'keep', b))

    def far_end(p, b, q):
        wait(F4.at[2 + b, ds(q * HB2, HB2), :], S(p + 's_far', 2 * b + q))

    def place(p, out, b, q, nq):
        nr = BLK // nq
        rr = ds(q * nr, nr)
        dst = out.at[dsm(r * TH + b * BLK + q * nr, nr, nr), :]
        mine, other = ob.at[b, rr, ds(c_odd * HB, HB)], ob.at[b, rr, ds((1 - c_odd) * HB, HB)]
        put(other, dst, S(p + 's_out', 4 * b + 2 * q), S(p + 'out'), col=cn, row=tau)

        @pl.when(r == tau)
        def _():
            copy(mine, dst, S(p + 'loc', 2 * b + q))

        @pl.when(r != tau)
        def _():
            put(mine, dst, S(p + 's_out', 4 * b + 2 * q + 1), S(p + 'out'), row=rp)

    def place_end(p, b, q, nq):
        part = ob.at[b, pl.ds(0, BLK // nq), pl.ds(0, HB)]
        wait(part, S(p + 's_out', 4 * b + 2 * q))

        @pl.when(r == tau)
        def _():
            wait(part, S(p + 'loc', 2 * b + q))

        @pl.when(r != tau)
        def _():
            wait(part, S(p + 's_out', 4 * b + 2 * q + 1))

    fcols = ds(f * HW, HW)

    def y_final(b):
        brow = ds(b * BLK, BLK)
        for q in range(2):
            wait(YFAR.at[ds(b * BLK + q * HB2, HB2), :], S('yfar', 2 * b + q))
        copy(YFAR.at[brow, :], f0, S('ld', 0))
        copy(YKEEP.at[brow, :], f1, S('ld', 1))
        copy(X.at[tau, dsm(r * TH + b * BLK, BLK, BLK), fcols], wx.at[0, :, pl.ds(0, HW)], S('ld', 2))
        wait(f0, S('ld', 0))
        wait(f1, S('ld', 1))
        wait(wx.at[0, :, pl.ds(0, HW)], S('ld', 2))

        def fin(i):
            rr = ds(i * ROWS, ROWS)
            ob[b, rr, :] = (wx[0, rr, :HW].astype(F32) + (f0[rr, :] + f1[rr, :]) + vec_v[2:3, fcols]).astype(BF16)
        loop(BLK // ROWS, fin)
        place('y', y_out, b, 0, 1)

    def services(t):
        @pl.when(t == 3)
        def _():
            with jax.named_scope('dwd_a3'):
                dwd_a(3)

    def da_all():
        def part(t, i):
            near = lax.div(t, NCH)
            tok = tau + i * (1 - near) * (1 - 2 * tau)
            chunk = t * (1 - near) + near * (2 * (t - NCH) + i)
            return near, tok, i * (1 - near), ds(chunk * BLK, BLK), near * o2 + (1 - near) * o

        def load(t, p):
            for i in range(2):
                _, tok, us, rows, start = part(t, i)
                copy(DY.at[tok, rows, :], wx.at[2 * p + i], S('ld', 2 * p + i))
                copy(SL.at[us, rows, ds(start, FH)], accU.at[2 * p + i], S('ld', 4 + 2 * p + i))

        def store(t, i):
            _, _, us, rows, start = part(t, i)
            copy(ob.at[i], DU.at[us, rows, ds(start, FH)], S('st', 4 + i))

        def stored():
            for i in range(2):
                wait(ob.at[i], S('st', 4 + i))

        n_steps = NCH + NCH // 2

        def step(t):
            near, _, _, _, start = part(t, 0)
            p = lax.rem(t, 2)
            services(t)
            for i in range(2):
                wait(wx.at[2 * p + i], S('ld', 2 * p + i))
                wait(accU.at[2 * p + i], S('ld', 4 + 2 * p + i))

            @pl.when(t < n_steps - 1)
            def _():
                load(t + 1, 1 - p)

            def tile(i, n):
                cols = ds(start + n * NTW, NTW)
                at = pl.ds(n * NTW, NTW)

                def product():
                    return lax.dot_general(wx[2 * p + i], wd_v[cols, :], NT, preferred_element_type=F32)

                def epilogue(acc):
                    du = (acc[:, :NTW] * accU[2 * p + i, :, at]).astype(BF16)
                    ob[i, :, at] = du
                    db_v[near, :, at] += jnp.sum(du.astype(F32).reshape(BLK // 8, 8, NTW), axis=0)
                return product, epilogue
            chain([tile(i, n) for i in range(2) for n in range(N_T)], {('before', 1): [lambda: pl.when(t > 0)(stored)]})
            for i in range(2):
                store(t, i)
        load(0, 0)
        loop(n_steps, step)
        stored()

    def rows_of(kb):
        return ds(lax.rem(kb, NCH) * BLK, BLK), lax.div(kb, NCH)

    d_col = (c, cn, cf, co)

    NB, NSLOT = 2 * NCH, 4

    def k_loop(load, use, width):
        for kb in range(NSLOT - 1):
            load(kb, wx.at[kb], S('ld', kb))

        def step(kb):
            slot = lax.rem(kb, NSLOT)

            @pl.when(kb + NSLOT - 1 < NB)
            def _():
                nxt = lax.rem(kb + NSLOT - 1, NSLOT)
                load(kb + NSLOT - 1, wx.at[nxt], S('ld', nxt))
            buf = wx.at[slot]
            wait(buf.at[:, pl.ds(0, width)], S('ld', slot))
            use(buf)
        loop(NB, step)

    def dwd_pass(js):
        def load(kb, buf, s_):
            rows, s = rows_of(kb)
            copy(A.at[s, rows, ds(o, FH)], buf.at[:, pl.ds(0, FH)], s_)
            for i, j in enumerate(js):
                copy(DY.at[tok_of(s), rows, ds(d_col[j] * HB, HB)], buf.at[:, pl.ds(FH + i * HB, HB)], s_)

        def use(buf):
            for i, j in enumerate(js):
                for m in range(2):
                    mm = slice(m * FH // 2, (m + 1) * FH // 2)
                    accD[j, mm, :] += lax.dot_general(buf[:, mm], buf[:, FH + i * HB:FH + (i + 1) * HB], TN, preferred_element_type=F32)
        for j in js:
            accD[j] = jnp.zeros((FH, HB), F32)
        k_loop(load, use, FH + len(js) * HB)

    def dwd_opp(j):
        put(accD.at[j, dsm(do * QF, QH, QH), :], r1D.at[j], S('d_so', 2 * j), S('d_r', 2 * j), depth=dn)
        put(accD.at[j, dsm(do * QF + QH, QH, QH), :], r2D.at[j], S('d_so', 2 * j + 1), S('d_r', 2 * j + 1), depth=df)

    def dwd_a(j):
        wait(r1D.at[j], S('d_r', 2 * j))
        rr = dsm(df * QF, QH, QH)
        accD[j, rr, :] += r1D[j]
        put(accD.at[j, ds(df * QF, QF), :], PFD.at[j], S('d_sa', 2 * j), S('d_p', 2 * j), depth=df)
        wait(r2D.at[j], S('d_r', 2 * j + 1))
        rr = dsm(dn * QF + QH, QH, QH)
        accD[j, rr, :] += r2D[j]
        put(accD.at[j, ds(dn * QF, QF), :], PND.at[j], S('d_sa', 2 * j + 1), S('d_p', 2 * j + 1), depth=dn)

    def dwd_rows(q, h, dd):
        return dsm((2 * q + h) * FH + dd * QF, QF, QF)

    def dwd_b(j):
        wait(PFD.at[j], S('d_p', 2 * j))
        wait(PND.at[j], S('d_p', 2 * j + 1))
        wait(PFD.at[j], S('d_sa', 2 * j))
        wait(PND.at[j], S('d_sa', 2 * j + 1))
        pf, pn = accD.at[j, ds(df * QF, QF), :], accD.at[j, ds(dn * QF, QF), :]
        copy(PFD.at[j], pf, S('ldb', 0))
        copy(PND.at[j], pn, S('ldb', 1))
        wait(pf, S('ldb', 0))
        wait(pn, S('ldb', 1))
        finD[j] = (accD[j, ds(d * QF, QF), :] + (pf[...] + pn[...])).astype(BF16)
        dst = gwd_out.at[dwd_rows(c_odd, r, d), :]
        if j:
            put(finD.at[j], dst, S('d_sf', j), S('d_out'), col=d_col[j], row=f)
        else:
            @pl.when(r == f)
            def _():
                copy(finD.at[0], dst, S('d_out'))

            @pl.when(r != f)
            def _():
                put(finD.at[0], dst, S('d_sf', 0), S('d_out'), row=rp)

    def gwd(i, dd, half=None):
        if half is None:
            return gwd_out.at[dsm(i * FH + dd * QF, QF, QF), :]
        return gwd_out.at[dsm(i * FH + dd * QF + half * QH, QH, QH), :]

    def gwd_send():
        wait(gwd_out.at[pl.ds(0, 4 * QF), :], S('d_out'))
        for i in range(4):
            put(gwd(i, d), gwd(i, d), S('d_sy', i), S('d_y', 0), depth=dn)
            put(gwd(i, d), gwd(i, d), S('d_sy', 4 + i), S('d_y', 1), depth=df)

    def gwd_relay():
        wait(gwd_out.at[pl.ds(0, 4 * QF), :], S('d_y', 0))
        for i in range(4):
            put(gwd(i, dn, 1), gwd(i, dn, 1), S('d_sr', i), S('d_o', 1), depth=df)
        wait(gwd_out.at[pl.ds(0, 4 * QF), :], S('d_y', 1))
        for i in range(4):
            put(gwd(i, df, 0), gwd(i, df, 0), S('d_sr', 4 + i), S('d_o', 0), depth=dn)

    def dwu_pass(dds):
        def load(kb, buf, s_):
            rows, s = rows_of(kb)
            copy(DU.at[s, rows, ds(o, FH)], buf.at[:, pl.ds(0, FH)], s_)
            for i, dd in enumerate(dds):
                copy(XN.at[s, rows, ds(dd * DQ, DQ)], buf.at[:, pl.ds(FH + i * DQ, DQ)], s_)

        def use(buf):
            for i, dd in enumerate(dds):
                for m in range(2):
                    mm = slice(m * FH // 2, (m + 1) * FH // 2)
                    accU[dd, :, mm] += lax.dot_general(buf[:, FH + i * DQ:FH + (i + 1) * DQ], buf[:, mm], TN, preferred_element_type=F32)
        for dd in dds:
            accU[dd] = jnp.zeros((DQ, FH), F32)
        k_loop(load, use, FH + len(dds) * DQ)

    def dwu_opp():
        put(accU.at[do, pl.ds(0, DH), :], r1U, S('u_so', 0), S('u_r', 0), depth=dn)
        put(accU.at[do, pl.ds(DH, DH), :], r2U, S('u_so', 1), S('u_r', 1), depth=df)

    def dwu_a():
        wait(r1U, S('u_r', 0))
        accU[df, :DH, :] += r1U[...]
        put(accU.at[df], PFU, S('u_sa', 0), S('u_p', 0), depth=df)
        wait(r2U, S('u_r', 1))
        accU[dn, DH:, :] += r2U[...]
        put(accU.at[dn], PNU, S('u_sa', 1), S('u_p', 1), depth=dn)

    def dwu_b():
        wait(PFU, S('u_p', 0))
        wait(PNU, S('u_p', 1))
        pf, pn = f0.at[pl.ds(0, DQ), pl.ds(0, FH)], f1.at[pl.ds(0, DQ), pl.ds(0, FH)]
        copy(PFU, pf, S('ldb', 0))
        copy(PNU, pn, S('ldb', 1))
        wait(pf, S('ldb', 0))
        wait(pn, S('ldb', 1))

        def fin(i):
            rr = ds(i * ROWS, ROWS)
            wx[3, rr, HW:HW + FH] = (accU[d, rr, :] + (f0[rr, :FH] + f1[rr, :FH])).astype(BF16)
        loop(DQ // ROWS, fin)
        dst = gwu_out.at[ds(d_odd * DQ, DQ), ds(r * FH, FH)]
        put(finU, dst, S('u_sf', 0), S('u_out', 1), depth=dn, row=dh)
        put(finU, dst, S('u_sf', 1), S('u_out', 2), depth=df, row=dh)

        @pl.when(r == dh)
        def _():
            copy(finU, dst, S('u_out', 0))

        @pl.when(r != dh)
        def _():
            put(finU, dst, S('u_sf', 2), S('u_out', 0), row=rp)

    def gwu(start, size):
        return gwu_out.at[dsm(start, size, size), :]

    def gwu_relay():
        @pl.when(r == dh)
        def _():
            wait(gwu(lax.rem(dn, 2) * DQ, DQ), S('u_out', 1))
            part = gwu(lax.rem(dn, 2) * DQ + DH, DH)
            put(part, part, S('u_sr'), S('u_o', 1), depth=df)

        @pl.when(r != dh)
        def _():
            wait(gwu(lax.rem(df, 2) * DQ, DQ), S('u_out', 2))
            part = gwu(lax.rem(df, 2) * DQ, DH)
            put(part, part, S('u_sr'), S('u_o', 0), depth=dn)

    def gwu_end():
        @pl.when(r == dh)
        def _():
            wait(gwu(d_odd * DQ, DQ), S('u_out', 0))

        @pl.when(r != dh)
        def _():
            wait(gwu(0, DH), S('u_o', 0))
            wait(gwu(0, DH), S('u_o', 1))

    lane = lax.broadcasted_iota(jnp.int32, (LROWS, 128), 1)

    SB = min(BLK, 128)
    NS = BLK // SB

    def stats_load():
        for b in range(2):
            copy(X.at[tau, dsm(r * TH + b * BLK, BLK, BLK), :], wx.at[b], S('ld', b))

    def stats_part(b):
        wait(wx.at[b], S('ld', b))

        def rows_step(i):
            rr = ds(i * LROWS, LROWS)
            _, mean, inv = norm_rows(wx.at[b], rr)
            s0, s1 = jnp.zeros((LROWS, 1), F32), jnp.zeros((LROWS, 1), F32)
            for col0, slot in ((f * HW, 1 - b), ((1 - f) * HW, 2 + b)):
                cols = ds(col0, HW)
                gh = F4[slot, rr, :] * vec_v[0:1, cols]
                s0 = s0 + jnp.sum(gh, axis=1, keepdims=True)
                s1 = s1 + jnp.sum(gh * ((wx[b, rr, cols].astype(F32) - mean) * inv), axis=1, keepdims=True)
            st_v[rr, :] = jnp.where(lane < 64, s0, s1)
            ms_v[b, rr, :] = jnp.where(lane < 64, mean, inv)
        loop(BLK // LROWS, rows_step)
        for t in range(NS):
            tr = st_v[t * SB:(t + 1) * SB, :].T
            sx_v[b, t:t + 1, :SB] = tr[0:1, :]
            sx_v[b, NS + t:NS + t + 1, :SB] = tr[64:65, :]
        put(sx_v.at[b], sr_v.at[b], S('s_st', b), S('r_st', b), col=cf)

    def stats_recv(b):
        wait(sr_v.at[b], S('r_st', b))
        for t in range(NS):
            for i in range(2):
                row = (sx_v[b, i * NS + t:i * NS + t + 1, :SB] + sr_v[b, i * NS + t:i * NS + t + 1, :SB]) * inv_w
                st2_v[i, t * SB:(t + 1) * SB, :] = jnp.broadcast_to(row, (128, SB)).T

    def dx_final(b, q):
        sub = ds(q * HB2, HB2)
        brow = ds(b * BLK + q * HB2, HB2)
        trow = dsm(r * TH + b * BLK + q * HB2, HB2, HB2)
        xb, gb = wx.at[b, sub, pl.ds(0, HW)], wx.at[2 + b, sub, pl.ds(0, HW)]
        copy(GKEEP.at[brow, :], F4.at[1, sub, :], S('ld', 1))
        copy(X.at[tau, trow, fcols], xb, S('ld', 2))
        copy(DY.at[tau, trow, fcols], gb, S('ld', 3))
        with jax.named_scope('d_far'):
            wait(GFAR.at[brow, :], S('dfar', 2 * b + q))
        copy(GFAR.at[brow, :], F4.at[0, sub, :], S('ld', 0))
        wait(F4.at[1, sub, :], S('ld', 1))
        wait(xb, S('ld', 2))
        wait(gb, S('ld', 3))
        wait(F4.at[0, sub, :], S('ld', 0))

        def rows_step(i):
            rr = dsm(q * HB2 + i * XROWS, XROWS, XROWS)
            mean, inv = ms_v[b, rr, 0:1], ms_v[b, rr, 64:65]
            xhat = (wx[b, rr, :HW].astype(F32) - mean) * inv
            dxn = F4[0, rr, :] + F4[1, rr, :]
            gh = dxn * vec_v[0:1, fcols]
            dx = wx[2 + b, rr, :HW].astype(F32) + inv * (gh - st2_v[0, rr, 0:1] - xhat * st2_v[1, rr, 0:1])
            ob[b, rr, :] = dx.astype(BF16)
            cs_v[0] += jnp.sum((dxn * xhat).reshape(XROWS // 8, 8, HW), axis=0)
            cs_v[1] += jnp.sum(dxn.reshape(XROWS // 8, 8, HW), axis=0)
        loop(HB2 // XROWS, rows_step)
        place('d', dx_out, b, q, 2)

    me = 2 * d + r
    peers = [dict(row=rp)] + [dict(depth=q, row=h) for q in (dn, df, do) for h in range(2)]
    near_in = sumr_v.at[8, :, pl.ds(0, 2 * HB)]

    def sums_1():
        cw = jnp.sum(cs_v[...], axis=1)
        for i in range(2):
            for q in range(2):
                @pl.when(c_odd == q)
                def _():
                    sum_v[0, :, i * HB:(i + 1) * HB] = cw[i:i + 1, q * HB:(q + 1) * HB]
                    sum_v[1, :, i * HB:(i + 1) * HB] = cw[i:i + 1, (1 - q) * HB:(2 - q) * HB]
        put(sum_v.at[1, :, pl.ds(0, 2 * HB)], near_in, S('s_sum', 0), S('r_sum', 0), col=cn)
        sum_v[0, :, 2 * HB:2 * HB + FB] = jnp.zeros((1, FB), F32)
        sum_v[0, :, dsm(2 * HB + r * FH, FH, HB)] = jnp.sum(db_v[0], axis=0, keepdims=True)
        sum_v[0, :, 2 * HB + FB:] = jnp.sum(bd_v[...], axis=0, keepdims=True)

    def sums_2():
        wait(near_in, S('r_sum', 0))
        sumr_v[me, :, :2 * HB] = sum_v[0, :, :2 * HB] + sumr_v[8, :, :2 * HB]
        sumr_v[me, :, 2 * HB:] = sum_v[0, :, 2 * HB:]
        for i, dev in enumerate(peers):
            put(sumr_v.at[me], sumr_v.at[me], S('s_sum', 1 + i), S('r_sum', 1), **dev)

    def sums_3():
        wait(sumr_v.at[pl.ds(0, 7)], S('r_sum', 1))
        total = sumr_v[0]
        for i in range(1, 8):
            total = total + sumr_v[i]
        sum_v[0] = total
        copy(sum_v.at[0], sum_out, S('l_small', 0))

    scope = jax.named_scope

    def g_ready(k):
        wait(DY.at[rp, ds(k * BLK, BLK), pl.ds(0, 2 * HB)], S('gd2d', k))

    def g_own(k):
        wait(reg(DY, k, c), S('gd2w', k))

    with scope('g0'):
        g_near_far(0)
    with scope('g_own'):
        loop(NCH, g_own)
    with scope('dwd_0'):
        dwd_pass((0,))
        dwd_opp(0)
    u_near_load()
    with scope('wuo'):
        wait(wuq(do, 0), S('r_wuy', 2))
        wait(wuq(do, 1), S('r_wuy', 3))
    with scope('u_near'):
        u_near()
    with scope('g12'):
        g_near_far(1)
        g_near_far(2)
    with scope('dwd_a0'):
        dwd_a(0)
    with scope('wd_wait'):
        wait(wd_v.at[pl.ds(0, 2 * FH), pl.ds(0, HB)], S('r_wd', 0))
        for g in range(2):
            for i in range(2, 4):
                wait(wd_bytes(g, QH), S('r_wdy', 4 * g + i))
    with scope('y_give'):
        give('y', A, tile_y, YGOT)
    with scope('g3'):
        g_near_far(3)
    with scope('y_keep_far'):
        keep_far('y', tile_y, YGOT, YFAR, 0, 2)
        keep_far('y', tile_y, YGOT, YFAR, 1, 2)
        give_end('y')
    with scope('g_ready'):
        loop(NCH, g_ready)
    with scope('dwd_12'):
        dwd_pass((1, 2))
        dwd_opp(1)
        dwd_opp(2)
    with scope('g_opp'):
        loop(NCH, g_opp)
        loop(NCH, g_opp_got)
    with scope('dwd_3'):
        dwd_pass((3,))
        dwd_opp(3)
    with scope('dwd_a12'):
        dwd_a(1)
        dwd_a(2)
    with scope('dwd_b0'):
        dwd_b(0)
    with scope('da'):
        da_all()
    with scope('dwd_b12'):
        dwd_b(1)
        dwd_b(2)
    with scope('d_give'):
        give('d', DU, tile_g, GGOT)
    with scope('dwd_b3'):
        dwd_b(3)
    with scope('gwd_send'):
        gwd_send()
    with scope('d_keep_far0'):
        for q in range(2):
            far_end('y', 0, q)
        keep_far('d', tile_g, GGOT, GFAR, 0, 2)
        wait(wx.at[3, :, pl.ds(0, FB)], S('ld', 3))
        give_end('d')
    with scope('dwu_01'):
        dwu_pass((do, df))
        dwu_opp()
    with scope('d_keep_far1'):
        copy(DU.at[0, dsm(r * TH + BLK, BLK, BLK), :], wx.at[3, :, pl.ds(0, FB)], S('ld', 3))
        for q in range(2):
            far_end('y', 1, q)
        keep_far('d', tile_g, GGOT, GFAR, 1, 1)
    with scope('dwu_23'):
        dwu_pass((dn, d))
    with scope('dwu_a'):
        dwu_a()
    with scope('d_keep_own'):
        stats_load()
        keep_own('d', DU, tile_g, GGOT, GKEEP, stats_part)
        far_put('d', GFAR, 1, 1)
    with scope('y_keep_own'):
        keep_own('y', A, tile_y, YGOT, YKEEP)
    with scope('gwd_relay'):
        gwd_relay()
    for b in range(2):
        with scope('y_final'):
            y_final(b)
    for b in range(2):
        with scope('place_end_y'):
            place_end('y', b, 0, 1)
        with scope('stats'):
            stats_recv(b)
        for q in range(2):
            if b and q:
                with scope('dwu_b'):
                    dwu_b()
            with scope('dx'):
                dx_final(b, q)
    with scope('sums_1'):
        sums_1()
    with scope('gwu_relay'):
        gwu_relay()
    with scope('sums_2'):
        sums_2()
    with scope('sums_3'):
        sums_3()

    with scope('gwu_end'):
        gwu_end()
    with scope('gwd_end'):
        wait(gwd_out.at[pl.ds(0, 4 * QH), :], S('d_o', 0))
    wait(gwd_out.at[pl.ds(0, 4 * QH), :], S('d_o', 1))
    for p, out in (('y', y_out), ('d', dx_out)):
        @pl.when(r == tau)
        def _():
            with scope('out_end'):
                wait(out.at[pl.ds(0, TH), :], S(p + 'out'))

        @pl.when(r != tau)
        def _():
            with scope('out_end'):
                wait(out, S(p + 'out'))
    wait(sum_out, S('l_small', 0))
    for b in range(2):
        for q in range(2):
            place_end('d', b, q, 2)
            far_end('d', b, q)
    for b in range(2):
        wait(sx_v.at[b], S('s_st', b))
    wait(sum_v.at[1, :, pl.ds(0, 2 * HB)], S('s_sum', 0))
    for i in range(7):
        wait(sumr_v.at[0], S('s_sum', 1 + i))
    wait(wun, S('s_wun'))

    @pl.when(r == f)
    def _():
        for s in range(2):
            wait(wd_own(s), S('s_wd0', s))
    for i in range(4):
        wait(wd_dst(0, c), S('s_wdx', i))
    wait(wu_own, S('s_wu'))
    for i in range(3):
        wait(vec_at, S('s_vec', i))
    wait(bu_at, S('s_vec', 3))
    for s in range(2):
        wait(wd_dst(s, cf), S('s_wdr', s))
    for i in range(2):
        wait(wuq(d), S('s_wuy', i))
        wait(wuq(d, 0), S('s_wuy', 2 + i))
    for i in range(12):
        wait(wdq(0, d, c), S('s_wdy', i))
        wait(wdq(0, d, c, 0), S('s_wdy', 12 + i))

    def sends(k):
        for z, Z in (('x', X), ('g', DY)):
            for n in ('s_near', 's_far', 's_rel'):
                wait(reg(Z, k, c), S(z + n, k))
            wait(Z.at[r, ds(k * BLK, BLK), :], S(z + 's_d2d', k))
    loop(NCH, sends)
    for i in range(8):
        wait(r1D.at[0], S('d_so', i))
        wait(gwd(0, d), S('d_sy', i))
        wait(gwd(0, d, 0), S('d_sr', i))
    for j in range(1, 4):
        wait(finD.at[j], S('d_sf', j))

    @pl.when(r != f)
    def _():
        wait(finD.at[0], S('d_sf', 0))
    for i in range(2):
        wait(r1U, S('u_so', i))
        wait(PFU, S('u_sa', i))
        wait(finU, S('u_sf', i))

    @pl.when(r != dh)
    def _():
        wait(finU, S('u_sf', 2))
    wait(gwu(0, DH), S('u_sr'))


def block_kernel(x, dy, wu, wd, vec, bu):
    (TK, HB), FH = x.shape, wu.shape[1] // 2
    W, HW, TH, BLK, QF, FB = 4 * HB, 2 * HB, TK // 2, TK // NCH, FH // 4, 2 * FH
    assert FB <= W and FH <= HW and W // 4 == BLK and QF <= BLK and FH == HW
    sd = jax.ShapeDtypeStruct
    NS = BLK // min(BLK, 128)
    outs = [sd((TK, HB), BF16), sd((TK, HB), BF16), sd((W // 2, FB), BF16), sd((4 * FH, HB), BF16), sd((1, 3 * HB + FB), F32)]
    n_out = len(outs)
    outs += [sd((2, TK, W), BF16)] * 3 + [sd((2, TK, FB), BF16)] * 2 + [sd((2, TK, FB), F32)]
    outs += [sd((TH, W), F32), sd((TH, HW), F32), sd((TH, HW), F32)] * 2
    outs += [sd((4, QF, HB), F32)] * 2 + [sd((W // 4, FH), F32)] * 2
    V = pltpu.VMEM
    scratch = [
        V((W, FB), BF16), V((FB, W), BF16), V((4, FH, HB), F32), V((4, W // 4, FH), F32),
        V((4, FH // 8, HB), F32), V((4, FH // 8, HB), F32), V((W // 8, FH), F32), V((W // 8, FH), F32),
        V((8, W), F32), V((8, FB), F32), V((4, BLK, W), BF16), V((4, BLK, HW), F32), V((2, BLK, HW), BF16),
        V((4, QF, HB), BF16), V((2, 8, FH), F32), V((2, 8, HW), F32),
        V((BLK, 128), F32), V((2, BLK, 128), F32), V((2, BLK, 128), F32), V((2, 2 * NS, 128), F32), V((2, 2 * NS, 128), F32),
        V((8, HB), F32), V((2, 1, 3 * HB + FB), F32), V((9, 1, 3 * HB + FB), F32),
        pltpu.SemaphoreType.DMA((N_SEM,)),
    ]
    res = pl.pallas_call(
        functools.partial(body, (TK, HB, FH)),
        out_shape=outs,
        in_specs=[pl.BlockSpec(memory_space=pl.ANY)] * 6,
        out_specs=[pl.BlockSpec(memory_space=pl.ANY)] * len(outs),
        scratch_shapes=scratch,
        compiler_params=pltpu.CompilerParams(collective_id=0, has_side_effects=True, vmem_limit_bytes=67043328),
        name='mlp_block',
    )(x, dy, wu, wd, vec, bu)
    return res[:n_out]


def solution(mesh):
    assert (mesh.shape['col'], mesh.shape['row'], mesh.shape['depth']) == (4, 2, 4)
    tok_spec = P(('dp', 'depth', 'row'), 'col')
    vec_spec = P('col')
    mat_spec = P('row', 'col')
    grad_vec = P(('dp', 'col'))
    grad_mat = P(('dp', 'row'), 'col')
    def local_pass(x_blk, gamma_blk, beta_blk, w_up_blk, b_up_blk, w_down_blk, b_down_blk, dy_blk):
        hb, fb = x_blk.shape[1], w_up_blk.shape[1]
        vec = jnp.stack([gamma_blk, beta_blk, b_down_blk.astype(F32)] + [jnp.zeros_like(gamma_blk)] * 5)
        bu = jnp.broadcast_to(b_up_blk.astype(F32)[None], (8, fb))
        y_blk, dx_blk, grad_w_up, grad_w_down, sums = block_kernel(x_blk, dy_blk, w_up_blk, w_down_blk, vec, bu)
        sums = sums[0]
        return (y_blk, dx_blk, sums[:hb], sums[hb:2 * hb], grad_w_up, sums[2 * hb:2 * hb + fb], grad_w_down, sums[2 * hb + fb:])

    return jax.shard_map(
        local_pass,
        mesh=mesh,
        in_specs=(tok_spec, vec_spec, vec_spec, mat_spec, vec_spec, mat_spec, vec_spec, tok_spec),
        out_specs=(tok_spec, tok_spec, grad_vec, grad_vec, grad_mat, grad_vec, grad_mat, grad_vec),
        check_vma=False,
    )
```

```python
import functools

import jax
import jax.numpy as jnp
from jax import lax
from jax.experimental import pallas as pl
from jax.experimental.pallas import tpu as pltpu
from jax.sharding import PartitionSpec as P

LN_EPS = 1e-5
F32 = jnp.float32
BF16 = jnp.bfloat16
MESH = pl.DeviceIdType.MESH
GELU_A = 0.7978845608028654
GELU_B = 0.044715
NCH = 4
ROWS = 16
LROWS = 64
XROWS = 32

NN = (((1,), (0,)), ((), ()))
NT = (((1,), (1,)), ((), ()))
TN = (((0,), (0,)), ((), ()))

SEMS = {}
for _z in ('x', 'g'):
    for _n in ('near', 'far', 'opp', 'd2d', 'd2w', 'd2o', 's_near', 's_far', 's_rel', 's_d2d'):
        SEMS[_z + _n] = NCH
    SEMS[_z + 'bounce'] = 2
for _p in ('y', 'd'):
    SEMS.update({_p + 's_give': 2, _p + 'got': 2, _p + 's_far': 4, _p + 'keep': 2, _p + 'far': 4, _p + 's_out': 8, _p + 'out': 1, _p + 'loc': 4})
SEMS.update(l_wu=1, s_wu=1, r_wu=1, s_wun=1, r_wun=1, s_wuy=4, r_wuy=4,
            s_wd0=2, s_wdx=4, r_wd=4, s_wdr=2, s_wdy=24, r_wdy=8,
            l_vec=2, s_vec=4, r_vec=2,
            ld=8, ldb=2, st=6, s_st=2, r_st=2, s_sum=8, r_sum=2,
            d_so=8, d_r=8, d_sa=8, d_p=8, d_sf=4, d_out=1, d_sy=8, d_y=2, d_sr=8, d_o=2,
            u_so=2, u_r=2, u_sa=2, u_p=2, u_sf=3, u_out=3, u_sr=1, u_o=2, l_small=2)
BASE = {}
_at = 0
for _n, _c in SEMS.items():
    BASE[_n] = _at
    _at += _c
N_SEM = _at


def gelu_and_slope(v):
    v2 = v * v
    t = jnp.tanh(v * (GELU_A + (GELU_A * GELU_B) * v2))
    q = (1.0 - t) * (GELU_A + (3.0 * GELU_A * GELU_B) * v2)
    return 0.5 * v * (1.0 + t), 0.5 * ((1.0 + t) * (1.0 + v * q))


def body(dims, x_ref, dy_ref, wu_ref, wd_ref, vec_ref, bu_ref,
         y_out, dx_out, gwu_out, gwd_out, sum_out,
         X, DY, XN, A, DU, SL, YGOT, YFAR, YKEEP, GGOT, GFAR, GKEEP, PFD, PND, PFU, PNU,
         wu_v, wd_v, accD, accU, r1D, r2D, r1U, r2U, vec_v, bu_v, wx, F4, ob, finD,
         db_v, cs_v, st_v, ms_v, st2_v, sx_v, sr_v, bd_v, sum_v, sumr_v, sem):
    TK, HB, FH = dims
    W, HW, TH, BLK, QF = 4 * HB, 2 * HB, TK // 2, TK // NCH, FH // 4
    RH, DQ, QH, DH, FB = W // 2, W // 4, FH // 8, W // 8, 2 * FH
    NTW = HB
    inv_w = 1.0 / W
    finU = wx.at[3, pl.ds(0, DQ), pl.ds(HW, FH)]
    f0, f1 = F4.at[0], F4.at[1]

    c, r, d = lax.axis_index('col'), lax.axis_index('row'), lax.axis_index('depth')
    c_odd, d_odd = lax.rem(c, 2), lax.rem(d, 2)
    cn, cf, co = c + 1 - 2 * c_odd, 3 - c, lax.rem(c + 2, 4)
    dn, df, do = d + 1 - 2 * d_odd, 3 - d, lax.rem(d + 2, 4)
    f, dh = lax.div(c, 2), lax.div(d, 2)
    tau = lax.rem(lax.div(c + 1, 2), 2)
    rp = 1 - r
    o, o2 = c_odd * FH, (1 - c_odd) * FH

    def S(name, i=0):
        return sem.at[BASE[name] + i]

    def ds(start, size):
        return pl.ds(pl.multiple_of(start, size), size)

    def dsm(start, size, mult):
        return pl.ds(pl.multiple_of(start, mult), size)

    def put(src, dst, ssem, rsem, **dev):
        pltpu.make_async_remote_copy(src_ref=src, dst_ref=dst, send_sem=ssem, recv_sem=rsem,
                                     device_id=dev, device_id_type=MESH).start()

    def copy(src, dst, s):
        pltpu.make_async_copy(src, dst, s).start()

    def wait(ref, s):
        pltpu.make_async_copy(ref, ref, s).wait()

    def loop(n, fn):
        def step(i, carry):
            fn(i)
            return carry
        lax.fori_loop(0, n, step, 0)

    bar = pltpu.get_barrier_semaphore()
    for dev in [dict(row=rp)] + [dict(row=h, **q) for h in range(2) for q in
                                 (dict(col=cn), dict(col=cf), dict(col=co), dict(depth=dn), dict(depth=df), dict(depth=do))]:
        pl.semaphore_signal(bar, inc=1, device_id=dev, device_id_type=MESH)
    pl.semaphore_wait(bar, 13)

    def wd_src(s, h):
        return wd_ref.at[dsm((2 * s + h) * FH + d * QF, QF, QF), :]

    def wd_dst(s, col):
        return wd_v.at[dsm(s * FH + d * QF, QF, QF), ds(col * HB, HB)]

    def reg(Z, k, col):
        return Z.at[r, ds(k * BLK, BLK), ds(col * HB, HB)]

    def send_own(z, z_ref, Z, which, chunks=(0, NCH)):
        def step(k):
            src = z_ref.at[ds(k * BLK, BLK), :]
            if 'near' in which:
                put(src, reg(Z, k, c), S(z + 's_near', k), S(z + 'near', k), col=cn)
            if 'far' in which:
                put(src, reg(Z, k, c), S(z + 's_far', k), S(z + 'far', k), col=cf)
            if 'd2d' in which:
                put(src, reg(Z, k, c), S(z + 's_d2d', k), S(z + ('d2d' if z == 'x' else 'd2w'), k), row=rp)
        for k in range(*chunks):
            step(k)

    def d2d(z, Z, k, col, s):
        put(reg(Z, k, col), reg(Z, k, col), S(z + 's_d2d', k), S(z + s, k), row=rp)

    vec_at = vec_v.at[:, :, ds(c * HB, HB)]
    copy(vec_ref, vec_at, S('l_vec', 0))
    put(vec_ref, vec_at, S('s_vec', 0), S('r_vec', 0), col=cn)
    put(vec_ref, vec_at, S('s_vec', 1), S('r_vec', 0), col=cf)
    put(vec_ref, vec_at, S('s_vec', 2), S('r_vec', 0), col=co)
    bu_src, bu_at = bu_ref.at[:, ds(r * FH, FH)], bu_v.at[:, ds(o, FH)]
    copy(bu_src, bu_at, S('l_vec', 1))
    put(bu_src, bu_at, S('s_vec', 3), S('r_vec', 1), col=cn)

    wu_own = wu_v.at[ds(r * RH, RH), ds(o, FH)]
    wd_own = lambda s: wd_v.at[pl.ds(s * FH, FH), ds(c * HB, HB)]

    @pl.when(r != f)
    def _():
        for s in range(2):
            for h in range(2):
                put(wd_src(s, h), wd_dst(s, c), S('s_wdx', 2 * s + h), S('r_wd', 2), col=cf, row=h)

    @pl.when(r == f)
    def _():
        for s in range(2):
            for h in range(2):
                put(wd_src(s, h), wd_dst(s, c), S('s_wdx', 2 * s + h), S('r_wd', 1), col=cn, row=h)
    send_own('x', x_ref, X, ('far',), (0, 2))
    send_own('x', x_ref, X, ('near',), (0, 1))
    put(wu_ref.at[:, ds(rp * FH, FH)], wu_own, S('s_wu'), S('r_wu'), row=rp)
    copy(wu_ref.at[:, ds(r * FH, FH)], wu_own, S('l_wu'))
    send_own('x', x_ref, X, ('d2d',))
    send_own('g', dy_ref, DY, ('d2d',))
    for i, z_ref in enumerate((x_ref, dy_ref)):
        for k in range(NCH):
            copy(z_ref.at[pl.ds(k * BLK, BLK), :], wx.at[i, :, pl.ds(k * HB, HB)], S('xg'[i] + 'bounce', 0))

    @pl.when(r == f)
    def _():
        for s in range(2):
            copy(wd_ref.at[dsm((2 * s + r) * FH, FH, FH), :], wd_own(s), S('r_wd', 0))
            put(wd_ref.at[dsm((2 * s + rp) * FH, FH, FH), :], wd_own(s), S('s_wd0', s), S('r_wd', 0), row=rp)

    for i, Z in enumerate((X, DY)):
        wait(wx.at[i], S('xg'[i] + 'bounce', 0))
        for k in range(NCH):
            copy(wx.at[i, :, pl.ds(k * HB, HB)], reg(Z, k, c), S('xg'[i] + 'bounce', 1))

    with jax.named_scope('wd_far'):
        wait(wd_v.at[pl.ds(0, 2 * QF), pl.ds(0, HB)], S('r_wd', 2))
    for s in range(2):
        put(wd_dst(s, cf), wd_dst(s, cf), S('s_wdr', s), S('r_wd', 3), col=cn)
    send_own('x', x_ref, X, ('near',), (1, NCH - 1))

    with jax.named_scope('wu_own'):
        wait(wu_own, S('l_wu'))
        wait(wu_v.at[ds(rp * RH, RH), ds(o, FH)], S('r_wu'))
    wun = wu_v.at[ds(d * DQ, DQ), ds(o, FH)]
    put(wun, wun, S('s_wun'), S('r_wun'), col=cn)
    send_own('x', x_ref, X, ('near',), (NCH - 1, NCH))

    db_v[...] = jnp.zeros_like(db_v)
    cs_v[...] = jnp.zeros_like(cs_v)
    bd_v[...] = jnp.zeros_like(bd_v)

    def dy_sum(i):
        rr = ds(i * ROWS, ROWS)
        part = jnp.sum(wx[1, rr, :].astype(F32).reshape(ROWS // 8, 8, W), axis=0)
        bd_v[...] += part[:, :HB] + part[:, HB:2 * HB] + part[:, 2 * HB:3 * HB] + part[:, 3 * HB:]
    with jax.named_scope('dy_sum'):
        loop(BLK // ROWS, dy_sum)

    def wuq(dd, half=None):
        if half is None:
            return wu_v.at[ds(dd * DQ, DQ), ds(o2, FH)]
        return wu_v.at[dsm(dd * DQ + half * DH, DH, DH), ds(o2, FH)]

    def wu_send():
        with jax.named_scope('wu_near'):
            wait(wuq(d), S('r_wun'))
        put(wuq(d), wuq(d), S('s_wuy', 0), S('r_wuy', 0), depth=dn)
        put(wuq(d), wuq(d), S('s_wuy', 1), S('r_wuy', 1), depth=df)

    def wu_relay():
        with jax.named_scope('wuy'):
            wait(wuq(dn), S('r_wuy', 0))
            wait(wuq(df), S('r_wuy', 1))
        put(wuq(dn, 1), wuq(dn, 1), S('s_wuy', 2), S('r_wuy', 3), depth=df)
        put(wuq(df, 0), wuq(df, 0), S('s_wuy', 3), S('r_wuy', 2), depth=dn)

    def wdq(s, dd, col, half=None):
        if half is None:
            return wd_v.at[dsm(s * FH + dd * QF, QF, QF), ds(col * HB, HB)]
        return wd_v.at[dsm(s * FH + dd * QF + half * QH, QH, QH), ds(col * HB, HB)]

    W_GROUPS = (((0, cn), (1, cf)), ((2, co),))

    def wd_send(g):
        if g == 0:
            wait(wd_v.at[pl.ds(0, 2 * QF), pl.ds(0, HB)], S('r_wd', 1))
        else:
            wait(wd_v.at[pl.ds(0, 2 * QF), pl.ds(0, HB)], S('r_wd', 3))
        for i, col in W_GROUPS[g]:
            for s in range(2):
                put(wdq(s, d, col), wdq(s, d, col), S('s_wdy', 4 * i + s), S('r_wdy', 4 * g), depth=dn)
                put(wdq(s, d, col), wdq(s, d, col), S('s_wdy', 4 * i + 2 + s), S('r_wdy', 4 * g + 1), depth=df)

    def wd_bytes(g, rows):
        return wd_v.at[pl.ds(0, 2 * rows), pl.ds(0, len(W_GROUPS[g]) * HB)]

    def wd_relay(g):
        for i in range(2):
            wait(wd_bytes(g, QF), S('r_wdy', 4 * g + i))
        for i, col in W_GROUPS[g]:
            for s in range(2):
                put(wdq(s, dn, col, 1), wdq(s, dn, col, 1), S('s_wdy', 12 + 4 * i + s), S('r_wdy', 4 * g + 3), depth=df)
                put(wdq(s, df, col, 0), wdq(s, df, col, 0), S('s_wdy', 12 + 4 * i + 2 + s), S('r_wdy', 4 * g + 2), depth=dn)

    def x_near(k):
        wait(reg(X, k, cn), S('xnear', k))
        put(reg(X, k, cn), reg(X, k, cn), S('xs_rel', k), S('xopp', k), col=cf)
        d2d('x', X, k, cn, 'd2d')

    with jax.named_scope('wd_send0'):
        wd_send(0)
    with jax.named_scope('x_near'):
        x_near(0)
    send_own('x', x_ref, X, ('far',), (2, 3))

    for i, Z in enumerate((X, DY)):
        wait(wx.at[i], S('xg'[i] + 'bounce', 1))
    wait(vec_at, S('l_vec', 0))
    wait(vec_v.at[:, :, pl.ds(0, 3 * HB)], S('r_vec', 0))
    wait(bu_at, S('l_vec', 1))
    wait(bu_at, S('r_vec', 1))

    def norm_rows(buf, rows):
        xf = buf[rows, :].astype(F32)
        mean = jnp.sum(xf, axis=1, keepdims=True) * inv_w
        cen = xf - mean
        inv = lax.rsqrt(jnp.sum(cen * cen, axis=1, keepdims=True) * inv_w + LN_EPS)
        return cen, mean, inv

    def tok_of(s):
        return tau + s * (1 - 2 * tau)

    N_T = FH // NTW

    def chain(tiles, hooks=None):
        hooks = hooks or {}

        def hook(what, i):
            for fn in hooks.get((what, i), ()):
                fn()
        for i, (product, _) in enumerate(tiles):
            hook('before', i)
            if i:
                tiles[i - 1][1](F4.at[(i - 1) % 2])
            F4[i % 2, :, :NTW] = product()
            hook('product', i)
            if i:
                hook('epilogue', i - 1)
        tiles[-1][1](F4.at[(len(tiles) - 1) % 2])
        hook('epilogue', len(tiles) - 1)

    def u_tile(src, i, n, start):
        cols = ds(start + n * NTW, NTW)
        at = pl.ds(n * NTW, NTW)

        def product():
            return lax.dot_general(wx[src], wu_v[:, cols], NN, preferred_element_type=F32)

        def epilogue(acc):
            u = (acc[:, :NTW] + bu_v[0:1, cols]).astype(BF16)
            a, slope = gelu_and_slope(u.astype(F32))
            ob[i, :, at] = a.astype(BF16)
            F4[2 + i, :, at] = slope
        return product, epilogue

    def u_store(i, s, rows, start):
        copy(ob.at[i], A.at[s, rows, ds(start, FH)], S('st', 2 + i))
        copy(F4.at[2 + i], SL.at[s, rows, ds(start, FH)], S('st', 4 + i))

    def u_stored():
        for i in range(2):
            wait(ob.at[i], S('st', 2 + i))
            wait(F4.at[2 + i], S('st', 4 + i))

    def phase1(k):
        @pl.when(k < NCH - 1)
        def _():
            with jax.named_scope('x_near'):
                x_near(k + 1)

        @pl.when(k == 0)
        def _():
            send_own('x', x_ref, X, ('far',), (3, 4))
            with jax.named_scope('wd_send1'):
                wd_send(1)

        @pl.when(k == 1)
        def _():
            with jax.named_scope('wd_relay0'):
                wd_relay(0)
            send_own('g', dy_ref, DY, ('near',))

        @pl.when(k == 2)
        def _():
            send_own('g', dy_ref, DY, ('far',))
            wu_send()
            with jax.named_scope('wd_relay1'):
                wd_relay(1)

        with jax.named_scope('x_far'):
            wait(reg(X, k, cf), S('xfar', k))
            d2d('x', X, k, cf, 'd2d')
        with jax.named_scope('x_opp'):
            wait(reg(X, k, co), S('xopp', k))
            d2d('x', X, k, co, 'd2d')

        rows = ds(k * BLK, BLK)
        with jax.named_scope('x_d2d'):
            wait(X.at[rp, rows, :], S('xd2d', k))

        @pl.when(k == NCH - 1)
        def _():
            wu_relay()

        @pl.when(k > 0)
        def _():
            for s in range(2):
                wait(wx.at[s], S('st', s))
        for s in range(2):
            copy(X.at[tok_of(s), rows, :], wx.at[s], S('ld', s))
        for s in range(2):
            wait(wx.at[s], S('ld', s))

            def ln(i):
                rr = ds(i * LROWS, LROWS)
                cen, _, inv = norm_rows(wx.at[s], rr)
                wx[s, rr, :] = (cen * inv * vec_v[0] + vec_v[1]).astype(BF16)
            with jax.named_scope('ln'):
                loop(BLK // LROWS, ln)
            copy(wx.at[s], XN.at[s, rows, :], S('st', s))
        pl.when(k > 0)(u_stored)
        with jax.named_scope('u_own'):
            chain([u_tile(i, i, n, o) for i in range(2) for n in range(N_T)])
        for s in range(2):
            u_store(s, s, rows, o)
    loop(NCH, phase1)
    for s in range(2):
        wait(wx.at[s], S('st', s))
    u_stored()

    def u_near_load():
        for b in range(NCH):
            copy(XN.at[0, pl.ds(b * BLK, BLK), :], wx.at[b], S('ld', b))

    def u_near():
        def step(kp):
            for i in range(2):
                wait(wx.at[2 * kp + i], S('ld', 2 * kp + i))
            chain([u_tile(2 * kp + i, i, n, o2) for i in range(2) for n in range(N_T)],
                  {('before', 1): [lambda: pl.when(kp > 0)(u_stored)]})
            for i in range(2):
                u_store(i, 0, ds((2 * kp + i) * BLK, BLK), o2)
        loop(NCH // 2, step)
        u_stored()

    def g_near_far(k):
        wait(reg(DY, k, cf), S('gfar', k))
        put(reg(DY, k, cf), reg(DY, k, cf), S('gs_rel', k), S('gopp', k), col=cn)
        d2d('g', DY, k, cf, 'd2d')
        wait(reg(DY, k, cn), S('gnear', k))
        d2d('g', DY, k, cn, 'd2d')

    def g_opp(k):
        wait(reg(DY, k, co), S('gopp', k))
        d2d('g', DY, k, co, 'd2o')

    def g_opp_got(k):
        wait(reg(DY, k, co), S('gd2o', k))

    def tile_y(lhs, col):
        return lax.dot_general(lhs, wd_v[:, dsm(col, NTW, NTW)], NN, preferred_element_type=F32)

    def tile_g(lhs, col):
        return lax.dot_general(lhs, wu_v[dsm(col, NTW, NTW), :], NT, preferred_element_type=F32)

    def give(p, src, tile, GOT):
        def blk(b):
            return src.at[0, dsm(rp * TH + b * BLK, BLK, BLK), :]
        for b in range(2):
            copy(blk(b), wx.at[b, :, pl.ds(0, FB)], S('ld', b))
        keep_load(src)

        def step(b):
            wait(wx.at[b, :, pl.ds(0, FB)], S('ld', b))

            def half(h):
                @pl.when(b == 1)
                def _():
                    wait(F4.at[h], S(p + 's_give', h))

                def n_tile(n):
                    F4[h, :, ds(n * NTW, NTW)] = tile(wx[b, :, :FB], h * HW + n * NTW)
                loop(HW // NTW, n_tile)
                put(F4.at[h], GOT.at[ds(b * BLK, BLK), ds(h * HW, HW)], S(p + 's_give', h), S(p + 'got', b), row=rp)
            loop(2, half)
        loop(2, step)

    HB2 = BLK // 2

    def keep_load(src):
        for b in range(2):
            copy(src.at[0, dsm(r * TH + b * BLK, BLK, BLK), :], wx.at[2 + b, :, pl.ds(0, FB)], S('ld', 2 + b))

    def got_load(GOT, b, col0, out, s_):
        copy(GOT.at[ds(b * BLK, BLK), ds(col0, HW)], F4.at[out], s_)

    def add_tiles(b, out, tile, col0):
        def n_tile(n):
            at = ds(n * NTW, NTW)
            F4[out, :, at] = F4[out, :, at] + tile(wx[2 + b, :, :FB], col0 + n * NTW)
        loop(HW // NTW, n_tile)

    def far_put(p, FAR, b, q):
        put(F4.at[2 + b, ds(q * HB2, HB2), :], FAR.at[ds(b * BLK + q * HB2, HB2), :], S(p + 's_far', 2 * b + q), S(p + 'far', 2 * b + q), col=cf)

    def give_end(p):
        for h in range(2):
            wait(F4.at[h], S(p + 's_give', h))

    def keep_far(p, tile, GOT, FAR, b, pieces):
        with jax.named_scope('got'):
            wait(GOT.at[ds(b * BLK, BLK), :], S(p + 'got', b))
        got_load(GOT, b, (1 - f) * HW, 2 + b, S('ld', 4 + b))
        wait(wx.at[2 + b, :, pl.ds(0, FB)], S('ld', 2 + b))
        wait(F4.at[2 + b], S('ld', 4 + b))
        add_tiles(b, 2 + b, tile, (1 - f) * HW)
        for q in range(pieces):
            far_put(p, FAR, b, q)

    def keep_own(p, src, tile, GOT, KEEP, after=None):
        keep_load(src)
        for b in range(2):
            got_load(GOT, b, f * HW, 1 - b, S('ld', 4 + b))

        def step(b):
            wait(wx.at[2 + b, :, pl.ds(0, FB)], S('ld', 2 + b))
            wait(F4.at[1 - b], S('ld', 4 + b))
            add_tiles(b, 1 - b, tile, f * HW)
            copy(F4.at[1 - b], KEEP.at[ds(b * BLK, BLK), :], S(p + 'keep', b))
            if after:
                after(b)
        loop(2, step)
        for b in range(2):
            wait(F4.at[b], S(p + 'keep', b))

    def far_end(p, b, q):
        wait(F4.at[2 + b, ds(q * HB2, HB2), :], S(p + 's_far', 2 * b + q))

    def place(p, out, b, q, nq):
        nr = BLK // nq
        rr = ds(q * nr, nr)
        dst = out.at[dsm(r * TH + b * BLK + q * nr, nr, nr), :]
        mine, other = ob.at[b, rr, ds(c_odd * HB, HB)], ob.at[b, rr, ds((1 - c_odd) * HB, HB)]
        put(other, dst, S(p + 's_out', 4 * b + 2 * q), S(p + 'out'), col=cn, row=tau)

        @pl.when(r == tau)
        def _():
            copy(mine, dst, S(p + 'loc', 2 * b + q))

        @pl.when(r != tau)
        def _():
            put(mine, dst, S(p + 's_out', 4 * b + 2 * q + 1), S(p + 'out'), row=rp)

    def place_end(p, b, q, nq):
        part = ob.at[b, pl.ds(0, BLK // nq), pl.ds(0, HB)]
        wait(part, S(p + 's_out', 4 * b + 2 * q))

        @pl.when(r == tau)
        def _():
            wait(part, S(p + 'loc', 2 * b + q))

        @pl.when(r != tau)
        def _():
            wait(part, S(p + 's_out', 4 * b + 2 * q + 1))

    fcols = ds(f * HW, HW)

    def y_final(b):
        brow = ds(b * BLK, BLK)
        for q in range(2):
            wait(YFAR.at[ds(b * BLK + q * HB2, HB2), :], S('yfar', 2 * b + q))
        copy(YFAR.at[brow, :], f0, S('ld', 0))
        copy(YKEEP.at[brow, :], f1, S('ld', 1))
        copy(X.at[tau, dsm(r * TH + b * BLK, BLK, BLK), fcols], wx.at[0, :, pl.ds(0, HW)], S('ld', 2))
        wait(f0, S('ld', 0))
        wait(f1, S('ld', 1))
        wait(wx.at[0, :, pl.ds(0, HW)], S('ld', 2))

        def fin(i):
            rr = ds(i * ROWS, ROWS)
            ob[b, rr, :] = (wx[0, rr, :HW].astype(F32) + (f0[rr, :] + f1[rr, :]) + vec_v[2, :, fcols]).astype(BF16)
        loop(BLK // ROWS, fin)
        place('y', y_out, b, 0, 1)

    def services(t):
        @pl.when(t == 3)
        def _():
            with jax.named_scope('dwd_a3'):
                dwd_a(3)

    def da_all():
        def part(t, i):
            near = lax.div(t, NCH)
            tok = tau + i * (1 - near) * (1 - 2 * tau)
            chunk = t * (1 - near) + near * (2 * (t - NCH) + i)
            return near, tok, i * (1 - near), ds(chunk * BLK, BLK), near * o2 + (1 - near) * o

        def load(t, p):
            for i in range(2):
                _, tok, us, rows, start = part(t, i)
                copy(DY.at[tok, rows, :], wx.at[2 * p + i], S('ld', 2 * p + i))
                copy(SL.at[us, rows, ds(start, FH)], accU.at[2 * p + i], S('ld', 4 + 2 * p + i))

        def store(t, i):
            _, _, us, rows, start = part(t, i)
            copy(ob.at[i], DU.at[us, rows, ds(start, FH)], S('st', 4 + i))

        def stored():
            for i in range(2):
                wait(ob.at[i], S('st', 4 + i))

        n_steps = NCH + NCH // 2

        def step(t):
            near, _, _, _, start = part(t, 0)
            p = lax.rem(t, 2)
            services(t)
            for i in range(2):
                wait(wx.at[2 * p + i], S('ld', 2 * p + i))
                wait(accU.at[2 * p + i], S('ld', 4 + 2 * p + i))

            @pl.when(t < n_steps - 1)
            def _():
                load(t + 1, 1 - p)

            def tile(i, n):
                cols = ds(start + n * NTW, NTW)
                at = pl.ds(n * NTW, NTW)

                def product():
                    return lax.dot_general(wx[2 * p + i], wd_v[cols, :], NT, preferred_element_type=F32)

                def epilogue(acc):
                    du = (acc[:, :NTW] * accU[2 * p + i, :, at]).astype(BF16)
                    ob[i, :, at] = du
                    db_v[near, :, at] += jnp.sum(du.astype(F32).reshape(BLK // 8, 8, NTW), axis=0)
                return product, epilogue
            chain([tile(i, n) for i in range(2) for n in range(N_T)], {('before', 1): [lambda: pl.when(t > 0)(stored)]})
            for i in range(2):
                store(t, i)
        load(0, 0)
        loop(n_steps, step)
        stored()

    def rows_of(kb):
        return ds(lax.rem(kb, NCH) * BLK, BLK), lax.div(kb, NCH)

    d_col = (c, cn, cf, co)

    NB, NSLOT = 2 * NCH, 4

    def k_loop(load, use, width):
        for kb in range(NSLOT - 1):
            load(kb, wx.at[kb], S('ld', kb))

        def step(kb):
            slot = lax.rem(kb, NSLOT)

            @pl.when(kb + NSLOT - 1 < NB)
            def _():
                nxt = lax.rem(kb + NSLOT - 1, NSLOT)
                load(kb + NSLOT - 1, wx.at[nxt], S('ld', nxt))
            buf = wx.at[slot]
            wait(buf.at[:, pl.ds(0, width)], S('ld', slot))
            use(buf)
        loop(NB, step)

    def dwd_pass(js):
        def load(kb, buf, s_):
            rows, s = rows_of(kb)
            copy(A.at[s, rows, ds(o, FH)], buf.at[:, pl.ds(0, FH)], s_)
            for i, j in enumerate(js):
                copy(DY.at[tok_of(s), rows, ds(d_col[j] * HB, HB)], buf.at[:, pl.ds(FH + i * HB, HB)], s_)

        def use(buf):
            for i, j in enumerate(js):
                for m in range(2):
                    mm = slice(m * FH // 2, (m + 1) * FH // 2)
                    accD[j, mm, :] += lax.dot_general(buf[:, mm], buf[:, FH + i * HB:FH + (i + 1) * HB], TN, preferred_element_type=F32)
        for j in js:
            accD[j] = jnp.zeros((FH, HB), F32)
        k_loop(load, use, FH + len(js) * HB)

    def dwd_opp(j):
        put(accD.at[j, dsm(do * QF, QH, QH), :], r1D.at[j], S('d_so', 2 * j), S('d_r', 2 * j), depth=dn)
        put(accD.at[j, dsm(do * QF + QH, QH, QH), :], r2D.at[j], S('d_so', 2 * j + 1), S('d_r', 2 * j + 1), depth=df)

    def dwd_a(j):
        wait(r1D.at[j], S('d_r', 2 * j))
        rr = dsm(df * QF, QH, QH)
        accD[j, rr, :] += r1D[j]
        put(accD.at[j, ds(df * QF, QF), :], PFD.at[j], S('d_sa', 2 * j), S('d_p', 2 * j), depth=df)
        wait(r2D.at[j], S('d_r', 2 * j + 1))
        rr = dsm(dn * QF + QH, QH, QH)
        accD[j, rr, :] += r2D[j]
        put(accD.at[j, ds(dn * QF, QF), :], PND.at[j], S('d_sa', 2 * j + 1), S('d_p', 2 * j + 1), depth=dn)

    def dwd_rows(q, h, dd):
        return dsm((2 * q + h) * FH + dd * QF, QF, QF)

    def dwd_b(j):
        wait(PFD.at[j], S('d_p', 2 * j))
        wait(PND.at[j], S('d_p', 2 * j + 1))
        wait(PFD.at[j], S('d_sa', 2 * j))
        wait(PND.at[j], S('d_sa', 2 * j + 1))
        pf, pn = accD.at[j, ds(df * QF, QF), :], accD.at[j, ds(dn * QF, QF), :]
        copy(PFD.at[j], pf, S('ldb', 0))
        copy(PND.at[j], pn, S('ldb', 1))
        wait(pf, S('ldb', 0))
        wait(pn, S('ldb', 1))
        finD[j] = (accD[j, ds(d * QF, QF), :] + (pf[...] + pn[...])).astype(BF16)
        dst = gwd_out.at[dwd_rows(c_odd, r, d), :]
        if j:
            put(finD.at[j], dst, S('d_sf', j), S('d_out'), col=d_col[j], row=f)
        else:
            @pl.when(r == f)
            def _():
                copy(finD.at[0], dst, S('d_out'))

            @pl.when(r != f)
            def _():
                put(finD.at[0], dst, S('d_sf', 0), S('d_out'), row=rp)

    def gwd(i, dd, half=None):
        if half is None:
            return gwd_out.at[dsm(i * FH + dd * QF, QF, QF), :]
        return gwd_out.at[dsm(i * FH + dd * QF + half * QH, QH, QH), :]

    def gwd_send():
        wait(gwd_out.at[pl.ds(0, 4 * QF), :], S('d_out'))
        for i in range(4):
            put(gwd(i, d), gwd(i, d), S('d_sy', i), S('d_y', 0), depth=dn)
            put(gwd(i, d), gwd(i, d), S('d_sy', 4 + i), S('d_y', 1), depth=df)

    def gwd_relay():
        wait(gwd_out.at[pl.ds(0, 4 * QF), :], S('d_y', 0))
        for i in range(4):
            put(gwd(i, dn, 1), gwd(i, dn, 1), S('d_sr', i), S('d_o', 1), depth=df)
        wait(gwd_out.at[pl.ds(0, 4 * QF), :], S('d_y', 1))
        for i in range(4):
            put(gwd(i, df, 0), gwd(i, df, 0), S('d_sr', 4 + i), S('d_o', 0), depth=dn)

    def dwu_pass(dds):
        def load(kb, buf, s_):
            rows, s = rows_of(kb)
            copy(DU.at[s, rows, ds(o, FH)], buf.at[:, pl.ds(0, FH)], s_)
            for i, dd in enumerate(dds):
                copy(XN.at[s, rows, ds(dd * DQ, DQ)], buf.at[:, pl.ds(FH + i * DQ, DQ)], s_)

        def use(buf):
            for i, dd in enumerate(dds):
                for m in range(2):
                    mm = slice(m * FH // 2, (m + 1) * FH // 2)
                    accU[dd, :, mm] += lax.dot_general(buf[:, FH + i * DQ:FH + (i + 1) * DQ], buf[:, mm], TN, preferred_element_type=F32)
        for dd in dds:
            accU[dd] = jnp.zeros((DQ, FH), F32)
        k_loop(load, use, FH + len(dds) * DQ)

    def dwu_opp():
        put(accU.at[do, pl.ds(0, DH), :], r1U, S('u_so', 0), S('u_r', 0), depth=dn)
        put(accU.at[do, pl.ds(DH, DH), :], r2U, S('u_so', 1), S('u_r', 1), depth=df)

    def dwu_a():
        wait(r1U, S('u_r', 0))
        accU[df, :DH, :] += r1U[...]
        put(accU.at[df], PFU, S('u_sa', 0), S('u_p', 0), depth=df)
        wait(r2U, S('u_r', 1))
        accU[dn, DH:, :] += r2U[...]
        put(accU.at[dn], PNU, S('u_sa', 1), S('u_p', 1), depth=dn)

    def dwu_b():
        wait(PFU, S('u_p', 0))
        wait(PNU, S('u_p', 1))
        pf, pn = f0.at[pl.ds(0, DQ), pl.ds(0, FH)], f1.at[pl.ds(0, DQ), pl.ds(0, FH)]
        copy(PFU, pf, S('ldb', 0))
        copy(PNU, pn, S('ldb', 1))
        wait(pf, S('ldb', 0))
        wait(pn, S('ldb', 1))

        def fin(i):
            rr = ds(i * ROWS, ROWS)
            wx[3, rr, HW:HW + FH] = (accU[d, rr, :] + (f0[rr, :FH] + f1[rr, :FH])).astype(BF16)
        loop(DQ // ROWS, fin)
        dst = gwu_out.at[ds(d_odd * DQ, DQ), ds(r * FH, FH)]
        put(finU, dst, S('u_sf', 0), S('u_out', 1), depth=dn, row=dh)
        put(finU, dst, S('u_sf', 1), S('u_out', 2), depth=df, row=dh)

        @pl.when(r == dh)
        def _():
            copy(finU, dst, S('u_out', 0))

        @pl.when(r != dh)
        def _():
            put(finU, dst, S('u_sf', 2), S('u_out', 0), row=rp)

    def gwu(start, size):
        return gwu_out.at[dsm(start, size, size), :]

    def gwu_relay():
        @pl.when(r == dh)
        def _():
            wait(gwu(lax.rem(dn, 2) * DQ, DQ), S('u_out', 1))
            part = gwu(lax.rem(dn, 2) * DQ + DH, DH)
            put(part, part, S('u_sr'), S('u_o', 1), depth=df)

        @pl.when(r != dh)
        def _():
            wait(gwu(lax.rem(df, 2) * DQ, DQ), S('u_out', 2))
            part = gwu(lax.rem(df, 2) * DQ, DH)
            put(part, part, S('u_sr'), S('u_o', 0), depth=dn)

    def gwu_end():
        @pl.when(r == dh)
        def _():
            wait(gwu(d_odd * DQ, DQ), S('u_out', 0))

        @pl.when(r != dh)
        def _():
            wait(gwu(0, DH), S('u_o', 0))
            wait(gwu(0, DH), S('u_o', 1))

    lane = lax.broadcasted_iota(jnp.int32, (LROWS, 128), 1)

    SB = min(BLK, 128)
    NS = BLK // SB

    def stats_load():
        for b in range(2):
            copy(X.at[tau, dsm(r * TH + b * BLK, BLK, BLK), :], wx.at[b], S('ld', b))

    def stats_part(b):
        wait(wx.at[b], S('ld', b))

        def rows_step(i):
            rr = ds(i * LROWS, LROWS)
            _, mean, inv = norm_rows(wx.at[b], rr)
            s0, s1 = jnp.zeros((LROWS, 1), F32), jnp.zeros((LROWS, 1), F32)
            for col0, slot in ((f * HW, 1 - b), ((1 - f) * HW, 2 + b)):
                cols = ds(col0, HW)
                gh = F4[slot, rr, :] * vec_v[0, :, cols]
                s0 = s0 + jnp.sum(gh, axis=1, keepdims=True)
                s1 = s1 + jnp.sum(gh * ((wx[b, rr, cols].astype(F32) - mean) * inv), axis=1, keepdims=True)
            st_v[rr, :] = jnp.where(lane < 64, s0, s1)
            ms_v[b, rr, :] = jnp.where(lane < 64, mean, inv)
        loop(BLK // LROWS, rows_step)
        for t in range(NS):
            tr = st_v[t * SB:(t + 1) * SB, :].T
            sx_v[b, t:t + 1, :SB] = tr[0:1, :]
            sx_v[b, NS + t:NS + t + 1, :SB] = tr[64:65, :]
        put(sx_v.at[b], sr_v.at[b], S('s_st', b), S('r_st', b), col=cf)

    def stats_recv(b):
        wait(sr_v.at[b], S('r_st', b))
        for t in range(NS):
            for i in range(2):
                row = (sx_v[b, i * NS + t:i * NS + t + 1, :SB] + sr_v[b, i * NS + t:i * NS + t + 1, :SB]) * inv_w
                st2_v[i, t * SB:(t + 1) * SB, :] = jnp.broadcast_to(row, (128, SB)).T

    def dx_final(b, q):
        sub = ds(q * HB2, HB2)
        brow = ds(b * BLK + q * HB2, HB2)
        trow = dsm(r * TH + b * BLK + q * HB2, HB2, HB2)
        xb, gb = wx.at[b, sub, pl.ds(0, HW)], wx.at[2 + b, sub, pl.ds(0, HW)]
        copy(GKEEP.at[brow, :], F4.at[1, sub, :], S('ld', 1))
        copy(X.at[tau, trow, fcols], xb, S('ld', 2))
        copy(DY.at[tau, trow, fcols], gb, S('ld', 3))
        with jax.named_scope('d_far'):
            wait(GFAR.at[brow, :], S('dfar', 2 * b + q))
        copy(GFAR.at[brow, :], F4.at[0, sub, :], S('ld', 0))
        wait(F4.at[1, sub, :], S('ld', 1))
        wait(xb, S('ld', 2))
        wait(gb, S('ld', 3))
        wait(F4.at[0, sub, :], S('ld', 0))

        def rows_step(i):
            rr = dsm(q * HB2 + i * XROWS, XROWS, XROWS)
            mean, inv = ms_v[b, rr, 0:1], ms_v[b, rr, 64:65]
            xhat = (wx[b, rr, :HW].astype(F32) - mean) * inv
            dxn = F4[0, rr, :] + F4[1, rr, :]
            gh = dxn * vec_v[0, :, fcols]
            dx = wx[2 + b, rr, :HW].astype(F32) + inv * (gh - st2_v[0, rr, 0:1] - xhat * st2_v[1, rr, 0:1])
            ob[b, rr, :] = dx.astype(BF16)
            cs_v[0] += jnp.sum((dxn * xhat).reshape(XROWS // 8, 8, HW), axis=0)
            cs_v[1] += jnp.sum(dxn.reshape(XROWS // 8, 8, HW), axis=0)
        loop(HB2 // XROWS, rows_step)
        place('d', dx_out, b, q, 2)

    me = 2 * d + r
    peers = [dict(row=rp)] + [dict(depth=q, row=h) for q in (dn, df, do) for h in range(2)]
    near_in = sumr_v.at[8, :, pl.ds(0, 2 * HB)]

    def sums_1():
        cw = jnp.sum(cs_v[...], axis=1)
        for i in range(2):
            for q in range(2):
                @pl.when(c_odd == q)
                def _():
                    sum_v[0, :, i * HB:(i + 1) * HB] = cw[i:i + 1, q * HB:(q + 1) * HB]
                    sum_v[1, :, i * HB:(i + 1) * HB] = cw[i:i + 1, (1 - q) * HB:(2 - q) * HB]
        put(sum_v.at[1, :, pl.ds(0, 2 * HB)], near_in, S('s_sum', 0), S('r_sum', 0), col=cn)
        sum_v[0, :, 2 * HB:2 * HB + FB] = jnp.zeros((1, FB), F32)
        sum_v[0, :, dsm(2 * HB + r * FH, FH, HB)] = jnp.sum(db_v[0], axis=0, keepdims=True)
        sum_v[0, :, 2 * HB + FB:] = jnp.sum(bd_v[...], axis=0, keepdims=True)

    def sums_2():
        wait(near_in, S('r_sum', 0))
        sumr_v[me, :, :2 * HB] = sum_v[0, :, :2 * HB] + sumr_v[8, :, :2 * HB]
        sumr_v[me, :, 2 * HB:] = sum_v[0, :, 2 * HB:]
        for i, dev in enumerate(peers):
            put(sumr_v.at[me], sumr_v.at[me], S('s_sum', 1 + i), S('r_sum', 1), **dev)

    def sums_3():
        wait(sumr_v.at[pl.ds(0, 7)], S('r_sum', 1))
        total = sumr_v[0]
        for i in range(1, 8):
            total = total + sumr_v[i]
        sum_v[0] = total
        copy(sum_v.at[0], sum_out, S('l_small', 0))

    scope = jax.named_scope

    def g_ready(k):
        wait(DY.at[rp, ds(k * BLK, BLK), pl.ds(0, 2 * HB)], S('gd2d', k))

    def g_own(k):
        wait(reg(DY, k, c), S('gd2w', k))

    with scope('g0'):
        g_near_far(0)
    with scope('g_own'):
        loop(NCH, g_own)
    with scope('dwd_0'):
        dwd_pass((0,))
        dwd_opp(0)
    u_near_load()
    with scope('wuo'):
        wait(wuq(do, 0), S('r_wuy', 2))
        wait(wuq(do, 1), S('r_wuy', 3))
    with scope('u_near'):
        u_near()
    with scope('g12'):
        g_near_far(1)
        g_near_far(2)
    with scope('dwd_a0'):
        dwd_a(0)
    with scope('wd_wait'):
        wait(wd_v.at[pl.ds(0, 2 * FH), pl.ds(0, HB)], S('r_wd', 0))
        for g in range(2):
            for i in range(2, 4):
                wait(wd_bytes(g, QH), S('r_wdy', 4 * g + i))
    with scope('y_give'):
        give('y', A, tile_y, YGOT)
    with scope('g3'):
        g_near_far(3)
    with scope('y_keep_far'):
        keep_far('y', tile_y, YGOT, YFAR, 0, 2)
        keep_far('y', tile_y, YGOT, YFAR, 1, 2)
        give_end('y')
    with scope('g_ready'):
        loop(NCH, g_ready)
    with scope('dwd_12'):
        dwd_pass((1, 2))
        dwd_opp(1)
        dwd_opp(2)
    with scope('g_opp'):
        loop(NCH, g_opp)
        loop(NCH, g_opp_got)
    with scope('dwd_3'):
        dwd_pass((3,))
        dwd_opp(3)
    with scope('dwd_a12'):
        dwd_a(1)
        dwd_a(2)
    with scope('dwd_b0'):
        dwd_b(0)
    with scope('da'):
        da_all()
    with scope('dwd_b12'):
        dwd_b(1)
        dwd_b(2)
    with scope('d_give'):
        give('d', DU, tile_g, GGOT)
    with scope('dwd_b3'):
        dwd_b(3)
    with scope('gwd_send'):
        gwd_send()
    with scope('d_keep_far0'):
        for q in range(2):
            far_end('y', 0, q)
        keep_far('d', tile_g, GGOT, GFAR, 0, 2)
        wait(wx.at[3, :, pl.ds(0, FB)], S('ld', 3))
        give_end('d')
    with scope('dwu_01'):
        dwu_pass((do, df))
        dwu_opp()
    with scope('dwu_23'):
        dwu_pass((dn, d))
    with scope('dwu_a'):
        dwu_a()
    with scope('d_keep_far1'):
        copy(DU.at[0, dsm(r * TH + BLK, BLK, BLK), :], wx.at[3, :, pl.ds(0, FB)], S('ld', 3))
        for q in range(2):
            far_end('y', 1, q)
        keep_far('d', tile_g, GGOT, GFAR, 1, 1)
    with scope('d_keep_own'):
        stats_load()
        keep_own('d', DU, tile_g, GGOT, GKEEP, stats_part)
        far_put('d', GFAR, 1, 1)
    with scope('y_keep_own'):
        keep_own('y', A, tile_y, YGOT, YKEEP)
    with scope('gwd_relay'):
        gwd_relay()
    with scope('y_final'):
        y_final(0)
    with scope('dwu_b'):
        dwu_b()
    with scope('y_final'):
        y_final(1)
    for b in range(2):
        with scope('place_end_y'):
            place_end('y', b, 0, 1)
        with scope('stats'):
            stats_recv(b)
        for q in range(2):
            if b and q:
                with scope('gwu_relay'):
                    gwu_relay()
            with scope('dx'):
                dx_final(b, q)
    with scope('sums_1'):
        sums_1()
    with scope('sums_2'):
        sums_2()
    with scope('sums_3'):
        sums_3()

    with scope('gwu_end'):
        gwu_end()
    with scope('gwd_end'):
        wait(gwd_out.at[pl.ds(0, 4 * QH), :], S('d_o', 0))
    wait(gwd_out.at[pl.ds(0, 4 * QH), :], S('d_o', 1))
    for p, out in (('y', y_out), ('d', dx_out)):
        @pl.when(r == tau)
        def _():
            with scope('out_end'):
                wait(out.at[pl.ds(0, TH), :], S(p + 'out'))

        @pl.when(r != tau)
        def _():
            with scope('out_end'):
                wait(out, S(p + 'out'))
    wait(sum_out, S('l_small', 0))
    for b in range(2):
        for q in range(2):
            place_end('d', b, q, 2)
            far_end('d', b, q)
    for b in range(2):
        wait(sx_v.at[b], S('s_st', b))
    wait(sum_v.at[1, :, pl.ds(0, 2 * HB)], S('s_sum', 0))
    for i in range(7):
        wait(sumr_v.at[0], S('s_sum', 1 + i))
    wait(wun, S('s_wun'))

    @pl.when(r == f)
    def _():
        for s in range(2):
            wait(wd_own(s), S('s_wd0', s))
    for i in range(4):
        wait(wd_dst(0, c), S('s_wdx', i))
    wait(wu_own, S('s_wu'))
    for i in range(3):
        wait(vec_at, S('s_vec', i))
    wait(bu_at, S('s_vec', 3))
    for s in range(2):
        wait(wd_dst(s, cf), S('s_wdr', s))
    for i in range(2):
        wait(wuq(d), S('s_wuy', i))
        wait(wuq(d, 0), S('s_wuy', 2 + i))
    for i in range(12):
        wait(wdq(0, d, c), S('s_wdy', i))
        wait(wdq(0, d, c, 0), S('s_wdy', 12 + i))

    def sends(k):
        for z, Z in (('x', X), ('g', DY)):
            for n in ('s_near', 's_far', 's_rel'):
                wait(reg(Z, k, c), S(z + n, k))
            wait(Z.at[r, ds(k * BLK, BLK), :], S(z + 's_d2d', k))
    loop(NCH, sends)
    for i in range(8):
        wait(r1D.at[0], S('d_so', i))
        wait(gwd(0, d), S('d_sy', i))
        wait(gwd(0, d, 0), S('d_sr', i))
    for j in range(1, 4):
        wait(finD.at[j], S('d_sf', j))

    @pl.when(r != f)
    def _():
        wait(finD.at[0], S('d_sf', 0))
    for i in range(2):
        wait(r1U, S('u_so', i))
        wait(PFU, S('u_sa', i))
        wait(finU, S('u_sf', i))

    @pl.when(r != dh)
    def _():
        wait(finU, S('u_sf', 2))
    wait(gwu(0, DH), S('u_sr'))


def block_kernel(x, dy, wu, wd, vec, bu):
    (TK, HB), FH = x.shape, wu.shape[1] // 2
    W, HW, TH, BLK, QF, FB = 4 * HB, 2 * HB, TK // 2, TK // NCH, FH // 4, 2 * FH
    assert FB <= W and FH <= HW and W // 4 == BLK and QF <= BLK and FH == HW
    sd = jax.ShapeDtypeStruct
    NS = BLK // min(BLK, 128)
    outs = [sd((TK, HB), BF16), sd((TK, HB), BF16), sd((W // 2, FB), BF16), sd((4 * FH, HB), BF16), sd((1, 3 * HB + FB), F32)]
    n_out = len(outs)
    outs += [sd((2, TK, W), BF16)] * 3 + [sd((2, TK, FB), BF16)] * 2 + [sd((2, TK, FB), F32)]
    outs += [sd((TH, W), F32), sd((TH, HW), F32), sd((TH, HW), F32)] * 2
    outs += [sd((4, QF, HB), F32)] * 2 + [sd((W // 4, FH), F32)] * 2
    V = pltpu.VMEM
    scratch = [
        V((W, FB), BF16), V((FB, W), BF16), V((4, FH, HB), F32), V((4, W // 4, FH), F32),
        V((4, FH // 8, HB), F32), V((4, FH // 8, HB), F32), V((W // 8, FH), F32), V((W // 8, FH), F32),
        V((3, 1, W), F32), V((1, FB), F32), V((4, BLK, W), BF16), V((4, BLK, HW), F32), V((2, BLK, HW), BF16),
        V((4, QF, HB), BF16), V((2, 8, FH), F32), V((2, 8, HW), F32),
        V((BLK, 128), F32), V((2, BLK, 128), F32), V((2, BLK, 128), F32), V((2, 2 * NS, 128), F32), V((2, 2 * NS, 128), F32),
        V((8, HB), F32), V((2, 1, 3 * HB + FB), F32), V((9, 1, 3 * HB + FB), F32),
        pltpu.SemaphoreType.DMA((N_SEM,)),
    ]
    res = pl.pallas_call(
        functools.partial(body, (TK, HB, FH)),
        out_shape=outs,
        in_specs=[pl.BlockSpec(memory_space=pl.ANY)] * 6,
        out_specs=[pl.BlockSpec(memory_space=pl.ANY)] * len(outs),
        scratch_shapes=scratch,
        compiler_params=pltpu.CompilerParams(collective_id=0, has_side_effects=True, vmem_limit_bytes=67043328),
        name='mlp_block',
    )(x, dy, wu, wd, vec, bu)
    return res[:n_out]


def solution(mesh):
    assert (mesh.shape['col'], mesh.shape['row'], mesh.shape['depth']) == (4, 2, 4)
    tok_spec = P(('dp', 'depth', 'row'), 'col')
    vec_spec = P('col')
    mat_spec = P('row', 'col')
    grad_vec = P(('dp', 'col'))
    grad_mat = P(('dp', 'row'), 'col')
    def local_pass(x_blk, gamma_blk, beta_blk, w_up_blk, b_up_blk, w_down_blk, b_down_blk, dy_blk):
        hb, fb = x_blk.shape[1], w_up_blk.shape[1]
        vec = jnp.stack([gamma_blk, beta_blk, b_down_blk.astype(F32)])[:, None]
        bu = b_up_blk.astype(F32)[None]
        y_blk, dx_blk, grad_w_up, grad_w_down, sums = block_kernel(x_blk, dy_blk, w_up_blk, w_down_blk, vec, bu)
        sums = sums[0]
        return (y_blk, dx_blk, sums[:hb], sums[hb:2 * hb], grad_w_up, sums[2 * hb:2 * hb + fb], grad_w_down, sums[2 * hb + fb:])

    return jax.shard_map(
        local_pass,
        mesh=mesh,
        in_specs=(tok_spec, vec_spec, vec_spec, mat_spec, vec_spec, mat_spec, vec_spec, tok_spec),
        out_specs=(tok_spec, tok_spec, grad_vec, grad_vec, grad_mat, grad_vec, grad_mat, grad_vec),
        check_vma=False,
    )
```

```python
import functools

import jax
import jax.numpy as jnp
from jax import lax
from jax.experimental import pallas as pl
from jax.experimental.pallas import tpu as pltpu
from jax.sharding import PartitionSpec as P

LN_EPS = 1e-5
F32 = jnp.float32
BF16 = jnp.bfloat16
MESH = pl.DeviceIdType.MESH
GELU_A = 0.7978845608028654
GELU_B = 0.044715
NCH = 4
ROWS = 16
LROWS = 64
XROWS = 32

NN = (((1,), (0,)), ((), ()))
NT = (((1,), (1,)), ((), ()))
TN = (((0,), (0,)), ((), ()))

SEMS = {}
for _z in ('x', 'g'):
    for _n in ('near', 'far', 'opp', 'd2d', 'd2w', 'd2o', 's_near', 's_far', 's_rel', 's_d2d'):
        SEMS[_z + _n] = NCH
    SEMS[_z + 'bounce'] = 2
for _p in ('y', 'd'):
    SEMS.update({_p + 's_give': 2, _p + 'got': 2, _p + 's_far': 4, _p + 'keep': 2, _p + 'far': 4, _p + 's_out': 8, _p + 'out': 1, _p + 'loc': 4})
SEMS.update(l_wu=1, s_wu=1, r_wu=1, s_wun=1, r_wun=1, s_wuy=4, r_wuy=4,
            s_wd0=2, s_wdx=4, r_wd=4, s_wdr=2, s_wdy=24, r_wdy=8,
            l_vec=2, s_vec=4, r_vec=2,
            ld=8, ldb=2, st=6, s_st=2, r_st=2, s_sum=8, r_sum=2,
            d_so=8, d_r=8, d_sa=8, d_p=8, d_sf=4, d_out=1, d_sy=8, d_y=2, d_sr=8, d_o=2,
            u_so=2, u_r=2, u_sa=2, u_p=2, u_sf=3, u_out=3, u_sr=1, u_o=2, l_small=2)
BASE = {}
_at = 0
for _n, _c in SEMS.items():
    BASE[_n] = _at
    _at += _c
N_SEM = _at


def gelu_and_slope(v):
    v2 = v * v
    t = jnp.tanh(v * (GELU_A + (GELU_A * GELU_B) * v2))
    q = (1.0 - t) * (GELU_A + (3.0 * GELU_A * GELU_B) * v2)
    return 0.5 * v * (1.0 + t), 0.5 * ((1.0 + t) * (1.0 + v * q))


def body(dims, x_ref, dy_ref, wu_ref, wd_ref, vec_ref, bu_ref,
         y_out, dx_out, gwu_out, gwd_out, sum_out,
         X, DY, XN, A, DU, SL, YGOT, YFAR, YKEEP, GGOT, GFAR, GKEEP, PFD, PND, PFU, PNU,
         wu_v, wd_v, accD, accU, r1D, r2D, r1U, r2U, vec_v, bu_v, wx, F4, ob, finD,
         db_v, cs_v, st_v, ms_v, st2_v, sx_v, sr_v, bd_v, sum_v, sumr_v, sem):
    TK, HB, FH = dims
    W, HW, TH, BLK, QF = 4 * HB, 2 * HB, TK // 2, TK // NCH, FH // 4
    RH, DQ, QH, DH, FB = W // 2, W // 4, FH // 8, W // 8, 2 * FH
    NTW = HB
    inv_w = 1.0 / W
    finU = wx.at[3, pl.ds(0, DQ), pl.ds(HW, FH)]
    f0, f1 = F4.at[0], F4.at[1]

    c, r, d = lax.axis_index('col'), lax.axis_index('row'), lax.axis_index('depth')
    c_odd, d_odd = lax.rem(c, 2), lax.rem(d, 2)
    cn, cf, co = c + 1 - 2 * c_odd, 3 - c, lax.rem(c + 2, 4)
    dn, df, do = d + 1 - 2 * d_odd, 3 - d, lax.rem(d + 2, 4)
    f, dh = lax.div(c, 2), lax.div(d, 2)
    tau = lax.rem(lax.div(c + 1, 2), 2)
    rp = 1 - r
    o, o2 = c_odd * FH, (1 - c_odd) * FH

    def S(name, i=0):
        return sem.at[BASE[name] + i]

    def ds(start, size):
        return pl.ds(pl.multiple_of(start, size), size)

    def dsm(start, size, mult):
        return pl.ds(pl.multiple_of(start, mult), size)

    def put(src, dst, ssem, rsem, **dev):
        pltpu.make_async_remote_copy(src_ref=src, dst_ref=dst, send_sem=ssem, recv_sem=rsem,
                                     device_id=dev, device_id_type=MESH).start()

    def copy(src, dst, s):
        pltpu.make_async_copy(src, dst, s).start()

    def wait(ref, s):
        pltpu.make_async_copy(ref, ref, s).wait()

    def loop(n, fn):
        def step(i, carry):
            fn(i)
            return carry
        lax.fori_loop(0, n, step, 0)

    bar = pltpu.get_barrier_semaphore()
    for dev in [dict(row=rp)] + [dict(row=h, **q) for h in range(2) for q in
                                 (dict(col=cn), dict(col=cf), dict(col=co), dict(depth=dn), dict(depth=df), dict(depth=do))]:
        pl.semaphore_signal(bar, inc=1, device_id=dev, device_id_type=MESH)
    pl.semaphore_wait(bar, 13)

    def wd_src(s, h):
        return wd_ref.at[dsm((2 * s + h) * FH + d * QF, QF, QF), :]

    def wd_dst(s, col):
        return wd_v.at[dsm(s * FH + d * QF, QF, QF), ds(col * HB, HB)]

    def reg(Z, k, col):
        return Z.at[r, ds(k * BLK, BLK), ds(col * HB, HB)]

    def send_own(z, z_ref, Z, which, chunks=(0, NCH)):
        def step(k):
            src = z_ref.at[ds(k * BLK, BLK), :]
            if 'near' in which:
                put(src, reg(Z, k, c), S(z + 's_near', k), S(z + 'near', k), col=cn)
            if 'far' in which:
                put(src, reg(Z, k, c), S(z + 's_far', k), S(z + 'far', k), col=cf)
            if 'd2d' in which:
                put(src, reg(Z, k, c), S(z + 's_d2d', k), S(z + ('d2d' if z == 'x' else 'd2w'), k), row=rp)
        for k in range(*chunks):
            step(k)

    def d2d(z, Z, k, col, s):
        put(reg(Z, k, col), reg(Z, k, col), S(z + 's_d2d', k), S(z + s, k), row=rp)

    vec_at = vec_v.at[:, :, ds(c * HB, HB)]
    copy(vec_ref, vec_at, S('l_vec', 0))
    put(vec_ref, vec_at, S('s_vec', 0), S('r_vec', 0), col=cn)
    put(vec_ref, vec_at, S('s_vec', 1), S('r_vec', 0), col=cf)
    put(vec_ref, vec_at, S('s_vec', 2), S('r_vec', 0), col=co)
    bu_src, bu_at = bu_ref.at[:, ds(r * FH, FH)], bu_v.at[:, ds(o, FH)]
    copy(bu_src, bu_at, S('l_vec', 1))
    put(bu_src, bu_at, S('s_vec', 3), S('r_vec', 1), col=cn)

    wu_own = wu_v.at[ds(r * RH, RH), ds(o, FH)]
    wd_own = lambda s: wd_v.at[pl.ds(s * FH, FH), ds(c * HB, HB)]

    @pl.when(r != f)
    def _():
        for s in range(2):
            for h in range(2):
                put(wd_src(s, h), wd_dst(s, c), S('s_wdx', 2 * s + h), S('r_wd', 2), col=cf, row=h)

    @pl.when(r == f)
    def _():
        for s in range(2):
            for h in range(2):
                put(wd_src(s, h), wd_dst(s, c), S('s_wdx', 2 * s + h), S('r_wd', 1), col=cn, row=h)
    send_own('x', x_ref, X, ('far',), (0, 2))
    send_own('x', x_ref, X, ('near',), (0, 1))
    put(wu_ref.at[:, ds(rp * FH, FH)], wu_own, S('s_wu'), S('r_wu'), row=rp)
    copy(wu_ref.at[:, ds(r * FH, FH)], wu_own, S('l_wu'))
    send_own('x', x_ref, X, ('d2d',))
    send_own('g', dy_ref, DY, ('d2d',))
    for i, z_ref in enumerate((x_ref, dy_ref)):
        for k in range(NCH):
            copy(z_ref.at[pl.ds(k * BLK, BLK), :], wx.at[i, :, pl.ds(k * HB, HB)], S('xg'[i] + 'bounce', 0))

    @pl.when(r == f)
    def _():
        for s in range(2):
            copy(wd_ref.at[dsm((2 * s + r) * FH, FH, FH), :], wd_own(s), S('r_wd', 0))
            put(wd_ref.at[dsm((2 * s + rp) * FH, FH, FH), :], wd_own(s), S('s_wd0', s), S('r_wd', 0), row=rp)

    for i, Z in enumerate((X, DY)):
        wait(wx.at[i], S('xg'[i] + 'bounce', 0))
        for k in range(NCH):
            copy(wx.at[i, :, pl.ds(k * HB, HB)], reg(Z, k, c), S('xg'[i] + 'bounce', 1))

    with jax.named_scope('wd_far'):
        wait(wd_v.at[pl.ds(0, 2 * QF), pl.ds(0, HB)], S('r_wd', 2))
    for s in range(2):
        put(wd_dst(s, cf), wd_dst(s, cf), S('s_wdr', s), S('r_wd', 3), col=cn)
    send_own('x', x_ref, X, ('near',), (1, NCH - 1))

    with jax.named_scope('wu_own'):
        wait(wu_own, S('l_wu'))
        wait(wu_v.at[ds(rp * RH, RH), ds(o, FH)], S('r_wu'))
    wun = wu_v.at[ds(d * DQ, DQ), ds(o, FH)]
    put(wun, wun, S('s_wun'), S('r_wun'), col=cn)
    send_own('x', x_ref, X, ('near',), (NCH - 1, NCH))

    db_v[...] = jnp.zeros_like(db_v)
    cs_v[...] = jnp.zeros_like(cs_v)
    bd_v[...] = jnp.zeros_like(bd_v)

    def dy_sum(i):
        rr = ds(i * ROWS, ROWS)
        part = jnp.sum(wx[1, rr, :].astype(F32).reshape(ROWS // 8, 8, W), axis=0)
        bd_v[...] += part[:, :HB] + part[:, HB:2 * HB] + part[:, 2 * HB:3 * HB] + part[:, 3 * HB:]
    with jax.named_scope('dy_sum'):
        loop(BLK // ROWS, dy_sum)

    def wuq(dd, half=None):
        if half is None:
            return wu_v.at[ds(dd * DQ, DQ), ds(o2, FH)]
        return wu_v.at[dsm(dd * DQ + half * DH, DH, DH), ds(o2, FH)]

    def wu_send():
        with jax.named_scope('wu_near'):
            wait(wuq(d), S('r_wun'))
        put(wuq(d), wuq(d), S('s_wuy', 0), S('r_wuy', 0), depth=dn)
        put(wuq(d), wuq(d), S('s_wuy', 1), S('r_wuy', 1), depth=df)

    def wu_relay():
        with jax.named_scope('wuy'):
            wait(wuq(dn), S('r_wuy', 0))
            wait(wuq(df), S('r_wuy', 1))
        put(wuq(dn, 1), wuq(dn, 1), S('s_wuy', 2), S('r_wuy', 3), depth=df)
        put(wuq(df, 0), wuq(df, 0), S('s_wuy', 3), S('r_wuy', 2), depth=dn)

    def wdq(s, dd, col, half=None):
        if half is None:
            return wd_v.at[dsm(s * FH + dd * QF, QF, QF), ds(col * HB, HB)]
        return wd_v.at[dsm(s * FH + dd * QF + half * QH, QH, QH), ds(col * HB, HB)]

    W_GROUPS = (((0, cn), (1, cf)), ((2, co),))

    def wd_send(g):
        if g == 0:
            wait(wd_v.at[pl.ds(0, 2 * QF), pl.ds(0, HB)], S('r_wd', 1))
        else:
            wait(wd_v.at[pl.ds(0, 2 * QF), pl.ds(0, HB)], S('r_wd', 3))
        for i, col in W_GROUPS[g]:
            for s in range(2):
                put(wdq(s, d, col), wdq(s, d, col), S('s_wdy', 4 * i + s), S('r_wdy', 4 * g), depth=dn)
                put(wdq(s, d, col), wdq(s, d, col), S('s_wdy', 4 * i + 2 + s), S('r_wdy', 4 * g + 1), depth=df)

    def wd_bytes(g, rows):
        return wd_v.at[pl.ds(0, 2 * rows), pl.ds(0, len(W_GROUPS[g]) * HB)]

    def wd_relay(g):
        for i in range(2):
            wait(wd_bytes(g, QF), S('r_wdy', 4 * g + i))
        for i, col in W_GROUPS[g]:
            for s in range(2):
                put(wdq(s, dn, col, 1), wdq(s, dn, col, 1), S('s_wdy', 12 + 4 * i + s), S('r_wdy', 4 * g + 3), depth=df)
                put(wdq(s, df, col, 0), wdq(s, df, col, 0), S('s_wdy', 12 + 4 * i + 2 + s), S('r_wdy', 4 * g + 2), depth=dn)

    def x_near(k):
        wait(reg(X, k, cn), S('xnear', k))
        put(reg(X, k, cn), reg(X, k, cn), S('xs_rel', k), S('xopp', k), col=cf)
        d2d('x', X, k, cn, 'd2d')

    with jax.named_scope('wd_send0'):
        wd_send(0)
    with jax.named_scope('x_near'):
        x_near(0)
    send_own('x', x_ref, X, ('far',), (2, 3))

    for i, Z in enumerate((X, DY)):
        wait(wx.at[i], S('xg'[i] + 'bounce', 1))
    wait(vec_at, S('l_vec', 0))
    wait(vec_v.at[:, :, pl.ds(0, 3 * HB)], S('r_vec', 0))
    wait(bu_at, S('l_vec', 1))
    wait(bu_at, S('r_vec', 1))

    def norm_rows(buf, rows):
        xf = buf[rows, :].astype(F32)
        mean = jnp.sum(xf, axis=1, keepdims=True) * inv_w
        cen = xf - mean
        inv = lax.rsqrt(jnp.sum(cen * cen, axis=1, keepdims=True) * inv_w + LN_EPS)
        return cen, mean, inv

    def tok_of(s):
        return tau + s * (1 - 2 * tau)

    N_T = FH // NTW

    def chain(tiles, hooks=None):
        hooks = hooks or {}

        def hook(what, i):
            for fn in hooks.get((what, i), ()):
                fn()
        for i, (product, _) in enumerate(tiles):
            hook('before', i)
            if i:
                tiles[i - 1][1](F4.at[(i - 1) % 2])
            F4[i % 2, :, :NTW] = product()
            hook('product', i)
            if i:
                hook('epilogue', i - 1)
        tiles[-1][1](F4.at[(len(tiles) - 1) % 2])
        hook('epilogue', len(tiles) - 1)

    def u_tile(src, i, n, start):
        cols = ds(start + n * NTW, NTW)
        at = pl.ds(n * NTW, NTW)

        def product():
            return lax.dot_general(wx[src], wu_v[:, cols], NN, preferred_element_type=F32)

        def epilogue(acc):
            u = (acc[:, :NTW] + bu_v[0:1, cols]).astype(BF16)
            a, slope = gelu_and_slope(u.astype(F32))
            ob[i, :, at] = a.astype(BF16)
            F4[2 + i, :, at] = slope
        return product, epilogue

    def u_store(i, s, rows, start):
        copy(ob.at[i], A.at[s, rows, ds(start, FH)], S('st', 2 + i))
        copy(F4.at[2 + i], SL.at[s, rows, ds(start, FH)], S('st', 4 + i))

    def u_stored():
        for i in range(2):
            wait(ob.at[i], S('st', 2 + i))
            wait(F4.at[2 + i], S('st', 4 + i))

    def phase1(k):
        @pl.when(k < NCH - 1)
        def _():
            with jax.named_scope('x_near'):
                x_near(k + 1)

        @pl.when(k == 0)
        def _():
            send_own('x', x_ref, X, ('far',), (3, 4))
            with jax.named_scope('wd_send1'):
                wd_send(1)

        @pl.when(k == 1)
        def _():
            with jax.named_scope('wd_relay0'):
                wd_relay(0)
            send_own('g', dy_ref, DY, ('near',))

        @pl.when(k == 2)
        def _():
            send_own('g', dy_ref, DY, ('far',))
            wu_send()
            with jax.named_scope('wd_relay1'):
                wd_relay(1)

        with jax.named_scope('x_far'):
            wait(reg(X, k, cf), S('xfar', k))
            d2d('x', X, k, cf, 'd2d')
        with jax.named_scope('x_opp'):
            wait(reg(X, k, co), S('xopp', k))
            d2d('x', X, k, co, 'd2d')

        rows = ds(k * BLK, BLK)
        with jax.named_scope('x_d2d'):
            wait(X.at[rp, rows, :], S('xd2d', k))

        @pl.when(k == NCH - 1)
        def _():
            wu_relay()

        @pl.when(k > 0)
        def _():
            for s in range(2):
                wait(wx.at[s], S('st', s))
        for s in range(2):
            copy(X.at[tok_of(s), rows, :], wx.at[s], S('ld', s))
        for s in range(2):
            wait(wx.at[s], S('ld', s))

            def ln(i):
                rr = ds(i * LROWS, LROWS)
                cen, _, inv = norm_rows(wx.at[s], rr)
                wx[s, rr, :] = (cen * inv * vec_v[0] + vec_v[1]).astype(BF16)
            with jax.named_scope('ln'):
                loop(BLK // LROWS, ln)
            copy(wx.at[s], XN.at[s, rows, :], S('st', s))
        pl.when(k > 0)(u_stored)
        with jax.named_scope('u_own'):
            chain([u_tile(i, i, n, o) for i in range(2) for n in range(N_T)])
        for s in range(2):
            u_store(s, s, rows, o)
    loop(NCH, phase1)
    for s in range(2):
        wait(wx.at[s], S('st', s))
    u_stored()

    def u_near_load():
        for b in range(NCH):
            copy(XN.at[0, pl.ds(b * BLK, BLK), :], wx.at[b], S('ld', b))

    def u_near():
        def step(kp):
            for i in range(2):
                wait(wx.at[2 * kp + i], S('ld', 2 * kp + i))
            chain([u_tile(2 * kp + i, i, n, o2) for i in range(2) for n in range(N_T)],
                  {('before', 1): [lambda: pl.when(kp > 0)(u_stored)]})
            for i in range(2):
                u_store(i, 0, ds((2 * kp + i) * BLK, BLK), o2)
        loop(NCH // 2, step)
        u_stored()

    def g_near_far(k):
        wait(reg(DY, k, cf), S('gfar', k))
        put(reg(DY, k, cf), reg(DY, k, cf), S('gs_rel', k), S('gopp', k), col=cn)
        d2d('g', DY, k, cf, 'd2d')
        wait(reg(DY, k, cn), S('gnear', k))
        d2d('g', DY, k, cn, 'd2d')

    def g_opp(k):
        wait(reg(DY, k, co), S('gopp', k))
        d2d('g', DY, k, co, 'd2o')

    def g_opp_got(k):
        wait(reg(DY, k, co), S('gd2o', k))

    def tile_y(lhs, col):
        return lax.dot_general(lhs, wd_v[:, dsm(col, NTW, NTW)], NN, preferred_element_type=F32)

    def tile_g(lhs, col):
        return lax.dot_general(lhs, wu_v[dsm(col, NTW, NTW), :], NT, preferred_element_type=F32)

    def give(p, src, tile, GOT):
        def blk(b):
            return src.at[0, dsm(rp * TH + b * BLK, BLK, BLK), :]
        for b in range(2):
            copy(blk(b), wx.at[b, :, pl.ds(0, FB)], S('ld', b))
        keep_load(src)

        def step(b):
            wait(wx.at[b, :, pl.ds(0, FB)], S('ld', b))

            def half(h):
                @pl.when(b == 1)
                def _():
                    wait(F4.at[h], S(p + 's_give', h))

                def n_tile(n):
                    F4[h, :, ds(n * NTW, NTW)] = tile(wx[b, :, :FB], h * HW + n * NTW)
                loop(HW // NTW, n_tile)
                put(F4.at[h], GOT.at[ds(b * BLK, BLK), ds(h * HW, HW)], S(p + 's_give', h), S(p + 'got', b), row=rp)
            loop(2, half)
        loop(2, step)

    HB2 = BLK // 2

    def keep_load(src):
        for b in range(2):
            copy(src.at[0, dsm(r * TH + b * BLK, BLK, BLK), :], wx.at[2 + b, :, pl.ds(0, FB)], S('ld', 2 + b))

    def got_load(GOT, b, col0, out, s_):
        copy(GOT.at[ds(b * BLK, BLK), ds(col0, HW)], F4.at[out], s_)

    def add_tiles(b, out, tile, col0):
        def n_tile(n):
            at = ds(n * NTW, NTW)
            F4[out, :, at] = F4[out, :, at] + tile(wx[2 + b, :, :FB], col0 + n * NTW)
        loop(HW // NTW, n_tile)

    def far_put(p, FAR, b, q):
        put(F4.at[2 + b, ds(q * HB2, HB2), :], FAR.at[ds(b * BLK + q * HB2, HB2), :], S(p + 's_far', 2 * b + q), S(p + 'far', 2 * b + q), col=cf)

    def give_end(p):
        for h in range(2):
            wait(F4.at[h], S(p + 's_give', h))

    def keep_far(p, tile, GOT, FAR, b, pieces):
        with jax.named_scope('got'):
            wait(GOT.at[ds(b * BLK, BLK), :], S(p + 'got', b))
        got_load(GOT, b, (1 - f) * HW, 2 + b, S('ld', 4 + b))
        wait(wx.at[2 + b, :, pl.ds(0, FB)], S('ld', 2 + b))
        wait(F4.at[2 + b], S('ld', 4 + b))
        add_tiles(b, 2 + b, tile, (1 - f) * HW)
        for q in range(pieces):
            far_put(p, FAR, b, q)

    def keep_own(p, src, tile, GOT, KEEP, after=None):
        keep_load(src)
        for b in range(2):
            got_load(GOT, b, f * HW, 1 - b, S('ld', 4 + b))

        def step(b):
            wait(wx.at[2 + b, :, pl.ds(0, FB)], S('ld', 2 + b))
            wait(F4.at[1 - b], S('ld', 4 + b))
            add_tiles(b, 1 - b, tile, f * HW)
            copy(F4.at[1 - b], KEEP.at[ds(b * BLK, BLK), :], S(p + 'keep', b))
            if after:
                after(b)
        loop(2, step)
        for b in range(2):
            wait(F4.at[b], S(p + 'keep', b))

    def far_end(p, b, q):
        wait(F4.at[2 + b, ds(q * HB2, HB2), :], S(p + 's_far', 2 * b + q))

    def place(p, out, b, q, nq):
        nr = BLK // nq
        rr = ds(q * nr, nr)
        dst = out.at[dsm(r * TH + b * BLK + q * nr, nr, nr), :]
        mine, other = ob.at[b, rr, ds(c_odd * HB, HB)], ob.at[b, rr, ds((1 - c_odd) * HB, HB)]
        put(other, dst, S(p + 's_out', 4 * b + 2 * q), S(p + 'out'), col=cn, row=tau)

        @pl.when(r == tau)
        def _():
            copy(mine, dst, S(p + 'loc', 2 * b + q))

        @pl.when(r != tau)
        def _():
            put(mine, dst, S(p + 's_out', 4 * b + 2 * q + 1), S(p + 'out'), row=rp)

    def place_end(p, b, q, nq):
        part = ob.at[b, pl.ds(0, BLK // nq), pl.ds(0, HB)]
        wait(part, S(p + 's_out', 4 * b + 2 * q))

        @pl.when(r == tau)
        def _():
            wait(part, S(p + 'loc', 2 * b + q))

        @pl.when(r != tau)
        def _():
            wait(part, S(p + 's_out', 4 * b + 2 * q + 1))

    fcols = ds(f * HW, HW)

    def y_final(b):
        brow = ds(b * BLK, BLK)
        for q in range(2):
            wait(YFAR.at[ds(b * BLK + q * HB2, HB2), :], S('yfar', 2 * b + q))
        copy(YFAR.at[brow, :], f0, S('ld', 0))
        copy(YKEEP.at[brow, :], f1, S('ld', 1))
        copy(X.at[tau, dsm(r * TH + b * BLK, BLK, BLK), fcols], wx.at[0, :, pl.ds(0, HW)], S('ld', 2))
        wait(f0, S('ld', 0))
        wait(f1, S('ld', 1))
        wait(wx.at[0, :, pl.ds(0, HW)], S('ld', 2))

        def fin(i):
            rr = ds(i * ROWS, ROWS)
            ob[b, rr, :] = (wx[0, rr, :HW].astype(F32) + (f0[rr, :] + f1[rr, :]) + vec_v[2, :, fcols]).astype(BF16)
        loop(BLK // ROWS, fin)
        place('y', y_out, b, 0, 1)

    def services(t):
        @pl.when(t == 3)
        def _():
            with jax.named_scope('dwd_a3'):
                dwd_a(3)

    def da_all():
        def part(t, i):
            near = lax.div(t, NCH)
            tok = tau + i * (1 - near) * (1 - 2 * tau)
            chunk = t * (1 - near) + near * (2 * (t - NCH) + i)
            return near, tok, i * (1 - near), ds(chunk * BLK, BLK), near * o2 + (1 - near) * o

        def load(t, p):
            for i in range(2):
                _, tok, us, rows, start = part(t, i)
                copy(DY.at[tok, rows, :], wx.at[2 * p + i], S('ld', 2 * p + i))
                copy(SL.at[us, rows, ds(start, FH)], accU.at[2 * p + i], S('ld', 4 + 2 * p + i))

        def store(t, i):
            _, _, us, rows, start = part(t, i)
            copy(ob.at[i], DU.at[us, rows, ds(start, FH)], S('st', 4 + i))

        def stored():
            for i in range(2):
                wait(ob.at[i], S('st', 4 + i))

        n_steps = NCH + NCH // 2

        def step(t):
            near, _, _, _, start = part(t, 0)
            p = lax.rem(t, 2)
            services(t)
            for i in range(2):
                wait(wx.at[2 * p + i], S('ld', 2 * p + i))
                wait(accU.at[2 * p + i], S('ld', 4 + 2 * p + i))

            @pl.when(t < n_steps - 1)
            def _():
                load(t + 1, 1 - p)

            def tile(i, n):
                cols = ds(start + n * NTW, NTW)
                at = pl.ds(n * NTW, NTW)

                def product():
                    return lax.dot_general(wx[2 * p + i], wd_v[cols, :], NT, preferred_element_type=F32)

                def epilogue(acc):
                    du = (acc[:, :NTW] * accU[2 * p + i, :, at]).astype(BF16)
                    ob[i, :, at] = du
                    db_v[near, :, at] += jnp.sum(du.astype(F32).reshape(BLK // 8, 8, NTW), axis=0)
                return product, epilogue
            chain([tile(i, n) for i in range(2) for n in range(N_T)], {('before', 1): [lambda: pl.when(t > 0)(stored)]})
            for i in range(2):
                store(t, i)
        load(0, 0)
        loop(n_steps, step)
        stored()

    def rows_of(kb):
        return ds(lax.rem(kb, NCH) * BLK, BLK), lax.div(kb, NCH)

    d_col = (c, cn, cf, co)

    NB, NSLOT = 2 * NCH, 4

    def k_loop(load, use, width):
        for kb in range(NSLOT - 1):
            load(kb, wx.at[kb], S('ld', kb))

        def step(kb):
            slot = lax.rem(kb, NSLOT)

            @pl.when(kb + NSLOT - 1 < NB)
            def _():
                nxt = lax.rem(kb + NSLOT - 1, NSLOT)
                load(kb + NSLOT - 1, wx.at[nxt], S('ld', nxt))
            buf = wx.at[slot]
            wait(buf.at[:, pl.ds(0, width)], S('ld', slot))
            use(buf)
        loop(NB, step)

    def dwd_pass(js):
        def load(kb, buf, s_):
            rows, s = rows_of(kb)
            copy(A.at[s, rows, ds(o, FH)], buf.at[:, pl.ds(0, FH)], s_)
            for i, j in enumerate(js):
                copy(DY.at[tok_of(s), rows, ds(d_col[j] * HB, HB)], buf.at[:, pl.ds(FH + i * HB, HB)], s_)

        def use(buf):
            for i, j in enumerate(js):
                for m in range(2):
                    mm = slice(m * FH // 2, (m + 1) * FH // 2)
                    accD[j, mm, :] += lax.dot_general(buf[:, mm], buf[:, FH + i * HB:FH + (i + 1) * HB], TN, preferred_element_type=F32)
        for j in js:
            accD[j] = jnp.zeros((FH, HB), F32)
        k_loop(load, use, FH + len(js) * HB)

    def dwd_opp(j):
        put(accD.at[j, dsm(do * QF, QH, QH), :], r1D.at[j], S('d_so', 2 * j), S('d_r', 2 * j), depth=dn)
        put(accD.at[j, dsm(do * QF + QH, QH, QH), :], r2D.at[j], S('d_so', 2 * j + 1), S('d_r', 2 * j + 1), depth=df)

    def dwd_a(j):
        wait(r1D.at[j], S('d_r', 2 * j))
        rr = dsm(df * QF, QH, QH)
        accD[j, rr, :] += r1D[j]
        put(accD.at[j, ds(df * QF, QF), :], PFD.at[j], S('d_sa', 2 * j), S('d_p', 2 * j), depth=df)
        wait(r2D.at[j], S('d_r', 2 * j + 1))
        rr = dsm(dn * QF + QH, QH, QH)
        accD[j, rr, :] += r2D[j]
        put(accD.at[j, ds(dn * QF, QF), :], PND.at[j], S('d_sa', 2 * j + 1), S('d_p', 2 * j + 1), depth=dn)

    def dwd_rows(q, h, dd):
        return dsm((2 * q + h) * FH + dd * QF, QF, QF)

    def dwd_b(j):
        wait(PFD.at[j], S('d_p', 2 * j))
        wait(PND.at[j], S('d_p', 2 * j + 1))
        wait(PFD.at[j], S('d_sa', 2 * j))
        wait(PND.at[j], S('d_sa', 2 * j + 1))
        pf, pn = accD.at[j, ds(df * QF, QF), :], accD.at[j, ds(dn * QF, QF), :]
        copy(PFD.at[j], pf, S('ldb', 0))
        copy(PND.at[j], pn, S('ldb', 1))
        wait(pf, S('ldb', 0))
        wait(pn, S('ldb', 1))
        finD[j] = (accD[j, ds(d * QF, QF), :] + (pf[...] + pn[...])).astype(BF16)
        dst = gwd_out.at[dwd_rows(c_odd, r, d), :]
        if j:
            put(finD.at[j], dst, S('d_sf', j), S('d_out'), col=d_col[j], row=f)
        else:
            @pl.when(r == f)
            def _():
                copy(finD.at[0], dst, S('d_out'))

            @pl.when(r != f)
            def _():
                put(finD.at[0], dst, S('d_sf', 0), S('d_out'), row=rp)

    def gwd(i, dd, half=None):
        if half is None:
            return gwd_out.at[dsm(i * FH + dd * QF, QF, QF), :]
        return gwd_out.at[dsm(i * FH + dd * QF + half * QH, QH, QH), :]

    def gwd_send():
        wait(gwd_out.at[pl.ds(0, 4 * QF), :], S('d_out'))
        for i in range(4):
            put(gwd(i, d), gwd(i, d), S('d_sy', i), S('d_y', 0), depth=dn)
            put(gwd(i, d), gwd(i, d), S('d_sy', 4 + i), S('d_y', 1), depth=df)

    def gwd_relay():
        wait(gwd_out.at[pl.ds(0, 4 * QF), :], S('d_y', 0))
        for i in range(4):
            put(gwd(i, dn, 1), gwd(i, dn, 1), S('d_sr', i), S('d_o', 1), depth=df)
        wait(gwd_out.at[pl.ds(0, 4 * QF), :], S('d_y', 1))
        for i in range(4):
            put(gwd(i, df, 0), gwd(i, df, 0), S('d_sr', 4 + i), S('d_o', 0), depth=dn)

    def dwu_pass(dds):
        def load(kb, buf, s_):
            rows, s = rows_of(kb)
            copy(DU.at[s, rows, ds(o, FH)], buf.at[:, pl.ds(0, FH)], s_)
            for i, dd in enumerate(dds):
                copy(XN.at[s, rows, ds(dd * DQ, DQ)], buf.at[:, pl.ds(FH + i * DQ, DQ)], s_)

        def use(buf):
            for i, dd in enumerate(dds):
                for m in range(2):
                    mm = slice(m * FH // 2, (m + 1) * FH // 2)
                    accU[dd, :, mm] += lax.dot_general(buf[:, FH + i * DQ:FH + (i + 1) * DQ], buf[:, mm], TN, preferred_element_type=F32)
        for dd in dds:
            accU[dd] = jnp.zeros((DQ, FH), F32)
        k_loop(load, use, FH + len(dds) * DQ)

    def dwu_opp():
        put(accU.at[do, pl.ds(0, DH), :], r1U, S('u_so', 0), S('u_r', 0), depth=dn)
        put(accU.at[do, pl.ds(DH, DH), :], r2U, S('u_so', 1), S('u_r', 1), depth=df)

    def dwu_a():
        wait(r1U, S('u_r', 0))
        accU[df, :DH, :] += r1U[...]
        put(accU.at[df], PFU, S('u_sa', 0), S('u_p', 0), depth=df)
        wait(r2U, S('u_r', 1))
        accU[dn, DH:, :] += r2U[...]
        put(accU.at[dn], PNU, S('u_sa', 1), S('u_p', 1), depth=dn)

    def dwu_b():
        wait(PFU, S('u_p', 0))
        wait(PNU, S('u_p', 1))
        pf, pn = f0.at[pl.ds(0, DQ), pl.ds(0, FH)], f1.at[pl.ds(0, DQ), pl.ds(0, FH)]
        copy(PFU, pf, S('ldb', 0))
        copy(PNU, pn, S('ldb', 1))
        wait(pf, S('ldb', 0))
        wait(pn, S('ldb', 1))

        def fin(i):
            rr = ds(i * ROWS, ROWS)
            wx[3, rr, HW:HW + FH] = (accU[d, rr, :] + (f0[rr, :FH] + f1[rr, :FH])).astype(BF16)
        loop(DQ // ROWS, fin)
        dst = gwu_out.at[ds(d_odd * DQ, DQ), ds(r * FH, FH)]
        put(finU, dst, S('u_sf', 0), S('u_out', 1), depth=dn, row=dh)
        put(finU, dst, S('u_sf', 1), S('u_out', 2), depth=df, row=dh)

        @pl.when(r == dh)
        def _():
            copy(finU, dst, S('u_out', 0))

        @pl.when(r != dh)
        def _():
            put(finU, dst, S('u_sf', 2), S('u_out', 0), row=rp)

    def gwu(start, size):
        return gwu_out.at[dsm(start, size, size), :]

    def gwu_relay():
        @pl.when(r == dh)
        def _():
            wait(gwu(lax.rem(dn, 2) * DQ, DQ), S('u_out', 1))
            part = gwu(lax.rem(dn, 2) * DQ + DH, DH)
            put(part, part, S('u_sr'), S('u_o', 1), depth=df)

        @pl.when(r != dh)
        def _():
            wait(gwu(lax.rem(df, 2) * DQ, DQ), S('u_out', 2))
            part = gwu(lax.rem(df, 2) * DQ, DH)
            put(part, part, S('u_sr'), S('u_o', 0), depth=dn)

    def gwu_end():
        @pl.when(r == dh)
        def _():
            wait(gwu(d_odd * DQ, DQ), S('u_out', 0))

        @pl.when(r != dh)
        def _():
            wait(gwu(0, DH), S('u_o', 0))
            wait(gwu(0, DH), S('u_o', 1))

    lane = lax.broadcasted_iota(jnp.int32, (LROWS, 128), 1)

    SB = min(BLK, 128)
    NS = BLK // SB

    def stats_load():
        for b in range(2):
            copy(X.at[tau, dsm(r * TH + b * BLK, BLK, BLK), :], wx.at[b], S('ld', b))

    def stats_part(b):
        wait(wx.at[b], S('ld', b))

        def rows_step(i):
            rr = ds(i * LROWS, LROWS)
            _, mean, inv = norm_rows(wx.at[b], rr)
            s0, s1 = jnp.zeros((LROWS, 1), F32), jnp.zeros((LROWS, 1), F32)
            for col0, slot in ((f * HW, 1 - b), ((1 - f) * HW, 2 + b)):
                cols = ds(col0, HW)
                gh = F4[slot, rr, :] * vec_v[0, :, cols]
                s0 = s0 + jnp.sum(gh, axis=1, keepdims=True)
                s1 = s1 + jnp.sum(gh * ((wx[b, rr, cols].astype(F32) - mean) * inv), axis=1, keepdims=True)
            st_v[rr, :] = jnp.where(lane < 64, s0, s1)
            ms_v[b, rr, :] = jnp.where(lane < 64, mean, inv)
        loop(BLK // LROWS, rows_step)
        for t in range(NS):
            tr = st_v[t * SB:(t + 1) * SB, :].T
            sx_v[b, t:t + 1, :SB] = tr[0:1, :]
            sx_v[b, NS + t:NS + t + 1, :SB] = tr[64:65, :]
        put(sx_v.at[b], sr_v.at[b], S('s_st', b), S('r_st', b), col=cf)

    def stats_recv(b):
        wait(sr_v.at[b], S('r_st', b))
        for t in range(NS):
            for i in range(2):
                row = (sx_v[b, i * NS + t:i * NS + t + 1, :SB] + sr_v[b, i * NS + t:i * NS + t + 1, :SB]) * inv_w
                st2_v[i, t * SB:(t + 1) * SB, :] = jnp.broadcast_to(row, (128, SB)).T

    def dx_final(b, q):
        sub = ds(q * HB2, HB2)
        brow = ds(b * BLK + q * HB2, HB2)
        trow = dsm(r * TH + b * BLK + q * HB2, HB2, HB2)
        xb, gb = wx.at[b, sub, pl.ds(0, HW)], wx.at[2 + b, sub, pl.ds(0, HW)]
        copy(GKEEP.at[brow, :], F4.at[1, sub, :], S('ld', 1))
        copy(X.at[tau, trow, fcols], xb, S('ld', 2))
        copy(DY.at[tau, trow, fcols], gb, S('ld', 3))
        with jax.named_scope('d_far'):
            wait(GFAR.at[brow, :], S('dfar', 2 * b + q))
        copy(GFAR.at[brow, :], F4.at[0, sub, :], S('ld', 0))
        wait(F4.at[1, sub, :], S('ld', 1))
        wait(xb, S('ld', 2))
        wait(gb, S('ld', 3))
        wait(F4.at[0, sub, :], S('ld', 0))

        def rows_step(i):
            rr = dsm(q * HB2 + i * XROWS, XROWS, XROWS)
            mean, inv = ms_v[b, rr, 0:1], ms_v[b, rr, 64:65]
            xhat = (wx[b, rr, :HW].astype(F32) - mean) * inv
            dxn = F4[0, rr, :] + F4[1, rr, :]
            gh = dxn * vec_v[0, :, fcols]
            dx = wx[2 + b, rr, :HW].astype(F32) + inv * (gh - st2_v[0, rr, 0:1] - xhat * st2_v[1, rr, 0:1])
            ob[b, rr, :] = dx.astype(BF16)
            cs_v[0] += jnp.sum((dxn * xhat).reshape(XROWS // 8, 8, HW), axis=0)
            cs_v[1] += jnp.sum(dxn.reshape(XROWS // 8, 8, HW), axis=0)
        loop(HB2 // XROWS, rows_step)
        place('d', dx_out, b, q, 2)

    me = 2 * d + r
    peers = [dict(row=rp)] + [dict(depth=q, row=h) for q in (dn, df, do) for h in range(2)]
    near_in = sumr_v.at[8, :, pl.ds(0, 2 * HB)]

    def sums_1():
        cw = jnp.sum(cs_v[...], axis=1)
        for i in range(2):
            for q in range(2):
                @pl.when(c_odd == q)
                def _():
                    sum_v[0, :, i * HB:(i + 1) * HB] = cw[i:i + 1, q * HB:(q + 1) * HB]
                    sum_v[1, :, i * HB:(i + 1) * HB] = cw[i:i + 1, (1 - q) * HB:(2 - q) * HB]
        put(sum_v.at[1, :, pl.ds(0, 2 * HB)], near_in, S('s_sum', 0), S('r_sum', 0), col=cn)
        sum_v[0, :, 2 * HB:2 * HB + FB] = jnp.zeros((1, FB), F32)
        sum_v[0, :, dsm(2 * HB + r * FH, FH, HB)] = jnp.sum(db_v[0], axis=0, keepdims=True)
        sum_v[0, :, 2 * HB + FB:] = jnp.sum(bd_v[...], axis=0, keepdims=True)

    def sums_2():
        wait(near_in, S('r_sum', 0))
        sumr_v[me, :, :2 * HB] = sum_v[0, :, :2 * HB] + sumr_v[8, :, :2 * HB]
        sumr_v[me, :, 2 * HB:] = sum_v[0, :, 2 * HB:]
        for i, dev in enumerate(peers):
            put(sumr_v.at[me], sumr_v.at[me], S('s_sum', 1 + i), S('r_sum', 1), **dev)

    def sums_3():
        wait(sumr_v.at[pl.ds(0, 7)], S('r_sum', 1))
        total = sumr_v[0]
        for i in range(1, 8):
            total = total + sumr_v[i]
        sum_v[0] = total
        copy(sum_v.at[0], sum_out, S('l_small', 0))

    scope = jax.named_scope

    def g_ready(k):
        wait(DY.at[rp, ds(k * BLK, BLK), pl.ds(0, 2 * HB)], S('gd2d', k))

    def g_own(k):
        wait(reg(DY, k, c), S('gd2w', k))

    with scope('g0'):
        g_near_far(0)
    with scope('g_own'):
        loop(NCH, g_own)
    with scope('dwd_0'):
        dwd_pass((0,))
        dwd_opp(0)
    u_near_load()
    with scope('wuo'):
        wait(wuq(do, 0), S('r_wuy', 2))
        wait(wuq(do, 1), S('r_wuy', 3))
    with scope('u_near'):
        u_near()
    with scope('g12'):
        g_near_far(1)
        g_near_far(2)
    with scope('dwd_a0'):
        dwd_a(0)
    with scope('wd_wait'):
        wait(wd_v.at[pl.ds(0, 2 * FH), pl.ds(0, HB)], S('r_wd', 0))
        for g in range(2):
            for i in range(2, 4):
                wait(wd_bytes(g, QH), S('r_wdy', 4 * g + i))
    with scope('y_give'):
        give('y', A, tile_y, YGOT)
    with scope('g3'):
        g_near_far(3)
    with scope('y_keep_far'):
        keep_far('y', tile_y, YGOT, YFAR, 0, 2)
        keep_far('y', tile_y, YGOT, YFAR, 1, 2)
        give_end('y')
    with scope('g_ready'):
        loop(NCH, g_ready)
    with scope('dwd_12'):
        dwd_pass((1, 2))
        dwd_opp(1)
        dwd_opp(2)
    with scope('g_opp'):
        loop(NCH, g_opp)
        loop(NCH, g_opp_got)
    with scope('dwd_3'):
        dwd_pass((3,))
        dwd_opp(3)
    with scope('dwd_a12'):
        dwd_a(1)
        dwd_a(2)
    with scope('dwd_b0'):
        dwd_b(0)
    with scope('da'):
        da_all()
    with scope('dwd_b12'):
        dwd_b(1)
        dwd_b(2)
    with scope('d_give'):
        give('d', DU, tile_g, GGOT)
    with scope('dwd_b3'):
        dwd_b(3)
    with scope('d_give_end'):
        for b in range(2):
            wait(wx.at[2 + b, :, pl.ds(0, FB)], S('ld', 2 + b))
        give_end('d')
    with scope('dwu_01'):
        dwu_pass((do, df))
        dwu_opp()
    with scope('gwd_send'):
        gwd_send()
    with scope('dwu_23'):
        dwu_pass((dn, d))
    keep_load(DU)
    for b in range(2):
        with scope('far_end_y'):
            for q in range(2):
                far_end('y', b, q)
        with scope('d_keep_far'):
            keep_far('d', tile_g, GGOT, GFAR, b, 2 - b)
    with scope('dwu_a'):
        dwu_a()
    with scope('d_keep_own'):
        stats_load()
        keep_own('d', DU, tile_g, GGOT, GKEEP, stats_part)
        far_put('d', GFAR, 1, 1)
    with scope('y_keep_own'):
        keep_own('y', A, tile_y, YGOT, YKEEP)
    with scope('gwd_relay'):
        gwd_relay()
    with scope('y_final'):
        y_final(0)
    with scope('dwu_b'):
        dwu_b()
    with scope('y_final'):
        y_final(1)
    for b in range(2):
        with scope('place_end_y'):
            place_end('y', b, 0, 1)
        with scope('stats'):
            stats_recv(b)
        for q in range(2):
            if b and q:
                with scope('gwu_relay'):
                    gwu_relay()
            with scope('dx'):
                dx_final(b, q)
    with scope('sums_1'):
        sums_1()
    with scope('sums_2'):
        sums_2()
    with scope('sums_3'):
        sums_3()

    with scope('gwu_end'):
        gwu_end()
    with scope('gwd_end'):
        wait(gwd_out.at[pl.ds(0, 4 * QH), :], S('d_o', 0))
    wait(gwd_out.at[pl.ds(0, 4 * QH), :], S('d_o', 1))
    for p, out in (('y', y_out), ('d', dx_out)):
        @pl.when(r == tau)
        def _():
            with scope('out_end'):
                wait(out.at[pl.ds(0, TH), :], S(p + 'out'))

        @pl.when(r != tau)
        def _():
            with scope('out_end'):
                wait(out, S(p + 'out'))
    wait(sum_out, S('l_small', 0))
    for b in range(2):
        for q in range(2):
            place_end('d', b, q, 2)
            far_end('d', b, q)
    for b in range(2):
        wait(sx_v.at[b], S('s_st', b))
    wait(sum_v.at[1, :, pl.ds(0, 2 * HB)], S('s_sum', 0))
    for i in range(7):
        wait(sumr_v.at[0], S('s_sum', 1 + i))
    wait(wun, S('s_wun'))

    @pl.when(r == f)
    def _():
        for s in range(2):
            wait(wd_own(s), S('s_wd0', s))
    for i in range(4):
        wait(wd_dst(0, c), S('s_wdx', i))
    wait(wu_own, S('s_wu'))
    for i in range(3):
        wait(vec_at, S('s_vec', i))
    wait(bu_at, S('s_vec', 3))
    for s in range(2):
        wait(wd_dst(s, cf), S('s_wdr', s))
    for i in range(2):
        wait(wuq(d), S('s_wuy', i))
        wait(wuq(d, 0), S('s_wuy', 2 + i))
    for i in range(12):
        wait(wdq(0, d, c), S('s_wdy', i))
        wait(wdq(0, d, c, 0), S('s_wdy', 12 + i))

    def sends(k):
        for z, Z in (('x', X), ('g', DY)):
            for n in ('s_near', 's_far', 's_rel'):
                wait(reg(Z, k, c), S(z + n, k))
            wait(Z.at[r, ds(k * BLK, BLK), :], S(z + 's_d2d', k))
    loop(NCH, sends)
    for i in range(8):
        wait(r1D.at[0], S('d_so', i))
        wait(gwd(0, d), S('d_sy', i))
        wait(gwd(0, d, 0), S('d_sr', i))
    for j in range(1, 4):
        wait(finD.at[j], S('d_sf', j))

    @pl.when(r != f)
    def _():
        wait(finD.at[0], S('d_sf', 0))
    for i in range(2):
        wait(r1U, S('u_so', i))
        wait(PFU, S('u_sa', i))
        wait(finU, S('u_sf', i))

    @pl.when(r != dh)
    def _():
        wait(finU, S('u_sf', 2))
    wait(gwu(0, DH), S('u_sr'))


def block_kernel(x, dy, wu, wd, vec, bu):
    (TK, HB), FH = x.shape, wu.shape[1] // 2
    W, HW, TH, BLK, QF, FB = 4 * HB, 2 * HB, TK // 2, TK // NCH, FH // 4, 2 * FH
    assert FB <= W and FH <= HW and W // 4 == BLK and QF <= BLK and FH == HW
    sd = jax.ShapeDtypeStruct
    NS = BLK // min(BLK, 128)
    outs = [sd((TK, HB), BF16), sd((TK, HB), BF16), sd((W // 2, FB), BF16), sd((4 * FH, HB), BF16), sd((1, 3 * HB + FB), F32)]
    n_out = len(outs)
    outs += [sd((2, TK, W), BF16)] * 3 + [sd((2, TK, FB), BF16)] * 2 + [sd((2, TK, FB), F32)]
    outs += [sd((TH, W), F32), sd((TH, HW), F32), sd((TH, HW), F32)] * 2
    outs += [sd((4, QF, HB), F32)] * 2 + [sd((W // 4, FH), F32)] * 2
    V = pltpu.VMEM
    scratch = [
        V((W, FB), BF16), V((FB, W), BF16), V((4, FH, HB), F32), V((4, W // 4, FH), F32),
        V((4, FH // 8, HB), F32), V((4, FH // 8, HB), F32), V((W // 8, FH), F32), V((W // 8, FH), F32),
        V((3, 1, W), F32), V((1, FB), F32), V((4, BLK, W), BF16), V((4, BLK, HW), F32), V((2, BLK, HW), BF16),
        V((4, QF, HB), BF16), V((2, 8, FH), F32), V((2, 8, HW), F32),
        V((BLK, 128), F32), V((2, BLK, 128), F32), V((2, BLK, 128), F32), V((2, 2 * NS, 128), F32), V((2, 2 * NS, 128), F32),
        V((8, HB), F32), V((2, 1, 3 * HB + FB), F32), V((9, 1, 3 * HB + FB), F32),
        pltpu.SemaphoreType.DMA((N_SEM,)),
    ]
    res = pl.pallas_call(
        functools.partial(body, (TK, HB, FH)),
        out_shape=outs,
        in_specs=[pl.BlockSpec(memory_space=pl.ANY)] * 6,
        out_specs=[pl.BlockSpec(memory_space=pl.ANY)] * len(outs),
        scratch_shapes=scratch,
        compiler_params=pltpu.CompilerParams(collective_id=0, has_side_effects=True, vmem_limit_bytes=67043328),
        name='mlp_block',
    )(x, dy, wu, wd, vec, bu)
    return res[:n_out]


def solution(mesh):
    assert (mesh.shape['col'], mesh.shape['row'], mesh.shape['depth']) == (4, 2, 4)
    tok_spec = P(('dp', 'depth', 'row'), 'col')
    vec_spec = P('col')
    mat_spec = P('row', 'col')
    grad_vec = P(('dp', 'col'))
    grad_mat = P(('dp', 'row'), 'col')
    def local_pass(x_blk, gamma_blk, beta_blk, w_up_blk, b_up_blk, w_down_blk, b_down_blk, dy_blk):
        hb, fb = x_blk.shape[1], w_up_blk.shape[1]
        vec = jnp.stack([gamma_blk, beta_blk, b_down_blk.astype(F32)])[:, None]
        bu = b_up_blk.astype(F32)[None]
        y_blk, dx_blk, grad_w_up, grad_w_down, sums = block_kernel(x_blk, dy_blk, w_up_blk, w_down_blk, vec, bu)
        sums = sums[0]
        return (y_blk, dx_blk, sums[:hb], sums[hb:2 * hb], grad_w_up, sums[2 * hb:2 * hb + fb], grad_w_down, sums[2 * hb + fb:])

    return jax.shard_map(
        local_pass,
        mesh=mesh,
        in_specs=(tok_spec, vec_spec, vec_spec, mat_spec, vec_spec, mat_spec, vec_spec, tok_spec),
        out_specs=(tok_spec, tok_spec, grad_vec, grad_vec, grad_mat, grad_vec, grad_mat, grad_vec),
        check_vma=False,
    )
```
